256 devices in a mesh: dp: 64 (over z, y, core), cp: 4 (over x).
Axes of the slice: x: 4, y: 4, z: 8, core: 2. Of those that a mesh axis runs over, the one named last changes fastest.
Arguments:
- x_in: bfloat16 [128, 2048, 640], P('dp', 'cp')
- grad_y: bfloat16 [128, 2048, 640], P('dp', 'cp')
- ln_gamma: float32 [640], replicated
- ln_beta: float32 [640], replicated
- w_q: bfloat16 [640, 8, 80], replicated
- w_k: bfloat16 [640, 8, 80], replicated
- w_v: bfloat16 [640, 8, 80], replicated
- w_o: bfloat16 [8, 80, 640], replicated
- b_o: float32 [640], replicated
Outputs:
- output 1: bfloat16 [128, 2048, 640], P('dp', 'cp')
- output 2: bfloat16 [128, 2048, 640], P('dp', 'cp')
- output 3: float32 [640], replicated
- output 4: float32 [640], replicated
- output 5: float32 [640, 8, 80], replicated
- output 6: float32 [640, 8, 80], replicated
- output 7: float32 [640, 8, 80], replicated
- output 8: float32 [8, 80, 640], replicated
- output 9: float32 [640], replicated
All inputs are finite; a program needn't handle non-finite values.
Results may differ from the reference program's by a relative error of at most 0.0149178.
Values are sent between devices in bfloat16 or wider.
A program may use at most 768 MiB of HBM per device.

```python
import math
import jax
import jax.numpy as jnp
from jax import lax

BATCH_TOTAL = 128
TOKENS_TOTAL = 2048
CHANNELS = 640
NUM_HEADS = 8
ROW_BLOCK = 128
HEAD_DIM = CHANNELS // NUM_HEADS
LN_EPS = 1e-5
SCORE_GAIN = (0.6 * math.log(TOKENS_TOTAL)) ** 0.25


def setup_inputs(seed: int = 0) -> dict:
    key_list = jax.random.split(jax.random.key(seed), 9)
    act_shape = (BATCH_TOTAL, TOKENS_TOTAL, CHANNELS)
    proj_shape = (CHANNELS, NUM_HEADS, HEAD_DIM)
    fan_scale = CHANNELS ** -0.5
    x_in = jax.random.normal(key_list[0], act_shape, jnp.float32)
    grad_y = jax.random.normal(key_list[1], act_shape, jnp.float32)
    ln_gamma = 1.0 + 0.3 * jax.random.normal(key_list[2], (CHANNELS,), jnp.float32)
    ln_beta = 0.3 * jax.random.normal(key_list[3], (CHANNELS,), jnp.float32)
    w_q = SCORE_GAIN * fan_scale * jax.random.normal(key_list[4], proj_shape, jnp.float32)
    w_k = SCORE_GAIN * fan_scale * jax.random.normal(key_list[5], proj_shape, jnp.float32)
    w_v = fan_scale * jax.random.normal(key_list[6], proj_shape, jnp.float32)
    w_o = fan_scale * jax.random.normal(key_list[7], (NUM_HEADS, HEAD_DIM, CHANNELS), jnp.float32)
    b_o = 0.5 * jax.random.normal(key_list[8], (CHANNELS,), jnp.float32)
    return {'x_in': x_in.astype(jnp.bfloat16), 'grad_y': grad_y.astype(jnp.bfloat16),
            'ln_gamma': ln_gamma, 'ln_beta': ln_beta,
            'w_q': w_q.astype(jnp.bfloat16), 'w_k': w_k.astype(jnp.bfloat16),
            'w_v': w_v.astype(jnp.bfloat16), 'w_o': w_o.astype(jnp.bfloat16), 'b_o': b_o}


def snap_bf16(values):
    return values.astype(jnp.bfloat16).astype(jnp.float32)


def attend_sample(q_sample, k_sample, v_sample):
    q_rows = q_sample.reshape(TOKENS_TOTAL // ROW_BLOCK, ROW_BLOCK, NUM_HEADS, HEAD_DIM)

    def block_out(q_blk):
        scores = jnp.einsum('rhd,khd->hrk', q_blk, k_sample) * (HEAD_DIM ** -0.5)
        weights = jax.nn.softmax(scores, axis=-1)
        return jnp.einsum('hrk,khd->rhd', weights, v_sample)

    out_rows = lax.map(jax.checkpoint(block_out), q_rows)
    return out_rows.reshape(TOKENS_TOTAL, NUM_HEADS, HEAD_DIM)


def block_forward(x_f, ln_gamma, ln_beta, w_q, w_k, w_v, w_o, b_o):
    tok_mean = jnp.mean(x_f, axis=-1, keepdims=True)
    centered = x_f - tok_mean
    tok_var = jnp.mean(centered * centered, axis=-1, keepdims=True)
    normed = snap_bf16(centered * lax.rsqrt(tok_var + LN_EPS) * ln_gamma + ln_beta)
    q_all = snap_bf16(jnp.einsum('bnc,chd->bnhd', normed, w_q))
    k_all = snap_bf16(jnp.einsum('bnc,chd->bnhd', normed, w_k))
    v_all = snap_bf16(jnp.einsum('bnc,chd->bnhd', normed, w_v))
    attn_out = snap_bf16(lax.map(lambda qkv_trio: attend_sample(qkv_trio[0], qkv_trio[1], qkv_trio[2]), (q_all, k_all, v_all)))
    return snap_bf16(x_f + jnp.einsum('bnhd,hdc->bnc', attn_out, w_o) + b_o)


def reference(x_in, grad_y, ln_gamma, ln_beta, w_q, w_k, w_v, w_o, b_o):
    y_f, pullback = jax.vjp(block_forward, x_in.astype(jnp.float32), ln_gamma, ln_beta,
                            w_q.astype(jnp.float32), w_k.astype(jnp.float32), w_v.astype(jnp.float32),
                            w_o.astype(jnp.float32), b_o)
    grad_list = pullback(grad_y.astype(jnp.float32))
    return (y_f.astype(jnp.bfloat16), grad_list[0].astype(jnp.bfloat16), grad_list[1], grad_list[2],
            grad_list[3], grad_list[4], grad_list[5], grad_list[6], grad_list[7])
```

```python
import functools
import math
import jax
import jax.numpy as jnp
from jax import lax
from jax.experimental import pallas as pl
from jax.experimental.pallas import tpu as pltpu
from jax.sharding import PartitionSpec as P

LN_EPS = 1e-5
KEY_TILE = 256
BF = jnp.bfloat16
F32 = jnp.float32


def dot_nn(lhs, rhs):
    return lax.dot_general(lhs, rhs, (((1,), (0,)), ((), ())), preferred_element_type=F32)


def dot_nt(lhs, rhs):
    return lax.dot_general(lhs, rhs, (((1,), (1,)), ((), ())), preferred_element_type=F32)


def dot_tn(lhs, rhs):
    return lax.dot_general(lhs, rhs, (((0,), (0,)), ((), ())), preferred_element_type=F32)


def attention_body(scale, qt_ref, kt_ref, vt_ref, do_ref, ot_ref, dq_ref, dk_ref, dv_ref,
                   k_s, v_s, s_s, p_s, ds_s, dk_acc, dv_acc):
    step = pl.program_id(1)
    rows = qt_ref.shape[1]
    tokens = kt_ref.shape[1]
    tiles = tokens // KEY_TILE
    log2_scale = scale * math.log2(math.e)

    @pl.when(step == 0)
    def _():
        k_s[...] = kt_ref[...].T
        v_s[...] = vt_ref[...].T
        dk_acc[...] = jnp.zeros_like(dk_acc)
        dv_acc[...] = jnp.zeros_like(dv_acc)

    q_t = qt_ref[...]
    do_t = do_ref[...]
    top = None
    for tile in range(tiles):
        keys = pl.ds(tile * KEY_TILE, KEY_TILE)
        scores = dot_nn(k_s[keys, :], q_t)
        s_s[keys, :] = scores
        part = jnp.max(scores.reshape(KEY_TILE // 8, 8, rows), axis=0)
        top = part if top is None else jnp.maximum(top, part)
    top = jnp.max(top, axis=0, keepdims=True) * log2_scale
    total = None
    for tile in range(tiles):
        keys = pl.ds(tile * KEY_TILE, KEY_TILE)
        probs = jnp.exp2(s_s[keys, :] * log2_scale - top)
        s_s[keys, :] = probs
        part = jnp.sum(probs.reshape(KEY_TILE // 8, 8, rows), axis=0)
        total = part if total is None else total + part
    recip = 1.0 / jnp.sum(total, axis=0, keepdims=True)
    for tile in range(tiles):
        keys = pl.ds(tile * KEY_TILE, KEY_TILE)
        p_s[keys, :] = (s_s[keys, :] * recip).astype(BF)
    out_t = dot_nn(vt_ref[...], p_s[...])
    ot_ref[...] = out_t.astype(BF)
    delta = jnp.sum(out_t * do_t.astype(F32), axis=0, keepdims=True)
    dv_acc[...] += dot_nt(do_t, p_s[...])
    for tile in range(tiles):
        keys = pl.ds(tile * KEY_TILE, KEY_TILE)
        d_probs = dot_nn(v_s[keys, :], do_t)
        ds_s[keys, :] = ((s_s[keys, :] * recip) * (d_probs - delta)).astype(BF)
    dq_ref[...] = (dot_nn(kt_ref[...], ds_s[...]) * scale).astype(BF)
    dk_acc[...] += dot_nt(q_t, ds_s[...])

    @pl.when(step == pl.num_programs(1) - 1)
    def _():
        dk_ref[...] = (dk_acc[...] * scale).astype(BF)
        dv_ref[...] = dv_acc[...].astype(BF)


def attention(q_t, k_t, v_t, do_t, head_dim, block=256):
    width, tokens = q_t.shape
    heads = width // head_dim
    row_spec = pl.BlockSpec((head_dim, block), lambda h, j: (h, j))
    full_spec = pl.BlockSpec((head_dim, tokens), lambda h, j: (h, 0))
    flops = 12 * heads * tokens * tokens * head_dim
    return pl.pallas_call(
        functools.partial(attention_body, head_dim ** -0.5),
        grid=(heads, tokens // block),
        in_specs=[row_spec, full_spec, full_spec, row_spec],
        out_specs=[row_spec, row_spec, full_spec, full_spec],
        out_shape=[jax.ShapeDtypeStruct((width, tokens), BF)] * 4,
        scratch_shapes=[pltpu.VMEM((tokens, head_dim), BF)] * 2 + [pltpu.VMEM((tokens, block), F32)]
        + [pltpu.VMEM((tokens, block), BF)] * 2 + [pltpu.VMEM((head_dim, tokens), F32)] * 2,
        compiler_params=pltpu.CompilerParams(vmem_limit_bytes=40 * 2 ** 20),
        cost_estimate=pl.CostEstimate(flops=flops, bytes_accessed=16 * width * tokens, transcendentals=heads * tokens * tokens),
        name='attention',
    )(q_t, k_t, v_t, do_t)


def solution(mesh):
    dp_size = mesh.shape['dp']
    cp_size = mesh.shape['cp']
    axes = ('dp', 'cp')
    act_spec = P('dp', 'cp', None)
    rep_spec = P()

    def index_of(dp, cp):
        return dp * cp_size + cp

    send_same, send_cross, swap = [], [], []
    for dp in range(dp_size):
        group, core = dp // 2, dp % 2
        for cp in range(cp_size):
            half, parity = cp // 2, cp % 2
            send_same.append((index_of(dp, cp), index_of(2 * group + half, 2 * core + parity)))
            send_cross.append((index_of(dp, cp), index_of(2 * group + half, 2 * core + 1 - parity)))
            swap.append((index_of(dp, cp), index_of(dp ^ 1, cp)))
    back_same = [(dst, src) for src, dst in send_same]
    back_cross = [(dst, src) for src, dst in send_cross]

    def device_step(x_in, grad_y, ln_gamma, ln_beta, w_q, w_k, w_v, w_o, b_o):
        channels = x_in.shape[2]
        num_heads, head_dim = w_q.shape[1], w_q.shape[2]
        half_heads = num_heads // 2
        width = half_heads * head_dim
        core = lax.rem(lax.axis_index('dp'), 2)
        parity = lax.rem(lax.axis_index('cp'), 2)

        def permute(value, pairs):
            return lax.ppermute(value, axes, pairs)

        def gather_image(band_pair):
            first = lax.dynamic_index_in_dim(band_pair, parity, 0, keepdims=False)
            second = lax.dynamic_index_in_dim(band_pair, 1 - parity, 0, keepdims=False)
            own_a, own_b = permute(first, send_same), permute(second, send_cross)
            return own_a, own_b, permute(own_a, swap), permute(own_b, swap)

        def scatter_image(own):
            half = own.shape[0] // 2
            same, cross = permute(own[:half], back_same), permute(own[half:], back_cross)
            return jnp.where(parity == 0, jnp.stack([same, cross]), jnp.stack([cross, same]))

        def head_slice(weight, which):
            return lax.dynamic_slice_in_dim(weight, which * half_heads, half_heads, 1).reshape(channels, width)

        def out_slice(which):
            return lax.dynamic_slice_in_dim(w_o, which * half_heads, half_heads, 0).reshape(width, channels)

        x_parts = gather_image(x_in)
        dy_parts = gather_image(grad_y)
        x_all = jnp.concatenate(x_parts, axis=0)
        dy_all = jnp.concatenate(dy_parts, axis=0)
        tokens = x_all.shape[0]
        own = tokens // 2

        x_f = x_all.astype(F32)
        mean = jnp.mean(x_f, axis=-1, keepdims=True)
        centered = x_f - mean
        inv_std = lax.rsqrt(jnp.mean(centered * centered, axis=-1, keepdims=True) + LN_EPS)
        normed = (centered * inv_std * ln_gamma + ln_beta).astype(BF)

        wq_mine, wk_mine, wv_mine = (head_slice(w, core) for w in (w_q, w_k, w_v))
        wq_other, wk_other, wv_other = (head_slice(w, 1 - core) for w in (w_q, w_k, w_v))
        wo_mine, wo_other = out_slice(core), out_slice(1 - core)

        def project(weight):
            return lax.dot_general(weight, normed, (((0,), (1,)), ((), ())), preferred_element_type=F32).astype(BF)

        q_t, k_t, v_t = project(wq_mine), project(wk_mine), project(wv_mine)
        do_t = dot_nt(wo_mine, dy_all).astype(BF)
        o_t, dq_t, dk_t, dv_t = attention(q_t, k_t, v_t, do_t, head_dim)

        o_peer = permute(o_t[:, own:], swap)
        y_f = x_all[:own].astype(F32) + (dot_tn(o_t[:, :own], wo_mine) + dot_tn(o_peer, wo_other)) + b_o
        y_out = scatter_image(y_f.astype(BF))

        dqkv_t = jnp.concatenate([dq_t, dk_t, dv_t], axis=0)
        dqkv_peer = permute(dqkv_t[:, own:], swap)
        w_mine = jnp.concatenate([wq_mine, wk_mine, wv_mine], axis=1)
        w_other = jnp.concatenate([wq_other, wk_other, wv_other], axis=1)
        d_normed = (lax.dot_general(dqkv_t[:, :own], w_mine, (((0,), (1,)), ((), ())), preferred_element_type=F32)
                    + lax.dot_general(dqkv_peer, w_other, (((0,), (1,)), ((), ())), preferred_element_type=F32))
        d_normed = d_normed.astype(BF).astype(F32)
        x_hat = centered[:own] * inv_std[:own]
        d_hat = d_normed * ln_gamma
        mean_one = jnp.mean(d_hat, axis=-1, keepdims=True)
        mean_two = jnp.mean(d_hat * x_hat, axis=-1, keepdims=True)
        dx = inv_std[:own] * (d_hat - mean_one - x_hat * mean_two)
        dx = (dy_all[:own].astype(F32) + dx).astype(BF)
        grad_x = scatter_image(dx)

        small = jnp.stack([jnp.sum(d_normed * x_hat, axis=0), jnp.sum(d_normed, axis=0),
                           jnp.sum(dy_all[:own].astype(F32), axis=0)])
        d_w = jnp.concatenate([dot_nn(dqkv_t, normed), dot_nn(o_t, dy_all)], axis=0)
        d_w = d_w.reshape(4, 1, width, channels)
        zero = jnp.zeros_like(d_w)
        both = jnp.where(core == 0, jnp.concatenate([d_w, zero], 1), jnp.concatenate([zero, d_w], 1))
        both, small = lax.psum((both, small), axes)
        both = both.reshape(4, num_heads, head_dim, channels)
        grads = [jnp.transpose(both[i], (2, 0, 1)) for i in range(3)]
        return (y_out, grad_x, small[0], small[1], grads[0], grads[1], grads[2], both[3], small[2])

    return jax.shard_map(device_step, mesh=mesh,
                         in_specs=(act_spec, act_spec) + (rep_spec,) * 7,
                         out_specs=(act_spec, act_spec) + (rep_spec,) * 7,
                         check_vma=False)
```

```python
import functools
import math
import jax
import jax.numpy as jnp
from jax import lax
from jax.experimental import pallas as pl
from jax.experimental.pallas import tpu as pltpu
from jax.sharding import PartitionSpec as P

LN_EPS = 1e-5
KEY_TILE = 256
BF = jnp.bfloat16
F32 = jnp.float32


def dot_nn(lhs, rhs):
    return lax.dot_general(lhs, rhs, (((1,), (0,)), ((), ())), preferred_element_type=F32)


def dot_nt(lhs, rhs):
    return lax.dot_general(lhs, rhs, (((1,), (1,)), ((), ())), preferred_element_type=F32)


def dot_tn(lhs, rhs):
    return lax.dot_general(lhs, rhs, (((0,), (0,)), ((), ())), preferred_element_type=F32)


def attention_body(scale, qt_ref, kt_ref, vt_ref, do_ref, ot_ref, dq_ref, dk_ref, dv_ref,
                   k_s, v_s, s_s, p_s, ds_s, dk_acc, dv_acc):
    step = pl.program_id(1)
    rows = qt_ref.shape[1]
    tokens = kt_ref.shape[1]
    tiles = tokens // KEY_TILE
    log2_scale = scale * math.log2(math.e)

    @pl.when(step == 0)
    def _():
        k_s[...] = kt_ref[...].T
        v_s[...] = vt_ref[...].T
        dk_acc[...] = jnp.zeros_like(dk_acc)
        dv_acc[...] = jnp.zeros_like(dv_acc)

    q_t = qt_ref[...]
    do_t = do_ref[...]
    top = None
    for tile in range(tiles):
        keys = pl.ds(tile * KEY_TILE, KEY_TILE)
        scores = dot_nn(k_s[keys, :], q_t)
        s_s[keys, :] = scores
        part = jnp.max(scores.reshape(KEY_TILE // 8, 8, rows), axis=0)
        top = part if top is None else jnp.maximum(top, part)
    top = jnp.max(top, axis=0, keepdims=True) * log2_scale
    total = None
    for tile in range(tiles):
        keys = pl.ds(tile * KEY_TILE, KEY_TILE)
        probs = jnp.exp2(s_s[keys, :] * log2_scale - top)
        s_s[keys, :] = probs
        part = jnp.sum(probs.reshape(KEY_TILE // 8, 8, rows), axis=0)
        total = part if total is None else total + part
    recip = 1.0 / jnp.sum(total, axis=0, keepdims=True)
    for tile in range(tiles):
        keys = pl.ds(tile * KEY_TILE, KEY_TILE)
        p_s[keys, :] = (s_s[keys, :] * recip).astype(BF)
    out_t = dot_nn(vt_ref[...], p_s[...])
    ot_ref[...] = out_t.astype(BF)
    delta = jnp.sum(out_t * do_t.astype(F32), axis=0, keepdims=True)
    dv_acc[...] += dot_nt(do_t, p_s[...])
    for tile in range(tiles):
        keys = pl.ds(tile * KEY_TILE, KEY_TILE)
        d_probs = dot_nn(v_s[keys, :], do_t)
        ds_s[keys, :] = ((s_s[keys, :] * recip) * (d_probs - delta)).astype(BF)
    dq_ref[...] = (dot_nn(kt_ref[...], ds_s[...]) * scale).astype(BF)
    dk_acc[...] += dot_nt(q_t, ds_s[...])

    @pl.when(step == pl.num_programs(1) - 1)
    def _():
        dk_ref[...] = (dk_acc[...] * scale).astype(BF)
        dv_ref[...] = dv_acc[...].astype(BF)


def attention(q_t, k_t, v_t, do_t, head_dim, block=256):
    width, tokens = q_t.shape
    heads = width // head_dim
    row_spec = pl.BlockSpec((head_dim, block), lambda h, j: (h, j))
    full_spec = pl.BlockSpec((head_dim, tokens), lambda h, j: (h, 0))
    flops = 12 * heads * tokens * tokens * head_dim
    return pl.pallas_call(
        functools.partial(attention_body, head_dim ** -0.5),
        grid=(heads, tokens // block),
        in_specs=[row_spec, full_spec, full_spec, row_spec],
        out_specs=[row_spec, row_spec, full_spec, full_spec],
        out_shape=[jax.ShapeDtypeStruct((width, tokens), BF)] * 4,
        scratch_shapes=[pltpu.VMEM((tokens, head_dim), BF)] * 2 + [pltpu.VMEM((tokens, block), F32)]
        + [pltpu.VMEM((tokens, block), BF)] * 2 + [pltpu.VMEM((head_dim, tokens), F32)] * 2,
        compiler_params=pltpu.CompilerParams(vmem_limit_bytes=40 * 2 ** 20),
        cost_estimate=pl.CostEstimate(flops=flops, bytes_accessed=16 * width * tokens, transcendentals=heads * tokens * tokens),
        name='attention',
    )(q_t, k_t, v_t, do_t)


MESH = pl.DeviceIdType.MESH
RING = 4


def ring_copies(src, relay, fin, sems, axis_pos, device_of, split, rows):
    send, recv = sems
    right, left, across = (lax.rem(axis_pos + k, RING) for k in (1, RING - 1, 2))
    low, high = pl.ds(0, split), pl.ds(split, rows - split)

    def copy(k, source, target, where):
        return pltpu.make_async_remote_copy(src_ref=source, dst_ref=target, send_sem=send.at[k], recv_sem=recv.at[k],
                                            device_id=device_of(where), device_id_type=MESH)

    return [copy(0, src.at[across, low], relay.at[low], right),
            copy(1, src.at[across, high], relay.at[high], left),
            copy(2, src.at[right, high], fin.at[0, high], right),
            copy(3, src.at[left, low], fin.at[1, low], left),
            copy(4, relay.at[low], fin.at[0, low], right),
            copy(5, relay.at[high], fin.at[1, high], left)]


def gather_copies(out, first, stride, rows, sems, axis_pos, device_of, split):
    send, recv = sems
    right, left = lax.rem(axis_pos + 1, RING), lax.rem(axis_pos + RING - 1, RING)

    def copy(k, block, begin, size, where):
        part = out.at[pl.ds(pl.multiple_of(first + block * stride + begin, 8), size)]
        return pltpu.make_async_remote_copy(src_ref=part, dst_ref=part, send_sem=send.at[k], recv_sem=recv.at[k],
                                            device_id=device_of(where), device_id_type=MESH)

    return [copy(0, axis_pos, 0, rows, right), copy(1, axis_pos, 0, rows, left),
            copy(2, left, 0, split, right), copy(3, right, split, rows - split, left)]


def all_reduce_body(depth, gp_ref, gq_ref, out_ref,
                    p_relay, p_fin, q_relay, q_fin, p2, q2, p2_relay, p2_fin, q2_relay, q2_fin,
                    z_src, z_recv, z_out, ring_sems, ag_sems, z_sems, swap_sems):
    dp, x = lax.axis_index('dp'), lax.axis_index('cp')
    core = lax.rem(dp, 2)
    y = lax.rem(dp // 2, RING)
    z = dp // (2 * RING)

    def at(zz, yy, cc):
        return (zz * RING + yy) * 2 + cc

    def on_x(pos):
        return (dp, pos)

    def on_y(pos):
        return (at(z, pos, core), x)

    def on_z(pos):
        return (at(pos, y, core), x)

    peer = (at(z, y, 1 - core), x)
    barrier = pltpu.get_barrier_semaphore()
    peers = [on_x(lax.rem(x + 1, RING)), on_x(lax.rem(x + RING - 1, RING)),
             on_y(lax.rem(y + 1, RING)), on_y(lax.rem(y + RING - 1, RING)), peer]
    peers += [on_z(lax.rem(z + d, depth)) for d in range(1, depth)]
    for device in peers:
        pl.semaphore_signal(barrier, inc=1, device_id=device, device_id_type=MESH)
    pl.semaphore_wait(barrier, len(peers))

    def sems(pool, k):
        return pool.at[0, k], pool.at[1, k]

    def two_rings(first, second):
        plans = [ring_copies(src, relay, fin, sm, pos, dev, split, rows)
                 for src, relay, fin, pos, dev, split, rows, sm in (first, second)]
        for k in range(4):
            for plan in plans:
                plan[k].start()
        for way, k in ((0, 4), (1, 5)):
            for plan, (src, relay, fin, pos, dev, split, rows, sm) in zip(plans, (first, second)):
                part = pl.ds(0, split) if way == 0 else pl.ds(split, rows - split)
                owner = lax.rem(pos + (1 if way == 0 else RING - 1), RING)
                plan[way].wait_recv()
                relay[part] = src[owner, part] + relay[part]
                plan[k].start()
        for k in (2, 3, 4, 5):
            for plan in plans:
                plan[k].wait_recv()
        for plan in plans:
            for copy in plan:
                copy.wait_send()

    two_rings((gp_ref, p_relay, p_fin, y, on_y, 88, 168, sems(ring_sems, 0)),
              (gq_ref, q_relay, q_fin, x, on_x, 80, 160, sems(ring_sems, 1)))
    tail = pl.ds(160, 8)
    for block in range(RING):
        rows = pl.ds(block * 40, 40)
        p2[block, pl.ds(0, 40)] = gp_ref[y, rows] + (p_fin[0, rows] + p_fin[1, rows])
        p2[block, pl.ds(40, 8)] = gp_ref[y, tail] + (p_fin[0, tail] + p_fin[1, tail])
        q2[block] = gq_ref[x, rows] + (q_fin[0, rows] + q_fin[1, rows])
    two_rings((p2, p2_relay, p2_fin, x, on_x, 24, 48, sems(ring_sems, 2)),
              (q2, q2_relay, q2_fin, y, on_y, 24, 40, sems(ring_sems, 3)))
    count = 0
    for src, fin, pos, rows in ((p2, p2_fin, x, 48), (q2, q2_fin, y, 40)):
        for i in range(rows // 8):
            r = pl.ds(i * 8, 8)
            for j in range(5):
                c = pl.ds(j * 128, 128)
                z_src[count] = src[pos, r, c] + (fin[0, r, c] + fin[1, r, c])
                count += 1
    z_src[count] = jnp.zeros((8, 128), F32)
    each = 56 // depth

    def z_copy(k, source, target, d):
        return pltpu.make_async_remote_copy(src_ref=source, dst_ref=target, send_sem=z_sems.at[0, k, d - 1],
                                            recv_sem=z_sems.at[1, k, d - 1], device_id=on_z(lax.rem(z + d, depth)),
                                            device_id_type=MESH)

    mine = pl.ds(z * each, each)
    copies = [z_copy(0, z_src.at[pl.ds(lax.rem(z + d, depth) * each, each)], z_recv.at[d - 1], d)
              for d in range(1, depth)]
    for copy in copies:
        copy.start()
    total = z_src[mine]
    for d, copy in enumerate(copies):
        copy.wait_recv()
        total = total + z_recv[d]
    z_out[mine] = total
    for copy in copies:
        copy.wait_send()
    copies = [z_copy(1, z_out.at[mine], z_out.at[mine], d) for d in range(1, depth)]
    for copy in copies:
        copy.start()
    for copy in copies:
        copy.wait_recv()
    for copy in copies:
        copy.wait_send()

    out = out_ref.at[core]
    p_first, q_first = y * 160, 640 + x * 160
    count = 0
    for first, rows in ((p_first + x * 40, 48), (q_first + y * 40, 40)):
        for i in range(rows // 8):
            for j in range(5):
                c = pl.ds(j * 128, 128)
                if i < 5:
                    out[pl.ds(pl.multiple_of(first + i * 8, 8), 8), c] = z_out[count]
                else:
                    out[pl.ds(1280, 8), c] = z_out[count]
                count += 1

    def two_gathers(first, second):
        plans = [gather_copies(out, base, stride, rows, sm, pos, dev, split)
                 for base, stride, rows, pos, dev, split, sm in (first, second)]
        for k in (0, 1):
            for plan in plans:
                plan[k].start()
        for k in (0, 1):
            for plan in plans:
                plan[k].wait_recv()
                plan[k + 2].start()
        for k in (2, 3):
            for plan in plans:
                plan[k].wait_recv()
        for plan in plans:
            for copy in plan:
                copy.wait_send()

    two_gathers((p_first, 40, 40, x, on_x, 24, sems(ag_sems, 0)), (q_first, 40, 40, y, on_y, 24, sems(ag_sems, 1)))
    two_gathers((0, 160, 160, y, on_y, 80, sems(ag_sems, 2)), (640, 160, 160, x, on_x, 80, sems(ag_sems, 3)))
    swap = pltpu.make_async_remote_copy(src_ref=out, dst_ref=out, send_sem=swap_sems.at[0], recv_sem=swap_sems.at[1],
                                        device_id=peer, device_id_type=MESH)
    swap.start()
    swap.wait()


def all_reduce(grad_p, grad_q, depth):
    channels = grad_p.shape[2]
    vm = lambda *shape: pltpu.VMEM(shape, F32)
    in_vmem = pl.BlockSpec(memory_space=pltpu.VMEM)
    dma = pltpu.SemaphoreType.DMA
    return pl.pallas_call(
        functools.partial(all_reduce_body, depth),
        in_specs=[in_vmem, in_vmem], out_specs=in_vmem,
        out_shape=jax.ShapeDtypeStruct((2, 1288, channels), F32),
        scratch_shapes=[vm(168, channels), vm(2, 168, channels), vm(160, channels), vm(2, 160, channels),
                        vm(RING, 48, channels), vm(RING, 40, channels), vm(48, channels), vm(2, 48, channels),
                        vm(40, channels), vm(2, 40, channels), vm(56, 8, 128), vm(max(depth - 1, 1), 56 // depth, 8, 128),
                        vm(56, 8, 128), dma((2, 4, 6)), dma((2, 4, 4)), dma((2, 2, max(depth - 1, 1))), dma((2,))],
        compiler_params=pltpu.CompilerParams(collective_id=0, has_side_effects=True, vmem_limit_bytes=40 * 2 ** 20),
        name='grad_all_reduce',
    )(grad_p, grad_q)


def solution(mesh):
    dp_size = mesh.shape['dp']
    cp_size = mesh.shape['cp']
    axes = ('dp', 'cp')
    act_spec = P('dp', 'cp', None)
    rep_spec = P()

    def index_of(dp, cp):
        return dp * cp_size + cp

    send_same, send_cross, swap = [], [], []
    for dp in range(dp_size):
        group, core = dp // 2, dp % 2
        for cp in range(cp_size):
            half, parity = cp // 2, cp % 2
            send_same.append((index_of(dp, cp), index_of(2 * group + half, 2 * core + parity)))
            send_cross.append((index_of(dp, cp), index_of(2 * group + half, 2 * core + 1 - parity)))
            swap.append((index_of(dp, cp), index_of(dp ^ 1, cp)))
    back_same = [(dst, src) for src, dst in send_same]
    back_cross = [(dst, src) for src, dst in send_cross]

    def device_step(x_in, grad_y, ln_gamma, ln_beta, w_q, w_k, w_v, w_o, b_o):
        channels = x_in.shape[2]
        num_heads, head_dim = w_q.shape[1], w_q.shape[2]
        half_heads = num_heads // 2
        width = half_heads * head_dim
        core = lax.rem(lax.axis_index('dp'), 2)
        parity = lax.rem(lax.axis_index('cp'), 2)

        def permute(value, pairs):
            return lax.ppermute(value, axes, pairs)

        def gather_image(band_pair):
            first = lax.dynamic_index_in_dim(band_pair, parity, 0, keepdims=False)
            second = lax.dynamic_index_in_dim(band_pair, 1 - parity, 0, keepdims=False)
            own_a, own_b = permute(first, send_same), permute(second, send_cross)
            return own_a, own_b, permute(own_a, swap), permute(own_b, swap)

        def scatter_image(own):
            half = own.shape[0] // 2
            same, cross = permute(own[:half], back_same), permute(own[half:], back_cross)
            return jnp.where(parity == 0, jnp.stack([same, cross]), jnp.stack([cross, same]))

        def head_slice(weight, which):
            return lax.dynamic_slice_in_dim(weight, which * half_heads, half_heads, 1).reshape(channels, width)

        def out_slice(which):
            return lax.dynamic_slice_in_dim(w_o, which * half_heads, half_heads, 0).reshape(width, channels)

        x_parts = gather_image(x_in)
        dy_parts = gather_image(grad_y)
        x_all = jnp.concatenate(x_parts, axis=0)
        dy_all = jnp.concatenate(dy_parts, axis=0)
        tokens = x_all.shape[0]
        own = tokens // 2

        x_f = x_all.astype(F32)
        mean = jnp.mean(x_f, axis=-1, keepdims=True)
        centered = x_f - mean
        inv_std = lax.rsqrt(jnp.mean(centered * centered, axis=-1, keepdims=True) + LN_EPS)
        normed = (centered * inv_std * ln_gamma + ln_beta).astype(BF)

        wq_mine, wk_mine, wv_mine = (head_slice(w, core) for w in (w_q, w_k, w_v))
        wq_other, wk_other, wv_other = (head_slice(w, 1 - core) for w in (w_q, w_k, w_v))
        wo_mine, wo_other = out_slice(core), out_slice(1 - core)

        def project(weight):
            return lax.dot_general(weight, normed, (((0,), (1,)), ((), ())), preferred_element_type=F32).astype(BF)

        q_t, k_t, v_t = project(wq_mine), project(wk_mine), project(wv_mine)
        do_t = dot_nt(wo_mine, dy_all).astype(BF)
        o_t, dq_t, dk_t, dv_t = attention(q_t, k_t, v_t, do_t, head_dim)

        o_peer = permute(o_t[:, own:], swap)
        y_f = x_all[:own].astype(F32) + (dot_tn(o_t[:, :own], wo_mine) + dot_tn(o_peer, wo_other)) + b_o
        y_out = scatter_image(y_f.astype(BF))

        dqkv_t = jnp.concatenate([dq_t, dk_t, dv_t], axis=0)
        dqkv_peer = permute(dqkv_t[:, own:], swap)
        w_mine = jnp.concatenate([wq_mine, wk_mine, wv_mine], axis=1)
        w_other = jnp.concatenate([wq_other, wk_other, wv_other], axis=1)
        d_normed = (lax.dot_general(dqkv_t[:, :own], w_mine, (((0,), (1,)), ((), ())), preferred_element_type=F32)
                    + lax.dot_general(dqkv_peer, w_other, (((0,), (1,)), ((), ())), preferred_element_type=F32))
        d_normed = d_normed.astype(BF).astype(F32)
        x_hat = centered[:own] * inv_std[:own]
        d_hat = d_normed * ln_gamma
        mean_one = jnp.mean(d_hat, axis=-1, keepdims=True)
        mean_two = jnp.mean(d_hat * x_hat, axis=-1, keepdims=True)
        dx = inv_std[:own] * (d_hat - mean_one - x_hat * mean_two)
        dx = (dy_all[:own].astype(F32) + dx).astype(BF)
        grad_x = scatter_image(dx)

        small = jnp.stack([jnp.sum(d_normed * x_hat, axis=0), jnp.sum(d_normed, axis=0),
                           jnp.sum(dy_all[:own].astype(F32), axis=0)])
        d_w = jnp.concatenate([dot_nn(dqkv_t, normed), dot_nn(o_t, dy_all)], axis=0)
        grad_p = jnp.concatenate([d_w[:640].reshape(4, 160, channels),
                                  jnp.broadcast_to(jnp.pad(small, ((0, 5), (0, 0))), (4, 8, channels))], axis=1)
        both = all_reduce(grad_p, d_w[640:].reshape(4, 160, channels), dp_size // 8)
        small = both[0, 1280:] + both[1, 1280:]
        both = jnp.transpose(both[:, :1280].reshape(2, 4, half_heads, head_dim, channels), (1, 0, 2, 3, 4))
        both = both.reshape(4, num_heads, head_dim, channels)
        grads = [jnp.transpose(both[i], (2, 0, 1)) for i in range(3)]
        return (y_out, grad_x, small[0], small[1], grads[0], grads[1], grads[2], both[3], small[2])

    return jax.shard_map(device_step, mesh=mesh,
                         in_specs=(act_spec, act_spec) + (rep_spec,) * 7,
                         out_specs=(act_spec, act_spec) + (rep_spec,) * 7,
                         check_vma=False)
```

```python
import functools
import math
import jax
import jax.numpy as jnp
from jax import lax
from jax.experimental import pallas as pl
from jax.experimental.pallas import tpu as pltpu
from jax.sharding import PartitionSpec as P


LN_EPS = 1e-5
KEY_TILE = 256
Q_BLOCK = 256
FOLD = 16
AUG = 96
BF = jnp.bfloat16
F32 = jnp.float32


def dot_nn(lhs, rhs):
    return lax.dot_general(lhs, rhs, (((1,), (0,)), ((), ())), preferred_element_type=F32)


def dot_nt(lhs, rhs):
    return lax.dot_general(lhs, rhs, (((1,), (1,)), ((), ())), preferred_element_type=F32)


def dot_tn(lhs, rhs):
    return lax.dot_general(lhs, rhs, (((0,), (0,)), ((), ())), preferred_element_type=F32)


def split_parts(value):
    high = value.astype(BF)
    rest = value - high.astype(F32)
    mid = rest.astype(BF)
    return high, mid, (rest - mid.astype(F32)).astype(BF)


def fold_rows(value, op):
    groups = value.reshape(value.shape[0] // FOLD, FOLD, value.shape[1])
    out = groups[0]
    for i in range(1, groups.shape[0]):
        out = op(out, groups[i])
    return out


def forward_body(scale, group, qt_ref, kt_ref, vt_ref, ot_ref, of_ref, lse_ref, k_s, v_s, *bufs):
    step = pl.program_id(1)
    zero = jnp.minimum(step, 0)
    dim, tokens = kt_ref.shape
    tiles = tokens // KEY_TILE
    log2_scale = scale * math.log2(math.e)

    @pl.when(step == 0)
    def _():
        k_t = kt_ref[...]
        k_s[...] = jnp.concatenate([k_t, k_t, k_t], axis=0).T
        v_s[0:dim, :] = vt_ref[...]
        v_s[dim:, :] = jnp.concatenate([jnp.ones((1, tokens), F32), jnp.zeros((AUG - dim - 1, tokens), F32)], axis=0).astype(BF)

    def rows(tile, base=None):
        return pl.ds(tile * KEY_TILE if base is None else pl.multiple_of(base + tile * KEY_TILE, KEY_TILE), KEY_TILE)

    def block(i):
        return pl.ds(pl.multiple_of((step * group + i) * Q_BLOCK, Q_BLOCK), Q_BLOCK)

    total = tiles * group
    lag = tiles + 1
    query, part, top, probs, out = {}, {}, {}, {}, {}
    for g in range(total + lag + 2):
        if g < total:
            i, t = divmod(g, tiles)
            if t == 0:
                query[i] = jnp.concatenate(split_parts(qt_ref[:, block(i)].astype(F32) * log2_scale), axis=0)
            scores = dot_nn(k_s[rows(t), :], query[i])
            bufs[i % len(bufs)][rows(t), :] = scores
            folded = fold_rows(scores, jnp.maximum)
            part[i] = folded if t == 0 else jnp.maximum(part[i], folded)
            if t == tiles - 1:
                top[i] = jnp.max(part[i], axis=0, keepdims=True)
        if lag <= g < total + lag:
            i, t = divmod(g - lag, tiles)
            probs[g - lag] = jnp.exp2(bufs[i % len(bufs)][rows(t, zero), :] - top[i]).astype(BF)
        if g >= lag + 2:
            i, t = divmod(g - lag - 2, tiles)
            part_out = dot_nn(v_s[:, rows(t)], probs[g - lag - 2])
            out[i] = part_out if t == 0 else out[i] + part_out
            if t == tiles - 1:
                denom = out[i][dim:dim + 1]
                normed = out[i][:dim] * (1.0 / denom)
                ot_ref[:, block(i)] = normed.astype(BF)
                of_ref[:, block(i)] = normed
                lse = (top[i] + jnp.log2(denom)) * (1.0 / log2_scale)
                lse_ref[:, block(i)] = jnp.concatenate([p.astype(F32) for p in split_parts(lse)] + [jnp.zeros((13, Q_BLOCK), F32)], axis=0).astype(BF)


def attention_forward(q_t, k_t, v_t, head_dim, group=4):
    width, tokens = q_t.shape
    heads = width // head_dim
    full = pl.BlockSpec((head_dim, tokens), lambda h, j: (h, 0))
    stat = pl.BlockSpec((16, tokens), lambda h, j: (h, 0))
    return pl.pallas_call(
        functools.partial(forward_body, head_dim ** -0.5, group),
        grid=(heads, tokens // (Q_BLOCK * group)),
        in_specs=[full] * 3, out_specs=[full, full, stat],
        out_shape=[jax.ShapeDtypeStruct((width, tokens), BF), jax.ShapeDtypeStruct((width, tokens), F32),
                   jax.ShapeDtypeStruct((heads * 16, tokens), BF)],
        scratch_shapes=[pltpu.VMEM((tokens, 3 * head_dim), BF), pltpu.VMEM((AUG, tokens), BF)]
        + [pltpu.VMEM((tokens, Q_BLOCK), F32)] * 3,
        compiler_params=pltpu.CompilerParams(vmem_limit_bytes=40 * 2 ** 20),
        cost_estimate=pl.CostEstimate(flops=4 * heads * tokens * tokens * head_dim, bytes_accessed=12 * width * tokens,
                                      transcendentals=heads * tokens * tokens),
        name='attention_forward',
    )(q_t, k_t, v_t)


def backward_body(scale, group, qt_ref, kt_ref, vt_ref, do_ref, lse_ref, delta_ref, grad_ref, k_s, v_s, dk_acc, dv_acc):
    step = pl.program_id(1)
    dim, tokens = kt_ref.shape
    tiles = tokens // KEY_TILE
    log2_scale = scale * math.log2(math.e)

    @pl.when(step == 0)
    def _():
        minus = jnp.concatenate([jnp.full((3, tokens), -1.0, F32), jnp.zeros((AUG - dim - 3, tokens), F32)], axis=0).astype(BF)
        k_s[...] = jnp.concatenate([kt_ref[...], minus], axis=0).T
        v_s[...] = jnp.concatenate([vt_ref[...], minus], axis=0).T
        dk_acc[...] = jnp.zeros_like(dk_acc)
        dv_acc[...] = jnp.zeros_like(dv_acc)

    def rows(tile):
        return pl.ds(tile * KEY_TILE, KEY_TILE)

    total = tiles * group
    ops, probs, d_scores, dq = {}, {}, {}, {}
    for g in range(total + 2):
        if g < total:
            i, t = divmod(g, tiles)
            if t == 0:
                cols = pl.ds(pl.multiple_of((step * group + i) * Q_BLOCK, Q_BLOCK), Q_BLOCK)
                q_t, do_t = qt_ref[:, cols], do_ref[:, cols]
                ops[i] = (cols, q_t, do_t, jnp.concatenate([q_t, lse_ref[:, cols]], axis=0),
                          jnp.concatenate([do_t, delta_ref[:, cols]], axis=0))
            scores = dot_nn(k_s[rows(t), :], ops[i][3])
            d_probs = dot_nn(v_s[rows(t), :], ops[i][4])
            prob = jnp.exp2(scores * log2_scale)
            probs[g] = prob.astype(BF)
            d_scores[g] = (prob * d_probs).astype(BF)
        if g >= 2:
            i, t = divmod(g - 2, tiles)
            cols, q_t, do_t = ops[i][:3]
            dv_acc[:, rows(t)] += dot_nt(do_t, probs[g - 2])
            part = dot_nn(kt_ref[:, rows(t)], d_scores[g - 2])
            dq[i] = part if t == 0 else dq[i] + part
            if t == tiles - 1:
                grad_ref[0, :, cols] = (dq[i] * scale).astype(BF)
            dk_acc[:, rows(t)] += dot_nt(q_t, d_scores[g - 2])

    @pl.when(step == pl.num_programs(1) - 1)
    def _():
        grad_ref[1] = (dk_acc[...] * scale).astype(BF)
        grad_ref[2] = dv_acc[...].astype(BF)


def attention_backward(q_t, k_t, v_t, do_t, lse, delta, head_dim, group=4):
    width, tokens = q_t.shape
    heads = width // head_dim
    full = pl.BlockSpec((head_dim, tokens), lambda h, j: (h, 0))
    stat = pl.BlockSpec((16, tokens), lambda h, j: (h, 0))
    return pl.pallas_call(
        functools.partial(backward_body, head_dim ** -0.5, group),
        grid=(heads, tokens // (Q_BLOCK * group)),
        in_specs=[full] * 4 + [stat] * 2,
        out_specs=pl.BlockSpec((3, head_dim, tokens), lambda h, j: (0, h, 0)),
        out_shape=jax.ShapeDtypeStruct((3, width, tokens), BF),
        scratch_shapes=[pltpu.VMEM((tokens, AUG), BF)] * 2 + [pltpu.VMEM((head_dim, tokens), F32)] * 2,
        compiler_params=pltpu.CompilerParams(vmem_limit_bytes=40 * 2 ** 20),
        cost_estimate=pl.CostEstimate(flops=10 * heads * tokens * tokens * head_dim, bytes_accessed=16 * width * tokens,
                                      transcendentals=heads * tokens * tokens),
        name='attention_backward',
    )(q_t, k_t, v_t, do_t, lse, delta)


MESH = pl.DeviceIdType.MESH
RING = 4


def ring_copies(src, relay, fin, sems, axis_pos, device_of, split, rows):
    send, recv = sems
    right, left, across = (lax.rem(axis_pos + k, RING) for k in (1, RING - 1, 2))
    low, high = pl.ds(0, split), pl.ds(split, rows - split)

    def copy(k, source, target, where):
        return pltpu.make_async_remote_copy(src_ref=source, dst_ref=target, send_sem=send.at[k], recv_sem=recv.at[k],
                                            device_id=device_of(where), device_id_type=MESH)

    return [copy(0, src.at[across, low], relay.at[low], right),
            copy(1, src.at[across, high], relay.at[high], left),
            copy(2, src.at[right, high], fin.at[0, high], right),
            copy(3, src.at[left, low], fin.at[1, low], left),
            copy(4, relay.at[low], fin.at[0, low], right),
            copy(5, relay.at[high], fin.at[1, high], left)]


def gather_copies(out, first, stride, rows, sems, axis_pos, device_of, split):
    send, recv = sems
    right, left = lax.rem(axis_pos + 1, RING), lax.rem(axis_pos + RING - 1, RING)

    def copy(k, block, begin, size, where):
        part = out.at[pl.ds(pl.multiple_of(first + block * stride + begin, 8), size)]
        return pltpu.make_async_remote_copy(src_ref=part, dst_ref=part, send_sem=send.at[k], recv_sem=recv.at[k],
                                            device_id=device_of(where), device_id_type=MESH)

    return [copy(0, axis_pos, 0, rows, right), copy(1, axis_pos, 0, rows, left),
            copy(2, left, 0, split, right), copy(3, right, split, rows - split, left)]


def all_reduce_body(depth, gp_ref, gq_ref, out_ref,
                    p_relay, p_fin, q_relay, q_fin, p2, q2, p2_relay, p2_fin, q2_relay, q2_fin,
                    z_src, z_recv, z_out, ring_sems, ag_sems, z_sems, swap_sems):
    dp, x = lax.axis_index('dp'), lax.axis_index('cp')
    core = lax.rem(dp, 2)
    y = lax.rem(dp // 2, RING)
    z = dp // (2 * RING)

    def at(zz, yy, cc):
        return (zz * RING + yy) * 2 + cc

    def on_x(pos):
        return (dp, pos)

    def on_y(pos):
        return (at(z, pos, core), x)

    def on_z(pos):
        return (at(pos, y, core), x)

    peer = (at(z, y, 1 - core), x)
    barrier = pltpu.get_barrier_semaphore()
    peers = [on_x(lax.rem(x + 1, RING)), on_x(lax.rem(x + RING - 1, RING)),
             on_y(lax.rem(y + 1, RING)), on_y(lax.rem(y + RING - 1, RING)), peer]
    peers += [on_z(lax.rem(z + d, depth)) for d in range(1, depth)]
    for device in peers:
        pl.semaphore_signal(barrier, inc=1, device_id=device, device_id_type=MESH)
    pl.semaphore_wait(barrier, len(peers))

    def sems(pool, k):
        return pool.at[0, k], pool.at[1, k]

    def two_rings(first, second):
        plans = [ring_copies(src, relay, fin, sm, pos, dev, split, rows)
                 for src, relay, fin, pos, dev, split, rows, sm in (first, second)]
        for k in range(4):
            for plan in plans:
                plan[k].start()
        for way, k in ((0, 4), (1, 5)):
            for plan, (src, relay, fin, pos, dev, split, rows, sm) in zip(plans, (first, second)):
                part = pl.ds(0, split) if way == 0 else pl.ds(split, rows - split)
                owner = lax.rem(pos + (1 if way == 0 else RING - 1), RING)
                plan[way].wait_recv()
                relay[part] = src[owner, part] + relay[part]
                plan[k].start()
        for k in (2, 3, 4, 5):
            for plan in plans:
                plan[k].wait_recv()
        for plan in plans:
            for copy in plan:
                copy.wait_send()

    two_rings((gp_ref, p_relay, p_fin, y, on_y, 88, 168, sems(ring_sems, 0)),
              (gq_ref, q_relay, q_fin, x, on_x, 80, 160, sems(ring_sems, 1)))
    tail = pl.ds(160, 8)
    for block in range(RING):
        rows = pl.ds(block * 40, 40)
        p2[block, pl.ds(0, 40)] = gp_ref[y, rows] + (p_fin[0, rows] + p_fin[1, rows])
        p2[block, pl.ds(40, 8)] = gp_ref[y, tail] + (p_fin[0, tail] + p_fin[1, tail])
        q2[block] = gq_ref[x, rows] + (q_fin[0, rows] + q_fin[1, rows])
    two_rings((p2, p2_relay, p2_fin, x, on_x, 24, 48, sems(ring_sems, 2)),
              (q2, q2_relay, q2_fin, y, on_y, 24, 40, sems(ring_sems, 3)))
    count = 0
    for src, fin, pos, rows in ((p2, p2_fin, x, 48), (q2, q2_fin, y, 40)):
        for i in range(rows // 8):
            r = pl.ds(i * 8, 8)
            for j in range(5):
                c = pl.ds(j * 128, 128)
                z_src[count] = src[pos, r, c] + (fin[0, r, c] + fin[1, r, c])
                count += 1
    z_src[count] = jnp.zeros((8, 128), F32)
    each = 56 // depth

    def z_copy(k, source, target, d):
        return pltpu.make_async_remote_copy(src_ref=source, dst_ref=target, send_sem=z_sems.at[0, k, d - 1],
                                            recv_sem=z_sems.at[1, k, d - 1], device_id=on_z(lax.rem(z + d, depth)),
                                            device_id_type=MESH)

    mine = pl.ds(z * each, each)
    copies = [z_copy(0, z_src.at[pl.ds(lax.rem(z + d, depth) * each, each)], z_recv.at[d - 1], d)
              for d in range(1, depth)]
    for copy in copies:
        copy.start()
    total = z_src[mine]
    for d, copy in enumerate(copies):
        copy.wait_recv()
        total = total + z_recv[d]
    z_out[mine] = total
    for copy in copies:
        copy.wait_send()
    copies = [z_copy(1, z_out.at[mine], z_out.at[mine], d) for d in range(1, depth)]
    for copy in copies:
        copy.start()
    for copy in copies:
        copy.wait_recv()
    for copy in copies:
        copy.wait_send()

    out = out_ref.at[core]
    p_first, q_first = y * 160, 640 + x * 160
    count = 0
    for first, rows in ((p_first + x * 40, 48), (q_first + y * 40, 40)):
        for i in range(rows // 8):
            for j in range(5):
                c = pl.ds(j * 128, 128)
                if i < 5:
                    out[pl.ds(pl.multiple_of(first + i * 8, 8), 8), c] = z_out[count]
                else:
                    out[pl.ds(1280, 8), c] = z_out[count]
                count += 1

    def two_gathers(first, second):
        plans = [gather_copies(out, base, stride, rows, sm, pos, dev, split)
                 for base, stride, rows, pos, dev, split, sm in (first, second)]
        for k in (0, 1):
            for plan in plans:
                plan[k].start()
        for k in (0, 1):
            for plan in plans:
                plan[k].wait_recv()
                plan[k + 2].start()
        for k in (2, 3):
            for plan in plans:
                plan[k].wait_recv()
        for plan in plans:
            for copy in plan:
                copy.wait_send()

    two_gathers((p_first, 40, 40, x, on_x, 24, sems(ag_sems, 0)), (q_first, 40, 40, y, on_y, 24, sems(ag_sems, 1)))
    two_gathers((0, 160, 160, y, on_y, 80, sems(ag_sems, 2)), (640, 160, 160, x, on_x, 80, sems(ag_sems, 3)))
    swap = pltpu.make_async_remote_copy(src_ref=out, dst_ref=out, send_sem=swap_sems.at[0], recv_sem=swap_sems.at[1],
                                        device_id=peer, device_id_type=MESH)
    swap.start()
    swap.wait()


def all_reduce(grad_p, grad_q, depth):
    channels = grad_p.shape[2]
    vm = lambda *shape: pltpu.VMEM(shape, F32)
    in_vmem = pl.BlockSpec(memory_space=pltpu.VMEM)
    dma = pltpu.SemaphoreType.DMA
    return pl.pallas_call(
        functools.partial(all_reduce_body, depth),
        in_specs=[in_vmem, in_vmem], out_specs=in_vmem,
        out_shape=jax.ShapeDtypeStruct((2, 1288, channels), F32),
        scratch_shapes=[vm(168, channels), vm(2, 168, channels), vm(160, channels), vm(2, 160, channels),
                        vm(RING, 48, channels), vm(RING, 40, channels), vm(48, channels), vm(2, 48, channels),
                        vm(40, channels), vm(2, 40, channels), vm(56, 8, 128), vm(max(depth - 1, 1), 56 // depth, 8, 128),
                        vm(56, 8, 128), dma((2, 4, 6)), dma((2, 4, 4)), dma((2, 2, max(depth - 1, 1))), dma((2,))],
        compiler_params=pltpu.CompilerParams(collective_id=0, has_side_effects=True, vmem_limit_bytes=40 * 2 ** 20),
        name='grad_all_reduce',
    )(grad_p, grad_q)


def solution(mesh):
    dp_size = mesh.shape['dp']
    cp_size = mesh.shape['cp']
    axes = ('dp', 'cp')
    act_spec = P('dp', 'cp', None)
    rep_spec = P()

    def index_of(dp, cp):
        return dp * cp_size + cp

    send_same, send_cross, swap = [], [], []
    for dp in range(dp_size):
        group, core = dp // 2, dp % 2
        for cp in range(cp_size):
            half, parity = cp // 2, cp % 2
            send_same.append((index_of(dp, cp), index_of(2 * group + half, 2 * core + parity)))
            send_cross.append((index_of(dp, cp), index_of(2 * group + half, 2 * core + 1 - parity)))
            swap.append((index_of(dp, cp), index_of(dp ^ 1, cp)))
    back_same = [(dst, src) for src, dst in send_same]
    back_cross = [(dst, src) for src, dst in send_cross]

    def device_step(x_in, grad_y, ln_gamma, ln_beta, w_q, w_k, w_v, w_o, b_o):
        channels = x_in.shape[2]
        num_heads, head_dim = w_q.shape[1], w_q.shape[2]
        half_heads = num_heads // 2
        width = half_heads * head_dim
        core = lax.rem(lax.axis_index('dp'), 2)
        parity = lax.rem(lax.axis_index('cp'), 2)

        def permute(value, pairs):
            return lax.ppermute(value, axes, pairs)

        def gather_image(band_pair):
            first = lax.dynamic_index_in_dim(band_pair, parity, 0, keepdims=False)
            second = lax.dynamic_index_in_dim(band_pair, 1 - parity, 0, keepdims=False)
            own_a, own_b = permute(first, send_same), permute(second, send_cross)
            return own_a, own_b, permute(own_a, swap), permute(own_b, swap)

        def scatter_image(own):
            half = own.shape[0] // 2
            same, cross = permute(own[:half], back_same), permute(own[half:], back_cross)
            return jnp.where(parity == 0, jnp.stack([same, cross]), jnp.stack([cross, same]))

        def head_slice(weight, which):
            return lax.dynamic_slice_in_dim(weight, which * half_heads, half_heads, 1).reshape(channels, width)

        def out_slice(which):
            return lax.dynamic_slice_in_dim(w_o, which * half_heads, half_heads, 0).reshape(width, channels)

        x_parts = gather_image(x_in)
        dy_parts = gather_image(grad_y)
        x_all = jnp.concatenate(x_parts, axis=0)
        dy_all = jnp.concatenate(dy_parts, axis=0)
        tokens = x_all.shape[0]
        own = tokens // 2

        x_f = x_all.astype(F32)
        mean = jnp.mean(x_f, axis=-1, keepdims=True)
        centered = x_f - mean
        inv_std = lax.rsqrt(jnp.mean(centered * centered, axis=-1, keepdims=True) + LN_EPS)
        normed = (centered * inv_std * ln_gamma + ln_beta).astype(BF)

        wq_mine, wk_mine, wv_mine = (head_slice(w, core) for w in (w_q, w_k, w_v))
        wq_other, wk_other, wv_other = (head_slice(w, 1 - core) for w in (w_q, w_k, w_v))
        wo_mine, wo_other = out_slice(core), out_slice(1 - core)

        def project(weight):
            return lax.dot_general(weight, normed, (((0,), (1,)), ((), ())), preferred_element_type=F32).astype(BF)

        q_t, k_t, v_t = project(wq_mine), project(wk_mine), project(wv_mine)
        o_t, o_f, lse = attention_forward(q_t, k_t, v_t, head_dim)
        o_peer = permute(o_t[:, own:], swap)
        do_t = dot_nt(wo_mine, dy_all).astype(BF)
        delta = jnp.sum((o_f * do_t.astype(F32)).reshape(half_heads, head_dim, tokens), axis=1)
        delta = jnp.pad(jnp.stack(split_parts(delta), axis=1), ((0, 0), (0, 13), (0, 0))).reshape(half_heads * 16, tokens)
        y_f = x_all[:own].astype(F32) + (dot_tn(o_t[:, :own], wo_mine) + dot_tn(o_peer, wo_other)) + b_o
        y_own, delta = lax.optimization_barrier((y_f.astype(BF), delta))
        y_same = permute(y_own[:own // 2], back_same)
        y_cross = permute(y_own[own // 2:], back_cross)
        dqkv_t = attention_backward(q_t, k_t, v_t, do_t, lse, delta, head_dim)
        y_out = jnp.where(parity == 0, jnp.stack([y_same, y_cross]), jnp.stack([y_cross, y_same]))
        dqkv_t = dqkv_t.reshape(3 * width, tokens)
        dqkv_peer = permute(dqkv_t[:, own:], swap)
        w_mine = jnp.concatenate([wq_mine, wk_mine, wv_mine], axis=1)
        w_other = jnp.concatenate([wq_other, wk_other, wv_other], axis=1)
        d_normed = (lax.dot_general(dqkv_t[:, :own], w_mine, (((0,), (1,)), ((), ())), preferred_element_type=F32)
                    + lax.dot_general(dqkv_peer, w_other, (((0,), (1,)), ((), ())), preferred_element_type=F32))
        d_normed = d_normed.astype(BF).astype(F32)
        x_hat = centered[:own] * inv_std[:own]
        d_hat = d_normed * ln_gamma
        mean_one = jnp.mean(d_hat, axis=-1, keepdims=True)
        mean_two = jnp.mean(d_hat * x_hat, axis=-1, keepdims=True)
        dx = inv_std[:own] * (d_hat - mean_one - x_hat * mean_two)
        dx = (dy_all[:own].astype(F32) + dx).astype(BF)
        grad_x = scatter_image(dx)

        small = jnp.stack([jnp.sum(d_normed * x_hat, axis=0), jnp.sum(d_normed, axis=0),
                           jnp.sum(dy_all[:own].astype(F32), axis=0)])
        d_w = jnp.concatenate([dot_nn(dqkv_t, normed), dot_nn(o_t, dy_all)], axis=0)
        grad_p = jnp.concatenate([d_w[:640].reshape(4, 160, channels),
                                  jnp.broadcast_to(jnp.pad(small, ((0, 5), (0, 0))), (4, 8, channels))], axis=1)
        both = all_reduce(grad_p, d_w[640:].reshape(4, 160, channels), dp_size // 8)
        small = both[0, 1280:] + both[1, 1280:]
        both = jnp.transpose(both[:, :1280].reshape(2, 4, half_heads, head_dim, channels), (1, 0, 2, 3, 4))
        both = both.reshape(4, num_heads, head_dim, channels)
        grads = [jnp.transpose(both[i], (2, 0, 1)) for i in range(3)]
        return (y_out, grad_x, small[0], small[1], grads[0], grads[1], grads[2], both[3], small[2])

    return jax.shard_map(device_step, mesh=mesh,
                         in_specs=(act_spec, act_spec) + (rep_spec,) * 7,
                         out_specs=(act_spec, act_spec) + (rep_spec,) * 7,
                         check_vma=False)
```

```python
import functools
import math
import jax
import jax.numpy as jnp
from jax import lax
from jax.experimental import pallas as pl
from jax.experimental.pallas import tpu as pltpu
from jax.sharding import PartitionSpec as P


LN_EPS = 1e-5
KEY_TILE = 256
Q_BLOCK = 256
FOLD = 16
AUG = 96
BF = jnp.bfloat16
F32 = jnp.float32


def dot_nn(lhs, rhs):
    return lax.dot_general(lhs, rhs, (((1,), (0,)), ((), ())), preferred_element_type=F32)


def dot_nt(lhs, rhs):
    return lax.dot_general(lhs, rhs, (((1,), (1,)), ((), ())), preferred_element_type=F32)


def dot_tn(lhs, rhs):
    return lax.dot_general(lhs, rhs, (((0,), (0,)), ((), ())), preferred_element_type=F32)


def split_parts(value):
    high = value.astype(BF)
    rest = value - high.astype(F32)
    mid = rest.astype(BF)
    return high, mid, (rest - mid.astype(F32)).astype(BF)


def fold_rows(value, op):
    groups = value.reshape(value.shape[0] // FOLD, FOLD, value.shape[1])
    out = groups[0]
    for i in range(1, groups.shape[0]):
        out = op(out, groups[i])
    return out


def forward_body(scale, group, qt_ref, kt_ref, vt_ref, ot_ref, of_ref, lse_ref, k_s, v_s, *bufs):
    step = pl.program_id(1)
    zero = jnp.minimum(step, 0)
    dim, tokens = kt_ref.shape
    tiles = tokens // KEY_TILE
    log2_scale = scale * math.log2(math.e)

    @pl.when(step == 0)
    def _():
        k_t = kt_ref[...]
        k_s[...] = jnp.concatenate([k_t, k_t, k_t], axis=0).T
        v_s[0:dim, :] = vt_ref[...]
        v_s[dim:, :] = jnp.concatenate([jnp.ones((1, tokens), F32), jnp.zeros((AUG - dim - 1, tokens), F32)], axis=0).astype(BF)

    def rows(tile, base=None):
        return pl.ds(tile * KEY_TILE if base is None else pl.multiple_of(base + tile * KEY_TILE, KEY_TILE), KEY_TILE)

    def block(i):
        return pl.ds(pl.multiple_of((step * group + i) * Q_BLOCK, Q_BLOCK), Q_BLOCK)

    total = tiles * group
    lag = tiles + 1
    query, part, top, probs, out = {}, {}, {}, {}, {}
    for g in range(total + lag + 2):
        if g < total:
            i, t = divmod(g, tiles)
            if t == 0:
                query[i] = jnp.concatenate(split_parts(qt_ref[:, block(i)].astype(F32) * log2_scale), axis=0)
            scores = dot_nn(k_s[rows(t), :], query[i])
            bufs[i % len(bufs)][rows(t), :] = scores
            folded = fold_rows(scores, jnp.maximum)
            part[i] = folded if t == 0 else jnp.maximum(part[i], folded)
            if t == tiles - 1:
                top[i] = jnp.max(part[i], axis=0, keepdims=True)
        if lag <= g < total + lag:
            i, t = divmod(g - lag, tiles)
            probs[g - lag] = jnp.exp2(bufs[i % len(bufs)][rows(t, zero), :] - top[i]).astype(BF)
        if g >= lag + 2:
            i, t = divmod(g - lag - 2, tiles)
            part_out = dot_nn(v_s[:, rows(t)], probs[g - lag - 2])
            out[i] = part_out if t == 0 else out[i] + part_out
            if t == tiles - 1:
                denom = out[i][dim:dim + 1]
                normed = out[i][:dim] * (1.0 / denom)
                ot_ref[:, block(i)] = normed.astype(BF)
                of_ref[:, block(i)] = normed
                lse = (top[i] + jnp.log2(denom)) * (1.0 / log2_scale)
                lse_ref[:, block(i)] = jnp.concatenate([p.astype(F32) for p in split_parts(lse)] + [jnp.zeros((13, Q_BLOCK), F32)], axis=0).astype(BF)


def attention_forward(q_t, k_t, v_t, head_dim, group=4):
    width, tokens = q_t.shape
    heads = width // head_dim
    full = pl.BlockSpec((head_dim, tokens), lambda h, j: (h, 0))
    stat = pl.BlockSpec((16, tokens), lambda h, j: (h, 0))
    return pl.pallas_call(
        functools.partial(forward_body, head_dim ** -0.5, group),
        grid=(heads, tokens // (Q_BLOCK * group)),
        in_specs=[full] * 3, out_specs=[full, full, stat],
        out_shape=[jax.ShapeDtypeStruct((width, tokens), BF), jax.ShapeDtypeStruct((width, tokens), F32),
                   jax.ShapeDtypeStruct((heads * 16, tokens), BF)],
        scratch_shapes=[pltpu.VMEM((tokens, 3 * head_dim), BF), pltpu.VMEM((AUG, tokens), BF)]
        + [pltpu.VMEM((tokens, Q_BLOCK), F32)] * 3,
        compiler_params=pltpu.CompilerParams(vmem_limit_bytes=40 * 2 ** 20),
        cost_estimate=pl.CostEstimate(flops=4 * heads * tokens * tokens * head_dim, bytes_accessed=12 * width * tokens,
                                      transcendentals=heads * tokens * tokens),
        name='attention_forward',
    )(q_t, k_t, v_t)


MESH = pl.DeviceIdType.MESH
RING = 4
ROUNDS = 5
ROUND_ROWS = 256
SPLIT = 384
ORDER = (('y', 'x'), ('y', 'x'), ('y', 'x'), ('y', 'y'), ('y', 'x'))


class Links:
    def __init__(self, depth):
        dp, self.x = lax.axis_index('dp'), lax.axis_index('cp')
        self.core = lax.rem(dp, 2)
        self.y = lax.rem(dp // 2, RING)
        self.z = dp // (2 * RING)
        self.depth = depth
        self.pos = {'x': self.x, 'y': self.y, 'z': self.z}
        self.size = {'x': RING, 'y': RING, 'z': depth}
        self.peer = self.at(core=1 - self.core)
        pair, odd = self.x // 2, lax.rem(self.x, 2)
        self.owners = [(pair, 2 * self.core + odd), (pair, 2 * self.core + 1 - odd)]
        self.workers = [(pair, 2 * self.core), (pair, 2 * self.core + 1)]

    def at(self, x=None, y=None, z=None, core=None):
        pick = lambda value, own: own if value is None else value
        return ((pick(z, self.z) * RING + pick(y, self.y)) * 2 + pick(core, self.core), pick(x, self.x))

    def step(self, axis, d):
        return self.at(**{axis: lax.rem(self.pos[axis] + d, self.size[axis])})

    def is_self(self, place):
        return jnp.logical_and(place[0] == self.core, place[1] == self.x)


def remote(source, target, send, recv, device):
    return pltpu.make_async_remote_copy(src_ref=source, dst_ref=target, send_sem=send, recv_sem=recv,
                                        device_id=device, device_id_type=MESH)


class GradReduce:
    def __init__(self, links, grad, out, result, bufs, sems):
        self.result = result
        self.links, self.grad, self.both, self.out = links, grad, out, out.at[links.core]
        (self.relay1, self.fin1, self.mid, self.relay2, self.fin2, self.z_src, self.z_recv, self.z_out) = bufs
        self.rs_sems, self.ag_sems, self.z_sems, self.swap_sems, self.store_sems = sems

    def axes(self, rnd, unit):
        first = ORDER[rnd][unit]
        return first, ('x' if first == 'y' else 'y')

    def scatter(self, rnd, unit, phase):
        links = self.links
        axis = self.axes(rnd, unit)[phase]
        pos = links.pos[axis]
        right, left, across = (lax.rem(pos + k, RING) for k in (1, RING - 1, 2))
        to_right, to_left = links.step(axis, 1), links.step(axis, RING - 1)
        low, high = pl.ds(0, SPLIT), pl.ds(SPLIT, 640 - SPLIT)
        if phase == 0:
            rows, relay, fin = 32, self.relay1.at[rnd, unit], self.fin1.at[rnd, unit]
            first = rnd * ROUND_ROWS + unit * 128
            src = lambda owner: self.grad.at[pl.ds(pl.multiple_of(first + owner * 32, 8), 32)]
        else:
            rows, relay, fin = 8, self.relay2.at[rnd, unit], self.fin2.at[rnd, unit]
            src = lambda owner: self.mid.at[rnd, unit, pl.ds(pl.multiple_of(owner * 8, 8), 8)]
        every = pl.ds(0, rows)
        send = lambda k: self.rs_sems.at[0, rnd, unit, phase, k]
        recv = lambda k: self.rs_sems.at[1, rnd, unit, phase, k]
        copies = [remote(src(across).at[every, low], relay.at[every, low], send(0), recv(0), to_right),
                  remote(src(across).at[every, high], relay.at[every, high], send(1), recv(1), to_left),
                  remote(src(right).at[every, high], fin.at[0, every, high], send(2), recv(2), to_right),
                  remote(src(left).at[every, low], fin.at[1, every, low], send(3), recv(3), to_left),
                  remote(relay.at[every, low], fin.at[0, every, low], send(4), recv(4), to_right),
                  remote(relay.at[every, high], fin.at[1, every, high], send(5), recv(5), to_left)]
        return copies, src, relay, fin, pos, right, left, low, high

    def scatter_start(self, rnd, unit, phase):
        copies = self.scatter(rnd, unit, phase)[0]
        for copy in copies[:4]:
            copy.start()

    def scatter_relay(self, rnd, unit, phase):
        copies, src, relay, _, _, right, left, low, high = self.scatter(rnd, unit, phase)
        for k, owner, cols in ((0, right, low), (1, left, high)):
            copies[k].wait_recv()
            relay[:, cols] = relay[:, cols] + src(owner)[:, cols]
            copies[4 + k].start()

    def scatter_end(self, rnd, unit, phase):
        copies, src, _, fin, pos = self.scatter(rnd, unit, phase)[:5]
        for k in (2, 3, 4, 5):
            copies[k].wait_recv()
        for copy in copies:
            copy.wait_send()
        return src(pos)[...] + (fin[0] + fin[1])

    def gather(self, rnd, unit, phase):
        links = self.links
        order = self.axes(rnd, unit)
        axis = order[phase]
        pos = links.pos[axis]
        rows = 32 if phase == 0 else 8
        first = rnd * ROUND_ROWS + unit * 128
        if phase == 1:
            first = first + links.pos[order[0]] * 32
        right, left = lax.rem(pos + 1, RING), lax.rem(pos + RING - 1, RING)
        to_right, to_left = links.step(axis, 1), links.step(axis, RING - 1)
        low, high, every = pl.ds(0, SPLIT), pl.ds(SPLIT, 640 - SPLIT), pl.ds(0, 640)

        def copy(k, block, cols, device):
            part = self.out.at[pl.ds(pl.multiple_of(first + block * rows, 8), rows), cols]
            return remote(part, part, self.ag_sems.at[0, rnd, unit, phase, k], self.ag_sems.at[1, rnd, unit, phase, k], device)

        return [copy(0, pos, every, to_right), copy(1, pos, every, to_left),
                copy(2, left, low, to_right), copy(3, right, high, to_left)]

    def gather_start(self, rnd, unit, phase):
        for copy in self.gather(rnd, unit, phase)[:2]:
            copy.start()

    def gather_relay(self, rnd, unit, phase):
        copies = self.gather(rnd, unit, phase)
        for k in (0, 1):
            copies[k].wait_recv()
            copies[k + 2].start()

    def gather_end(self, rnd, unit, phase):
        copies = self.gather(rnd, unit, phase)
        for k in (2, 3):
            copies[k].wait_recv()
        for copy in copies:
            copy.wait_send()

    def z_copies(self, rnd, way):
        links = self.links
        each = 16 // links.depth
        send, recv = self.z_sems.at[0, rnd, way], self.z_sems.at[1, rnd, way]
        mine = pl.ds(links.z * each, each)
        copies = []
        for d in range(1, links.depth):
            far = lax.rem(links.z + d, links.depth)
            if way == 0:
                source, target = self.z_src.at[rnd, pl.ds(far * each, each)], self.z_recv.at[rnd, d - 1]
            else:
                source = target = self.z_out.at[rnd, mine]
            copies.append(remote(source, target, send, recv, links.step('z', d)))
        return copies, mine

    def z_wait(self, rnd, way):
        if self.links.depth > 1:
            whole = self.z_recv.at[rnd]
            all_of = remote(whole, whole, self.z_sems.at[0, rnd, way], self.z_sems.at[1, rnd, way], self.links.step('z', 1))
            all_of.wait_recv()
            all_of.wait_send()

    def swap(self, rnd):
        part = self.out.at[pl.ds(rnd * ROUND_ROWS, ROUND_ROWS)]
        return remote(part, part, self.swap_sems.at[0, rnd], self.swap_sems.at[1, rnd], self.links.peer)

    def stage(self, rnd, k):
        units = (0, 1)
        if k == 0:
            for u in units:
                self.scatter_start(rnd, u, 0)
        elif k == 1:
            for u in units:
                self.scatter_relay(rnd, u, 0)
        elif k == 2:
            for u in units:
                self.mid[rnd, u] = self.scatter_end(rnd, u, 0)
                self.scatter_start(rnd, u, 1)
        elif k == 3:
            for u in units:
                self.scatter_relay(rnd, u, 1)
        elif k == 4:
            for u in units:
                total = self.scatter_end(rnd, u, 1)
                for j in range(5):
                    self.z_src[rnd, u * 5 + j] = total[:, j * 128:(j + 1) * 128]
            self.z_src[rnd, pl.ds(10, 6)] = jnp.zeros((6, 8, 128), F32)
            for copy in self.z_copies(rnd, 0)[0]:
                copy.start()
        elif k == 5:
            self.z_wait(rnd, 0)
            copies, mine = self.z_copies(rnd, 1)
            total = self.z_src[rnd, mine]
            for d in range(self.links.depth - 1):
                total = total + self.z_recv[rnd, d]
            self.z_out[rnd, mine] = total
            for copy in copies:
                copy.start()
        elif k == 6:
            self.z_wait(rnd, 1)
            for u in units:
                order = self.axes(rnd, u)
                first = rnd * ROUND_ROWS + u * 128 + self.links.pos[order[0]] * 32 + self.links.pos[order[1]] * 8
                for j in range(5):
                    self.out[pl.ds(pl.multiple_of(first, 8), 8), pl.ds(j * 128, 128)] = self.z_out[rnd, u * 5 + j]
                self.gather_start(rnd, u, 1)
        elif k == 7:
            for u in units:
                self.gather_relay(rnd, u, 1)
        elif k == 8:
            for u in units:
                self.gather_end(rnd, u, 1)
                self.gather_start(rnd, u, 0)
        elif k == 9:
            for u in units:
                self.gather_relay(rnd, u, 0)
        elif k == 10:
            for u in units:
                self.gather_end(rnd, u, 0)
            self.swap(rnd).start()
        else:
            self.swap(rnd).wait()
            self.store(rnd).start()

    def store(self, rnd):
        rows = pl.ds(rnd * ROUND_ROWS, ROUND_ROWS)
        return pltpu.make_async_copy(self.both.at[:, rows], self.result.at[:, rows], self.store_sems.at[rnd])


def backward_body(scale, group, depth, qt_ref, kt_ref, vt_ref, do_ref, lse_ref, delta_ref,
                  normed_ref, dy_ref, ot_ref, x_ref, wt_ref, gamma_ref, gx_ref, out_ref, small_ref,
                  k_s, v_s, dk_acc, dv_acc, grads, grads_peer, d_w, d_w_all, dx_s,
                  relay1, fin1, mid, relay2, fin2, z_src, z_recv, z_out, small_s, small_recv,
                  rs_sems, ag_sems, z_sems, swap_sems, store_sems, grad_sems, gx_send, gx_recv, small_sems):
    head, step = pl.program_id(0), pl.program_id(1)
    heads, steps = 4, kt_ref.shape[1] // (Q_BLOCK * group)
    now = head * steps + step
    dim, tokens = kt_ref.shape
    own = tokens // 2
    width = heads * dim
    tiles = tokens // KEY_TILE
    log2_scale = scale * math.log2(math.e)
    links = Links(depth)
    reduce = GradReduce(links, d_w, d_w_all, out_ref, (relay1, fin1, mid, relay2, fin2, z_src, z_recv, z_out),
                        (rs_sems, ag_sems, z_sems, swap_sems, store_sems))
    head_rows = pl.ds(pl.multiple_of(head * dim, 16), dim)

    def swap_grads(h):
        rows = pl.ds(pl.multiple_of(h * dim, 16), dim)
        return remote(grads.at[:, rows, pl.ds(own, own)], grads_peer.at[:, rows], grad_sems.at[0, h], grad_sems.at[1, h], links.peer)

    @pl.when(now == 0)
    def _():
        barrier = pltpu.get_barrier_semaphore()
        fixed = [links.peer]
        fixed += [links.step(axis, d) for axis in ('x', 'y') for d in (1, 2, 3)]
        fixed += [links.step('z', d) for d in range(1, depth)]
        for device in fixed:
            pl.semaphore_signal(barrier, inc=1, device_id=device, device_id_type=MESH)
        count = len(fixed)
        for place in links.owners + links.workers:
            other = jnp.logical_not(links.is_self(place))
            count = count + other.astype(jnp.int32)

            @pl.when(other)
            def _():
                pl.semaphore_signal(barrier, inc=1, device_id=links.at(core=place[0], x=place[1]), device_id_type=MESH)
        pl.semaphore_wait(barrier, count)
        d_w[pl.ds(0, width)] = dot_nn(ot_ref[...], dy_ref[...])

    for at in range(heads * steps):
        todo = [(rnd, at - rnd * steps) for rnd in range(ROUNDS - 1) if 0 <= at - rnd * steps <= 11]
        if todo:
            @pl.when(now == at)
            def _():
                for rnd, k in todo:
                    reduce.stage(rnd, k)

    @pl.when(step == 0)
    def _():
        minus = jnp.concatenate([jnp.full((3, tokens), -1.0, F32), jnp.zeros((AUG - dim - 3, tokens), F32)], axis=0).astype(BF)
        k_s[...] = jnp.concatenate([kt_ref[...], minus], axis=0).T
        v_s[...] = jnp.concatenate([vt_ref[...], minus], axis=0).T
        dk_acc[...] = jnp.zeros_like(dk_acc)
        dv_acc[...] = jnp.zeros_like(dv_acc)

    def rows_of(tile):
        return pl.ds(tile * KEY_TILE, KEY_TILE)

    total = tiles * group
    ops, probs, d_scores, dq = {}, {}, {}, {}
    for g in range(total + 2):
        if g < total:
            i, t = divmod(g, tiles)
            if t == 0:
                cols = pl.ds(pl.multiple_of((step * group + i) * Q_BLOCK, Q_BLOCK), Q_BLOCK)
                q_t, do_t = qt_ref[:, cols], do_ref[:, cols]
                ops[i] = (cols, q_t, do_t, jnp.concatenate([q_t, lse_ref[:, cols]], axis=0),
                          jnp.concatenate([do_t, delta_ref[:, cols]], axis=0))
            scores = dot_nn(k_s[rows_of(t), :], ops[i][3])
            d_probs = dot_nn(v_s[rows_of(t), :], ops[i][4])
            prob = jnp.exp2(scores * log2_scale)
            probs[g] = prob.astype(BF)
            d_scores[g] = (prob * d_probs).astype(BF)
        if g >= 2:
            i, t = divmod(g - 2, tiles)
            cols, q_t, do_t = ops[i][:3]
            dv_acc[:, rows_of(t)] += dot_nt(do_t, probs[g - 2])
            part = dot_nn(kt_ref[:, rows_of(t)], d_scores[g - 2])
            dq[i] = part if t == 0 else dq[i] + part
            if t == tiles - 1:
                grads[0, head_rows, cols] = (dq[i] * scale).astype(BF)
            dk_acc[:, rows_of(t)] += dot_nt(q_t, d_scores[g - 2])

    @pl.when(step == steps - 1)
    def _():
        grads[1, head_rows] = (dk_acc[...] * scale).astype(BF)
        grads[2, head_rows] = dv_acc[...].astype(BF)
        stacked = jnp.concatenate([grads[0, head_rows], grads[1, head_rows], grads[2, head_rows]], axis=0)
        d_w[pl.ds(pl.multiple_of(width + head * (3 * dim), 8), 3 * dim)] = dot_nn(stacked, normed_ref[...])
        swap_grads(head).start()

    @pl.when(now == heads * steps - 1)
    def _():
        def tail(slot):
            last = heads * steps + slot
            for rnd in range(ROUNDS):
                if 0 <= last - rnd * steps <= 11:
                    reduce.stage(rnd, last - rnd * steps)

        tail(0)
        for h in range(heads):
            swap_grads(h).wait()
        gamma = gamma_ref[...]
        sums = [jnp.zeros((1, 640), F32)] * 3
        band = own // 2
        piece = band // 2
        odd = lax.rem(links.x, 2)

        def send_dx(i, start):
            core, x = links.owners[i // 2]
            source = dx_s.at[pl.ds(i * piece, piece)]
            target = gx_ref.at[odd, pl.ds((i % 2) * piece, piece)]
            far = remote(source, target, gx_send.at[i], gx_recv.at[odd, i % 2], links.at(core=core, x=x))
            near = pltpu.make_async_copy(source, target, gx_recv.at[odd, i % 2])
            here = links.is_self((core, x))

            @pl.when(jnp.logical_not(here))
            def _():
                far.start() if start else far.wait_send()

            if start:
                @pl.when(here)
                def _():
                    near.start()

        for i in range(4):
            toks = pl.ds(i * piece, piece)
            mine = jnp.concatenate([grads[k, :, toks] for k in range(3)], axis=0)
            theirs = jnp.concatenate([grads_peer[k, :, toks] for k in range(3)], axis=0)
            d_normed = (dot_tn(mine, wt_ref[0]) + dot_tn(theirs, wt_ref[1])).astype(BF).astype(F32)
            x_f = x_ref[toks].astype(F32)
            centered = x_f - jnp.mean(x_f, axis=-1, keepdims=True)
            inv_std = lax.rsqrt(jnp.mean(centered * centered, axis=-1, keepdims=True) + LN_EPS)
            x_hat = centered * inv_std
            d_hat = d_normed * gamma
            mean_one = jnp.mean(d_hat, axis=-1, keepdims=True)
            mean_two = jnp.mean(d_hat * x_hat, axis=-1, keepdims=True)
            dy_f = dy_ref[toks].astype(F32)
            dx_s[toks] = (dy_f + inv_std * (d_hat - mean_one - x_hat * mean_two)).astype(BF)
            send_dx(i, True)
            for k, term in enumerate((d_normed * x_hat, d_normed, dy_f)):
                sums[k] = sums[k] + jnp.sum(term, axis=0, keepdims=True)
            tail(1 + i)

        for k in range(3):
            for j in range(5):
                small_s[0, pl.ds(k * 5 + j, 1)] = sums[k][:, j * 128:(j + 1) * 128]
        small_s[0, pl.ds(15, 1)] = jnp.zeros((1, 128), F32)
        first = 0
        for hop, axis in enumerate(('x', 'y', 'z', 'core')):
            far = [links.peer] if axis == 'core' else [links.step(axis, d) for d in range(1, links.size[axis])]
            copies = [remote(small_s.at[hop], small_recv.at[first + d], small_sems.at[0, first + d], small_sems.at[1, first + d], device)
                      for d, device in enumerate(far)]
            for copy in copies:
                copy.start()
            tail(5 + hop)
            acc = small_s[hop]
            for d, copy in enumerate(copies):
                copy.wait_recv()
                acc = acc + small_recv[first + d]
            for copy in copies:
                copy.wait_send()
            if hop < 3:
                small_s[hop + 1] = acc
            else:
                small_ref[...] = acc
            first += len(far)
        for slot in range(9, 12):
            tail(slot)
        for rnd in range(ROUNDS):
            reduce.store(rnd).wait()
        for i in range(4):
            send_dx(i, False)
        for m in range(2):
            for i in range(2):
                part = gx_ref.at[m, pl.ds(i * piece, piece)]
                pltpu.make_async_copy(part, part, gx_recv.at[m, i]).wait()


def attention_backward(q_t, k_t, v_t, do_t, lse, delta, normed, dy, o_t, x_own, w_t, gamma, head_dim, depth, group=2):
    width, tokens = q_t.shape
    heads = width // head_dim
    channels = normed.shape[1]
    own = tokens // 2
    full = pl.BlockSpec((head_dim, tokens), lambda h, j: (h, 0))
    stat = pl.BlockSpec((16, tokens), lambda h, j: (h, 0))

    def whole(shape):
        return pl.BlockSpec(shape, lambda h, j: (0,) * len(shape), pipeline_mode=pl.Buffered(1))

    vm = lambda *shape: pltpu.VMEM(shape, F32)
    dma = pltpu.SemaphoreType.DMA
    far = max(depth - 1, 1)
    return pl.pallas_call(
        functools.partial(backward_body, head_dim ** -0.5, group, depth),
        grid=(heads, tokens // (Q_BLOCK * group)),
        in_specs=[full] * 4 + [stat] * 2 + [whole(a.shape) for a in (normed, dy, o_t, x_own, w_t, gamma)],
        out_specs=[pl.BlockSpec(memory_space=pl.ANY)] * 2 + [whole((16, 128))],
        out_shape=[jax.ShapeDtypeStruct((2, own // 2, channels), BF), jax.ShapeDtypeStruct((2, 1280, channels), F32),
                   jax.ShapeDtypeStruct((16, 128), F32)],
        scratch_shapes=[pltpu.VMEM((tokens, AUG), BF)] * 2 + [vm(head_dim, tokens)] * 2
        + [pltpu.VMEM((3, width, tokens), BF), pltpu.VMEM((3, width, own), BF), vm(1280, channels), vm(2, 1280, channels), pltpu.VMEM((own, channels), BF),
           vm(ROUNDS, 2, 32, channels), vm(ROUNDS, 2, 2, 32, channels), vm(ROUNDS, 2, 32, channels),
           vm(ROUNDS, 2, 8, channels), vm(ROUNDS, 2, 2, 8, channels), vm(ROUNDS, 16, 8, 128),
           vm(ROUNDS, far, 16 // depth, 8, 128), vm(ROUNDS, 16, 8, 128), vm(4, 16, 128), vm(7 + far, 16, 128),
           dma((2, ROUNDS, 2, 2, 6)), dma((2, ROUNDS, 2, 2, 4)), dma((2, ROUNDS, 2)), dma((2, ROUNDS)), dma((ROUNDS,)), dma((2, 4)),
           dma((4,)), dma((2, 2)), dma((2, 7 + far))],
        compiler_params=pltpu.CompilerParams(collective_id=0, has_side_effects=True, vmem_limit_bytes=60 * 2 ** 20),
        cost_estimate=pl.CostEstimate(flops=10 * heads * tokens * tokens * head_dim, bytes_accessed=16 * width * tokens,
                                      transcendentals=heads * tokens * tokens),
        name='attention_backward',
    )(q_t, k_t, v_t, do_t, lse, delta, normed, dy, o_t, x_own, w_t, gamma)


def solution(mesh):
    dp_size = mesh.shape['dp']
    cp_size = mesh.shape['cp']
    axes = ('dp', 'cp')
    act_spec = P('dp', 'cp', None)
    rep_spec = P()

    def index_of(dp, cp):
        return dp * cp_size + cp

    send_same, send_cross, swap = [], [], []
    for dp in range(dp_size):
        group, core = dp // 2, dp % 2
        for cp in range(cp_size):
            half, parity = cp // 2, cp % 2
            send_same.append((index_of(dp, cp), index_of(2 * group + half, 2 * core + parity)))
            send_cross.append((index_of(dp, cp), index_of(2 * group + half, 2 * core + 1 - parity)))
            swap.append((index_of(dp, cp), index_of(dp ^ 1, cp)))
    back_same = [(dst, src) for src, dst in send_same]
    back_cross = [(dst, src) for src, dst in send_cross]

    def device_step(x_in, grad_y, ln_gamma, ln_beta, w_q, w_k, w_v, w_o, b_o):
        channels = x_in.shape[2]
        num_heads, head_dim = w_q.shape[1], w_q.shape[2]
        half_heads = num_heads // 2
        width = half_heads * head_dim
        core = lax.rem(lax.axis_index('dp'), 2)
        parity = lax.rem(lax.axis_index('cp'), 2)

        def permute(value, pairs):
            return lax.ppermute(value, axes, pairs)

        def gather_image(band_pair):
            first = lax.dynamic_index_in_dim(band_pair, parity, 0, keepdims=False)
            second = lax.dynamic_index_in_dim(band_pair, 1 - parity, 0, keepdims=False)
            own_a, own_b = permute(first, send_same), permute(second, send_cross)
            return own_a, own_b, permute(own_a, swap), permute(own_b, swap)

        def head_slice(weight, which):
            return lax.dynamic_slice_in_dim(weight, which * half_heads, half_heads, 1).reshape(channels, width)

        def out_slice(which):
            return lax.dynamic_slice_in_dim(w_o, which * half_heads, half_heads, 0).reshape(width, channels)

        x_parts = gather_image(x_in)
        dy_parts = gather_image(grad_y)
        x_all = jnp.concatenate(x_parts, axis=0)
        dy_all = jnp.concatenate(dy_parts, axis=0)
        tokens = x_all.shape[0]
        own = tokens // 2

        x_f = x_all.astype(F32)
        mean = jnp.mean(x_f, axis=-1, keepdims=True)
        centered = x_f - mean
        inv_std = lax.rsqrt(jnp.mean(centered * centered, axis=-1, keepdims=True) + LN_EPS)
        normed = (centered * inv_std * ln_gamma + ln_beta).astype(BF)

        wq_mine, wk_mine, wv_mine = (head_slice(w, core) for w in (w_q, w_k, w_v))
        wq_other, wk_other, wv_other = (head_slice(w, 1 - core) for w in (w_q, w_k, w_v))
        wo_mine, wo_other = out_slice(core), out_slice(1 - core)

        w_t = jnp.stack([jnp.concatenate([wq_mine, wk_mine, wv_mine], axis=1).T,
                         jnp.concatenate([wq_other, wk_other, wv_other], axis=1).T])

        def project(weight):
            return lax.dot_general(weight, normed, (((0,), (1,)), ((), ())), preferred_element_type=F32).astype(BF)

        q_t, k_t, v_t = project(wq_mine), project(wk_mine), project(wv_mine)
        o_t, o_f, lse = attention_forward(q_t, k_t, v_t, head_dim)
        o_peer = permute(o_t[:, own:], swap)
        do_t = dot_nt(wo_mine, dy_all).astype(BF)
        delta = jnp.sum((o_f * do_t.astype(F32)).reshape(half_heads, head_dim, tokens), axis=1)
        delta = jnp.pad(jnp.stack(split_parts(delta), axis=1), ((0, 0), (0, 13), (0, 0))).reshape(half_heads * 16, tokens)
        y_f = x_all[:own].astype(F32) + (dot_tn(o_t[:, :own], wo_mine) + dot_tn(o_peer, wo_other)) + b_o
        y_own, delta = lax.optimization_barrier((y_f.astype(BF), delta))
        y_same = permute(y_own[:own // 2], back_same)
        y_cross = permute(y_own[own // 2:], back_cross)
        grad_x, both, small = attention_backward(q_t, k_t, v_t, do_t, lse, delta, normed, dy_all, o_t, x_all[:own], w_t,
                                                 ln_gamma.reshape(1, channels), head_dim, dp_size // 8)
        y_out = jnp.where(parity == 0, jnp.stack([y_same, y_cross]), jnp.stack([y_cross, y_same]))
        small = small[:15].reshape(3, channels)
        grad_wo = both[:, :width].reshape(num_heads, head_dim, channels)
        both = both[:, width:].reshape(num_heads, 3, head_dim, channels)
        grads = [jnp.transpose(both[:, i], (2, 0, 1)) for i in range(3)]
        return (y_out, grad_x, small[0], small[1], grads[0], grads[1], grads[2], grad_wo, small[2])

    return jax.shard_map(device_step, mesh=mesh,
                         in_specs=(act_spec, act_spec) + (rep_spec,) * 7,
                         out_specs=(act_spec, act_spec) + (rep_spec,) * 7,
                         check_vma=False)
```

```python
import functools
import math
import jax
import jax.numpy as jnp
from jax import lax
from jax.experimental import pallas as pl
from jax.experimental.pallas import tpu as pltpu
from jax.sharding import PartitionSpec as P


LN_EPS = 1e-5
KEY_TILE = 256
Q_BLOCK = 256
FOLD = 16
AUG = 96
BF = jnp.bfloat16
F32 = jnp.float32


def dot_nn(lhs, rhs):
    return lax.dot_general(lhs, rhs, (((1,), (0,)), ((), ())), preferred_element_type=F32)


def dot_nt(lhs, rhs):
    return lax.dot_general(lhs, rhs, (((1,), (1,)), ((), ())), preferred_element_type=F32)


def dot_tn(lhs, rhs):
    return lax.dot_general(lhs, rhs, (((0,), (0,)), ((), ())), preferred_element_type=F32)


def split_parts(value):
    high = value.astype(BF)
    rest = value - high.astype(F32)
    mid = rest.astype(BF)
    return high, mid, (rest - mid.astype(F32)).astype(BF)


def fold_rows(value, op):
    groups = value.reshape(value.shape[0] // FOLD, FOLD, value.shape[1])
    out = groups[0]
    for i in range(1, groups.shape[0]):
        out = op(out, groups[i])
    return out


def forward_body(scale, group, qt_ref, kt_ref, vt_ref, ot_ref, of_ref, lse_ref, k_s, v_s, *bufs):
    step = pl.program_id(1)
    zero = jnp.minimum(step, 0)
    dim, tokens = kt_ref.shape
    tiles = tokens // KEY_TILE
    log2_scale = scale * math.log2(math.e)

    @pl.when(step == 0)
    def _():
        k_t = kt_ref[...]
        k_s[...] = jnp.concatenate([k_t, k_t, k_t], axis=0).T
        v_s[0:dim, :] = vt_ref[...]
        v_s[dim:, :] = jnp.concatenate([jnp.ones((1, tokens), F32), jnp.zeros((AUG - dim - 1, tokens), F32)], axis=0).astype(BF)

    def rows(tile, base=None):
        return pl.ds(tile * KEY_TILE if base is None else pl.multiple_of(base + tile * KEY_TILE, KEY_TILE), KEY_TILE)

    def block(i):
        return pl.ds(pl.multiple_of((step * group + i) * Q_BLOCK, Q_BLOCK), Q_BLOCK)

    total = tiles * group
    lag = tiles + 1
    query, part, top, probs, out = {}, {}, {}, {}, {}
    for g in range(total + lag + 2):
        if g < total:
            i, t = divmod(g, tiles)
            if t == 0:
                query[i] = jnp.concatenate(split_parts(qt_ref[:, block(i)].astype(F32) * log2_scale), axis=0)
            scores = dot_nn(k_s[rows(t), :], query[i])
            bufs[i % len(bufs)][rows(t), :] = scores
            folded = fold_rows(scores, jnp.maximum)
            part[i] = folded if t == 0 else jnp.maximum(part[i], folded)
            if t == tiles - 1:
                top[i] = jnp.max(part[i], axis=0, keepdims=True)
        if lag <= g < total + lag:
            i, t = divmod(g - lag, tiles)
            probs[g - lag] = jnp.exp2(bufs[i % len(bufs)][rows(t, zero), :] - top[i]).astype(BF)
        if g >= lag + 2:
            i, t = divmod(g - lag - 2, tiles)
            part_out = dot_nn(v_s[:, rows(t)], probs[g - lag - 2])
            out[i] = part_out if t == 0 else out[i] + part_out
            if t == tiles - 1:
                denom = out[i][dim:dim + 1]
                normed = out[i][:dim] * (1.0 / denom)
                ot_ref[:, block(i)] = normed.astype(BF)
                of_ref[:, block(i)] = normed
                lse = (top[i] + jnp.log2(denom)) * (1.0 / log2_scale)
                lse_ref[:, block(i)] = jnp.concatenate([p.astype(F32) for p in split_parts(lse)] + [jnp.zeros((13, Q_BLOCK), F32)], axis=0).astype(BF)


def attention_forward(q_t, k_t, v_t, head_dim, group=4):
    width, tokens = q_t.shape
    heads = width // head_dim
    full = pl.BlockSpec((head_dim, tokens), lambda h, j: (h, 0))
    stat = pl.BlockSpec((16, tokens), lambda h, j: (h, 0))
    return pl.pallas_call(
        functools.partial(forward_body, head_dim ** -0.5, group),
        grid=(heads, tokens // (Q_BLOCK * group)),
        in_specs=[full] * 3, out_specs=[full, full, stat],
        out_shape=[jax.ShapeDtypeStruct((width, tokens), BF), jax.ShapeDtypeStruct((width, tokens), F32),
                   jax.ShapeDtypeStruct((heads * 16, tokens), BF)],
        scratch_shapes=[pltpu.VMEM((tokens, 3 * head_dim), BF), pltpu.VMEM((AUG, tokens), BF)]
        + [pltpu.VMEM((tokens, Q_BLOCK), F32)] * 3,
        compiler_params=pltpu.CompilerParams(vmem_limit_bytes=40 * 2 ** 20),
        cost_estimate=pl.CostEstimate(flops=4 * heads * tokens * tokens * head_dim, bytes_accessed=12 * width * tokens,
                                      transcendentals=heads * tokens * tokens),
        name='attention_forward',
    )(q_t, k_t, v_t)


MESH = pl.DeviceIdType.MESH
RING = 4
ROUNDS = 5
ROUND_ROWS = 256
STAGES = 8
ORDER = (('y', 'x'), ('y', 'x'), ('y', 'x'), ('y', 'y'), ('y', 'x'))


class Links:
    def __init__(self, depth):
        dp, self.x = lax.axis_index('dp'), lax.axis_index('cp')
        self.core = lax.rem(dp, 2)
        self.y = lax.rem(dp // 2, RING)
        self.z = dp // (2 * RING)
        self.depth = depth
        self.pos = {'x': self.x, 'y': self.y, 'z': self.z}
        self.size = {'x': RING, 'y': RING, 'z': depth}
        self.peer = self.at(core=1 - self.core)
        pair, odd = self.x // 2, lax.rem(self.x, 2)
        self.owners = [(pair, 2 * self.core + odd), (pair, 2 * self.core + 1 - odd)]
        self.workers = [(pair, 2 * self.core), (pair, 2 * self.core + 1)]

    def at(self, x=None, y=None, z=None, core=None):
        pick = lambda value, own: own if value is None else value
        return ((pick(z, self.z) * RING + pick(y, self.y)) * 2 + pick(core, self.core), pick(x, self.x))

    def step(self, axis, d):
        return self.at(**{axis: lax.rem(self.pos[axis] + d, self.size[axis])})

    def is_self(self, place):
        return jnp.logical_and(place[0] == self.core, place[1] == self.x)


def remote(source, target, send, recv, device):
    return pltpu.make_async_remote_copy(src_ref=source, dst_ref=target, send_sem=send, recv_sem=recv,
                                        device_id=device, device_id_type=MESH)


class GradReduce:
    def __init__(self, links, grad, out, result, bufs, sems):
        self.links, self.grad, self.both, self.out, self.result = links, grad, out, out.at[links.core], result
        self.recv1, self.recv2, self.mid, self.z_src, self.z_recv, self.z_out = bufs
        self.rs_sems, self.ag_sems, self.z_sems, self.swap_sems, self.store_sems = sems

    def axes(self, rnd, unit):
        first = ORDER[rnd][unit]
        return first, ('x' if first == 'y' else 'y')

    def block(self, rnd, unit, phase):
        first = rnd * ROUND_ROWS + unit * 128
        if phase == 0:
            return first, 32
        return first + self.links.pos[self.axes(rnd, unit)[0]] * 32, 8

    def landing(self, rnd, unit, phase):
        return (self.recv1 if phase == 0 else self.recv2).at[rnd, unit]

    def wait_all(self, rnd, unit, phase, sems):
        whole = self.landing(rnd, unit, phase)
        every = remote(whole, whole, sems.at[0, rnd, unit, phase], sems.at[1, rnd, unit, phase], self.links.peer)
        every.wait_recv()
        every.wait_send()

    def source(self, rnd, unit, phase, owner):
        if phase == 0:
            first, rows = self.block(rnd, unit, 0)
            return self.grad.at[pl.ds(pl.multiple_of(first + owner * rows, 8), rows)]
        return self.mid.at[rnd, unit, pl.ds(pl.multiple_of(owner * 8, 8), 8)]

    def scatter_start(self, rnd, unit, phase):
        axis = self.axes(rnd, unit)[phase]
        for d in (2, 1, 3):
            owner = lax.rem(self.links.pos[axis] + d, RING)
            remote(self.source(rnd, unit, phase, owner), self.landing(rnd, unit, phase).at[d - 1],
                   self.rs_sems.at[0, rnd, unit, phase], self.rs_sems.at[1, rnd, unit, phase], self.links.step(axis, d)).start()

    def scatter_end(self, rnd, unit, phase):
        self.wait_all(rnd, unit, phase, self.rs_sems)
        landing = self.landing(rnd, unit, phase)
        mine = self.source(rnd, unit, phase, self.links.pos[self.axes(rnd, unit)[phase]])
        return (mine[...] + landing[0]) + (landing[1] + landing[2])

    def gather_start(self, rnd, unit, phase):
        axis = self.axes(rnd, unit)[phase]
        first, rows = self.block(rnd, unit, phase)
        part = self.out.at[pl.ds(pl.multiple_of(first + self.links.pos[axis] * rows, 8), rows)]
        for d in (2, 1, 3):
            remote(part, part, self.ag_sems.at[0, rnd, unit, phase], self.ag_sems.at[1, rnd, unit, phase],
                   self.links.step(axis, d)).start()

    def z_copies(self, rnd, way):
        links = self.links
        each = 16 // links.depth
        send, recv = self.z_sems.at[0, rnd, way], self.z_sems.at[1, rnd, way]
        mine = pl.ds(links.z * each, each)
        copies = []
        for d in range(1, links.depth):
            far = lax.rem(links.z + d, links.depth)
            if way == 0:
                source, target = self.z_src.at[rnd, pl.ds(far * each, each)], self.z_recv.at[rnd, d - 1]
            else:
                source = target = self.z_out.at[rnd, mine]
            copies.append(remote(source, target, send, recv, links.step('z', d)))
        return copies, mine

    def z_wait(self, rnd, way):
        if self.links.depth > 1:
            whole = self.z_recv.at[rnd]
            all_of = remote(whole, whole, self.z_sems.at[0, rnd, way], self.z_sems.at[1, rnd, way], self.links.step('z', 1))
            all_of.wait_recv()
            all_of.wait_send()

    def swap(self, rnd):
        part = self.out.at[pl.ds(rnd * ROUND_ROWS, ROUND_ROWS)]
        return remote(part, part, self.swap_sems.at[0, rnd], self.swap_sems.at[1, rnd], self.links.peer)

    def store(self, rnd):
        rows = pl.ds(rnd * ROUND_ROWS, ROUND_ROWS)
        return pltpu.make_async_copy(self.both.at[:, rows], self.result.at[:, rows], self.store_sems.at[rnd])

    def stage(self, rnd, k):
        units = (0, 1)
        if k == 0:
            for u in units:
                self.scatter_start(rnd, u, 0)
        elif k == 1:
            for u in units:
                self.mid[rnd, u] = self.scatter_end(rnd, u, 0)
                self.scatter_start(rnd, u, 1)
        elif k == 2:
            for u in units:
                total = self.scatter_end(rnd, u, 1)
                for j in range(5):
                    self.z_src[rnd, u * 5 + j] = total[:, j * 128:(j + 1) * 128]
            self.z_src[rnd, pl.ds(10, 6)] = jnp.zeros((6, 8, 128), F32)
            for copy in self.z_copies(rnd, 0)[0]:
                copy.start()
        elif k == 3:
            self.z_wait(rnd, 0)
            copies, mine = self.z_copies(rnd, 1)
            total = self.z_src[rnd, mine]
            for d in range(self.links.depth - 1):
                total = total + self.z_recv[rnd, d]
            self.z_out[rnd, mine] = total
            for copy in copies:
                copy.start()
        elif k == 4:
            self.z_wait(rnd, 1)
            for u in units:
                first = self.block(rnd, u, 1)[0] + self.links.pos[self.axes(rnd, u)[1]] * 8
                for j in range(5):
                    self.out[pl.ds(pl.multiple_of(first, 8), 8), pl.ds(j * 128, 128)] = self.z_out[rnd, u * 5 + j]
                self.gather_start(rnd, u, 1)
        elif k == 5:
            for u in units:
                self.wait_all(rnd, u, 1, self.ag_sems)
                self.gather_start(rnd, u, 0)
        elif k == 6:
            for u in units:
                self.wait_all(rnd, u, 0, self.ag_sems)
            self.swap(rnd).start()
        else:
            self.swap(rnd).wait()
            self.store(rnd).start()


def backward_body(scale, group, depth, qt_ref, kt_ref, vt_ref, do_ref, lse_ref, delta_ref,
                  normed_hbm, dy_hbm, ot_hbm, x_hbm, wt_hbm, gamma_ref, gx_ref, out_ref, small_ref,
                  normed_ref, dy_ref, ot_ref, x_ref, wt_ref, load_sems,
                  k_s, v_s, dk_acc, dv_acc, grads, grads_peer, d_w, d_w_all, dx_s,
                  recv1, recv2, mid, z_src, z_recv, z_out, small_s, small_recv,
                  rs_sems, ag_sems, z_sems, swap_sems, store_sems, grad_sems, gx_send, gx_recv, small_sems):
    head, step = pl.program_id(0), pl.program_id(1)
    heads, steps = 4, kt_ref.shape[1] // (Q_BLOCK * group)
    now = head * steps + step
    dim, tokens = kt_ref.shape
    own = tokens // 2
    width = heads * dim
    tiles = tokens // KEY_TILE
    log2_scale = scale * math.log2(math.e)
    links = Links(depth)
    reduce = GradReduce(links, d_w, d_w_all, out_ref, (recv1, recv2, mid, z_src, z_recv, z_out),
                        (rs_sems, ag_sems, z_sems, swap_sems, store_sems))
    head_rows = pl.ds(pl.multiple_of(head * dim, 16), dim)

    def swap_grads(h):
        rows = pl.ds(pl.multiple_of(h * dim, 16), dim)
        return remote(grads.at[:, rows, pl.ds(own, own)], grads_peer.at[:, rows], grad_sems.at[0, h], grad_sems.at[1, h], links.peer)

    fixed = [links.peer]
    fixed += [links.step(axis, d) for axis in ('x', 'y') for d in (1, 2, 3)]
    fixed += [links.step('z', d) for d in range(1, depth)]
    places = links.owners + links.workers
    peer_count = len(fixed)
    for place in places:
        peer_count = peer_count + jnp.logical_not(links.is_self(place)).astype(jnp.int32)
    loads = [pltpu.make_async_copy(source, target, load_sems.at[i]) for i, (source, target) in enumerate(
        ((ot_hbm, ot_ref), (dy_hbm, dy_ref), (normed_hbm, normed_ref), (x_hbm, x_ref), (wt_hbm, wt_ref)))]

    @pl.when(now == 0)
    def _():
        barrier = pltpu.get_barrier_semaphore()
        for device in fixed:
            pl.semaphore_signal(barrier, inc=1, device_id=device, device_id_type=MESH)
        for place in places:
            other = jnp.logical_not(links.is_self(place))

            @pl.when(other)
            def _():
                pl.semaphore_signal(barrier, inc=1, device_id=links.at(core=place[0], x=place[1]), device_id_type=MESH)
        for load in loads:
            load.start()

    @pl.when(now == 1)
    def _():
        pl.semaphore_wait(pltpu.get_barrier_semaphore(), peer_count)
        loads[0].wait()
        loads[1].wait()
        d_w[pl.ds(0, width)] = dot_nn(ot_ref[...], dy_ref[...])

    end = heads * steps
    plan, ahead = {}, [0] * ROUNDS
    for at in range(1, end + STAGES):
        due = []
        for rnd in range(ROUNDS):
            wait = at - max(rnd * steps, 1)
            if ahead[rnd] < STAGES and wait >= 0 and (at >= end or wait % 2 == 0):
                due.append((rnd, ahead[rnd]))
                ahead[rnd] += 1
        plan[at] = due if at > end else due[::-1]

    for at in range(1, heads * steps):
        todo = plan[at]
        if todo:
            @pl.when(now == at)
            def _():
                for rnd, k in todo:
                    reduce.stage(rnd, k)

    @pl.when(step == 0)
    def _():
        minus = jnp.concatenate([jnp.full((3, tokens), -1.0, F32), jnp.zeros((AUG - dim - 3, tokens), F32)], axis=0).astype(BF)
        k_s[...] = jnp.concatenate([kt_ref[...], minus], axis=0).T
        v_s[...] = jnp.concatenate([vt_ref[...], minus], axis=0).T
        dk_acc[...] = jnp.zeros_like(dk_acc)
        dv_acc[...] = jnp.zeros_like(dv_acc)

    def rows_of(tile):
        return pl.ds(tile * KEY_TILE, KEY_TILE)

    total = tiles * group
    ops, probs, d_scores, dq = {}, {}, {}, {}
    for g in range(total + 2):
        if g < total:
            i, t = divmod(g, tiles)
            if t == 0:
                cols = pl.ds(pl.multiple_of((step * group + i) * Q_BLOCK, Q_BLOCK), Q_BLOCK)
                q_t, do_t = qt_ref[:, cols], do_ref[:, cols]
                ops[i] = (cols, q_t, do_t, jnp.concatenate([q_t, lse_ref[:, cols]], axis=0),
                          jnp.concatenate([do_t, delta_ref[:, cols]], axis=0))
            scores = dot_nn(k_s[rows_of(t), :], ops[i][3])
            d_probs = dot_nn(v_s[rows_of(t), :], ops[i][4])
            prob = jnp.exp2(scores * log2_scale)
            probs[g] = prob.astype(BF)
            d_scores[g] = (prob * d_probs).astype(BF)
        if g >= 2:
            i, t = divmod(g - 2, tiles)
            cols, q_t, do_t = ops[i][:3]
            dv_acc[:, rows_of(t)] += dot_nt(do_t, probs[g - 2])
            part = dot_nn(kt_ref[:, rows_of(t)], d_scores[g - 2])
            dq[i] = part if t == 0 else dq[i] + part
            if t == tiles - 1:
                grads[0, head_rows, cols] = (dq[i] * scale).astype(BF)
            dk_acc[:, rows_of(t)] += dot_nt(q_t, d_scores[g - 2])

    @pl.when(step == steps - 1)
    def _():
        grads[1, head_rows] = (dk_acc[...] * scale).astype(BF)
        grads[2, head_rows] = dv_acc[...].astype(BF)

        @pl.when(head == 0)
        def _():
            loads[2].wait()

        stacked = jnp.concatenate([grads[0, head_rows], grads[1, head_rows], grads[2, head_rows]], axis=0)
        d_w[pl.ds(pl.multiple_of(width + head * (3 * dim), 8), 3 * dim)] = dot_nn(stacked, normed_ref[...])
        swap_grads(head).start()

    @pl.when(now == heads * steps - 1)
    def _():
        def tail(slot):
            last = heads * steps + slot
            for rnd, k in plan[last]:
                reduce.stage(rnd, k)

        tail(0)
        for h in range(heads):
            swap_grads(h).wait()
        loads[3].wait()
        loads[4].wait()
        gamma = gamma_ref[...]
        sums = [jnp.zeros((1, 640), F32)] * 3
        band = own // 2
        piece = band // 2
        odd = lax.rem(links.x, 2)

        def send_dx(i, start):
            core, x = links.owners[i // 2]
            source = dx_s.at[pl.ds(i * piece, piece)]
            target = gx_ref.at[odd, pl.ds((i % 2) * piece, piece)]
            far = remote(source, target, gx_send.at[i], gx_recv.at[odd, i % 2], links.at(core=core, x=x))
            near = pltpu.make_async_copy(source, target, gx_recv.at[odd, i % 2])
            here = links.is_self((core, x))

            @pl.when(jnp.logical_not(here))
            def _():
                far.start() if start else far.wait_send()

            if start:
                @pl.when(here)
                def _():
                    near.start()

        for i in range(4):
            toks = pl.ds(i * piece, piece)
            mine = jnp.concatenate([grads[k, :, toks] for k in range(3)], axis=0)
            theirs = jnp.concatenate([grads_peer[k, :, toks] for k in range(3)], axis=0)
            d_normed = (dot_tn(mine, wt_ref[0]) + dot_tn(theirs, wt_ref[1])).astype(BF).astype(F32)
            x_f = x_ref[toks].astype(F32)
            centered = x_f - jnp.mean(x_f, axis=-1, keepdims=True)
            inv_std = lax.rsqrt(jnp.mean(centered * centered, axis=-1, keepdims=True) + LN_EPS)
            x_hat = centered * inv_std
            d_hat = d_normed * gamma
            mean_one = jnp.mean(d_hat, axis=-1, keepdims=True)
            mean_two = jnp.mean(d_hat * x_hat, axis=-1, keepdims=True)
            dy_f = dy_ref[toks].astype(F32)
            dx_s[toks] = (dy_f + inv_std * (d_hat - mean_one - x_hat * mean_two)).astype(BF)
            send_dx(i, True)
            for k, term in enumerate((d_normed * x_hat, d_normed, dy_f)):
                sums[k] = sums[k] + jnp.sum(term, axis=0, keepdims=True)
            tail(1 + i)

        for k in range(3):
            for j in range(5):
                small_s[0, pl.ds(k * 5 + j, 1)] = sums[k][:, j * 128:(j + 1) * 128]
        small_s[0, pl.ds(15, 1)] = jnp.zeros((1, 128), F32)
        first = 0
        for hop, axis in enumerate(('x', 'y', 'z', 'core')):
            far = [links.peer] if axis == 'core' else [links.step(axis, d) for d in range(1, links.size[axis])]
            copies = [remote(small_s.at[hop], small_recv.at[first + d], small_sems.at[0, first + d], small_sems.at[1, first + d], device)
                      for d, device in enumerate(far)]
            for copy in copies:
                copy.start()
            if 5 + hop < STAGES:
                tail(5 + hop)
            acc = small_s[hop]
            for d, copy in enumerate(copies):
                copy.wait_recv()
                acc = acc + small_recv[first + d]
            for copy in copies:
                copy.wait_send()
            if hop < 3:
                small_s[hop + 1] = acc
            else:
                small_ref[...] = acc
            first += len(far)
        for rnd in range(ROUNDS):
            reduce.store(rnd).wait()
        for i in range(4):
            send_dx(i, False)
        for m in range(2):
            for i in range(2):
                part = gx_ref.at[m, pl.ds(i * piece, piece)]
                pltpu.make_async_copy(part, part, gx_recv.at[m, i]).wait()


def attention_backward(q_t, k_t, v_t, do_t, lse, delta, normed, dy, o_t, x_own, w_t, gamma, head_dim, depth, group=2):
    width, tokens = q_t.shape
    heads = width // head_dim
    channels = normed.shape[1]
    own = tokens // 2
    full = pl.BlockSpec((head_dim, tokens), lambda h, j: (h, 0))
    stat = pl.BlockSpec((16, tokens), lambda h, j: (h, 0))

    def whole(shape):
        return pl.BlockSpec(shape, lambda h, j: (0,) * len(shape), pipeline_mode=pl.Buffered(1))

    vm = lambda *shape: pltpu.VMEM(shape, F32)
    dma = pltpu.SemaphoreType.DMA
    far = max(depth - 1, 1)
    return pl.pallas_call(
        functools.partial(backward_body, head_dim ** -0.5, group, depth),
        grid=(heads, tokens // (Q_BLOCK * group)),
        in_specs=[full] * 4 + [stat] * 2 + [pl.BlockSpec(memory_space=pl.ANY)] * 5 + [whole(gamma.shape)],
        out_specs=[pl.BlockSpec(memory_space=pl.ANY)] * 2 + [whole((16, 128))],
        out_shape=[jax.ShapeDtypeStruct((2, own // 2, channels), BF), jax.ShapeDtypeStruct((2, 1280, channels), F32),
                   jax.ShapeDtypeStruct((16, 128), F32)],
        scratch_shapes=[pltpu.VMEM(a.shape, BF) for a in (normed, dy, o_t, x_own, w_t)] + [dma((5,))]
        + [pltpu.VMEM((tokens, AUG), BF)] * 2 + [vm(head_dim, tokens)] * 2
        + [pltpu.VMEM((3, width, tokens), BF), pltpu.VMEM((3, width, own), BF), vm(1280, channels), vm(2, 1280, channels), pltpu.VMEM((own, channels), BF),
           vm(ROUNDS, 2, 3, 32, channels), vm(ROUNDS, 2, 3, 8, channels), vm(ROUNDS, 2, 32, channels), vm(ROUNDS, 16, 8, 128),
           vm(ROUNDS, far, 16 // depth, 8, 128), vm(ROUNDS, 16, 8, 128), vm(4, 16, 128), vm(7 + far, 16, 128),
           dma((2, ROUNDS, 2, 2)), dma((2, ROUNDS, 2, 2)), dma((2, ROUNDS, 2)), dma((2, ROUNDS)), dma((ROUNDS,)), dma((2, 4)),
           dma((4,)), dma((2, 2)), dma((2, 7 + far))],
        compiler_params=pltpu.CompilerParams(collective_id=0, has_side_effects=True, vmem_limit_bytes=60 * 2 ** 20),
        cost_estimate=pl.CostEstimate(flops=10 * heads * tokens * tokens * head_dim, bytes_accessed=16 * width * tokens,
                                      transcendentals=heads * tokens * tokens),
        name='attention_backward',
    )(q_t, k_t, v_t, do_t, lse, delta, normed, dy, o_t, x_own, w_t, gamma)


def solution(mesh):
    dp_size = mesh.shape['dp']
    cp_size = mesh.shape['cp']
    axes = ('dp', 'cp')
    act_spec = P('dp', 'cp', None)
    rep_spec = P()

    def index_of(dp, cp):
        return dp * cp_size + cp

    send_same, send_cross, swap = [], [], []
    for dp in range(dp_size):
        group, core = dp // 2, dp % 2
        for cp in range(cp_size):
            half, parity = cp // 2, cp % 2
            send_same.append((index_of(dp, cp), index_of(2 * group + half, 2 * core + parity)))
            send_cross.append((index_of(dp, cp), index_of(2 * group + half, 2 * core + 1 - parity)))
            swap.append((index_of(dp, cp), index_of(dp ^ 1, cp)))
    back_same = [(dst, src) for src, dst in send_same]
    back_cross = [(dst, src) for src, dst in send_cross]

    def device_step(x_in, grad_y, ln_gamma, ln_beta, w_q, w_k, w_v, w_o, b_o):
        channels = x_in.shape[2]
        num_heads, head_dim = w_q.shape[1], w_q.shape[2]
        half_heads = num_heads // 2
        width = half_heads * head_dim
        core = lax.rem(lax.axis_index('dp'), 2)
        parity = lax.rem(lax.axis_index('cp'), 2)

        def permute(value, pairs):
            return lax.ppermute(value, axes, pairs)

        def gather_image(band_pair):
            first = lax.dynamic_index_in_dim(band_pair, parity, 0, keepdims=False)
            second = lax.dynamic_index_in_dim(band_pair, 1 - parity, 0, keepdims=False)
            own_a, own_b = permute(first, send_same), permute(second, send_cross)
            return own_a, own_b, permute(own_a, swap), permute(own_b, swap)

        def head_slice(weight, which):
            return lax.dynamic_slice_in_dim(weight, which * half_heads, half_heads, 1).reshape(channels, width)

        def out_slice(which):
            return lax.dynamic_slice_in_dim(w_o, which * half_heads, half_heads, 0).reshape(width, channels)

        x_parts = gather_image(x_in)
        dy_parts = gather_image(grad_y)
        x_all = jnp.concatenate(x_parts, axis=0)
        dy_all = jnp.concatenate(dy_parts, axis=0)
        tokens = x_all.shape[0]
        own = tokens // 2

        x_f = x_all.astype(F32)
        mean = jnp.mean(x_f, axis=-1, keepdims=True)
        centered = x_f - mean
        inv_std = lax.rsqrt(jnp.mean(centered * centered, axis=-1, keepdims=True) + LN_EPS)
        normed = (centered * inv_std * ln_gamma + ln_beta).astype(BF)

        wq_mine, wk_mine, wv_mine = (head_slice(w, core) for w in (w_q, w_k, w_v))
        wq_other, wk_other, wv_other = (head_slice(w, 1 - core) for w in (w_q, w_k, w_v))
        wo_mine, wo_other = out_slice(core), out_slice(1 - core)

        w_t = jnp.stack([jnp.concatenate([wq_mine, wk_mine, wv_mine], axis=1).T,
                         jnp.concatenate([wq_other, wk_other, wv_other], axis=1).T])

        def project(weight):
            return lax.dot_general(weight, normed, (((0,), (1,)), ((), ())), preferred_element_type=F32).astype(BF)

        q_t, k_t, v_t = project(wq_mine), project(wk_mine), project(wv_mine)
        o_t, o_f, lse = attention_forward(q_t, k_t, v_t, head_dim)
        o_peer = permute(o_t[:, own:], swap)
        do_t = dot_nt(wo_mine, dy_all).astype(BF)
        delta = jnp.sum((o_f * do_t.astype(F32)).reshape(half_heads, head_dim, tokens), axis=1)
        delta = jnp.pad(jnp.stack(split_parts(delta), axis=1), ((0, 0), (0, 13), (0, 0))).reshape(half_heads * 16, tokens)
        y_f = x_all[:own].astype(F32) + (dot_tn(o_t[:, :own], wo_mine) + dot_tn(o_peer, wo_other)) + b_o
        y_own, delta = lax.optimization_barrier((y_f.astype(BF), delta))
        y_same = permute(y_own[:own // 2], back_same)
        y_cross = permute(y_own[own // 2:], back_cross)
        grad_x, both, small = attention_backward(q_t, k_t, v_t, do_t, lse, delta, normed, dy_all, o_t, x_all[:own], w_t,
                                                 ln_gamma.reshape(1, channels), head_dim, dp_size // 8)
        y_out = jnp.where(parity == 0, jnp.stack([y_same, y_cross]), jnp.stack([y_cross, y_same]))
        small = small[:15].reshape(3, channels)
        grad_wo = both[:, :width].reshape(num_heads, head_dim, channels)
        both = both[:, width:].reshape(num_heads, 3, head_dim, channels)
        grads = [jnp.transpose(both[:, i], (2, 0, 1)) for i in range(3)]
        return (y_out, grad_x, small[0], small[1], grads[0], grads[1], grads[2], grad_wo, small[2])

    return jax.shard_map(device_step, mesh=mesh,
                         in_specs=(act_spec, act_spec) + (rep_spec,) * 7,
                         out_specs=(act_spec, act_spec) + (rep_spec,) * 7,
                         check_vma=False)
```

```python
import functools
import math
import jax
import jax.numpy as jnp
from jax import lax
from jax.experimental import pallas as pl
from jax.experimental.pallas import tpu as pltpu
from jax.sharding import PartitionSpec as P

LN_EPS = 1e-5
KEY_TILE = 256
Q_BLOCK = 256
FOLD = 16
AUG = 96
VMEM_BYTES = 67043328
BF = jnp.bfloat16
F32 = jnp.float32


def dot_nn(lhs, rhs):
    return lax.dot_general(lhs, rhs, (((1,), (0,)), ((), ())), preferred_element_type=F32)


def dot_nt(lhs, rhs):
    return lax.dot_general(lhs, rhs, (((1,), (1,)), ((), ())), preferred_element_type=F32)


def dot_tn(lhs, rhs):
    return lax.dot_general(lhs, rhs, (((0,), (0,)), ((), ())), preferred_element_type=F32)


def split_parts(value):
    high = value.astype(BF)
    rest = value - high.astype(F32)
    mid = rest.astype(BF)
    return high, mid, (rest - mid.astype(F32)).astype(BF)


def fold_rows(value, op):
    groups = value.reshape(value.shape[0] // FOLD, FOLD, value.shape[1])
    out = groups[0]
    for i in range(1, groups.shape[0]):
        out = op(out, groups[i])
    return out


MESH = pl.DeviceIdType.MESH
RING = 4
ROUNDS = 5
ROUND_ROWS = 256
STAGES = 8
PIECES = 4
ORDER = (('y', 'x'), ('y', 'x'), ('y', 'x'), ('y', 'y'), ('y', 'x'))


class Links:
    def __init__(self, depth):
        dp, self.x = lax.axis_index('dp'), lax.axis_index('cp')
        self.core = lax.rem(dp, 2)
        self.y = lax.rem(dp // 2, RING)
        self.z = dp // (2 * RING)
        self.depth = depth
        self.pos = {'x': self.x, 'y': self.y, 'z': self.z}
        self.size = {'x': RING, 'y': RING, 'z': depth}
        self.peer = self.at(core=1 - self.core)
        pair, odd = self.x // 2, lax.rem(self.x, 2)
        self.owners = [(pair, 2 * self.core + odd), (pair, 2 * self.core + 1 - odd)]
        self.workers = [(pair, 2 * self.core), (pair, 2 * self.core + 1)]

    def at(self, x=None, y=None, z=None, core=None):
        pick = lambda value, own: own if value is None else value
        return ((pick(z, self.z) * RING + pick(y, self.y)) * 2 + pick(core, self.core), pick(x, self.x))

    def step(self, axis, d):
        return self.at(**{axis: lax.rem(self.pos[axis] + d, self.size[axis])})

    def is_self(self, place):
        return jnp.logical_and(place[0] == self.core, place[1] == self.x)


def remote(source, target, send, recv, device):
    return pltpu.make_async_remote_copy(src_ref=source, dst_ref=target, send_sem=send, recv_sem=recv,
                                        device_id=device, device_id_type=MESH)


class GradReduce:
    def __init__(self, links, grad, out, result, bufs, sems):
        self.links, self.grad, self.both, self.out, self.result = links, grad, out, out.at[links.core], result
        self.recv1, self.recv2, self.mid, self.z_src, self.z_recv, self.z_out = bufs
        self.rs_sems, self.ag_sems, self.z_sems, self.swap_sems, self.store_sems = sems

    def axes(self, rnd, unit):
        first = ORDER[rnd][unit]
        return first, ('x' if first == 'y' else 'y')

    def block(self, rnd, unit, phase):
        first = rnd * ROUND_ROWS + unit * 128
        if phase == 0:
            return first, 32
        return first + self.links.pos[self.axes(rnd, unit)[0]] * 32, 8

    def landing(self, rnd, unit, phase):
        return (self.recv1 if phase == 0 else self.recv2).at[rnd, unit]

    def wait_all(self, rnd, unit, phase, sems):
        whole = self.landing(rnd, unit, phase)
        every = remote(whole, whole, sems.at[0, rnd, unit, phase], sems.at[1, rnd, unit, phase], self.links.peer)
        every.wait_recv()
        every.wait_send()

    def source(self, rnd, unit, phase, owner):
        if phase == 0:
            first, rows = self.block(rnd, unit, 0)
            return self.grad.at[pl.ds(pl.multiple_of(first + owner * rows, 8), rows)]
        return self.mid.at[rnd, unit, pl.ds(pl.multiple_of(owner * 8, 8), 8)]

    def scatter_start(self, rnd, unit, phase):
        axis = self.axes(rnd, unit)[phase]
        for d in (2, 1, 3):
            owner = lax.rem(self.links.pos[axis] + d, RING)
            remote(self.source(rnd, unit, phase, owner), self.landing(rnd, unit, phase).at[d - 1],
                   self.rs_sems.at[0, rnd, unit, phase], self.rs_sems.at[1, rnd, unit, phase], self.links.step(axis, d)).start()

    def scatter_end(self, rnd, unit, phase):
        self.wait_all(rnd, unit, phase, self.rs_sems)
        landing = self.landing(rnd, unit, phase)
        mine = self.source(rnd, unit, phase, self.links.pos[self.axes(rnd, unit)[phase]])
        return (mine[...] + landing[0]) + (landing[1] + landing[2])

    def gather_start(self, rnd, unit, phase):
        axis = self.axes(rnd, unit)[phase]
        first, rows = self.block(rnd, unit, phase)
        part = self.out.at[pl.ds(pl.multiple_of(first + self.links.pos[axis] * rows, 8), rows)]
        for d in (2, 1, 3):
            remote(part, part, self.ag_sems.at[0, rnd, unit, phase], self.ag_sems.at[1, rnd, unit, phase],
                   self.links.step(axis, d)).start()

    def z_copies(self, rnd, way):
        links = self.links
        each = 16 // links.depth
        send, recv = self.z_sems.at[0, rnd, way], self.z_sems.at[1, rnd, way]
        mine = pl.ds(links.z * each, each)
        copies = []
        for d in range(1, links.depth):
            far = lax.rem(links.z + d, links.depth)
            if way == 0:
                source, target = self.z_src.at[rnd, pl.ds(far * each, each)], self.z_recv.at[rnd, d - 1]
            else:
                source = target = self.z_out.at[rnd, mine]
            copies.append(remote(source, target, send, recv, links.step('z', d)))
        return copies, mine

    def z_wait(self, rnd, way):
        if self.links.depth > 1:
            whole = self.z_recv.at[rnd]
            all_of = remote(whole, whole, self.z_sems.at[0, rnd, way], self.z_sems.at[1, rnd, way], self.links.step('z', 1))
            all_of.wait_recv()
            all_of.wait_send()

    def swap(self, rnd):
        part = self.out.at[pl.ds(rnd * ROUND_ROWS, ROUND_ROWS)]
        return remote(part, part, self.swap_sems.at[0, rnd], self.swap_sems.at[1, rnd], self.links.peer)

    def store(self, rnd):
        rows = pl.ds(rnd * ROUND_ROWS, ROUND_ROWS)
        return pltpu.make_async_copy(self.both.at[:, rows], self.result.at[:, rows], self.store_sems.at[rnd])

    def stage(self, rnd, k):
        units = (0, 1)
        if k == 0:
            for u in units:
                self.scatter_start(rnd, u, 0)
        elif k == 1:
            for u in units:
                self.mid[rnd, u] = self.scatter_end(rnd, u, 0)
                self.scatter_start(rnd, u, 1)
        elif k == 2:
            for u in units:
                total = self.scatter_end(rnd, u, 1)
                for j in range(5):
                    self.z_src[rnd, u * 5 + j] = total[:, j * 128:(j + 1) * 128]
            self.z_src[rnd, pl.ds(10, 6)] = jnp.zeros((6, 8, 128), F32)
            for copy in self.z_copies(rnd, 0)[0]:
                copy.start()
        elif k == 3:
            self.z_wait(rnd, 0)
            copies, mine = self.z_copies(rnd, 1)
            total = self.z_src[rnd, mine]
            for d in range(self.links.depth - 1):
                total = total + self.z_recv[rnd, d]
            self.z_out[rnd, mine] = total
            for copy in copies:
                copy.start()
        elif k == 4:
            self.z_wait(rnd, 1)
            for u in units:
                first = self.block(rnd, u, 1)[0] + self.links.pos[self.axes(rnd, u)[1]] * 8
                for j in range(5):
                    self.out[pl.ds(pl.multiple_of(first, 8), 8), pl.ds(j * 128, 128)] = self.z_out[rnd, u * 5 + j]
                self.gather_start(rnd, u, 1)
        elif k == 5:
            for u in units:
                self.wait_all(rnd, u, 1, self.ag_sems)
                self.gather_start(rnd, u, 0)
        elif k == 6:
            for u in units:
                self.wait_all(rnd, u, 0, self.ag_sems)
            self.swap(rnd).start()
        else:
            self.swap(rnd).wait()
            self.store(rnd).start()


def layer_norm(x_ref, rows):
    x_f = x_ref[rows].astype(F32)
    centered = x_f - jnp.mean(x_f, axis=-1, keepdims=True)
    inv_std = lax.rsqrt(jnp.mean(centered * centered, axis=-1, keepdims=True) + LN_EPS)
    return centered * inv_std, inv_std


def padded(parts, rows):
    filled = [part.astype(F32) for part in parts]
    used = sum(part.shape[0] for part in filled)
    return jnp.concatenate(filled + [jnp.zeros((rows - used, filled[0].shape[1]), F32)], axis=0).astype(BF)


def wait_for(ref, sem):
    pltpu.make_async_copy(ref, ref, sem).wait()


def block_body(dim, depth, x_hbm, dy_hbm, wt_hbm, wo_hbm, gamma_ref, beta_ref, bo_ref, y_ref, gx_ref, dw_ref, small_ref,
               x_s, normed_s, dy_s, wt_s, wo_s, q_s, k_s, v_s, do_s, o_s, of_s, o_peer, lse_s, kf_s, vf_s, buf_a, buf_b, buf_c,
               kb_s, vb_s, dk_acc, dv_acc, grads, grads_peer, d_w, d_w_all, dx_s, y_s,
               recv1, recv2, mid, z_src, z_recv, z_out, small_s, small_recv,
               load_sems, in_send, in_recv, pass_send, pass_recv, o_sems, grad_sems, out_send, out_recv, small_sems,
               rs_sems, ag_sems, z_sems, swap_sems, store_sems):
    now = pl.program_id(0)
    links = Links(depth)
    width, tokens = q_s.shape
    heads, tiles = width // dim, tokens // KEY_TILE
    own, band = tokens // 2, tokens // 4
    scale = dim ** -0.5
    log2_scale = scale * math.log2(math.e)
    fwd_group, bwd_group = 4, 2
    fwd_steps, bwd_steps = tiles // fwd_group, tiles // bwd_group
    middle = 1 + heads * fwd_steps
    odd = lax.rem(links.x, 2)
    reduce = GradReduce(links, d_w, d_w_all, dw_ref, (recv1, recv2, mid, z_src, z_recv, z_out),
                        (rs_sems, ag_sems, z_sems, swap_sems, store_sems))
    end = heads * bwd_steps + 1
    plan, ahead = {}, [0] * ROUNDS
    for at in range(end + STAGES):
        due = []
        for rnd in range(ROUNDS):
            age = at - (rnd * bwd_steps + 1 if rnd else 0)
            if ahead[rnd] < STAGES and age >= 0 and (at >= end or age % 2 == 0):
                due.append((rnd, ahead[rnd]))
                ahead[rnd] += 1
        plan[at] = due[::-1]

    def tile_rows(tile, base=None):
        return pl.ds(tile * KEY_TILE if base is None else pl.multiple_of(base + tile * KEY_TILE, KEY_TILE), KEY_TILE)

    def head_rows(head, rows=dim):
        return pl.ds(pl.multiple_of(head * rows, 16), rows)

    def q_cols(index):
        return pl.ds(pl.multiple_of(index * Q_BLOCK, Q_BLOCK), Q_BLOCK)

    def my_half(side):
        return pl.ds(pl.multiple_of((links.core if side == 0 else 1 - links.core) * width, 16), width)

    loads = [pltpu.make_async_copy(wt_hbm.at[k, my_half(side)], wt_s.at[side, pl.ds(k * width, width)], load_sems.at[side, k])
             for side in range(2) for k in range(3)]
    loads += [pltpu.make_async_copy(wo_hbm.at[my_half(side)], wo_s.at[side], load_sems.at[side, 3]) for side in range(2)]

    def maybe_far(place, source, target, send, recv, start):
        core, x = place
        here = links.is_self(place)
        far = remote(source, target, send, recv, links.at(core=core, x=x))
        near = pltpu.make_async_copy(source, target, recv)

        @pl.when(jnp.logical_not(here))
        def _():
            far.start() if start else far.wait_send()

        if start:
            @pl.when(here)
            def _():
                near.start()

    piece = band // PIECES

    def deliver(which, m, c, start):
        slot = lax.rem(links.x + m, 2)
        source = (dy_hbm if which else x_hbm).at[m, pl.ds(c * piece, piece)]
        target = (dy_s if which else x_s).at[pl.ds(pl.multiple_of(slot * band + c * piece, 16), piece)]
        maybe_far(links.workers[m], source, target, in_send.at[which, m, c], in_recv.at[which, slot, c], start)

    def hand_over(which, slot, c):
        rows = dy_s if which else x_s
        first = slot * band + c * piece
        return remote(rows.at[pl.ds(first, piece)], rows.at[pl.ds(own + first, piece)],
                      pass_send.at[which, slot, c], pass_recv.at[which, slot, c], links.peer)

    def arrive(which, slot, c):
        with jax.named_scope(f'arrive{which}{slot}{c}'):
            wait_for((dy_s if which else x_s).at[pl.ds(slot * band + c * piece, piece)], in_recv.at[which, slot, c])
        hand_over(which, slot, c).start()

    def swap_out(head):
        rows = head_rows(head)
        return remote(o_s.at[rows, pl.ds(own, own)], o_peer.at[rows], o_sems.at[0, head], o_sems.at[1, head], links.peer)

    def swap_grads(head):
        rows = head_rows(head)
        return remote(grads.at[:, rows, pl.ds(own, own)], grads_peer.at[:, rows], grad_sems.at[0, head], grad_sems.at[1, head],
                      links.peer)

    part = band // 2

    def send_home(which, i, start):
        source = (dx_s if which else y_s).at[pl.ds(i * part, part)]
        target = (gx_ref if which else y_ref).at[odd, pl.ds((i % 2) * part, part)]
        maybe_far(links.owners[i // 2], source, target, out_send.at[which, i], out_recv.at[which, odd, i % 2], start)

    def received_home(which):
        for m in range(2):
            for i in range(2):
                wait_for((gx_ref if which else y_ref).at[m, pl.ds(i * part, part)], out_recv.at[which, m, i])

    @pl.when(now == 0)
    def _():
        barrier = pltpu.get_barrier_semaphore()
        fixed = [links.peer]
        fixed += [links.step(axis, d) for axis in ('x', 'y') for d in range(1, RING)]
        fixed += [links.step('z', d) for d in range(1, depth)]
        for device in fixed:
            pl.semaphore_signal(barrier, inc=1, device_id=device, device_id_type=MESH)
        count = len(fixed)
        for place in links.owners + links.workers:
            other = jnp.logical_not(links.is_self(place))
            count = count + other.astype(jnp.int32)

            @pl.when(other)
            def _():
                pl.semaphore_signal(barrier, inc=1, device_id=links.at(core=place[0], x=place[1]), device_id_type=MESH)
        for load in loads:
            load.start()
        with jax.named_scope('barrier'):
            pl.semaphore_wait(barrier, count)
        for which in range(2):
            for c in range(PIECES):
                for m in range(2):
                    deliver(which, m, c, True)
        for load in loads:
            load.wait()

        def normalize(first):
            rows = pl.ds(first, piece)
            normed_s[rows] = (layer_norm(x_s, rows)[0] * gamma_ref[...] + beta_ref[...]).astype(BF)

        for c in range(PIECES):
            for slot in range(2):
                arrive(0, slot, c)
                normalize(slot * band + c * piece)
            for slot in range(2):
                with jax.named_scope(f'handed{slot}{c}'):
                    hand_over(0, slot, c).wait_recv()
                normalize(own + slot * band + c * piece)
            if c % 2:
                for b in range(4):
                    cols = pl.ds(b * band + (c - 1) * piece, 2 * piece)
                    normed = normed_s[cols]
                    for k, out in enumerate((q_s, k_s, v_s)):
                        out[:, cols] = dot_nt(wt_s[0, pl.ds(k * width, width)], normed).astype(BF)

    for c in range(PIECES):
        @pl.when(now == (c + 1) * middle // (PIECES + 1) + 1)
        def _():
            for slot in range(2):
                arrive(1, slot, c)

    @pl.when(jnp.logical_and(now > 0, now < middle))
    def _():
        head, step = (now - 1) // fwd_steps, lax.rem(now - 1, fwd_steps)
        zero = jnp.minimum(now, 0)
        rows = head_rows(head)

        @pl.when(step == 0)
        def _():
            k_t = k_s[rows]
            kf_s[...] = jnp.concatenate([k_t, k_t, k_t], axis=0).T
            vf_s[0:dim] = v_s[rows]
            vf_s[dim:] = padded([jnp.ones((1, tokens), F32)], AUG - dim)

        bufs = (buf_a, buf_b, buf_c)
        total, lag = tiles * fwd_group, tiles + 1
        query, high, top, probs, out = {}, {}, {}, {}, {}
        for g in range(total + lag + 2):
            if g < total:
                i, t = divmod(g, tiles)
                if t == 0:
                    query[i] = jnp.concatenate(split_parts(q_s[rows, q_cols(step * fwd_group + i)].astype(F32) * log2_scale), axis=0)
                scores = dot_nn(kf_s[tile_rows(t)], query[i])
                bufs[i % 3][tile_rows(t)] = scores
                folded = fold_rows(scores, jnp.maximum)
                high[i] = folded if t == 0 else jnp.maximum(high[i], folded)
                if t == tiles - 1:
                    top[i] = jnp.max(high[i], axis=0, keepdims=True)
            if lag <= g < total + lag:
                i, t = divmod(g - lag, tiles)
                probs[g - lag] = jnp.exp2(bufs[i % 3][tile_rows(t, zero)] - top[i]).astype(BF)
            if g >= lag + 2:
                i, t = divmod(g - lag - 2, tiles)
                product = dot_nn(vf_s[:, tile_rows(t)], probs[g - lag - 2])
                out[i] = product if t == 0 else out[i] + product
                if t == tiles - 1:
                    cols = q_cols(step * fwd_group + i)
                    denom = out[i][dim:dim + 1]
                    value = out[i][:dim] * (1.0 / denom)
                    o_s[rows, cols] = value.astype(BF)
                    of_s[rows, cols] = value
                    lse = (top[i] + jnp.log2(denom)) * (1.0 / log2_scale)
                    lse_s[head_rows(head, 16), cols] = padded(split_parts(lse), 16)

        @pl.when(step == fwd_steps - 1)
        def _():
            swap_out(head).start()

    @pl.when(now == middle)
    def _():
        with jax.named_scope('dyhanded'):
            for c in range(PIECES):
                for slot in range(2):
                    hand_over(1, slot, c).wait_recv()
        d_w[pl.ds(0, width)] = dot_nn(o_s[...], dy_s[...])
        for rnd, k in plan[0]:
            reduce.stage(rnd, k)
        with jax.named_scope('oswap'):
            for head in range(heads):
                swap_out(head).wait()
        for i in range(4):
            toks = pl.ds(i * part, part)
            product = dot_tn(o_s[:, toks], wo_s[0]) + dot_tn(o_peer[:, toks], wo_s[1])
            y_s[toks] = (x_s[toks].astype(F32) + product + bo_ref[...]).astype(BF)
            send_home(0, i, True)
        for i in range(tiles):
            cols = pl.ds(i * KEY_TILE, KEY_TILE)
            do_s[:, cols] = dot_nt(wo_s[0], dy_s[cols]).astype(BF)
        with jax.named_scope('middlesends'):
            for which in range(2):
                for c in range(PIECES):
                    for m in range(2):
                        deliver(which, m, c, False)
                        hand_over(which, m, c).wait_send()

    for at in range(1, end):
        todo = plan[at]
        if todo:
            @pl.when(now == middle + at)
            def _():
                with jax.named_scope(f'step{at}'):
                    for rnd, k in todo:
                        reduce.stage(rnd, k)

    @pl.when(now > middle)
    def _():
        since = now - middle - 1
        head, step = since // bwd_steps, lax.rem(since, bwd_steps)
        rows = head_rows(head)

        @pl.when(step == 0)
        def _():
            minus = padded([jnp.full((3, tokens), -1.0, F32)], AUG - dim)
            kb_s[...] = jnp.concatenate([k_s[rows], minus], axis=0).T
            vb_s[...] = jnp.concatenate([v_s[rows], minus], axis=0).T
            dk_acc[...] = jnp.zeros_like(dk_acc)
            dv_acc[...] = jnp.zeros_like(dv_acc)

        total = tiles * bwd_group
        ops, probs, d_scores, dq = {}, {}, {}, {}
        for g in range(total + 2):
            if g < total:
                i, t = divmod(g, tiles)
                if t == 0:
                    cols = q_cols(step * bwd_group + i)
                    q_t, do_t = q_s[rows, cols], do_s[rows, cols]
                    delta = jnp.sum(of_s[rows, cols] * do_t.astype(F32), axis=0, keepdims=True)
                    ops[i] = (cols, q_t, do_t, jnp.concatenate([q_t, lse_s[head_rows(head, 16), cols]], axis=0),
                              jnp.concatenate([do_t, padded(split_parts(delta), 16)], axis=0))
                scores = dot_nn(kb_s[tile_rows(t)], ops[i][3])
                d_probs = dot_nn(vb_s[tile_rows(t)], ops[i][4])
                prob = jnp.exp2(scores * log2_scale)
                probs[g] = prob.astype(BF)
                d_scores[g] = (prob * d_probs).astype(BF)
            if g >= 2:
                i, t = divmod(g - 2, tiles)
                cols, q_t, do_t = ops[i][:3]
                dv_acc[:, tile_rows(t)] += dot_nt(do_t, probs[g - 2])
                product = dot_nn(k_s[rows, tile_rows(t)], d_scores[g - 2])
                dq[i] = product if t == 0 else dq[i] + product
                if t == tiles - 1:
                    grads[0, rows, cols] = (dq[i] * scale).astype(BF)
                dk_acc[:, tile_rows(t)] += dot_nt(q_t, d_scores[g - 2])

        @pl.when(step == bwd_steps - 1)
        def _():
            grads[1, rows] = (dk_acc[...] * scale).astype(BF)
            grads[2, rows] = dv_acc[...].astype(BF)
            swap_grads(head).start()
            stacked = jnp.concatenate([grads[0, rows], grads[1, rows], grads[2, rows]], axis=0)
            d_w[pl.ds(pl.multiple_of(width + head * (3 * dim), 8), 3 * dim)] = dot_nn(stacked, normed_s[...])

    @pl.when(now == middle + end - 1)
    def _():
        def tail(slot):
            for rnd, k in plan[end + slot]:
                with jax.named_scope(f'tail{slot}r{rnd}k{k}'):
                    reduce.stage(rnd, k)

        tail(0)
        with jax.named_scope('gradswap'):
            for head in range(heads):
                swap_grads(head).wait()
        gamma = gamma_ref[...]
        sums = [jnp.zeros((1, 640), F32)] * 3
        for i in range(4):
            toks = pl.ds(i * part, part)
            mine = jnp.concatenate([grads[k, :, toks] for k in range(3)], axis=0)
            theirs = jnp.concatenate([grads_peer[k, :, toks] for k in range(3)], axis=0)
            d_normed = (dot_tn(mine, wt_s[0]) + dot_tn(theirs, wt_s[1])).astype(BF).astype(F32)
            x_hat, inv_std = layer_norm(x_s, toks)
            d_hat = d_normed * gamma
            mean_one = jnp.mean(d_hat, axis=-1, keepdims=True)
            mean_two = jnp.mean(d_hat * x_hat, axis=-1, keepdims=True)
            dy_f = dy_s[toks].astype(F32)
            dx_s[toks] = (dy_f + inv_std * (d_hat - mean_one - x_hat * mean_two)).astype(BF)
            send_home(1, i, True)
            for k, term in enumerate((d_normed * x_hat, d_normed, dy_f)):
                sums[k] = sums[k] + jnp.sum(term, axis=0, keepdims=True)
            if i == 1:
                tail(1)

        for k in range(3):
            for j in range(5):
                small_s[0, pl.ds(k * 5 + j, 1)] = sums[k][:, j * 128:(j + 1) * 128]
        small_s[0, pl.ds(15, 1)] = jnp.zeros((1, 128), F32)
        first = 0
        for hop, axis in enumerate(('x', 'y', 'z', 'core')):
            far = [links.peer] if axis == 'core' else [links.step(axis, d) for d in range(1, links.size[axis])]
            copies = [remote(small_s.at[hop], small_recv.at[first + d], small_sems.at[0, first + d], small_sems.at[1, first + d], device)
                      for d, device in enumerate(far)]
            for copy in copies:
                copy.start()
            tail(2 + hop)
            acc = small_s[hop]
            with jax.named_scope(f'small{hop}'):
                for copy in copies:
                    copy.wait_recv()
            for d in range(len(copies)):
                acc = acc + small_recv[first + d]
            for copy in copies:
                copy.wait_send()
            if axis == 'core':
                small_ref[...] = acc
            else:
                small_s[hop + 1] = acc
            first += len(far)
        for slot in range(6, STAGES):
            tail(slot)
        with jax.named_scope('home'):
            for which in range(2):
                for i in range(4):
                    send_home(which, i, False)
                received_home(which)
        for rnd in range(ROUNDS):
            reduce.store(rnd).wait()


def attention_block(x_in, grad_y, w_t, w_o, gamma, beta, b_o, dim, depth):
    rows, channels = x_in.shape[1:]
    tokens, own = 4 * rows, 2 * rows
    width = w_o.shape[0] // 2
    heads = width // dim
    total = 4 * width
    half = lambda *shape: pltpu.VMEM(shape, BF)
    full = lambda *shape: pltpu.VMEM(shape, F32)
    dma = lambda *shape: pltpu.SemaphoreType.DMA(shape)
    anywhere = pl.BlockSpec(memory_space=pl.ANY)
    vector = pl.BlockSpec((1, channels), lambda i: (0, 0))
    far = max(depth - 1, 1)
    tiles = tokens // KEY_TILE
    return pl.pallas_call(
        functools.partial(block_body, dim, depth),
        grid=(2 + heads * (tiles // 4 + tiles // 2),),
        in_specs=[anywhere] * 4 + [vector] * 3,
        out_specs=[anywhere] * 3 + [pl.BlockSpec((16, 128), lambda i: (0, 0))],
        out_shape=[jax.ShapeDtypeStruct(x_in.shape, BF)] * 2
        + [jax.ShapeDtypeStruct((2, total, channels), F32), jax.ShapeDtypeStruct((16, 128), F32)],
        scratch_shapes=[half(tokens, channels)] * 3 + [half(2, 3 * width, channels), half(2, width, channels)]
        + [half(width, tokens)] * 5 + [full(width, tokens), half(width, own), half(16 * heads, tokens),
                                       half(tokens, 3 * dim), half(AUG, tokens)]
        + [full(tokens, Q_BLOCK)] * 3 + [half(tokens, AUG)] * 2 + [full(dim, tokens)] * 2
        + [half(3, width, tokens), half(3, width, own), full(total, channels), full(2, total, channels)]
        + [half(own, channels)] * 2
        + [full(ROUNDS, 2, 3, 32, channels), full(ROUNDS, 2, 3, 8, channels), full(ROUNDS, 2, 32, channels), full(ROUNDS, 16, 8, 128),
           full(ROUNDS, far, 16 // depth, 8, 128), full(ROUNDS, 16, 8, 128), full(4, 16, 128), full(7 + far, 16, 128),
           dma(2, 4)] + [dma(2, 2, PIECES)] * 4 + [dma(2, heads)] * 2
        + [dma(2, 4), dma(2, 2, 2), dma(2, 7 + far)] + [dma(2, ROUNDS, 2, 2)] * 2 + [dma(2, ROUNDS, 2), dma(2, ROUNDS), dma(ROUNDS)],
        compiler_params=pltpu.CompilerParams(collective_id=0, has_side_effects=True, vmem_limit_bytes=VMEM_BYTES),
        name='attention_block',
    )(x_in, grad_y, w_t, w_o, gamma, beta, b_o)


def solution(mesh):
    depth = mesh.shape['dp'] // (2 * RING)
    act_spec, rep_spec = P('dp', 'cp', None), P()

    def device_step(x_in, grad_y, ln_gamma, ln_beta, w_q, w_k, w_v, w_o, b_o):
        channels, num_heads, head_dim = w_q.shape
        w_t = jnp.stack([jnp.transpose(w, (1, 2, 0)).reshape(num_heads * head_dim, channels) for w in (w_q, w_k, w_v)])
        vectors = [vector.reshape(1, channels) for vector in (ln_gamma, ln_beta, b_o)]
        y_out, grad_x, d_w, small = attention_block(x_in, grad_y, w_t, w_o.reshape(num_heads * head_dim, channels), *vectors,
                                                    head_dim, depth)
        small = small[:15].reshape(3, channels)
        width = num_heads * head_dim // 2
        grad_wo = d_w[:, :width].reshape(num_heads, head_dim, channels)
        d_w = d_w[:, width:].reshape(num_heads, 3, head_dim, channels)
        grads = [jnp.transpose(d_w[:, i], (2, 0, 1)) for i in range(3)]
        return (y_out, grad_x, small[0], small[1], *grads, grad_wo, small[2])

    specs = (act_spec, act_spec) + (rep_spec,) * 7
    return jax.shard_map(device_step, mesh=mesh, in_specs=specs, out_specs=specs, check_vma=False)
```

```python
import functools
import math
import jax
import jax.numpy as jnp
from jax import lax
from jax.experimental import pallas as pl
from jax.experimental.pallas import tpu as pltpu
from jax.sharding import PartitionSpec as P

LN_EPS = 1e-5
KEY_TILE = 256
Q_BLOCK = 256
FOLD = 16
AUG = 96
VMEM_BYTES = 67043328
BF = jnp.bfloat16
F32 = jnp.float32


def dot_nn(lhs, rhs):
    return lax.dot_general(lhs, rhs, (((1,), (0,)), ((), ())), preferred_element_type=F32)


def dot_nt(lhs, rhs):
    return lax.dot_general(lhs, rhs, (((1,), (1,)), ((), ())), preferred_element_type=F32)


def dot_tn(lhs, rhs):
    return lax.dot_general(lhs, rhs, (((0,), (0,)), ((), ())), preferred_element_type=F32)


def split_parts(value):
    high = value.astype(BF)
    rest = value - high.astype(F32)
    mid = rest.astype(BF)
    return high, mid, (rest - mid.astype(F32)).astype(BF)


def fold_rows(value, op):
    groups = value.reshape(value.shape[0] // FOLD, FOLD, value.shape[1])
    out = groups[0]
    for i in range(1, groups.shape[0]):
        out = op(out, groups[i])
    return out


MESH = pl.DeviceIdType.MESH
RING = 4
ROUNDS = 5
ROUND_ROWS = 256
STAGES = 8
PIECES = 4
SENDS = 16
ORDER = (('y', 'x'), ('y', 'x'), ('y', 'x'), ('y', 'y'), ('y', 'x'))


class Links:
    def __init__(self, depth):
        dp, self.x = lax.axis_index('dp'), lax.axis_index('cp')
        self.core = lax.rem(dp, 2)
        self.y = lax.rem(dp // 2, RING)
        self.z = dp // (2 * RING)
        self.depth = depth
        self.pos = {'x': self.x, 'y': self.y, 'z': self.z}
        self.size = {'x': RING, 'y': RING, 'z': depth}
        self.peer = self.at(core=1 - self.core)
        pair, odd = self.x // 2, lax.rem(self.x, 2)
        self.owners = [(pair, 2 * self.core + odd), (pair, 2 * self.core + 1 - odd)]
        self.workers = [(pair, 2 * self.core), (pair, 2 * self.core + 1)]

    def at(self, x=None, y=None, z=None, core=None):
        pick = lambda value, own: own if value is None else value
        return ((pick(z, self.z) * RING + pick(y, self.y)) * 2 + pick(core, self.core), pick(x, self.x))

    def step(self, axis, d):
        return self.at(**{axis: lax.rem(self.pos[axis] + d, self.size[axis])})

    def is_self(self, place):
        return jnp.logical_and(place[0] == self.core, place[1] == self.x)


def remote(source, target, send, recv, device):
    return pltpu.make_async_remote_copy(src_ref=source, dst_ref=target, send_sem=send, recv_sem=recv,
                                        device_id=device, device_id_type=MESH)


class GradReduce:
    def __init__(self, links, grad, out, result, bufs, sems):
        self.links, self.grad, self.both, self.out, self.result = links, grad, out, out.at[links.core], result
        self.recv1, self.recv2, self.mid, self.z_src, self.z_recv, self.z_out = bufs
        self.rs_sems, self.ag_sems, self.z_sems, self.swap_sems, self.store_sems = sems

    def axes(self, rnd, unit):
        first = ORDER[rnd][unit]
        return first, ('x' if first == 'y' else 'y')

    def block(self, rnd, unit, phase):
        first = rnd * ROUND_ROWS + unit * 128
        if phase == 0:
            return first, 32
        return first + self.links.pos[self.axes(rnd, unit)[0]] * 32, 8

    def landing(self, rnd, unit, phase):
        return (self.recv1 if phase == 0 else self.recv2).at[rnd, unit]

    def wait_all(self, rnd, unit, phase, sems):
        whole = self.landing(rnd, unit, phase)
        every = remote(whole, whole, sems.at[0, rnd, unit, phase], sems.at[1, rnd, unit, phase], self.links.peer)
        every.wait_recv()
        every.wait_send()

    def source(self, rnd, unit, phase, owner):
        if phase == 0:
            first, rows = self.block(rnd, unit, 0)
            return self.grad.at[pl.ds(pl.multiple_of(first + owner * rows, 8), rows)]
        return self.mid.at[rnd, unit, pl.ds(pl.multiple_of(owner * 8, 8), 8)]

    def scatter_start(self, rnd, unit, phase):
        axis = self.axes(rnd, unit)[phase]
        for d in (2, 1, 3):
            owner = lax.rem(self.links.pos[axis] + d, RING)
            remote(self.source(rnd, unit, phase, owner), self.landing(rnd, unit, phase).at[d - 1],
                   self.rs_sems.at[0, rnd, unit, phase], self.rs_sems.at[1, rnd, unit, phase], self.links.step(axis, d)).start()

    def scatter_end(self, rnd, unit, phase):
        self.wait_all(rnd, unit, phase, self.rs_sems)
        landing = self.landing(rnd, unit, phase)
        mine = self.source(rnd, unit, phase, self.links.pos[self.axes(rnd, unit)[phase]])
        return (mine[...] + landing[0]) + (landing[1] + landing[2])

    def gather_start(self, rnd, unit, phase):
        axis = self.axes(rnd, unit)[phase]
        first, rows = self.block(rnd, unit, phase)
        part = self.out.at[pl.ds(pl.multiple_of(first + self.links.pos[axis] * rows, 8), rows)]
        for d in (2, 1, 3):
            remote(part, part, self.ag_sems.at[0, rnd, unit, phase], self.ag_sems.at[1, rnd, unit, phase],
                   self.links.step(axis, d)).start()

    def z_copies(self, rnd, way):
        links = self.links
        each = 16 // links.depth
        send, recv = self.z_sems.at[0, rnd, way], self.z_sems.at[1, rnd, way]
        mine = pl.ds(links.z * each, each)
        copies = []
        for d in range(1, links.depth):
            far = lax.rem(links.z + d, links.depth)
            if way == 0:
                source, target = self.z_src.at[rnd, pl.ds(far * each, each)], self.z_recv.at[rnd, d - 1]
            else:
                source = target = self.z_out.at[rnd, mine]
            copies.append(remote(source, target, send, recv, links.step('z', d)))
        return copies, mine

    def z_wait(self, rnd, way):
        if self.links.depth > 1:
            whole = self.z_recv.at[rnd]
            all_of = remote(whole, whole, self.z_sems.at[0, rnd, way], self.z_sems.at[1, rnd, way], self.links.step('z', 1))
            all_of.wait_recv()
            all_of.wait_send()

    def swap(self, rnd):
        part = self.out.at[pl.ds(rnd * ROUND_ROWS, ROUND_ROWS)]
        return remote(part, part, self.swap_sems.at[0, rnd], self.swap_sems.at[1, rnd], self.links.peer)

    def store(self, rnd):
        rows = pl.ds(rnd * ROUND_ROWS, ROUND_ROWS)
        return pltpu.make_async_copy(self.both.at[:, rows], self.result.at[:, rows], self.store_sems.at[rnd])

    def stage(self, rnd, k):
        units = (0, 1)
        if k == 0:
            for u in units:
                self.scatter_start(rnd, u, 0)
        elif k == 1:
            for u in units:
                self.mid[rnd, u] = self.scatter_end(rnd, u, 0)
                self.scatter_start(rnd, u, 1)
        elif k == 2:
            for u in units:
                total = self.scatter_end(rnd, u, 1)
                for j in range(5):
                    self.z_src[rnd, u * 5 + j] = total[:, j * 128:(j + 1) * 128]
            self.z_src[rnd, pl.ds(10, 6)] = jnp.zeros((6, 8, 128), F32)
            for copy in self.z_copies(rnd, 0)[0]:
                copy.start()
        elif k == 3:
            self.z_wait(rnd, 0)
            copies, mine = self.z_copies(rnd, 1)
            total = self.z_src[rnd, mine]
            for d in range(self.links.depth - 1):
                total = total + self.z_recv[rnd, d]
            self.z_out[rnd, mine] = total
            for copy in copies:
                copy.start()
        elif k == 4:
            self.z_wait(rnd, 1)
            for u in units:
                first = self.block(rnd, u, 1)[0] + self.links.pos[self.axes(rnd, u)[1]] * 8
                for j in range(5):
                    self.out[pl.ds(pl.multiple_of(first, 8), 8), pl.ds(j * 128, 128)] = self.z_out[rnd, u * 5 + j]
                self.gather_start(rnd, u, 1)
        elif k == 5:
            for u in units:
                self.wait_all(rnd, u, 1, self.ag_sems)
                self.gather_start(rnd, u, 0)
        elif k == 6:
            for u in units:
                self.wait_all(rnd, u, 0, self.ag_sems)
            self.swap(rnd).start()
        else:
            self.swap(rnd).wait()
            self.store(rnd).start()


def layer_norm(x_ref, rows):
    x_f = x_ref[rows].astype(F32)
    centered = x_f - jnp.mean(x_f, axis=-1, keepdims=True)
    inv_std = lax.rsqrt(jnp.mean(centered * centered, axis=-1, keepdims=True) + LN_EPS)
    return centered * inv_std, inv_std


def padded(parts, rows):
    filled = [part.astype(F32) for part in parts]
    used = sum(part.shape[0] for part in filled)
    return jnp.concatenate(filled + [jnp.zeros((rows - used, filled[0].shape[1]), F32)], axis=0).astype(BF)


def wait_for(ref, sem):
    pltpu.make_async_copy(ref, ref, sem).wait()


def block_body(dim, depth, x_hbm, dy_hbm, wt_hbm, wo_hbm, vectors, y_ref, gx_ref, dw_ref, small_ref,
               x_s, normed_s, dy_s, wt_s, wo_s, q_s, k_s, v_s, do_s, o_s, of_s, o_peer, lse_s, kf_s, vf_s, buf_a, buf_b, buf_c,
               kb_s, vb_s, dk_acc, dv_acc, grads, grads_peer, d_w, d_w_all, dx_s, y_s,
               recv1, recv2, mid, z_src, z_recv, z_out, small_s, small_recv,
               load_sems, in_send, in_recv, pass_send, pass_recv, o_sems, grad_sems, out_send, out_recv, small_sems,
               rs_sems, ag_sems, z_sems, swap_sems, store_sems):
    links = Links(depth)
    width, tokens = q_s.shape
    heads, tiles = width // dim, tokens // KEY_TILE
    own, band = tokens // 2, tokens // 4
    scale = dim ** -0.5
    log2_scale = scale * math.log2(math.e)
    fwd_group, bwd_group = 4, 2
    fwd_steps, bwd_steps = tiles // fwd_group, tiles // bwd_group
    zero = jnp.minimum(links.x, 0)
    odd = lax.rem(links.x, 2)
    reduce = GradReduce(links, d_w, d_w_all, dw_ref, (recv1, recv2, mid, z_src, z_recv, z_out),
                        (rs_sems, ag_sems, z_sems, swap_sems, store_sems))
    end = heads * bwd_steps + 1
    plan, ahead = {}, [0] * ROUNDS
    for at in range(end + STAGES):
        due = []
        for rnd in range(ROUNDS):
            age = at - (rnd * bwd_steps + 1 if rnd else 0)
            if ahead[rnd] < STAGES and age >= 0 and (at >= end or age % 2 == 0):
                due.append((rnd, ahead[rnd]))
                ahead[rnd] += 1
        plan[at] = due[::-1]

    def tile_rows(tile, base=None):
        return pl.ds(tile * KEY_TILE if base is None else pl.multiple_of(base + tile * KEY_TILE, KEY_TILE), KEY_TILE)

    def head_rows(head, rows=dim):
        return pl.ds(pl.multiple_of(head * rows, 16), rows)

    def q_cols(index):
        return pl.ds(pl.multiple_of(index * Q_BLOCK, Q_BLOCK), Q_BLOCK)

    def my_half(side):
        return pl.ds(pl.multiple_of((links.core if side == 0 else 1 - links.core) * width, 16), width)

    loads = [pltpu.make_async_copy(wt_hbm.at[k, my_half(side)], wt_s.at[side, pl.ds(k * width, width)], load_sems.at[side, k])
             for side in range(2) for k in range(3)]
    loads += [pltpu.make_async_copy(wo_hbm.at[my_half(side)], wo_s.at[side], load_sems.at[side, 3]) for side in range(2)]

    def maybe_far(place, source, target, send, recv, start):
        core, x = place
        here = links.is_self(place)
        far = remote(source, target, send, recv, links.at(core=core, x=x))
        near = pltpu.make_async_copy(source, target, recv)

        @pl.when(jnp.logical_not(here))
        def _():
            far.start() if start else far.wait_send()

        if start:
            @pl.when(here)
            def _():
                near.start()

    piece = band // PIECES

    def deliver(which, m, c, start):
        slot = lax.rem(links.x + m, 2)
        source = (dy_hbm if which else x_hbm).at[m, pl.ds(c * piece, piece)]
        target = (dy_s if which else x_s).at[pl.ds(pl.multiple_of(slot * band + c * piece, 16), piece)]
        maybe_far(links.workers[m], source, target, in_send.at[which, m, c], in_recv.at[which, slot, c], start)

    def hand_over(which, slot, c):
        rows = dy_s if which else x_s
        first = slot * band + c * piece
        return remote(rows.at[pl.ds(first, piece)], rows.at[pl.ds(own + first, piece)],
                      pass_send.at[which, slot, c], pass_recv.at[which, slot, c], links.peer)

    def arrive(which, slot, c):
        with jax.named_scope(f'arrive{which}{slot}{c}'):
            wait_for((dy_s if which else x_s).at[pl.ds(slot * band + c * piece, piece)], in_recv.at[which, slot, c])
        hand_over(which, slot, c).start()

    def swap_out(head):
        rows = head_rows(head)
        return remote(o_s.at[rows, pl.ds(own, own)], o_peer.at[rows], o_sems.at[0, head], o_sems.at[1, head], links.peer)

    def swap_grads(head):
        rows = head_rows(head)
        return remote(grads.at[:, rows, pl.ds(own, own)], grads_peer.at[:, rows], grad_sems.at[0, head], grad_sems.at[1, head],
                      links.peer)

    part = band // 2
    portion = own // SENDS

    def send_home(which, i, start):
        cut = SENDS // 2
        second, inner = i // cut, lax.rem(i, cut)
        source = (dx_s if which else y_s).at[pl.ds(pl.multiple_of(i * portion, 16), portion)]
        target = (gx_ref if which else y_ref).at[odd, pl.ds(pl.multiple_of(inner * portion, 16), portion)]
        (core, x0), (_, x1) = links.owners
        maybe_far((core, jnp.where(second == 0, x0, x1)), source, target, out_send.at[which, i],
                  out_recv.at[which, odd, inner], start)

    def received_home(which):
        for m in range(2):
            for i in range(SENDS // 2):
                wait_for((gx_ref if which else y_ref).at[m, pl.ds(i * portion, portion)], out_recv.at[which, m, i])

    barrier = pltpu.get_barrier_semaphore()
    fixed = [links.peer]
    fixed += [links.step(axis, d) for axis in ('x', 'y') for d in range(1, RING)]
    fixed += [links.step('z', d) for d in range(1, depth)]
    for device in fixed:
        pl.semaphore_signal(barrier, inc=1, device_id=device, device_id_type=MESH)
    count = len(fixed)
    for place in links.owners + links.workers:
        other = jnp.logical_not(links.is_self(place))
        count = count + other.astype(jnp.int32)

        @pl.when(other)
        def _():
            pl.semaphore_signal(barrier, inc=1, device_id=links.at(core=place[0], x=place[1]), device_id_type=MESH)
    for load in loads:
        load.start()
    with jax.named_scope('barrier'):
        pl.semaphore_wait(barrier, count)
    for which in range(2):
        for c in range(PIECES):
            for m in range(2):
                deliver(which, m, c, True)
    for load in loads:
        load.wait()

    def normalize(first):
        rows = pl.ds(first, piece)
        normed_s[rows] = (layer_norm(x_s, rows)[0] * vectors[0:1] + vectors[1:2]).astype(BF)

    for c in range(PIECES + 1):
        if c < PIECES:
            for slot in range(2):
                arrive(0, slot, c)
            for slot in range(2):
                normalize(slot * band + c * piece)
        if c:
            for slot in range(2):
                with jax.named_scope(f'handed{slot}{c}'):
                    hand_over(0, slot, c - 1).wait_recv()
                normalize(own + slot * band + (c - 1) * piece)
            if c % 2 == 0:
                for b in range(4):
                    cols = pl.ds(b * band + (c - 2) * piece, 2 * piece)
                    normed = normed_s[cols]
                    for k, out in enumerate((q_s, k_s, v_s)):
                        out[:, cols] = dot_nt(wt_s[0, pl.ds(k * width, width)], normed).astype(BF)

    def forward_step(now, carry):
        head, step = now // fwd_steps, lax.rem(now, fwd_steps)
        rows = head_rows(head)
        for c in range(PIECES):
            @pl.when(now == (c + 1) * heads * fwd_steps // (PIECES + 1))
            def _():
                for slot in range(2):
                    arrive(1, slot, c)

        @pl.when(step == 0)
        def _():
            k_t = k_s[rows]
            kf_s[...] = jnp.concatenate([k_t, k_t, k_t], axis=0).T
            vf_s[0:dim] = v_s[rows]
            vf_s[dim:] = padded([jnp.ones((1, tokens), F32)], AUG - dim)

        bufs = (buf_a, buf_b, buf_c)
        total, lag = tiles * fwd_group, tiles + 1
        query, high, top, probs, out = {}, {}, {}, {}, {}
        for g in range(total + lag + 2):
            if g < total:
                i, t = divmod(g, tiles)
                if t == 0:
                    query[i] = jnp.concatenate(split_parts(q_s[rows, q_cols(step * fwd_group + i)].astype(F32) * log2_scale), axis=0)
                scores = dot_nn(kf_s[tile_rows(t)], query[i])
                bufs[i % 3][tile_rows(t)] = scores
                folded = fold_rows(scores, jnp.maximum)
                high[i] = folded if t == 0 else jnp.maximum(high[i], folded)
                if t == tiles - 1:
                    top[i] = jnp.max(high[i], axis=0, keepdims=True)
            if lag <= g < total + lag:
                i, t = divmod(g - lag, tiles)
                probs[g - lag] = jnp.exp2(bufs[i % 3][tile_rows(t, zero)] - top[i]).astype(BF)
            if g >= lag + 2:
                i, t = divmod(g - lag - 2, tiles)
                product = dot_nn(vf_s[:, tile_rows(t)], probs[g - lag - 2])
                out[i] = product if t == 0 else out[i] + product
                if t == tiles - 1:
                    cols = q_cols(step * fwd_group + i)
                    denom = out[i][dim:dim + 1]
                    value = out[i][:dim] * (1.0 / denom)
                    o_s[rows, cols] = value.astype(BF)
                    of_s[rows, cols] = value
                    lse = (top[i] + jnp.log2(denom)) * (1.0 / log2_scale)
                    lse_s[head_rows(head, 16), cols] = padded(split_parts(lse), 16)

        @pl.when(step == fwd_steps - 1)
        def _():
            swap_out(head).start()

        return carry

    lax.fori_loop(0, heads * fwd_steps, forward_step, 0)
    with jax.named_scope('dyhanded'):
        for c in range(PIECES):
            for slot in range(2):
                hand_over(1, slot, c).wait_recv()
    d_w[pl.ds(0, width)] = dot_nn(o_s[...], dy_s[...])
    for rnd, k in plan[0]:
        reduce.stage(rnd, k)
    with jax.named_scope('oswap'):
        for head in range(heads):
            swap_out(head).wait()
    for i in range(4):
        toks = pl.ds(i * part, part)
        product = dot_tn(o_s[:, toks], wo_s[0]) + dot_tn(o_peer[:, toks], wo_s[1])
        y_s[toks] = (x_s[toks].astype(F32) + product + vectors[2:3]).astype(BF)
    for i in range(tiles):
        cols = pl.ds(i * KEY_TILE, KEY_TILE)
        do_s[:, cols] = dot_nt(wo_s[0], dy_s[cols]).astype(BF)
    with jax.named_scope('middlesends'):
        for which in range(2):
            for c in range(PIECES):
                for m in range(2):
                    deliver(which, m, c, False)
                    hand_over(which, m, c).wait_send()

    def backward_step(now, carry):
        head, step = now // bwd_steps, lax.rem(now, bwd_steps)
        rows = head_rows(head)
        for at in range(end - 1):
            todo = plan[at + 1]
            if todo:
                @pl.when(now == at)
                def _():
                    with jax.named_scope(f'step{at}'):
                        for rnd, k in todo:
                            reduce.stage(rnd, k)
        share = SENDS // (heads * bwd_steps)
        for i in range(share):
            send_home(0, now * share + i, True)

        @pl.when(step == 0)
        def _():
            minus = padded([jnp.full((3, tokens), -1.0, F32)], AUG - dim)
            kb_s[...] = jnp.concatenate([k_s[rows], minus], axis=0).T
            vb_s[...] = jnp.concatenate([v_s[rows], minus], axis=0).T
            dk_acc[...] = jnp.zeros_like(dk_acc)
            dv_acc[...] = jnp.zeros_like(dv_acc)

        total = tiles * bwd_group
        ops, probs, d_scores, dq = {}, {}, {}, {}
        for g in range(total + 2):
            if g < total:
                i, t = divmod(g, tiles)
                if t == 0:
                    cols = q_cols(step * bwd_group + i)
                    q_t, do_t = q_s[rows, cols], do_s[rows, cols]
                    delta = jnp.sum(of_s[rows, cols] * do_t.astype(F32), axis=0, keepdims=True)
                    ops[i] = (cols, q_t, do_t, jnp.concatenate([q_t, lse_s[head_rows(head, 16), cols]], axis=0),
                              jnp.concatenate([do_t, padded(split_parts(delta), 16)], axis=0))
                scores = dot_nn(kb_s[tile_rows(t)], ops[i][3])
                d_probs = dot_nn(vb_s[tile_rows(t)], ops[i][4])
                prob = jnp.exp2(scores * log2_scale)
                probs[g] = prob.astype(BF)
                d_scores[g] = (prob * d_probs).astype(BF)
            if g >= 2:
                i, t = divmod(g - 2, tiles)
                cols, q_t, do_t = ops[i][:3]
                dv_acc[:, tile_rows(t)] += dot_nt(do_t, probs[g - 2])
                product = dot_nn(k_s[rows, tile_rows(t)], d_scores[g - 2])
                dq[i] = product if t == 0 else dq[i] + product
                if t == tiles - 1:
                    grads[0, rows, cols] = (dq[i] * scale).astype(BF)
                dk_acc[:, tile_rows(t)] += dot_nt(q_t, d_scores[g - 2])

        @pl.when(step == bwd_steps - 1)
        def _():
            grads[1, rows] = (dk_acc[...] * scale).astype(BF)
            grads[2, rows] = dv_acc[...].astype(BF)
            swap_grads(head).start()
            stacked = jnp.concatenate([grads[0, rows], grads[1, rows], grads[2, rows]], axis=0)
            d_w[pl.ds(pl.multiple_of(width + head * (3 * dim), 8), 3 * dim)] = dot_nn(stacked, normed_s[...])

        return carry

    lax.fori_loop(0, heads * bwd_steps, backward_step, 0)

    def tail(slot):
        for rnd, k in plan[end + slot]:
            with jax.named_scope(f'tail{slot}r{rnd}k{k}'):
                reduce.stage(rnd, k)

    def spread(share):
        for i in range(2):
            send_home(1, share * 2 + i, True)

    tail(0)
    with jax.named_scope('gradswap'):
        for head in range(heads):
            swap_grads(head).wait()
    gamma = vectors[0:1]
    sums = [jnp.zeros((1, 640), F32)] * 3
    for i in range(4):
        toks = pl.ds(i * part, part)
        mine = jnp.concatenate([grads[k, :, toks] for k in range(3)], axis=0)
        theirs = jnp.concatenate([grads_peer[k, :, toks] for k in range(3)], axis=0)
        d_normed = (dot_tn(mine, wt_s[0]) + dot_tn(theirs, wt_s[1])).astype(BF).astype(F32)
        x_hat, inv_std = layer_norm(x_s, toks)
        d_hat = d_normed * gamma
        mean_one = jnp.mean(d_hat, axis=-1, keepdims=True)
        mean_two = jnp.mean(d_hat * x_hat, axis=-1, keepdims=True)
        dy_f = dy_s[toks].astype(F32)
        dx_s[toks] = (dy_f + inv_std * (d_hat - mean_one - x_hat * mean_two)).astype(BF)
        if i < 2:
            spread(i)
        for k, term in enumerate((d_normed * x_hat, d_normed, dy_f)):
            sums[k] = sums[k] + jnp.sum(term, axis=0, keepdims=True)

    for k in range(3):
        for j in range(5):
            small_s[0, pl.ds(k * 5 + j, 1)] = sums[k][:, j * 128:(j + 1) * 128]
    small_s[0, pl.ds(15, 1)] = jnp.zeros((1, 128), F32)
    first, waiting = 0, None
    for hop, axis in enumerate(('z', 'y', 'core', 'x', '')):
        if waiting:
            acc = small_s[hop - 1]
            with jax.named_scope(f'small{hop}'):
                for copy in waiting:
                    copy.wait_recv()
            for d in range(len(waiting)):
                acc = acc + small_recv[first + d]
            for copy in waiting:
                copy.wait_send()
            if axis:
                small_s[hop] = acc
            else:
                small_ref[...] = acc
            first += len(waiting)
        elif hop:
            small_s[hop] = small_s[hop - 1]
        if axis:
            far = [links.peer] if axis == 'core' else [links.step(axis, d) for d in range(1, links.size[axis])]
            waiting = [remote(small_s.at[hop], small_recv.at[first + d], small_sems.at[0, first + d], small_sems.at[1, first + d],
                              device) for d, device in enumerate(far)]
            for copy in waiting:
                copy.start()
            tail(1 + hop)
            if hop < 3:
                for i in range(2):
                    spread(2 + 2 * hop + i)
    for slot in range(5, STAGES):
        tail(slot)
    with jax.named_scope('home'):
        for which in range(2):
            for i in range(SENDS):
                send_home(which, i, False)
            received_home(which)
    with jax.named_scope('stored'):
        for rnd in range(ROUNDS):
            reduce.store(rnd).wait()


def attention_block(x_in, grad_y, w_t, w_o, vectors, dim, depth):
    rows, channels = x_in.shape[1:]
    tokens, own = 4 * rows, 2 * rows
    width = w_o.shape[0] // 2
    heads = width // dim
    total = 4 * width
    half = lambda *shape: pltpu.VMEM(shape, BF)
    full = lambda *shape: pltpu.VMEM(shape, F32)
    dma = lambda *shape: pltpu.SemaphoreType.DMA(shape)
    anywhere = pl.BlockSpec(memory_space=pl.ANY)
    in_vmem = pl.BlockSpec(memory_space=pltpu.VMEM)
    far = max(depth - 1, 1)
    return pl.pallas_call(
        functools.partial(block_body, dim, depth),
        in_specs=[anywhere] * 4 + [in_vmem],
        out_specs=[anywhere] * 3 + [in_vmem],
        out_shape=[jax.ShapeDtypeStruct(x_in.shape, BF)] * 2
        + [jax.ShapeDtypeStruct((2, total, channels), F32), jax.ShapeDtypeStruct((16, 128), F32)],
        scratch_shapes=[half(tokens, channels)] * 3 + [half(2, 3 * width, channels), half(2, width, channels)]
        + [half(width, tokens)] * 5 + [full(width, tokens), half(width, own), half(16 * heads, tokens),
                                       half(tokens, 3 * dim), half(AUG, tokens)]
        + [full(tokens, Q_BLOCK)] * 3 + [half(tokens, AUG)] * 2 + [full(dim, tokens)] * 2
        + [half(3, width, tokens), half(3, width, own), full(total, channels), full(2, total, channels)]
        + [half(own, channels)] * 2
        + [full(ROUNDS, 2, 3, 32, channels), full(ROUNDS, 2, 3, 8, channels), full(ROUNDS, 2, 32, channels), full(ROUNDS, 16, 8, 128),
           full(ROUNDS, far, 16 // depth, 8, 128), full(ROUNDS, 16, 8, 128), full(4, 16, 128), full(7 + far, 16, 128),
           dma(2, 4)] + [dma(2, 2, PIECES)] * 4 + [dma(2, heads)] * 2
        + [dma(2, SENDS), dma(2, 2, SENDS // 2), dma(2, 7 + far)] + [dma(2, ROUNDS, 2, 2)] * 2 + [dma(2, ROUNDS, 2), dma(2, ROUNDS), dma(ROUNDS)],
        compiler_params=pltpu.CompilerParams(collective_id=0, has_side_effects=True, vmem_limit_bytes=VMEM_BYTES),
        name='attention_block',
    )(x_in, grad_y, w_t, w_o, vectors)


def solution(mesh):
    depth = mesh.shape['dp'] // (2 * RING)
    act_spec, rep_spec = P('dp', 'cp', None), P()

    def device_step(x_in, grad_y, ln_gamma, ln_beta, w_q, w_k, w_v, w_o, b_o):
        channels, num_heads, head_dim = w_q.shape
        w_t = jnp.stack([jnp.transpose(w, (1, 2, 0)).reshape(num_heads * head_dim, channels) for w in (w_q, w_k, w_v)])
        vectors = jnp.stack([ln_gamma, ln_beta, b_o])
        y_out, grad_x, d_w, small = attention_block(x_in, grad_y, w_t, w_o.reshape(num_heads * head_dim, channels), vectors,
                                                    head_dim, depth)
        small = small[:15].reshape(3, channels)
        width = num_heads * head_dim // 2
        grad_wo = d_w[:, :width].reshape(num_heads, head_dim, channels)
        d_w = d_w[:, width:].reshape(num_heads, 3, head_dim, channels)
        grads = [jnp.transpose(d_w[:, i], (2, 0, 1)) for i in range(3)]
        return (y_out, grad_x, small[0], small[1], *grads, grad_wo, small[2])

    specs = (act_spec, act_spec) + (rep_spec,) * 7
    return jax.shard_map(device_step, mesh=mesh, in_specs=specs, out_specs=specs, check_vma=False)
```

```python
import functools
import math
import jax
import jax.numpy as jnp
from jax import lax
from jax.experimental import pallas as pl
from jax.experimental.pallas import tpu as pltpu
from jax.sharding import PartitionSpec as P

LN_EPS = 1e-5
KEY_TILE = 256
Q_BLOCK = 256
FOLD = 16
AUG = 96
VMEM_BYTES = 67043328
BF = jnp.bfloat16
F32 = jnp.float32


def dot_nn(lhs, rhs):
    return lax.dot_general(lhs, rhs, (((1,), (0,)), ((), ())), preferred_element_type=F32)


def dot_nt(lhs, rhs):
    return lax.dot_general(lhs, rhs, (((1,), (1,)), ((), ())), preferred_element_type=F32)


def dot_tn(lhs, rhs):
    return lax.dot_general(lhs, rhs, (((0,), (0,)), ((), ())), preferred_element_type=F32)


def split_parts(value):
    high = value.astype(BF)
    rest = value - high.astype(F32)
    mid = rest.astype(BF)
    return high, mid, (rest - mid.astype(F32)).astype(BF)


def fold_rows(value, op):
    groups = value.reshape(value.shape[0] // FOLD, FOLD, value.shape[1])
    out = groups[0]
    for i in range(1, groups.shape[0]):
        out = op(out, groups[i])
    return out


MESH = pl.DeviceIdType.MESH
RING = 4
ROUNDS = 5
ROUND_ROWS = 256
STAGES = 8
PIECES = 4
SENDS = 16
ORDER = ('y', 'x')


class Links:
    def __init__(self, depth):
        dp, self.x = lax.axis_index('dp'), lax.axis_index('cp')
        self.core = lax.rem(dp, 2)
        self.y = lax.rem(dp // 2, RING)
        self.z = dp // (2 * RING)
        self.depth = depth
        self.pos = {'x': self.x, 'y': self.y, 'z': self.z}
        self.size = {'x': RING, 'y': RING, 'z': depth}
        self.peer = self.at(core=1 - self.core)
        pair, odd = self.x // 2, lax.rem(self.x, 2)
        self.owners = [(pair, 2 * self.core + odd), (pair, 2 * self.core + 1 - odd)]
        self.workers = [(pair, 2 * self.core), (pair, 2 * self.core + 1)]

    def at(self, x=None, y=None, z=None, core=None):
        pick = lambda value, own: own if value is None else value
        return ((pick(z, self.z) * RING + pick(y, self.y)) * 2 + pick(core, self.core), pick(x, self.x))

    def step(self, axis, d):
        return self.at(**{axis: lax.rem(self.pos[axis] + d, self.size[axis])})

    def is_self(self, place):
        return jnp.logical_and(place[0] == self.core, place[1] == self.x)


def remote(source, target, send, recv, device):
    return pltpu.make_async_remote_copy(src_ref=source, dst_ref=target, send_sem=send, recv_sem=recv,
                                        device_id=device, device_id_type=MESH)


class GradReduce:
    def __init__(self, links, grad, out, result, bufs, sems):
        self.links, self.grad, self.both, self.out, self.result = links, grad, out, out.at[links.core], result
        self.recv1, self.recv2, self.mid, self.z_src, self.z_recv, self.z_out = bufs
        self.rs_sems, self.ag_sems, self.z_sems, self.swap_sems, self.store_sems = sems

    def axes(self, rnd, unit):
        first = ORDER[unit]
        return first, ('x' if first == 'y' else 'y')

    def block(self, rnd, unit, phase):
        first = rnd * ROUND_ROWS + unit * 128
        if phase == 0:
            return first, 32
        return first + self.links.pos[self.axes(rnd, unit)[0]] * 32, 8

    def landing(self, rnd, unit, phase):
        return (self.recv1 if phase == 0 else self.recv2).at[rnd, unit]

    def wait_all(self, rnd, unit, phase, sems):
        whole = self.landing(rnd, unit, phase)
        every = remote(whole, whole, sems.at[0, rnd, unit, phase], sems.at[1, rnd, unit, phase], self.links.peer)
        every.wait_recv()
        every.wait_send()

    def source(self, rnd, unit, phase, owner):
        if phase == 0:
            first, rows = self.block(rnd, unit, 0)
            return self.grad.at[pl.ds(pl.multiple_of(first + owner * rows, 8), rows)]
        return self.mid.at[rnd, unit, pl.ds(pl.multiple_of(owner * 8, 8), 8)]

    def scatter_start(self, rnd, unit, phase):
        axis = self.axes(rnd, unit)[phase]
        for d in (2, 1, 3):
            owner = lax.rem(self.links.pos[axis] + d, RING)
            remote(self.source(rnd, unit, phase, owner), self.landing(rnd, unit, phase).at[d - 1],
                   self.rs_sems.at[0, rnd, unit, phase], self.rs_sems.at[1, rnd, unit, phase], self.links.step(axis, d)).start()

    def scatter_end(self, rnd, unit, phase):
        self.wait_all(rnd, unit, phase, self.rs_sems)
        landing = self.landing(rnd, unit, phase)
        mine = self.source(rnd, unit, phase, self.links.pos[self.axes(rnd, unit)[phase]])
        return (mine[...] + landing[0]) + (landing[1] + landing[2])

    def gather_start(self, rnd, unit, phase):
        axis = self.axes(rnd, unit)[phase]
        first, rows = self.block(rnd, unit, phase)
        part = self.out.at[pl.ds(pl.multiple_of(first + self.links.pos[axis] * rows, 8), rows)]
        for d in (2, 1, 3):
            remote(part, part, self.ag_sems.at[0, rnd, unit, phase], self.ag_sems.at[1, rnd, unit, phase],
                   self.links.step(axis, d)).start()

    def z_copies(self, rnd, way):
        links = self.links
        each = 16 // links.depth
        send, recv = self.z_sems.at[0, rnd, way], self.z_sems.at[1, rnd, way]
        mine = pl.ds(links.z * each, each)
        copies = []
        for d in range(1, links.depth):
            far = lax.rem(links.z + d, links.depth)
            if way == 0:
                source, target = self.z_src.at[rnd, pl.ds(far * each, each)], self.z_recv.at[rnd, d - 1]
            else:
                source = target = self.z_out.at[rnd, mine]
            copies.append(remote(source, target, send, recv, links.step('z', d)))
        return copies, mine

    def z_wait(self, rnd, way):
        if self.links.depth > 1:
            whole = self.z_recv.at[rnd]
            all_of = remote(whole, whole, self.z_sems.at[0, rnd, way], self.z_sems.at[1, rnd, way], self.links.step('z', 1))
            all_of.wait_recv()
            all_of.wait_send()

    def swap(self, rnd):
        part = self.out.at[pl.ds(rnd * ROUND_ROWS, ROUND_ROWS)]
        return remote(part, part, self.swap_sems.at[0, rnd], self.swap_sems.at[1, rnd], self.links.peer)

    def store(self, rnd):
        rows = pl.ds(rnd * ROUND_ROWS, ROUND_ROWS)
        return pltpu.make_async_copy(self.both.at[:, rows], self.result.at[:, rows], self.store_sems.at[rnd])

    def stage(self, rnd, k):
        units = (0, 1)
        if k == 0:
            for u in units:
                self.scatter_start(rnd, u, 0)
        elif k == 1:
            for u in units:
                self.mid[rnd, u] = self.scatter_end(rnd, u, 0)
                self.scatter_start(rnd, u, 1)
        elif k == 2:
            for u in units:
                total = self.scatter_end(rnd, u, 1)
                for j in range(5):
                    self.z_src[rnd, u * 5 + j] = total[:, j * 128:(j + 1) * 128]
            self.z_src[rnd, pl.ds(10, 6)] = jnp.zeros((6, 8, 128), F32)
            for copy in self.z_copies(rnd, 0)[0]:
                copy.start()
        elif k == 3:
            self.z_wait(rnd, 0)
            copies, mine = self.z_copies(rnd, 1)
            total = self.z_src[rnd, mine]
            for d in range(self.links.depth - 1):
                total = total + self.z_recv[rnd, d]
            self.z_out[rnd, mine] = total
            for copy in copies:
                copy.start()
        elif k == 4:
            self.z_wait(rnd, 1)
            for u in units:
                first = self.block(rnd, u, 1)[0] + self.links.pos[self.axes(rnd, u)[1]] * 8
                for j in range(5):
                    self.out[pl.ds(pl.multiple_of(first, 8), 8), pl.ds(j * 128, 128)] = self.z_out[rnd, u * 5 + j]
                self.gather_start(rnd, u, 1)
        elif k == 5:
            for u in units:
                self.wait_all(rnd, u, 1, self.ag_sems)
                self.gather_start(rnd, u, 0)
        elif k == 6:
            for u in units:
                self.wait_all(rnd, u, 0, self.ag_sems)
            self.swap(rnd).start()
        else:
            self.swap(rnd).wait()
            self.store(rnd).start()


def layer_norm(x_ref, rows):
    x_f = x_ref[rows].astype(F32)
    centered = x_f - jnp.mean(x_f, axis=-1, keepdims=True)
    inv_std = lax.rsqrt(jnp.mean(centered * centered, axis=-1, keepdims=True) + LN_EPS)
    return centered * inv_std, inv_std


def padded(parts, rows):
    filled = [part.astype(F32) for part in parts]
    used = sum(part.shape[0] for part in filled)
    return jnp.concatenate(filled + [jnp.zeros((rows - used, filled[0].shape[1]), F32)], axis=0).astype(BF)


def wait_for(ref, sem):
    pltpu.make_async_copy(ref, ref, sem).wait()


def block_body(dim, depth, x_hbm, dy_hbm, wt_hbm, wo_hbm, vectors, y_ref, gx_ref, dw_ref, small_ref,
               x_s, normed_s, dy_s, wt_s, wo_s, q_s, k_s, v_s, do_s, o_s, of_s, o_peer, lse_s, kf_s, vf_s, buf_a, buf_b, buf_c,
               kb_s, vb_s, dk_acc, dv_acc, grads, grads_peer, d_w, d_w_all, dx_s, y_s,
               recv1, recv2, mid, z_src, z_recv, z_out, small_s, small_recv,
               load_sems, in_send, in_recv, pass_send, pass_recv, o_sems, grad_sems, out_send, out_recv, small_sems,
               rs_sems, ag_sems, z_sems, swap_sems, store_sems):
    links = Links(depth)
    width, tokens = q_s.shape
    heads, tiles = width // dim, tokens // KEY_TILE
    own, band = tokens // 2, tokens // 4
    scale = dim ** -0.5
    log2_scale = scale * math.log2(math.e)
    fwd_group, bwd_group = 4, 4
    fwd_steps, bwd_steps = tiles // fwd_group, tiles // bwd_group
    zero = jnp.minimum(links.x, 0)
    odd = lax.rem(links.x, 2)
    reduce = GradReduce(links, d_w, d_w_all, dw_ref, (recv1, recv2, mid, z_src, z_recv, z_out),
                        (rs_sems, ag_sems, z_sems, swap_sems, store_sems))
    end = heads * bwd_steps + 1
    plan = {}
    for rnd in range(ROUNDS):
        at = rnd * bwd_steps + 1 if rnd else 0
        for k in range(STAGES):
            at += 0 if k == 0 else 2 if k in (1, 6) and rnd < ROUNDS - 1 else 1
            plan.setdefault(at, []).insert(0, (rnd, k))
    slots = max(plan) + 1 - end

    def tile_rows(tile, base=None):
        return pl.ds(tile * KEY_TILE if base is None else pl.multiple_of(base + tile * KEY_TILE, KEY_TILE), KEY_TILE)

    def head_rows(head, rows=dim):
        return pl.ds(pl.multiple_of(head * rows, 16), rows)

    def q_cols(index):
        return pl.ds(pl.multiple_of(index * Q_BLOCK, Q_BLOCK), Q_BLOCK)

    def my_half(side):
        return pl.ds(pl.multiple_of((links.core if side == 0 else 1 - links.core) * width, 16), width)

    loads = [pltpu.make_async_copy(wt_hbm.at[k, my_half(side)], wt_s.at[side, pl.ds(k * width, width)], load_sems.at[side, k])
             for side in range(2) for k in range(3)]
    loads += [pltpu.make_async_copy(wo_hbm.at[my_half(side)], wo_s.at[side], load_sems.at[side, 3]) for side in range(2)]

    def maybe_far(place, source, target, send, recv, start):
        core, x = place
        here = links.is_self(place)
        far = remote(source, target, send, recv, links.at(core=core, x=x))
        near = pltpu.make_async_copy(source, target, recv)

        @pl.when(jnp.logical_not(here))
        def _():
            far.start() if start else far.wait_send()

        if start:
            @pl.when(here)
            def _():
                near.start()

    piece = band // PIECES

    def deliver(which, m, c, start):
        slot = lax.rem(links.x + m, 2)
        source = (dy_hbm if which else x_hbm).at[m, pl.ds(c * piece, piece)]
        target = (dy_s if which else x_s).at[pl.ds(pl.multiple_of(slot * band + c * piece, 16), piece)]
        maybe_far(links.workers[m], source, target, in_send.at[which, m, c], in_recv.at[which, slot, c], start)

    def hand_over(which, slot, c):
        rows = dy_s if which else x_s
        first = slot * band + c * piece
        return remote(rows.at[pl.ds(first, piece)], rows.at[pl.ds(own + first, piece)],
                      pass_send.at[which, slot, c], pass_recv.at[which, slot, c], links.peer)

    def arrive(which, slot, c):
        with jax.named_scope(f'arrive{which}{slot}{c}'):
            wait_for((dy_s if which else x_s).at[pl.ds(slot * band + c * piece, piece)], in_recv.at[which, slot, c])
        hand_over(which, slot, c).start()

    def swap_out(head):
        rows = head_rows(head)
        return remote(o_s.at[rows, pl.ds(own, own)], o_peer.at[rows], o_sems.at[0, head], o_sems.at[1, head], links.peer)

    def swap_grads(head):
        rows = head_rows(head)
        return remote(grads.at[:, rows, pl.ds(own, own)], grads_peer.at[:, rows], grad_sems.at[0, head], grad_sems.at[1, head],
                      links.peer)

    part = band // 2
    portion = own // SENDS

    def send_home(which, i, start):
        cut = SENDS // 2
        second, inner = i // cut, lax.rem(i, cut)
        source = (dx_s if which else y_s).at[pl.ds(pl.multiple_of(i * portion, 16), portion)]
        target = (gx_ref if which else y_ref).at[odd, pl.ds(pl.multiple_of(inner * portion, 16), portion)]
        (core, x0), (_, x1) = links.owners
        maybe_far((core, jnp.where(second == 0, x0, x1)), source, target, out_send.at[which, i],
                  out_recv.at[which, odd, inner], start)

    def received_home(which):
        for m in range(2):
            for i in range(SENDS // 2):
                wait_for((gx_ref if which else y_ref).at[m, pl.ds(i * portion, portion)], out_recv.at[which, m, i])

    barrier = pltpu.get_barrier_semaphore()
    fixed = [links.peer]
    fixed += [links.step(axis, d) for axis in ('x', 'y') for d in range(1, RING)]
    fixed += [links.step('z', d) for d in range(1, depth)]
    for device in fixed:
        pl.semaphore_signal(barrier, inc=1, device_id=device, device_id_type=MESH)
    count = len(fixed)
    for place in links.owners + links.workers:
        other = jnp.logical_not(links.is_self(place))
        count = count + other.astype(jnp.int32)

        @pl.when(other)
        def _():
            pl.semaphore_signal(barrier, inc=1, device_id=links.at(core=place[0], x=place[1]), device_id_type=MESH)
    for load in loads:
        load.start()
    with jax.named_scope('barrier'):
        pl.semaphore_wait(barrier, count)
    for c in range(PIECES):
        for m in range(2):
            deliver(0, m, c, True)
    for load in loads:
        load.wait()

    def normalize(first):
        rows = pl.ds(first, piece)
        normed_s[rows] = (layer_norm(x_s, rows)[0] * vectors[0:1] + vectors[1:2]).astype(BF)

    for c in range(PIECES + 1):
        if c < PIECES:
            for slot in range(2):
                arrive(0, slot, c)
            if c == PIECES - 1:
                for i in range(PIECES):
                    for m in range(2):
                        deliver(1, m, i, True)
            for slot in range(2):
                normalize(slot * band + c * piece)
        if c:
            for slot in range(2):
                with jax.named_scope(f'handed{slot}{c}'):
                    hand_over(0, slot, c - 1).wait_recv()
                normalize(own + slot * band + (c - 1) * piece)
            if c % 2 == 0:
                for b in range(4):
                    cols = pl.ds(b * band + (c - 2) * piece, 2 * piece)
                    normed = normed_s[cols]
                    for k, out in enumerate((q_s, k_s, v_s)):
                        out[:, cols] = dot_nt(wt_s[0, pl.ds(k * width, width)], normed).astype(BF)

    def forward_step(now, carry):
        head, step = now // fwd_steps, lax.rem(now, fwd_steps)
        rows = head_rows(head)
        for c in range(PIECES):
            @pl.when(now == (c + 1) * heads * fwd_steps // (PIECES + 1))
            def _():
                for slot in range(2):
                    arrive(1, slot, c)

        @pl.when(step == 0)
        def _():
            k_t = k_s[rows]
            kf_s[...] = jnp.concatenate([k_t, k_t, k_t], axis=0).T
            vf_s[0:dim] = v_s[rows]
            vf_s[dim:] = padded([jnp.ones((1, tokens), F32)], AUG - dim)

        bufs = (buf_a, buf_b, buf_c)
        total, lag = tiles * fwd_group, tiles + 1
        query, high, top, probs, out = {}, {}, {}, {}, {}
        for g in range(total + lag + 2):
            if g < total:
                i, t = divmod(g, tiles)
                if t == 0:
                    query[i] = jnp.concatenate(split_parts(q_s[rows, q_cols(step * fwd_group + i)].astype(F32) * log2_scale), axis=0)
                scores = dot_nn(kf_s[tile_rows(t)], query[i])
                bufs[i % 3][tile_rows(t)] = scores
                folded = fold_rows(scores, jnp.maximum)
                high[i] = folded if t == 0 else jnp.maximum(high[i], folded)
                if t == tiles - 1:
                    top[i] = jnp.max(high[i], axis=0, keepdims=True)
            if lag <= g < total + lag:
                i, t = divmod(g - lag, tiles)
                probs[g - lag] = jnp.exp2(bufs[i % 3][tile_rows(t, zero)] - top[i]).astype(BF)
            if g >= lag + 2:
                i, t = divmod(g - lag - 2, tiles)
                product = dot_nn(vf_s[:, tile_rows(t)], probs[g - lag - 2])
                out[i] = product if t == 0 else out[i] + product
                if t == tiles - 1:
                    cols = q_cols(step * fwd_group + i)
                    denom = out[i][dim:dim + 1]
                    value = out[i][:dim] * (1.0 / denom)
                    o_s[rows, cols] = value.astype(BF)
                    of_s[rows, cols] = value
                    lse = (top[i] + jnp.log2(denom)) * (1.0 / log2_scale)
                    lse_s[head_rows(head, 16), cols] = padded(split_parts(lse), 16)

        @pl.when(step == fwd_steps - 1)
        def _():
            swap_out(head).start()

        return carry

    lax.fori_loop(0, heads * fwd_steps, forward_step, 0)
    with jax.named_scope('dyhanded'):
        for c in range(PIECES):
            for slot in range(2):
                hand_over(1, slot, c).wait_recv()
    d_w[pl.ds(0, width)] = dot_nn(o_s[...], dy_s[...])
    for rnd, k in plan[0]:
        reduce.stage(rnd, k)
    with jax.named_scope('oswap'):
        for head in range(heads):
            swap_out(head).wait()
    for i in range(4):
        toks = pl.ds(i * part, part)
        product = dot_tn(o_s[:, toks], wo_s[0]) + dot_tn(o_peer[:, toks], wo_s[1])
        y_s[toks] = (x_s[toks].astype(F32) + product + vectors[2:3]).astype(BF)
    for i in range(tiles):
        cols = pl.ds(i * KEY_TILE, KEY_TILE)
        do_s[:, cols] = dot_nt(wo_s[0], dy_s[cols]).astype(BF)
    with jax.named_scope('middlesends'):
        for which in range(2):
            for c in range(PIECES):
                for m in range(2):
                    deliver(which, m, c, False)
                    hand_over(which, m, c).wait_send()

    def backward_step(now, carry):
        head, step = now // bwd_steps, lax.rem(now, bwd_steps)
        rows = head_rows(head)
        for at in range(end - 1):
            todo = plan.get(at + 1)
            if todo:
                @pl.when(now == at)
                def _():
                    with jax.named_scope(f'step{at}'):
                        for rnd, k in todo:
                            reduce.stage(rnd, k)
        share = SENDS // (heads * bwd_steps)
        for i in range(share):
            send_home(0, now * share + i, True)

        @pl.when(step == 0)
        def _():
            minus = padded([jnp.full((3, tokens), -1.0, F32)], AUG - dim)
            kb_s[...] = jnp.concatenate([k_s[rows], minus], axis=0).T
            vb_s[...] = jnp.concatenate([v_s[rows], minus], axis=0).T
            dk_acc[...] = jnp.zeros_like(dk_acc)
            dv_acc[...] = jnp.zeros_like(dv_acc)

        total = tiles * bwd_group
        ops, probs, d_scores, dq = {}, {}, {}, {}
        for g in range(total + 2):
            if g < total:
                i, t = divmod(g, tiles)
                if t == 0:
                    cols = q_cols(step * bwd_group + i)
                    q_t, do_t = q_s[rows, cols], do_s[rows, cols]
                    delta = jnp.sum(of_s[rows, cols] * do_t.astype(F32), axis=0, keepdims=True)
                    ops[i] = (cols, q_t, do_t, jnp.concatenate([q_t, lse_s[head_rows(head, 16), cols]], axis=0),
                              jnp.concatenate([do_t, padded(split_parts(delta), 16)], axis=0))
                scores = dot_nn(kb_s[tile_rows(t)], ops[i][3])
                d_probs = dot_nn(vb_s[tile_rows(t)], ops[i][4])
                prob = jnp.exp2(scores * log2_scale)
                probs[g] = prob.astype(BF)
                d_scores[g] = (prob * d_probs).astype(BF)
            if g >= 2:
                i, t = divmod(g - 2, tiles)
                cols, q_t, do_t = ops[i][:3]
                dv_acc[:, tile_rows(t)] += dot_nt(do_t, probs[g - 2])
                product = dot_nn(k_s[rows, tile_rows(t)], d_scores[g - 2])
                dq[i] = product if t == 0 else dq[i] + product
                if t == tiles - 1:
                    grads[0, rows, cols] = (dq[i] * scale).astype(BF)
                dk_acc[:, tile_rows(t)] += dot_nt(q_t, d_scores[g - 2])

        @pl.when(step == bwd_steps - 1)
        def _():
            grads[1, rows] = (dk_acc[...] * scale).astype(BF)
            grads[2, rows] = dv_acc[...].astype(BF)
            swap_grads(head).start()
            stacked = jnp.concatenate([grads[0, rows], grads[1, rows], grads[2, rows]], axis=0)
            d_w[pl.ds(pl.multiple_of(width + head * (3 * dim), 8), 3 * dim)] = dot_nn(stacked, normed_s[...])

        return carry

    lax.fori_loop(0, heads * bwd_steps, backward_step, 0)

    def tail(slot):
        for rnd, k in plan.get(end + slot, ()):
            reduce.stage(rnd, k)

    def spread(share):
        for i in range(2):
            send_home(1, share * 2 + i, True)

    tail(0)
    with jax.named_scope('gradswap'):
        for head in range(heads):
            swap_grads(head).wait()
    gamma = vectors[0:1]
    sums = [jnp.zeros((1, 640), F32)] * 3
    for i in range(4):
        toks = pl.ds(i * part, part)
        mine = jnp.concatenate([grads[k, :, toks] for k in range(3)], axis=0)
        theirs = jnp.concatenate([grads_peer[k, :, toks] for k in range(3)], axis=0)
        d_normed = (dot_tn(mine, wt_s[0]) + dot_tn(theirs, wt_s[1])).astype(BF).astype(F32)
        x_hat, inv_std = layer_norm(x_s, toks)
        d_hat = d_normed * gamma
        mean_one = jnp.mean(d_hat, axis=-1, keepdims=True)
        mean_two = jnp.mean(d_hat * x_hat, axis=-1, keepdims=True)
        dy_f = dy_s[toks].astype(F32)
        dx_s[toks] = (dy_f + inv_std * (d_hat - mean_one - x_hat * mean_two)).astype(BF)
        spread(i)
        for k, term in enumerate((d_normed * x_hat, d_normed, dy_f)):
            sums[k] = sums[k] + jnp.sum(term, axis=0, keepdims=True)

    for k in range(3):
        for j in range(5):
            small_s[0, pl.ds(k * 5 + j, 1)] = sums[k][:, j * 128:(j + 1) * 128]
    small_s[0, pl.ds(15, 1)] = jnp.zeros((1, 128), F32)
    first, waiting = 0, None
    for hop, axis in enumerate(('z', 'y', 'core', 'x', '')):
        if waiting:
            acc = small_s[hop - 1]
            with jax.named_scope(f'small{hop}'):
                for copy in waiting:
                    copy.wait_recv()
            for d in range(len(waiting)):
                acc = acc + small_recv[first + d]
            for copy in waiting:
                copy.wait_send()
            if axis:
                small_s[hop] = acc
            else:
                small_ref[...] = acc
            first += len(waiting)
        elif hop:
            small_s[hop] = small_s[hop - 1]
        if axis:
            far = [links.peer] if axis == 'core' else [links.step(axis, d) for d in range(1, links.size[axis])]
            waiting = [remote(small_s.at[hop], small_recv.at[first + d], small_sems.at[0, first + d], small_sems.at[1, first + d],
                              device) for d, device in enumerate(far)]
            for copy in waiting:
                copy.start()
            tail(1 + hop)
            if hop < 2:
                for i in range(2):
                    spread(4 + 2 * hop + i)
    for slot in range(5, slots):
        tail(slot)
    with jax.named_scope('home'):
        for which in range(2):
            for i in range(SENDS):
                send_home(which, i, False)
            received_home(which)
    with jax.named_scope('stored'):
        for rnd in range(ROUNDS):
            reduce.store(rnd).wait()


def attention_block(x_in, grad_y, w_t, w_o, vectors, dim, depth):
    rows, channels = x_in.shape[1:]
    tokens, own = 4 * rows, 2 * rows
    width = w_o.shape[0] // 2
    heads = width // dim
    total = 4 * width
    half = lambda *shape: pltpu.VMEM(shape, BF)
    full = lambda *shape: pltpu.VMEM(shape, F32)
    dma = lambda *shape: pltpu.SemaphoreType.DMA(shape)
    anywhere = pl.BlockSpec(memory_space=pl.ANY)
    in_vmem = pl.BlockSpec(memory_space=pltpu.VMEM)
    far = max(depth - 1, 1)
    return pl.pallas_call(
        functools.partial(block_body, dim, depth),
        in_specs=[anywhere] * 4 + [in_vmem],
        out_specs=[anywhere] * 3 + [in_vmem],
        out_shape=[jax.ShapeDtypeStruct(x_in.shape, BF)] * 2
        + [jax.ShapeDtypeStruct((2, total, channels), F32), jax.ShapeDtypeStruct((16, 128), F32)],
        scratch_shapes=[half(tokens, channels)] * 3 + [half(2, 3 * width, channels), half(2, width, channels)]
        + [half(width, tokens)] * 5 + [full(width, tokens), half(width, own), half(16 * heads, tokens),
                                       half(tokens, 3 * dim), half(AUG, tokens)]
        + [full(tokens, Q_BLOCK)] * 3 + [half(tokens, AUG)] * 2 + [full(dim, tokens)] * 2
        + [half(3, width, tokens), half(3, width, own), full(total, channels), full(2, total, channels)]
        + [half(own, channels)] * 2
        + [full(ROUNDS, 2, 3, 32, channels), full(ROUNDS, 2, 3, 8, channels), full(ROUNDS, 2, 32, channels), full(ROUNDS, 16, 8, 128),
           full(ROUNDS, far, 16 // depth, 8, 128), full(ROUNDS, 16, 8, 128), full(4, 16, 128), full(7 + far, 16, 128),
           dma(2, 4)] + [dma(2, 2, PIECES)] * 4 + [dma(2, heads)] * 2
        + [dma(2, SENDS), dma(2, 2, SENDS // 2), dma(2, 7 + far)] + [dma(2, ROUNDS, 2, 2)] * 2 + [dma(2, ROUNDS, 2), dma(2, ROUNDS), dma(ROUNDS)],
        compiler_params=pltpu.CompilerParams(collective_id=0, has_side_effects=True, vmem_limit_bytes=VMEM_BYTES),
        name='attention_block',
    )(x_in, grad_y, w_t, w_o, vectors)


def solution(mesh):
    depth = mesh.shape['dp'] // (2 * RING)
    act_spec, rep_spec = P('dp', 'cp', None), P()

    def device_step(x_in, grad_y, ln_gamma, ln_beta, w_q, w_k, w_v, w_o, b_o):
        channels, num_heads, head_dim = w_q.shape
        w_t = jnp.stack([jnp.transpose(w, (1, 2, 0)).reshape(num_heads * head_dim, channels) for w in (w_q, w_k, w_v)])
        vectors = jnp.stack([ln_gamma, ln_beta, b_o])
        y_out, grad_x, d_w, small = attention_block(x_in, grad_y, w_t, w_o.reshape(num_heads * head_dim, channels), vectors,
                                                    head_dim, depth)
        small = small[:15].reshape(3, channels)
        width = num_heads * head_dim // 2
        grad_wo = d_w[:, :width].reshape(num_heads, head_dim, channels)
        d_w = d_w[:, width:].reshape(num_heads, 3, head_dim, channels)
        grads = [jnp.transpose(d_w[:, i], (2, 0, 1)) for i in range(3)]
        return (y_out, grad_x, small[0], small[1], *grads, grad_wo, small[2])

    specs = (act_spec, act_spec) + (rep_spec,) * 7
    return jax.shard_map(device_step, mesh=mesh, in_specs=specs, out_specs=specs, check_vma=False)
```

```python
import functools
import math
import jax
import jax.numpy as jnp
from jax import lax
from jax.experimental import pallas as pl
from jax.experimental.pallas import tpu as pltpu
from jax.sharding import PartitionSpec as P

LN_EPS = 1e-5
KEY_TILE = 256
Q_BLOCK = 256
FOLD = 16
AUG = 96
VMEM_BYTES = 67043328
BF = jnp.bfloat16
F32 = jnp.float32


def dot_nn(lhs, rhs):
    return lax.dot_general(lhs, rhs, (((1,), (0,)), ((), ())), preferred_element_type=F32)


def dot_nt(lhs, rhs):
    return lax.dot_general(lhs, rhs, (((1,), (1,)), ((), ())), preferred_element_type=F32)


def dot_tn(lhs, rhs):
    return lax.dot_general(lhs, rhs, (((0,), (0,)), ((), ())), preferred_element_type=F32)


def split_parts(value):
    high = value.astype(BF)
    rest = value - high.astype(F32)
    mid = rest.astype(BF)
    return high, mid, (rest - mid.astype(F32)).astype(BF)


def fold_rows(value, op):
    groups = value.reshape(value.shape[0] // FOLD, FOLD, value.shape[1])
    out = groups[0]
    for i in range(1, groups.shape[0]):
        out = op(out, groups[i])
    return out


MESH = pl.DeviceIdType.MESH
RING = 4
ROUNDS = 5
ROUND_ROWS = 256
STAGES = 8
PIECES = 4
SENDS = 16
ORDER = ('y', 'x')


class Links:
    def __init__(self, depth):
        dp, self.x = lax.axis_index('dp'), lax.axis_index('cp')
        self.core = lax.rem(dp, 2)
        self.y = lax.rem(dp // 2, RING)
        self.z = dp // (2 * RING)
        self.depth = depth
        self.pos = {'x': self.x, 'y': self.y, 'z': self.z}
        self.size = {'x': RING, 'y': RING, 'z': depth}
        self.peer = self.at(core=1 - self.core)
        pair, odd = self.x // 2, lax.rem(self.x, 2)
        self.owners = [(pair, 2 * self.core + odd), (pair, 2 * self.core + 1 - odd)]
        self.workers = [(pair, 2 * self.core), (pair, 2 * self.core + 1)]

    def at(self, x=None, y=None, z=None, core=None):
        pick = lambda value, own: own if value is None else value
        return ((pick(z, self.z) * RING + pick(y, self.y)) * 2 + pick(core, self.core), pick(x, self.x))

    def step(self, axis, d):
        return self.at(**{axis: lax.rem(self.pos[axis] + d, self.size[axis])})

    def is_self(self, place):
        return jnp.logical_and(place[0] == self.core, place[1] == self.x)


def remote(source, target, send, recv, device):
    return pltpu.make_async_remote_copy(src_ref=source, dst_ref=target, send_sem=send, recv_sem=recv,
                                        device_id=device, device_id_type=MESH)


def wait_for(ref, sem):
    pltpu.make_async_copy(ref, ref, sem).wait()


class GradReduce:
    def __init__(self, links, dim, grad, out, results, bufs, sems):
        self.links, self.grad, self.both, self.out = links, grad, out, out.at[links.core]
        width = grad.shape[0] // 4
        self.pieces = [(0, width, results[0], 0)]
        self.pieces += [(width + (3 * head + k) * dim, dim, results[1 + k], head * dim) for head in range(width // dim) for k in range(3)]
        self.recv1, self.recv2, self.mid, self.z_src, self.z_recv, self.z_out = bufs
        self.rs_sems, self.ag_sems, self.z_sems, self.swap_sems, self.store_sems = sems

    def axes(self, rnd, unit):
        first = ORDER[unit]
        return first, ('x' if first == 'y' else 'y')

    def block(self, rnd, unit, phase):
        first = rnd * ROUND_ROWS + unit * 128
        if phase == 0:
            return first, 32
        return first + self.links.pos[self.axes(rnd, unit)[0]] * 32, 8

    def landing(self, rnd, unit, phase):
        return (self.recv1 if phase == 0 else self.recv2).at[rnd, unit]

    def wait_all(self, rnd, unit, phase, sems):
        whole = self.landing(rnd, unit, phase)
        every = remote(whole, whole, sems.at[0, rnd, unit, phase], sems.at[1, rnd, unit, phase], self.links.peer)
        every.wait_recv()
        every.wait_send()

    def source(self, rnd, unit, phase, owner):
        if phase == 0:
            first, rows = self.block(rnd, unit, 0)
            return self.grad.at[pl.ds(pl.multiple_of(first + owner * rows, 8), rows)]
        return self.mid.at[rnd, unit, pl.ds(pl.multiple_of(owner * 8, 8), 8)]

    def scatter_start(self, rnd, unit, phase):
        axis = self.axes(rnd, unit)[phase]
        for d in (2, 1, 3):
            owner = lax.rem(self.links.pos[axis] + d, RING)
            remote(self.source(rnd, unit, phase, owner), self.landing(rnd, unit, phase).at[d - 1],
                   self.rs_sems.at[0, rnd, unit, phase], self.rs_sems.at[1, rnd, unit, phase], self.links.step(axis, d)).start()

    def scatter_end(self, rnd, unit, phase):
        self.wait_all(rnd, unit, phase, self.rs_sems)
        landing = self.landing(rnd, unit, phase)
        mine = self.source(rnd, unit, phase, self.links.pos[self.axes(rnd, unit)[phase]])
        return (mine[...] + landing[0]) + (landing[1] + landing[2])

    def gather_start(self, rnd, unit, phase):
        axis = self.axes(rnd, unit)[phase]
        first, rows = self.block(rnd, unit, phase)
        part = self.out.at[pl.ds(pl.multiple_of(first + self.links.pos[axis] * rows, 8), rows)]
        for d in (2, 1, 3):
            remote(part, part, self.ag_sems.at[0, rnd, unit, phase], self.ag_sems.at[1, rnd, unit, phase],
                   self.links.step(axis, d)).start()

    def z_copies(self, rnd, way):
        links = self.links
        each = 16 // links.depth
        send, recv = self.z_sems.at[0, rnd, way], self.z_sems.at[1, rnd, way]
        mine = pl.ds(links.z * each, each)
        copies = []
        for d in range(1, links.depth):
            far = lax.rem(links.z + d, links.depth)
            if way == 0:
                source, target = self.z_src.at[rnd, pl.ds(far * each, each)], self.z_recv.at[rnd, d - 1]
            else:
                source = target = self.z_out.at[rnd, mine]
            copies.append(remote(source, target, send, recv, links.step('z', d)))
        return copies, mine

    def z_wait(self, rnd, way):
        if self.links.depth > 1:
            whole = self.z_recv.at[rnd]
            all_of = remote(whole, whole, self.z_sems.at[0, rnd, way], self.z_sems.at[1, rnd, way], self.links.step('z', 1))
            all_of.wait_recv()
            all_of.wait_send()

    def swap(self, rnd):
        part = self.out.at[pl.ds(rnd * ROUND_ROWS, ROUND_ROWS)]
        return remote(part, part, self.swap_sems.at[0, rnd], self.swap_sems.at[1, rnd], self.links.peer)

    def store(self, rnd):
        begin = rnd * ROUND_ROWS
        half = self.both.shape[1] // 4
        for first, rows, result, place in self.pieces:
            low, high = max(first, begin), min(first + rows, begin + ROUND_ROWS)
            for core in range(2):
                if low < high:
                    target = result.at[pl.ds(core * half + place + low - first, high - low)]
                    pltpu.make_async_copy(self.both.at[core, pl.ds(low, high - low)], target, self.store_sems.at[rnd]).start()

    def stored(self, rnd):
        wait_for(self.both.at[:, pl.ds(rnd * ROUND_ROWS, ROUND_ROWS)], self.store_sems.at[rnd])

    def stage(self, rnd, k):
        units = (0, 1)
        if k == 0:
            for u in units:
                self.scatter_start(rnd, u, 0)
        elif k == 1:
            for u in units:
                self.mid[rnd, u] = self.scatter_end(rnd, u, 0)
                self.scatter_start(rnd, u, 1)
        elif k == 2:
            for u in units:
                total = self.scatter_end(rnd, u, 1)
                for j in range(5):
                    self.z_src[rnd, u * 5 + j] = total[:, j * 128:(j + 1) * 128]
            self.z_src[rnd, pl.ds(10, 6)] = jnp.zeros((6, 8, 128), F32)
            for copy in self.z_copies(rnd, 0)[0]:
                copy.start()
        elif k == 3:
            self.z_wait(rnd, 0)
            copies, mine = self.z_copies(rnd, 1)
            total = self.z_src[rnd, mine]
            for d in range(self.links.depth - 1):
                total = total + self.z_recv[rnd, d]
            self.z_out[rnd, mine] = total
            for copy in copies:
                copy.start()
        elif k == 4:
            self.z_wait(rnd, 1)
            for u in units:
                first = self.block(rnd, u, 1)[0] + self.links.pos[self.axes(rnd, u)[1]] * 8
                for j in range(5):
                    self.out[pl.ds(pl.multiple_of(first, 8), 8), pl.ds(j * 128, 128)] = self.z_out[rnd, u * 5 + j]
                self.gather_start(rnd, u, 1)
        elif k == 5:
            for u in units:
                self.wait_all(rnd, u, 1, self.ag_sems)
                self.gather_start(rnd, u, 0)
        elif k == 6:
            for u in units:
                self.wait_all(rnd, u, 0, self.ag_sems)
            self.swap(rnd).start()
        else:
            self.swap(rnd).wait()
            self.store(rnd)


def layer_norm(x_ref, rows):
    x_f = x_ref[rows].astype(F32)
    centered = x_f - jnp.mean(x_f, axis=-1, keepdims=True)
    inv_std = lax.rsqrt(jnp.mean(centered * centered, axis=-1, keepdims=True) + LN_EPS)
    return centered * inv_std, inv_std


def padded(parts, rows):
    filled = [part.astype(F32) for part in parts]
    used = sum(part.shape[0] for part in filled)
    return jnp.concatenate(filled + [jnp.zeros((rows - used, filled[0].shape[1]), F32)], axis=0).astype(BF)


def block_body(dim, depth, x_hbm, dy_hbm, wq_hbm, wk_hbm, wv_hbm, wo_hbm, gamma_ref, beta_ref, bo_ref,
               y_ref, gx_ref, dq_ref, dk_ref, dv_ref, dwo_ref, small_ref,
               x_s, normed_s, dy_s, wt_s, wo_s, q_s, k_s, v_s, do_s, o_s, of_s, o_peer, lse_s, kf_s, vf_s, buf_a, buf_b, buf_c,
               kb_s, vb_s, dk_acc, dv_acc, grads, grads_peer, d_w, d_w_all, dx_s, y_s,
               recv1, recv2, mid, z_src, z_recv, z_out, small_s, small_recv,
               load_sems, in_send, in_recv, pass_send, pass_recv, o_sems, grad_sems, out_send, out_recv, small_sems,
               rs_sems, ag_sems, z_sems, swap_sems, store_sems):
    links = Links(depth)
    width, tokens = q_s.shape
    heads, tiles = width // dim, tokens // KEY_TILE
    own, band = tokens // 2, tokens // 4
    scale = dim ** -0.5
    log2_scale = scale * math.log2(math.e)
    fwd_group, bwd_group = 4, 4
    fwd_steps, bwd_steps = tiles // fwd_group, tiles // bwd_group
    zero = jnp.minimum(links.x, 0)
    gamma, beta, bias = (ref[...].reshape(1, ref.shape[0]) for ref in (gamma_ref, beta_ref, bo_ref))
    odd = lax.rem(links.x, 2)
    reduce = GradReduce(links, dim, d_w, d_w_all, (dwo_ref, dq_ref, dk_ref, dv_ref), (recv1, recv2, mid, z_src, z_recv, z_out),
                        (rs_sems, ag_sems, z_sems, swap_sems, store_sems))
    end = heads * bwd_steps + 1
    plan = {}
    for rnd in range(ROUNDS):
        at = rnd * bwd_steps + 1 if rnd else 0
        for k in range(STAGES):
            at += 0 if k == 0 else 2 if k in (1, 6) and rnd < ROUNDS - 1 else 1
            plan.setdefault(at, []).insert(0, (rnd, k))
    slots = max(plan) + 1 - end

    def tile_rows(tile, base=None):
        return pl.ds(tile * KEY_TILE if base is None else pl.multiple_of(base + tile * KEY_TILE, KEY_TILE), KEY_TILE)

    def head_rows(head, rows=dim):
        return pl.ds(pl.multiple_of(head * rows, 16), rows)

    def q_cols(index):
        return pl.ds(pl.multiple_of(index * Q_BLOCK, Q_BLOCK), Q_BLOCK)

    def my_half(side):
        return pl.ds(pl.multiple_of((links.core if side == 0 else 1 - links.core) * width, 16), width)

    loads = [pltpu.make_async_copy(w_hbm.at[my_half(side)], wt_s.at[side, pl.ds(k * width, width)], load_sems.at[side, k])
             for side in range(2) for k, w_hbm in enumerate((wq_hbm, wk_hbm, wv_hbm))]
    loads += [pltpu.make_async_copy(wo_hbm.at[my_half(side)], wo_s.at[side], load_sems.at[side, 3]) for side in range(2)]

    def maybe_far(place, source, target, send, recv, start):
        core, x = place
        here = links.is_self(place)
        far = remote(source, target, send, recv, links.at(core=core, x=x))
        near = pltpu.make_async_copy(source, target, recv)

        @pl.when(jnp.logical_not(here))
        def _():
            far.start() if start else far.wait_send()

        if start:
            @pl.when(here)
            def _():
                near.start()

    piece = band // PIECES

    def deliver(which, m, c, start):
        slot = lax.rem(links.x + m, 2)
        source = (dy_hbm if which else x_hbm).at[m, pl.ds(c * piece, piece)]
        target = (dy_s if which else x_s).at[pl.ds(pl.multiple_of(slot * band + c * piece, 16), piece)]
        maybe_far(links.workers[m], source, target, in_send.at[which, m, c], in_recv.at[which, slot, c], start)

    def hand_over(which, slot, c):
        rows = dy_s if which else x_s
        first = slot * band + c * piece
        return remote(rows.at[pl.ds(first, piece)], rows.at[pl.ds(own + first, piece)],
                      pass_send.at[which, slot, c], pass_recv.at[which, slot, c], links.peer)

    def arrive(which, slot, c):
        with jax.named_scope(f'arrive{which}{slot}{c}'):
            wait_for((dy_s if which else x_s).at[pl.ds(slot * band + c * piece, piece)], in_recv.at[which, slot, c])
        hand_over(which, slot, c).start()

    def swap_out(head):
        rows = head_rows(head)
        return remote(o_s.at[rows, pl.ds(own, own)], o_peer.at[rows], o_sems.at[0, head], o_sems.at[1, head], links.peer)

    def swap_grads(head):
        rows = head_rows(head)
        return remote(grads.at[:, rows, pl.ds(own, own)], grads_peer.at[:, rows], grad_sems.at[0, head], grad_sems.at[1, head],
                      links.peer)

    part = band // 2
    portion = own // SENDS

    def send_home(which, i, start):
        cut = SENDS // 2
        second, inner = i // cut, lax.rem(i, cut)
        source = (dx_s if which else y_s).at[pl.ds(pl.multiple_of(i * portion, 16), portion)]
        target = (gx_ref if which else y_ref).at[odd, pl.ds(pl.multiple_of(inner * portion, 16), portion)]
        (core, x0), (_, x1) = links.owners
        maybe_far((core, jnp.where(second == 0, x0, x1)), source, target, out_send.at[which, i],
                  out_recv.at[which, odd, inner], start)

    def received_home(which):
        for m in range(2):
            for i in range(SENDS // 2):
                wait_for((gx_ref if which else y_ref).at[m, pl.ds(i * portion, portion)], out_recv.at[which, m, i])

    barrier = pltpu.get_barrier_semaphore()
    fixed = [links.peer]
    fixed += [links.step(axis, d) for axis in ('x', 'y') for d in range(1, RING)]
    fixed += [links.step('z', d) for d in range(1, depth)]
    for device in fixed:
        pl.semaphore_signal(barrier, inc=1, device_id=device, device_id_type=MESH)
    count = len(fixed)
    for place in links.owners + links.workers:
        other = jnp.logical_not(links.is_self(place))
        count = count + other.astype(jnp.int32)

        @pl.when(other)
        def _():
            pl.semaphore_signal(barrier, inc=1, device_id=links.at(core=place[0], x=place[1]), device_id_type=MESH)
    for load in loads:
        load.start()
    with jax.named_scope('barrier'):
        pl.semaphore_wait(barrier, count)
    for c in range(PIECES):
        for m in range(2):
            deliver(0, m, c, True)
    for load in loads:
        load.wait()

    def normalize(first):
        rows = pl.ds(first, piece)
        normed_s[rows] = (layer_norm(x_s, rows)[0] * gamma + beta).astype(BF)

    for c in range(PIECES + 1):
        if c < PIECES:
            for slot in range(2):
                arrive(0, slot, c)
            if c == PIECES - 1:
                for i in range(PIECES):
                    for m in range(2):
                        deliver(1, m, i, True)
            for slot in range(2):
                normalize(slot * band + c * piece)
        if c:
            for slot in range(2):
                with jax.named_scope(f'handed{slot}{c}'):
                    hand_over(0, slot, c - 1).wait_recv()
                normalize(own + slot * band + (c - 1) * piece)
            if c % 2 == 0:
                for b in range(4):
                    cols = pl.ds(b * band + (c - 2) * piece, 2 * piece)
                    normed = normed_s[cols]
                    for k, out in enumerate((q_s, k_s, v_s)):
                        out[:, cols] = dot_nt(wt_s[0, pl.ds(k * width, width)], normed).astype(BF)

    def forward_step(now, carry):
        head, step = now // fwd_steps, lax.rem(now, fwd_steps)
        rows = head_rows(head)
        for c in range(PIECES):
            @pl.when(now == (c + 1) * heads * fwd_steps // (PIECES + 1))
            def _():
                for slot in range(2):
                    arrive(1, slot, c)

        @pl.when(step == 0)
        def _():
            k_t = k_s[rows]
            kf_s[...] = jnp.concatenate([k_t, k_t, k_t], axis=0).T
            vf_s[0:dim] = v_s[rows]
            vf_s[dim:] = padded([jnp.ones((1, tokens), F32)], AUG - dim)

        bufs = (buf_a, buf_b, buf_c)
        total, lag = tiles * fwd_group, tiles + 1
        query, high, top, probs, out = {}, {}, {}, {}, {}
        for g in range(total + lag + 2):
            if g < total:
                i, t = divmod(g, tiles)
                if t == 0:
                    query[i] = jnp.concatenate(split_parts(q_s[rows, q_cols(step * fwd_group + i)].astype(F32) * log2_scale), axis=0)
                scores = dot_nn(kf_s[tile_rows(t)], query[i])
                bufs[i % 3][tile_rows(t)] = scores
                folded = fold_rows(scores, jnp.maximum)
                high[i] = folded if t == 0 else jnp.maximum(high[i], folded)
                if t == tiles - 1:
                    top[i] = jnp.max(high[i], axis=0, keepdims=True)
            if lag <= g < total + lag:
                i, t = divmod(g - lag, tiles)
                probs[g - lag] = jnp.exp2(bufs[i % 3][tile_rows(t, zero)] - top[i]).astype(BF)
            if g >= lag + 2:
                i, t = divmod(g - lag - 2, tiles)
                product = dot_nn(vf_s[:, tile_rows(t)], probs[g - lag - 2])
                out[i] = product if t == 0 else out[i] + product
                if t == tiles - 1:
                    cols = q_cols(step * fwd_group + i)
                    denom = out[i][dim:dim + 1]
                    value = out[i][:dim] * (1.0 / denom)
                    o_s[rows, cols] = value.astype(BF)
                    of_s[rows, cols] = value
                    lse = (top[i] + jnp.log2(denom)) * (1.0 / log2_scale)
                    lse_s[head_rows(head, 16), cols] = padded(split_parts(lse), 16)

        @pl.when(step == fwd_steps - 1)
        def _():
            swap_out(head).start()

        return carry

    lax.fori_loop(0, heads * fwd_steps, forward_step, 0)
    with jax.named_scope('dyhanded'):
        for c in range(PIECES):
            for slot in range(2):
                hand_over(1, slot, c).wait_recv()
    d_w[pl.ds(0, width)] = dot_nn(o_s[...], dy_s[...])
    for rnd, k in plan[0]:
        reduce.stage(rnd, k)
    with jax.named_scope('oswap'):
        for head in range(heads):
            swap_out(head).wait()
    for i in range(4):
        toks = pl.ds(i * part, part)
        product = dot_tn(o_s[:, toks], wo_s[0]) + dot_tn(o_peer[:, toks], wo_s[1])
        y_s[toks] = (x_s[toks].astype(F32) + product + bias).astype(BF)
    for i in range(tiles):
        cols = pl.ds(i * KEY_TILE, KEY_TILE)
        do_s[:, cols] = dot_nt(wo_s[0], dy_s[cols]).astype(BF)
    with jax.named_scope('middlesends'):
        for which in range(2):
            for c in range(PIECES):
                for m in range(2):
                    deliver(which, m, c, False)
                    hand_over(which, m, c).wait_send()

    def backward_step(now, carry):
        head, step = now // bwd_steps, lax.rem(now, bwd_steps)
        rows = head_rows(head)
        for at in range(end - 1):
            todo = plan.get(at + 1)
            if todo:
                @pl.when(now == at)
                def _():
                    with jax.named_scope(f'step{at}'):
                        for rnd, k in todo:
                            reduce.stage(rnd, k)
        share = SENDS // (heads * bwd_steps)
        for i in range(share):
            send_home(0, now * share + i, True)

        @pl.when(step == 0)
        def _():
            minus = padded([jnp.full((3, tokens), -1.0, F32)], AUG - dim)
            kb_s[...] = jnp.concatenate([k_s[rows], minus], axis=0).T
            vb_s[...] = jnp.concatenate([v_s[rows], minus], axis=0).T
            dk_acc[...] = jnp.zeros_like(dk_acc)
            dv_acc[...] = jnp.zeros_like(dv_acc)

        total = tiles * bwd_group
        ops, probs, d_scores, dq = {}, {}, {}, {}
        for g in range(total + 2):
            if g < total:
                i, t = divmod(g, tiles)
                if t == 0:
                    cols = q_cols(step * bwd_group + i)
                    q_t, do_t = q_s[rows, cols], do_s[rows, cols]
                    delta = jnp.sum(of_s[rows, cols] * do_t.astype(F32), axis=0, keepdims=True)
                    ops[i] = (cols, q_t, do_t, jnp.concatenate([q_t, lse_s[head_rows(head, 16), cols]], axis=0),
                              jnp.concatenate([do_t, padded(split_parts(delta), 16)], axis=0))
                scores = dot_nn(kb_s[tile_rows(t)], ops[i][3])
                d_probs = dot_nn(vb_s[tile_rows(t)], ops[i][4])
                prob = jnp.exp2(scores * log2_scale)
                probs[g] = prob.astype(BF)
                d_scores[g] = (prob * d_probs).astype(BF)
            if g >= 2:
                i, t = divmod(g - 2, tiles)
                cols, q_t, do_t = ops[i][:3]
                dv_acc[:, tile_rows(t)] += dot_nt(do_t, probs[g - 2])
                product = dot_nn(k_s[rows, tile_rows(t)], d_scores[g - 2])
                dq[i] = product if t == 0 else dq[i] + product
                if t == tiles - 1:
                    grads[0, rows, cols] = (dq[i] * scale).astype(BF)
                dk_acc[:, tile_rows(t)] += dot_nt(q_t, d_scores[g - 2])

        @pl.when(step == bwd_steps - 1)
        def _():
            grads[1, rows] = (dk_acc[...] * scale).astype(BF)
            grads[2, rows] = dv_acc[...].astype(BF)
            swap_grads(head).start()
            stacked = jnp.concatenate([grads[0, rows], grads[1, rows], grads[2, rows]], axis=0)
            d_w[pl.ds(pl.multiple_of(width + head * (3 * dim), 8), 3 * dim)] = dot_nn(stacked, normed_s[...])

        return carry

    lax.fori_loop(0, heads * bwd_steps, backward_step, 0)

    def tail(slot):
        for rnd, k in plan.get(end + slot, ()):
            with jax.named_scope(f'tail{slot}r{rnd}k{k}'):
                reduce.stage(rnd, k)

    tail(0)
    with jax.named_scope('gradswap'):
        for head in range(heads):
            swap_grads(head).wait()
    sums = [jnp.zeros((1, 640), F32)] * 3
    for i in range(4):
        toks = pl.ds(i * part, part)
        mine = jnp.concatenate([grads[k, :, toks] for k in range(3)], axis=0)
        theirs = jnp.concatenate([grads_peer[k, :, toks] for k in range(3)], axis=0)
        d_normed = (dot_tn(mine, wt_s[0]) + dot_tn(theirs, wt_s[1])).astype(BF).astype(F32)
        x_hat, inv_std = layer_norm(x_s, toks)
        d_hat = d_normed * gamma
        mean_one = jnp.mean(d_hat, axis=-1, keepdims=True)
        mean_two = jnp.mean(d_hat * x_hat, axis=-1, keepdims=True)
        dy_f = dy_s[toks].astype(F32)
        dx_s[toks] = (dy_f + inv_std * (d_hat - mean_one - x_hat * mean_two)).astype(BF)
        for k, term in enumerate((d_normed * x_hat, d_normed, dy_f)):
            sums[k] = sums[k] + jnp.sum(term, axis=0, keepdims=True)

    for k in range(3):
        for j in range(5):
            small_s[0, pl.ds(k * 5 + j, 1)] = sums[k][:, j * 128:(j + 1) * 128]
    small_s[0, pl.ds(15, 1)] = jnp.zeros((1, 128), F32)
    first, waiting = 0, None
    for hop, axis in enumerate(('z', 'y', 'core', 'x', '')):
        if waiting:
            acc = small_s[hop - 1]
            with jax.named_scope(f'small{hop}'):
                for copy in waiting:
                    copy.wait_recv()
            for d in range(len(waiting)):
                acc = acc + small_recv[first + d]
            for copy in waiting:
                copy.wait_send()
            if axis:
                small_s[hop] = acc
            else:
                small_ref[...] = acc
            first += len(waiting)
        elif hop:
            small_s[hop] = small_s[hop - 1]
        if axis:
            far = [links.peer] if axis == 'core' else [links.step(axis, d) for d in range(1, links.size[axis])]
            waiting = [remote(small_s.at[hop], small_recv.at[first + d], small_sems.at[0, first + d], small_sems.at[1, first + d],
                              device) for d, device in enumerate(far)]
            for copy in waiting:
                copy.start()
            tail(1 + hop)
            if hop == 0:
                for i in range(SENDS):
                    send_home(1, i, True)
    for slot in range(5, slots):
        tail(slot)
    with jax.named_scope('home'):
        for which in range(2):
            for i in range(SENDS):
                send_home(which, i, False)
            received_home(which)
    with jax.named_scope('stored'):
        for rnd in range(ROUNDS):
            reduce.stored(rnd)


def attention_block(x_in, grad_y, weights, vectors, dim, depth):
    rows, channels = x_in.shape[1:]
    tokens, own = 4 * rows, 2 * rows
    width = weights[0].shape[0] // 2
    heads = width // dim
    total = 4 * width
    half = lambda *shape: pltpu.VMEM(shape, BF)
    full = lambda *shape: pltpu.VMEM(shape, F32)
    dma = lambda *shape: pltpu.SemaphoreType.DMA(shape)
    anywhere = pl.BlockSpec(memory_space=pl.ANY)
    in_vmem = pl.BlockSpec(memory_space=pltpu.VMEM)
    far = max(depth - 1, 1)
    return pl.pallas_call(
        functools.partial(block_body, dim, depth),
        in_specs=[anywhere] * 6 + [in_vmem] * 3,
        out_specs=[anywhere] * 6 + [in_vmem],
        out_shape=[jax.ShapeDtypeStruct(x_in.shape, BF)] * 2
        + [jax.ShapeDtypeStruct(weights[0].shape, F32)] * 4 + [jax.ShapeDtypeStruct((16, 128), F32)],
        scratch_shapes=[half(tokens, channels)] * 3 + [half(2, 3 * width, channels), half(2, width, channels)]
        + [half(width, tokens)] * 5 + [full(width, tokens), half(width, own), half(16 * heads, tokens),
                                       half(tokens, 3 * dim), half(AUG, tokens)]
        + [full(tokens, Q_BLOCK)] * 3 + [half(tokens, AUG)] * 2 + [full(dim, tokens)] * 2
        + [half(3, width, tokens), half(3, width, own), full(total, channels), full(2, total, channels)]
        + [half(own, channels)] * 2
        + [full(ROUNDS, 2, 3, 32, channels), full(ROUNDS, 2, 3, 8, channels), full(ROUNDS, 2, 32, channels), full(ROUNDS, 16, 8, 128),
           full(ROUNDS, far, 16 // depth, 8, 128), full(ROUNDS, 16, 8, 128), full(4, 16, 128), full(7 + far, 16, 128),
           dma(2, 4)] + [dma(2, 2, PIECES)] * 4 + [dma(2, heads)] * 2
        + [dma(2, SENDS), dma(2, 2, SENDS // 2), dma(2, 7 + far)] + [dma(2, ROUNDS, 2, 2)] * 2 + [dma(2, ROUNDS, 2), dma(2, ROUNDS), dma(ROUNDS)],
        compiler_params=pltpu.CompilerParams(collective_id=0, has_side_effects=True, vmem_limit_bytes=VMEM_BYTES),
        name='attention_block',
    )(x_in, grad_y, *weights, *vectors)


def solution(mesh):
    depth = mesh.shape['dp'] // (2 * RING)
    act_spec, rep_spec = P('dp', 'cp', None), P()

    def device_step(x_in, grad_y, ln_gamma, ln_beta, w_q, w_k, w_v, w_o, b_o):
        channels, num_heads, head_dim = w_q.shape
        flat = (num_heads * head_dim, channels)
        weights = [jnp.transpose(w, (1, 2, 0)).reshape(flat) for w in (w_q, w_k, w_v)] + [w_o.reshape(flat)]
        y_out, grad_x, *grads, grad_wo, small = attention_block(x_in, grad_y, weights, (ln_gamma, ln_beta, b_o), head_dim, depth)
        small = small[:15].reshape(3, channels)
        grads = [jnp.transpose(grad.reshape(num_heads, head_dim, channels), (2, 0, 1)) for grad in grads]
        return (y_out, grad_x, small[0], small[1], *grads, grad_wo.reshape(num_heads, head_dim, channels), small[2])

    specs = (act_spec, act_spec) + (rep_spec,) * 7
    return jax.shard_map(device_step, mesh=mesh, in_specs=specs, out_specs=specs, check_vma=False)
```

```python
import functools
import math
import jax
import jax.numpy as jnp
from jax import lax
from jax.experimental import pallas as pl
from jax.experimental.pallas import tpu as pltpu
from jax.sharding import PartitionSpec as P

LN_EPS = 1e-5
KEY_TILE = 256
Q_BLOCK = 256
FOLD = 16
AUG = 96
VMEM_BYTES = 67043328
BF = jnp.bfloat16
F32 = jnp.float32


def dot_nn(lhs, rhs):
    return lax.dot_general(lhs, rhs, (((1,), (0,)), ((), ())), preferred_element_type=F32)


def dot_nt(lhs, rhs):
    return lax.dot_general(lhs, rhs, (((1,), (1,)), ((), ())), preferred_element_type=F32)


def dot_tn(lhs, rhs):
    return lax.dot_general(lhs, rhs, (((0,), (0,)), ((), ())), preferred_element_type=F32)


def split_parts(value):
    high = value.astype(BF)
    rest = value - high.astype(F32)
    mid = rest.astype(BF)
    return high, mid, (rest - mid.astype(F32)).astype(BF)


def fold_rows(value, op):
    groups = value.reshape(value.shape[0] // FOLD, FOLD, value.shape[1])
    out = groups[0]
    for i in range(1, groups.shape[0]):
        out = op(out, groups[i])
    return out


MESH = pl.DeviceIdType.MESH
RING = 4
ROUNDS = 5
ROUND_ROWS = 256
STAGES = 8
PIECES = 4
SENDS = 16
CUTS = 4
ORDER = ('yy', 'yx', 'yy', 'yy', 'yx')


class Links:
    def __init__(self, depth):
        dp, self.x = lax.axis_index('dp'), lax.axis_index('cp')
        self.core = lax.rem(dp, 2)
        self.y = lax.rem(dp // 2, RING)
        self.z = dp // (2 * RING)
        self.depth = depth
        self.pos = {'x': self.x, 'y': self.y, 'z': self.z}
        self.size = {'x': RING, 'y': RING, 'z': depth}
        self.peer = self.at(core=1 - self.core)
        pair, odd = self.x // 2, lax.rem(self.x, 2)
        self.owners = [(pair, 2 * self.core + odd), (pair, 2 * self.core + 1 - odd)]
        self.workers = [(pair, 2 * self.core), (pair, 2 * self.core + 1)]

    def at(self, x=None, y=None, z=None, core=None):
        pick = lambda value, own: own if value is None else value
        return ((pick(z, self.z) * RING + pick(y, self.y)) * 2 + pick(core, self.core), pick(x, self.x))

    def step(self, axis, d):
        return self.at(**{axis: lax.rem(self.pos[axis] + d, self.size[axis])})

    def is_self(self, place):
        return jnp.logical_and(place[0] == self.core, place[1] == self.x)


def remote(source, target, send, recv, device):
    return pltpu.make_async_remote_copy(src_ref=source, dst_ref=target, send_sem=send, recv_sem=recv,
                                        device_id=device, device_id_type=MESH)


def wait_for(ref, sem):
    pltpu.make_async_copy(ref, ref, sem).wait()


class GradReduce:
    def __init__(self, links, dim, grad, out, results, bufs, sems):
        self.links, self.grad, self.both, self.out = links, grad, out, out.at[links.core]
        width = grad.shape[0] // 4
        self.pieces = [(0, width, results[0], 0)]
        self.pieces += [(width + (3 * head + k) * dim, dim, results[1 + k], head * dim) for head in range(width // dim) for k in range(3)]
        self.recv1, self.recv2, self.mid, self.z_src, self.z_recv, self.z_out = bufs
        self.rs_sems, self.ag_sems, self.z_sems, self.swap_sems, self.store_sems = sems

    def axes(self, rnd, unit):
        first = ORDER[rnd][unit]
        return first, ('x' if first == 'y' else 'y')

    def block(self, rnd, unit, phase):
        first = rnd * ROUND_ROWS + unit * 128
        if phase == 0:
            return first, 32
        return first + self.links.pos[self.axes(rnd, unit)[0]] * 32, 8

    def landing(self, rnd, unit, phase):
        return (self.recv1 if phase == 0 else self.recv2).at[rnd, unit]

    def wait_all(self, rnd, unit, phase, sems):
        whole = self.landing(rnd, unit, phase)
        every = remote(whole, whole, sems.at[0, rnd, unit, phase], sems.at[1, rnd, unit, phase], self.links.peer)
        every.wait_recv()
        every.wait_send()

    def source(self, rnd, unit, phase, owner):
        if phase == 0:
            first, rows = self.block(rnd, unit, 0)
            return self.grad.at[pl.ds(pl.multiple_of(first + owner * rows, 8), rows)]
        return self.mid.at[rnd, unit, pl.ds(pl.multiple_of(owner * 8, 8), 8)]

    def scatter_start(self, rnd, unit, phase):
        axis = self.axes(rnd, unit)[phase]
        for d in (2, 1, 3):
            owner = lax.rem(self.links.pos[axis] + d, RING)
            remote(self.source(rnd, unit, phase, owner), self.landing(rnd, unit, phase).at[d - 1],
                   self.rs_sems.at[0, rnd, unit, phase], self.rs_sems.at[1, rnd, unit, phase], self.links.step(axis, d)).start()

    def scatter_end(self, rnd, unit, phase):
        self.wait_all(rnd, unit, phase, self.rs_sems)
        landing = self.landing(rnd, unit, phase)
        mine = self.source(rnd, unit, phase, self.links.pos[self.axes(rnd, unit)[phase]])
        return (mine[...] + landing[0]) + (landing[1] + landing[2])

    def gather_start(self, rnd, unit, phase):
        axis = self.axes(rnd, unit)[phase]
        first, rows = self.block(rnd, unit, phase)
        part = self.out.at[pl.ds(pl.multiple_of(first + self.links.pos[axis] * rows, 8), rows)]
        for d in (2, 1, 3):
            remote(part, part, self.ag_sems.at[0, rnd, unit, phase], self.ag_sems.at[1, rnd, unit, phase],
                   self.links.step(axis, d)).start()

    def z_copies(self, rnd, way):
        links = self.links
        each = 16 // links.depth
        send, recv = self.z_sems.at[0, rnd, way], self.z_sems.at[1, rnd, way]
        mine = pl.ds(links.z * each, each)
        copies = []
        for d in range(1, links.depth):
            far = lax.rem(links.z + d, links.depth)
            if way == 0:
                source, target = self.z_src.at[rnd, pl.ds(far * each, each)], self.z_recv.at[rnd, d - 1]
            else:
                source = target = self.z_out.at[rnd, mine]
            copies.append(remote(source, target, send, recv, links.step('z', d)))
        return copies, mine

    def z_wait(self, rnd, way):
        if self.links.depth > 1:
            whole = self.z_recv.at[rnd]
            all_of = remote(whole, whole, self.z_sems.at[0, rnd, way], self.z_sems.at[1, rnd, way], self.links.step('z', 1))
            all_of.wait_recv()
            all_of.wait_send()

    def swap(self, rnd):
        part = self.out.at[pl.ds(rnd * ROUND_ROWS, ROUND_ROWS)]
        return remote(part, part, self.swap_sems.at[0, rnd], self.swap_sems.at[1, rnd], self.links.peer)

    def store(self, rnd):
        begin = rnd * ROUND_ROWS
        half = self.both.shape[1] // 4
        for first, rows, result, place in self.pieces:
            low, high = max(first, begin), min(first + rows, begin + ROUND_ROWS)
            for core in range(2):
                if low < high:
                    target = result.at[pl.ds(core * half + place + low - first, high - low)]
                    pltpu.make_async_copy(self.both.at[core, pl.ds(low, high - low)], target, self.store_sems.at[rnd]).start()

    def stored(self, rnd):
        wait_for(self.both.at[:, pl.ds(rnd * ROUND_ROWS, ROUND_ROWS)], self.store_sems.at[rnd])

    def stage(self, rnd, k):
        units = (0, 1)
        if k == 0:
            for u in units:
                self.scatter_start(rnd, u, 0)
        elif k == 1:
            for u in units:
                self.mid[rnd, u] = self.scatter_end(rnd, u, 0)
                self.scatter_start(rnd, u, 1)
        elif k == 2:
            for u in units:
                total = self.scatter_end(rnd, u, 1)
                for j in range(5):
                    self.z_src[rnd, u * 5 + j] = total[:, j * 128:(j + 1) * 128]
            self.z_src[rnd, pl.ds(10, 6)] = jnp.zeros((6, 8, 128), F32)
            for copy in self.z_copies(rnd, 0)[0]:
                copy.start()
        elif k == 3:
            self.z_wait(rnd, 0)
            copies, mine = self.z_copies(rnd, 1)
            total = self.z_src[rnd, mine]
            for d in range(self.links.depth - 1):
                total = total + self.z_recv[rnd, d]
            self.z_out[rnd, mine] = total
            for copy in copies:
                copy.start()
        elif k == 4:
            self.z_wait(rnd, 1)
            for u in units:
                first = self.block(rnd, u, 1)[0] + self.links.pos[self.axes(rnd, u)[1]] * 8
                for j in range(5):
                    self.out[pl.ds(pl.multiple_of(first, 8), 8), pl.ds(j * 128, 128)] = self.z_out[rnd, u * 5 + j]
                self.gather_start(rnd, u, 1)
        elif k == 5:
            for u in units:
                self.wait_all(rnd, u, 1, self.ag_sems)
                self.gather_start(rnd, u, 0)
        elif k == 6:
            for u in units:
                self.wait_all(rnd, u, 0, self.ag_sems)
            self.swap(rnd).start()
        else:
            self.swap(rnd).wait()
            self.store(rnd)


def layer_norm(x_ref, rows):
    x_f = x_ref[rows].astype(F32)
    centered = x_f - jnp.mean(x_f, axis=-1, keepdims=True)
    inv_std = lax.rsqrt(jnp.mean(centered * centered, axis=-1, keepdims=True) + LN_EPS)
    return centered * inv_std, inv_std


def padded(parts, rows):
    filled = [part.astype(F32) for part in parts]
    used = sum(part.shape[0] for part in filled)
    return jnp.concatenate(filled + [jnp.zeros((rows - used, filled[0].shape[1]), F32)], axis=0).astype(BF)


def block_body(dim, depth, x_hbm, dy_hbm, wq_hbm, wk_hbm, wv_hbm, wo_hbm, gamma_ref, beta_ref, bo_ref,
               y_ref, gx_ref, dq_ref, dk_ref, dv_ref, dwo_ref, small_ref,
               x_s, normed_s, dy_s, wt_s, wo_s, q_s, k_s, v_s, do_s, o_s, of_s, o_peer, lse_s, kf_s, vf_s, buf_a, buf_b, buf_c,
               kb_s, vb_s, dk_acc, dv_acc, grads, grads_peer, d_w, d_w_all, dx_s, y_s,
               recv1, recv2, mid, z_src, z_recv, z_out, small_s, small_recv,
               load_sems, in_send, in_recv, pass_send, pass_recv, o_sems, grad_sems, out_send, out_recv, small_sems,
               rs_sems, ag_sems, z_sems, swap_sems, store_sems):
    links = Links(depth)
    width, tokens = q_s.shape
    heads, tiles = width // dim, tokens // KEY_TILE
    own, band = tokens // 2, tokens // 4
    scale = dim ** -0.5
    log2_scale = scale * math.log2(math.e)
    fwd_group, bwd_group = 4, 4
    fwd_steps, bwd_steps = tiles // fwd_group, tiles // bwd_group
    zero = jnp.minimum(links.x, 0)
    gamma, beta, bias = (ref[...].reshape(1, ref.shape[0]) for ref in (gamma_ref, beta_ref, bo_ref))
    odd = lax.rem(links.x, 2)
    reduce = GradReduce(links, dim, d_w, d_w_all, (dwo_ref, dq_ref, dk_ref, dv_ref), (recv1, recv2, mid, z_src, z_recv, z_out),
                        (rs_sems, ag_sems, z_sems, swap_sems, store_sems))
    end = heads * bwd_steps + 1
    plan = {}
    for rnd in range(ROUNDS):
        at = rnd * bwd_steps + 1 if rnd else 0
        for k in range(STAGES):
            at += 0 if k == 0 else 2 if k in (1, 5) and rnd < ROUNDS - 1 else 1
            plan.setdefault(at, []).insert(0, (rnd, k))
    slots = max(plan) + 1 - end

    def tile_rows(tile, base=None):
        return pl.ds(tile * KEY_TILE if base is None else pl.multiple_of(base + tile * KEY_TILE, KEY_TILE), KEY_TILE)

    def head_rows(head, rows=dim):
        return pl.ds(pl.multiple_of(head * rows, 16), rows)

    def q_cols(index):
        return pl.ds(pl.multiple_of(index * Q_BLOCK, Q_BLOCK), Q_BLOCK)

    def my_half(side):
        return pl.ds(pl.multiple_of((links.core if side == 0 else 1 - links.core) * width, 16), width)

    loads = [pltpu.make_async_copy(w_hbm.at[my_half(side)], wt_s.at[side, pl.ds(k * width, width)], load_sems.at[side, k])
             for side in range(2) for k, w_hbm in enumerate((wq_hbm, wk_hbm, wv_hbm))]
    loads += [pltpu.make_async_copy(wo_hbm.at[my_half(side)], wo_s.at[side], load_sems.at[side, 3]) for side in range(2)]

    def maybe_far(place, source, target, send, recv, start):
        core, x = place
        here = links.is_self(place)
        far = remote(source, target, send, recv, links.at(core=core, x=x))
        near = pltpu.make_async_copy(source, target, recv)

        @pl.when(jnp.logical_not(here))
        def _():
            far.start() if start else far.wait_send()

        if start:
            @pl.when(here)
            def _():
                near.start()

    piece = band // PIECES

    def deliver(which, m, c, start):
        slot = lax.rem(links.x + m, 2)
        source = (dy_hbm if which else x_hbm).at[m, pl.ds(c * piece, piece)]
        target = (dy_s if which else x_s).at[pl.ds(pl.multiple_of(slot * band + c * piece, 16), piece)]
        maybe_far(links.workers[m], source, target, in_send.at[which, m, c], in_recv.at[which, slot, c], start)

    def hand_over(which, slot, c):
        rows = dy_s if which else x_s
        first = slot * band + c * piece
        return remote(rows.at[pl.ds(first, piece)], rows.at[pl.ds(own + first, piece)],
                      pass_send.at[which, slot, c], pass_recv.at[which, slot, c], links.peer)

    def arrive(which, slot, c):
        with jax.named_scope(f'arrive{which}{slot}{c}'):
            wait_for((dy_s if which else x_s).at[pl.ds(slot * band + c * piece, piece)], in_recv.at[which, slot, c])
        hand_over(which, slot, c).start()

    def swap_out(head):
        rows = head_rows(head)
        return remote(o_s.at[rows, pl.ds(own, own)], o_peer.at[rows], o_sems.at[0, head], o_sems.at[1, head], links.peer)

    def swap_grads(head):
        rows = head_rows(head)
        return remote(grads.at[:, rows, pl.ds(own, own)], grads_peer.at[:, rows], grad_sems.at[0, head], grad_sems.at[1, head],
                      links.peer)

    part = band // 2
    portion = own // SENDS

    def send_home(which, i, start):
        cut = SENDS // 2
        second, inner = i // cut, lax.rem(i, cut)
        source = (dx_s if which else y_s).at[pl.ds(pl.multiple_of(i * portion, 16), portion)]
        target = (gx_ref if which else y_ref).at[odd, pl.ds(pl.multiple_of(inner * portion, 16), portion)]
        (core, x0), (_, x1) = links.owners
        maybe_far((core, jnp.where(second == 0, x0, x1)), source, target, out_send.at[which, i],
                  out_recv.at[which, odd, inner], start)

    def received_home(which):
        for m in range(2):
            for i in range(SENDS // 2):
                wait_for((gx_ref if which else y_ref).at[m, pl.ds(i * portion, portion)], out_recv.at[which, m, i])

    barrier = pltpu.get_barrier_semaphore()
    fixed = [links.peer]
    fixed += [links.step(axis, d) for axis in ('x', 'y') for d in range(1, RING)]
    fixed += [links.step('z', d) for d in range(1, depth)]
    for device in fixed:
        pl.semaphore_signal(barrier, inc=1, device_id=device, device_id_type=MESH)
    count = len(fixed)
    for place in links.owners + links.workers:
        other = jnp.logical_not(links.is_self(place))
        count = count + other.astype(jnp.int32)

        @pl.when(other)
        def _():
            pl.semaphore_signal(barrier, inc=1, device_id=links.at(core=place[0], x=place[1]), device_id_type=MESH)
    for load in loads:
        load.start()
    with jax.named_scope('barrier'):
        pl.semaphore_wait(barrier, count)
    for c in range(PIECES):
        for m in range(2):
            deliver(0, m, c, True)
    for load in loads:
        load.wait()

    def normalize(first):
        rows = pl.ds(first, piece)
        normed_s[rows] = (layer_norm(x_s, rows)[0] * gamma + beta).astype(BF)

    for c in range(PIECES + 1):
        if c < PIECES:
            for slot in range(2):
                arrive(0, slot, c)
            if c == PIECES - 1:
                for i in range(PIECES):
                    for m in range(2):
                        deliver(1, m, i, True)
            for slot in range(2):
                normalize(slot * band + c * piece)
        if c:
            for slot in range(2):
                with jax.named_scope(f'handed{slot}{c}'):
                    hand_over(0, slot, c - 1).wait_recv()
                normalize(own + slot * band + (c - 1) * piece)
            if c % 2 == 0:
                for b in range(4):
                    cols = pl.ds(b * band + (c - 2) * piece, 2 * piece)
                    normed = normed_s[cols]
                    for k, out in enumerate((q_s, k_s, v_s)):
                        out[:, cols] = dot_nt(wt_s[0, pl.ds(k * width, width)], normed).astype(BF)

    def forward_step(now, carry):
        head, step = now // fwd_steps, lax.rem(now, fwd_steps)
        rows = head_rows(head)
        for c in range(PIECES):
            @pl.when(now == (c + 1) * heads * fwd_steps // (PIECES + 1))
            def _():
                for slot in range(2):
                    arrive(1, slot, c)

        @pl.when(step == 0)
        def _():
            k_t = k_s[rows]
            kf_s[...] = jnp.concatenate([k_t, k_t, k_t], axis=0).T
            vf_s[0:dim] = v_s[rows]
            vf_s[dim:] = padded([jnp.ones((1, tokens), F32)], AUG - dim)

        bufs = (buf_a, buf_b, buf_c)
        total, lag = tiles * fwd_group, tiles + 1
        query, high, top, probs, out = {}, {}, {}, {}, {}
        for g in range(total + lag + 2):
            if g < total:
                i, t = divmod(g, tiles)
                if t == 0:
                    query[i] = jnp.concatenate(split_parts(q_s[rows, q_cols(step * fwd_group + i)].astype(F32) * log2_scale), axis=0)
                scores = dot_nn(kf_s[tile_rows(t)], query[i])
                bufs[i % 3][tile_rows(t)] = scores
                folded = fold_rows(scores, jnp.maximum)
                high[i] = folded if t == 0 else jnp.maximum(high[i], folded)
                if t == tiles - 1:
                    top[i] = jnp.max(high[i], axis=0, keepdims=True)
            if lag <= g < total + lag:
                i, t = divmod(g - lag, tiles)
                probs[g - lag] = jnp.exp2(bufs[i % 3][tile_rows(t, zero)] - top[i]).astype(BF)
            if g >= lag + 2:
                i, t = divmod(g - lag - 2, tiles)
                product = dot_nn(vf_s[:, tile_rows(t)], probs[g - lag - 2])
                out[i] = product if t == 0 else out[i] + product
                if t == tiles - 1:
                    cols = q_cols(step * fwd_group + i)
                    denom = out[i][dim:dim + 1]
                    value = out[i][:dim] * (1.0 / denom)
                    o_s[rows, cols] = value.astype(BF)
                    of_s[rows, cols] = value
                    lse = (top[i] + jnp.log2(denom)) * (1.0 / log2_scale)
                    lse_s[head_rows(head, 16), cols] = padded(split_parts(lse), 16)

        @pl.when(step == fwd_steps - 1)
        def _():
            swap_out(head).start()

        return carry

    lax.fori_loop(0, heads * fwd_steps, forward_step, 0)
    with jax.named_scope('dyhanded'):
        for c in range(PIECES):
            for slot in range(2):
                hand_over(1, slot, c).wait_recv()
    d_w[pl.ds(0, width)] = dot_nn(o_s[...], dy_s[...])
    for rnd, k in plan[0]:
        reduce.stage(rnd, k)
    with jax.named_scope('oswap'):
        for head in range(heads):
            swap_out(head).wait()
    for i in range(4):
        toks = pl.ds(i * part, part)
        product = dot_tn(o_s[:, toks], wo_s[0]) + dot_tn(o_peer[:, toks], wo_s[1])
        y_s[toks] = (x_s[toks].astype(F32) + product + bias).astype(BF)
    for i in range(tiles):
        cols = pl.ds(i * KEY_TILE, KEY_TILE)
        do_s[:, cols] = dot_nt(wo_s[0], dy_s[cols]).astype(BF)
    with jax.named_scope('middlesends'):
        for which in range(2):
            for c in range(PIECES):
                for m in range(2):
                    deliver(which, m, c, False)
                    hand_over(which, m, c).wait_send()

    def backward_step(now, carry):
        head, step = now // bwd_steps, lax.rem(now, bwd_steps)
        rows = head_rows(head)
        for at in range(end - 1):
            todo = plan.get(at + 1)
            if todo:
                @pl.when(now == at)
                def _():
                    with jax.named_scope(f'step{at}'):
                        for rnd, k in todo:
                            reduce.stage(rnd, k)
        share = SENDS // (heads * bwd_steps)
        for i in range(share):
            send_home(0, now * share + i, True)

        @pl.when(step == 0)
        def _():
            minus = padded([jnp.full((3, tokens), -1.0, F32)], AUG - dim)
            kb_s[...] = jnp.concatenate([k_s[rows], minus], axis=0).T
            vb_s[...] = jnp.concatenate([v_s[rows], minus], axis=0).T
            dk_acc[...] = jnp.zeros_like(dk_acc)
            dv_acc[...] = jnp.zeros_like(dv_acc)

        total = tiles * bwd_group
        ops, probs, d_scores, dq = {}, {}, {}, {}
        for g in range(total + 2):
            if g < total:
                i, t = divmod(g, tiles)
                if t == 0:
                    cols = q_cols(step * bwd_group + i)
                    q_t, do_t = q_s[rows, cols], do_s[rows, cols]
                    delta = jnp.sum(of_s[rows, cols] * do_t.astype(F32), axis=0, keepdims=True)
                    ops[i] = (cols, q_t, do_t, jnp.concatenate([q_t, lse_s[head_rows(head, 16), cols]], axis=0),
                              jnp.concatenate([do_t, padded(split_parts(delta), 16)], axis=0))
                scores = dot_nn(kb_s[tile_rows(t)], ops[i][3])
                d_probs = dot_nn(vb_s[tile_rows(t)], ops[i][4])
                prob = jnp.exp2(scores * log2_scale)
                probs[g] = prob.astype(BF)
                d_scores[g] = (prob * d_probs).astype(BF)
            if g >= 2:
                i, t = divmod(g - 2, tiles)
                cols, q_t, do_t = ops[i][:3]
                dv_acc[:, tile_rows(t)] += dot_nt(do_t, probs[g - 2])
                product = dot_nn(k_s[rows, tile_rows(t)], d_scores[g - 2])
                dq[i] = product if t == 0 else dq[i] + product
                if t == tiles - 1:
                    grads[0, rows, cols] = (dq[i] * scale).astype(BF)
                dk_acc[:, tile_rows(t)] += dot_nt(q_t, d_scores[g - 2])

        @pl.when(step == bwd_steps - 1)
        def _():
            grads[1, rows] = (dk_acc[...] * scale).astype(BF)
            grads[2, rows] = dv_acc[...].astype(BF)
            swap_grads(head).start()
            stacked = jnp.concatenate([grads[0, rows], grads[1, rows], grads[2, rows]], axis=0)
            d_w[pl.ds(pl.multiple_of(width + head * (3 * dim), 8), 3 * dim)] = dot_nn(stacked, normed_s[...])

        return carry

    lax.fori_loop(0, heads * bwd_steps, backward_step, 0)

    def tail(slot):
        for rnd, k in plan.get(end + slot, ()):
            with jax.named_scope(f'tail{slot}r{rnd}k{k}'):
                reduce.stage(rnd, k)

    tail(0)
    with jax.named_scope('gradswap'):
        for head in range(heads):
            swap_grads(head).wait()
    sums = [jnp.zeros((1, 640), F32)] * 3
    for i in range(4):
        toks = pl.ds(i * part, part)
        mine = jnp.concatenate([grads[k, :, toks] for k in range(3)], axis=0)
        theirs = jnp.concatenate([grads_peer[k, :, toks] for k in range(3)], axis=0)
        d_normed = (dot_tn(mine, wt_s[0]) + dot_tn(theirs, wt_s[1])).astype(BF).astype(F32)
        x_hat, inv_std = layer_norm(x_s, toks)
        d_hat = d_normed * gamma
        mean_one = jnp.mean(d_hat, axis=-1, keepdims=True)
        mean_two = jnp.mean(d_hat * x_hat, axis=-1, keepdims=True)
        dy_f = dy_s[toks].astype(F32)
        dx_s[toks] = (dy_f + inv_std * (d_hat - mean_one - x_hat * mean_two)).astype(BF)
        for k, term in enumerate((d_normed * x_hat, d_normed, dy_f)):
            sums[k] = sums[k] + jnp.sum(term, axis=0, keepdims=True)

    for k in range(3):
        for j in range(5):
            small_s[0, pl.ds(k * 5 + j, 1)] = sums[k][:, j * 128:(j + 1) * 128]
    small_s[0, pl.ds(15, 1)] = jnp.zeros((1, 128), F32)
    small_copy = pltpu.make_async_copy(small_s.at[0], small_ref, load_sems.at[0, 0])
    first, waiting = 0, None
    for hop, axis in enumerate(('z', 'y', 'core', 'x', '')):
        if waiting:
            acc = small_s[hop - 1]
            with jax.named_scope(f'small{hop}'):
                for copy in waiting:
                    copy.wait_recv()
            for d in range(len(waiting)):
                acc = acc + small_recv[first + d]
            for copy in waiting:
                copy.wait_send()
            if axis:
                small_s[hop] = acc
            else:
                small_s[0] = acc
                small_copy.start()
            first += len(waiting)
        elif hop:
            small_s[hop] = small_s[hop - 1]
        if axis:
            far = [links.peer] if axis == 'core' else [links.step(axis, d) for d in range(1, links.size[axis])]
            waiting = [remote(small_s.at[hop], small_recv.at[first + d], small_sems.at[0, first + d], small_sems.at[1, first + d],
                              device) for d, device in enumerate(far)]
            for copy in waiting:
                copy.start()
            tail(1 + hop)
            if hop == 0:
                for i in range(SENDS):
                    send_home(1, i, True)
    for slot in range(5, slots):
        tail(slot)
    with jax.named_scope('home'):
        for which in range(2):
            for i in range(SENDS):
                send_home(which, i, False)
            received_home(which)
    with jax.named_scope('stored'):
        for rnd in range(ROUNDS):
            reduce.stored(rnd)
    small_copy.wait()


def attention_block(x_in, grad_y, weights, vectors, dim, depth):
    rows, channels = x_in.shape[1:]
    tokens, own = 4 * rows, 2 * rows
    width = weights[0].shape[0] // 2
    heads = width // dim
    total = 4 * width
    half = lambda *shape: pltpu.VMEM(shape, BF)
    full = lambda *shape: pltpu.VMEM(shape, F32)
    dma = lambda *shape: pltpu.SemaphoreType.DMA(shape)
    anywhere = pl.BlockSpec(memory_space=pl.ANY)
    in_vmem = pl.BlockSpec(memory_space=pltpu.VMEM)
    far = max(depth - 1, 1)
    return pl.pallas_call(
        functools.partial(block_body, dim, depth),
        in_specs=[anywhere] * 6 + [in_vmem] * 3,
        out_specs=[anywhere] * 7,
        out_shape=[jax.ShapeDtypeStruct(x_in.shape, BF)] * 2
        + [jax.ShapeDtypeStruct(weights[0].shape, F32)] * 4 + [jax.ShapeDtypeStruct((16, 128), F32)],
        scratch_shapes=[half(tokens, channels)] * 3 + [half(2, 3 * width, channels), half(2, width, channels)]
        + [half(width, tokens)] * 5 + [full(width, tokens), half(width, own), half(16 * heads, tokens),
                                       half(tokens, 3 * dim), half(AUG, tokens)]
        + [full(tokens, Q_BLOCK)] * 3 + [half(tokens, AUG)] * 2 + [full(dim, tokens)] * 2
        + [half(3, width, tokens), half(3, width, own), full(total, channels), full(2, total, channels)]
        + [half(own, channels)] * 2
        + [full(ROUNDS, 2, 3, 32, channels), full(ROUNDS, 2, 3, 8, channels), full(ROUNDS, 2, 32, channels), full(ROUNDS, 16, 8, 128),
           full(ROUNDS, far, 16 // depth, 8, 128), full(ROUNDS, 16, 8, 128), full(4, 16, 128), full(7 + far, 16, 128),
           dma(2, 4)] + [dma(2, 2, PIECES)] * 4 + [dma(2, heads)] * 2
        + [dma(2, SENDS), dma(2, 2, SENDS // 2), dma(2, 7 + far)] + [dma(2, ROUNDS, 2, 2)] * 2 + [dma(2, ROUNDS, 2), dma(2, ROUNDS), dma(ROUNDS)],
        compiler_params=pltpu.CompilerParams(collective_id=0, has_side_effects=True, vmem_limit_bytes=VMEM_BYTES),
        name='attention_block',
    )(x_in, grad_y, *weights, *vectors)


def settle_body(count, *refs):
    sources, targets, bufs, sems = refs[:count], refs[count:2 * count], refs[2 * count:3 * count], refs[3 * count]
    cuts = []
    for i, (source, target, buf) in enumerate(zip(sources, targets, bufs)):
        rows = source.shape[0] // CUTS
        for c in range(CUTS):
            part = pl.ds(c * rows, rows)
            cuts.append((pltpu.make_async_copy(source.at[part], buf.at[part], sems.at[0, i, c]),
                         pltpu.make_async_copy(buf.at[part], target.at[part], sems.at[1, i, c])))
    for read, _ in cuts:
        read.start()
    for read, write in cuts:
        read.wait()
        write.start()
    for _, write in cuts:
        write.wait()


def settle(arrays):
    anywhere = pl.BlockSpec(memory_space=pl.ANY)
    count = len(arrays)
    return pl.pallas_call(
        functools.partial(settle_body, count),
        in_specs=[anywhere] * count, out_specs=[anywhere] * count,
        out_shape=[jax.ShapeDtypeStruct(a.shape, a.dtype) for a in arrays],
        scratch_shapes=[pltpu.VMEM(a.shape, a.dtype) for a in arrays] + [pltpu.SemaphoreType.DMA((2, count, CUTS))],
        compiler_params=pltpu.CompilerParams(vmem_limit_bytes=VMEM_BYTES),
        name='settle',
    )(*arrays)


def solution(mesh):
    depth = mesh.shape['dp'] // (2 * RING)
    act_spec, rep_spec = P('dp', 'cp', None), P()

    def device_step(x_in, grad_y, ln_gamma, ln_beta, w_q, w_k, w_v, w_o, b_o):
        channels, num_heads, head_dim = w_q.shape
        flat = (num_heads * head_dim, channels)
        weights = [jnp.transpose(w, (1, 2, 0)).reshape(flat) for w in (w_q, w_k, w_v)] + [w_o.reshape(flat)]
        y_out, grad_x, *grads, grad_wo, small = attention_block(x_in, grad_y, weights, (ln_gamma, ln_beta, b_o), head_dim, depth)
        rows = (2 * y_out.shape[1], channels)
        moved = settle([y_out.reshape(rows), grad_x.reshape(rows), *grads, grad_wo])
        y_out, grad_x = (a.reshape(x_in.shape) for a in moved[:2])
        grads, grad_wo = moved[2:5], moved[5]
        small = small[:15].reshape(3, channels)
        grads = [jnp.transpose(grad.reshape(num_heads, head_dim, channels), (2, 0, 1)) for grad in grads]
        return (y_out, grad_x, small[0], small[1], *grads, grad_wo.reshape(num_heads, head_dim, channels), small[2])

    specs = (act_spec, act_spec) + (rep_spec,) * 7
    return jax.shard_map(device_step, mesh=mesh, in_specs=specs, out_specs=specs, check_vma=False)
```

```python
import functools
import math
import jax
import jax.numpy as jnp
from jax import lax
from jax.experimental import pallas as pl
from jax.experimental.pallas import tpu as pltpu
from jax.sharding import PartitionSpec as P

LN_EPS = 1e-5
KEY_TILE = 256
Q_BLOCK = 256
FOLD = 16
AUG = 96
VMEM_BYTES = 67043328
BF = jnp.bfloat16
F32 = jnp.float32


def dot_nn(lhs, rhs):
    return lax.dot_general(lhs, rhs, (((1,), (0,)), ((), ())), preferred_element_type=F32)


def dot_nt(lhs, rhs):
    return lax.dot_general(lhs, rhs, (((1,), (1,)), ((), ())), preferred_element_type=F32)


def dot_tn(lhs, rhs):
    return lax.dot_general(lhs, rhs, (((0,), (0,)), ((), ())), preferred_element_type=F32)


def split_parts(value):
    high = value.astype(BF)
    rest = value - high.astype(F32)
    mid = rest.astype(BF)
    return high, mid, (rest - mid.astype(F32)).astype(BF)


def fold_rows(value, op):
    groups = value.reshape(value.shape[0] // FOLD, FOLD, value.shape[1])
    out = groups[0]
    for i in range(1, groups.shape[0]):
        out = op(out, groups[i])
    return out


MESH = pl.DeviceIdType.MESH
RING = 4
ROUNDS = 5
ROUND_ROWS = 256
STAGES = 8
SPARE = ((0, 1), (1, 1), (2, 1), (3, 1), (0, 6), (1, 6), (2, 6), (3, 5))
PIECES = 4
SENDS = 16
CUTS = 4
ORDER = ('yx', 'yx', 'yy', 'yx', 'yx')


class Links:
    def __init__(self, depth):
        dp, self.x = lax.axis_index('dp'), lax.axis_index('cp')
        self.core = lax.rem(dp, 2)
        self.y = lax.rem(dp // 2, RING)
        self.z = dp // (2 * RING)
        self.depth = depth
        self.pos = {'x': self.x, 'y': self.y, 'z': self.z}
        self.size = {'x': RING, 'y': RING, 'z': depth}
        self.peer = self.at(core=1 - self.core)
        pair, odd = self.x // 2, lax.rem(self.x, 2)
        self.owners = [(pair, 2 * self.core + odd), (pair, 2 * self.core + 1 - odd)]
        self.workers = [(pair, 2 * self.core), (pair, 2 * self.core + 1)]

    def at(self, x=None, y=None, z=None, core=None):
        pick = lambda value, own: own if value is None else value
        return ((pick(z, self.z) * RING + pick(y, self.y)) * 2 + pick(core, self.core), pick(x, self.x))

    def step(self, axis, d):
        return self.at(**{axis: lax.rem(self.pos[axis] + d, self.size[axis])})

    def is_self(self, place):
        return jnp.logical_and(place[0] == self.core, place[1] == self.x)


def remote(source, target, send, recv, device):
    return pltpu.make_async_remote_copy(src_ref=source, dst_ref=target, send_sem=send, recv_sem=recv,
                                        device_id=device, device_id_type=MESH)


def wait_for(ref, sem):
    pltpu.make_async_copy(ref, ref, sem).wait()


class GradReduce:
    def __init__(self, links, dim, grad, out, results, bufs, sems):
        self.links, self.grad, self.both, self.out = links, grad, out, out.at[links.core]
        width = grad.shape[0] // 4
        self.pieces = [(0, width, results[0], 0)]
        self.pieces += [(width + (3 * head + k) * dim, dim, results[1 + k], head * dim) for head in range(width // dim) for k in range(3)]
        self.recv1, self.recv2, self.mid, self.z_src, self.z_recv, self.z_out = bufs
        self.rs_sems, self.ag_sems, self.z_sems, self.swap_sems, self.store_sems = sems

    def axes(self, rnd, unit):
        first = ORDER[rnd][unit]
        return first, ('x' if first == 'y' else 'y')

    def block(self, rnd, unit, phase):
        first = rnd * ROUND_ROWS + unit * 128
        if phase == 0:
            return first, 32
        return first + self.links.pos[self.axes(rnd, unit)[0]] * 32, 8

    def landing(self, rnd, unit, phase):
        return (self.recv1 if phase == 0 else self.recv2).at[rnd, unit]

    def wait_all(self, rnd, unit, phase, sems):
        whole = self.landing(rnd, unit, phase)
        every = remote(whole, whole, sems.at[0, rnd, unit, phase], sems.at[1, rnd, unit, phase], self.links.peer)
        every.wait_recv()
        every.wait_send()

    def source(self, rnd, unit, phase, owner):
        if phase == 0:
            first, rows = self.block(rnd, unit, 0)
            return self.grad.at[pl.ds(pl.multiple_of(first + owner * rows, 8), rows)]
        return self.mid.at[rnd, unit, pl.ds(pl.multiple_of(owner * 8, 8), 8)]

    def scatter_start(self, rnd, unit, phase):
        axis = self.axes(rnd, unit)[phase]
        for d in (2, 1, 3):
            owner = lax.rem(self.links.pos[axis] + d, RING)
            remote(self.source(rnd, unit, phase, owner), self.landing(rnd, unit, phase).at[d - 1],
                   self.rs_sems.at[0, rnd, unit, phase], self.rs_sems.at[1, rnd, unit, phase], self.links.step(axis, d)).start()

    def scatter_end(self, rnd, unit, phase):
        self.wait_all(rnd, unit, phase, self.rs_sems)
        landing = self.landing(rnd, unit, phase)
        mine = self.source(rnd, unit, phase, self.links.pos[self.axes(rnd, unit)[phase]])
        return (mine[...] + landing[0]) + (landing[1] + landing[2])

    def gather_start(self, rnd, unit, phase):
        axis = self.axes(rnd, unit)[phase]
        first, rows = self.block(rnd, unit, phase)
        part = self.out.at[pl.ds(pl.multiple_of(first + self.links.pos[axis] * rows, 8), rows)]
        for d in (2, 1, 3):
            remote(part, part, self.ag_sems.at[0, rnd, unit, phase], self.ag_sems.at[1, rnd, unit, phase],
                   self.links.step(axis, d)).start()

    def z_copies(self, rnd, way):
        links = self.links
        each = 16 // links.depth
        send, recv = self.z_sems.at[0, rnd, way], self.z_sems.at[1, rnd, way]
        mine = pl.ds(links.z * each, each)
        copies = []
        for d in range(1, links.depth):
            far = lax.rem(links.z + d, links.depth)
            if way == 0:
                source, target = self.z_src.at[rnd, pl.ds(far * each, each)], self.z_recv.at[rnd, d - 1]
            else:
                source = target = self.z_out.at[rnd, mine]
            copies.append(remote(source, target, send, recv, links.step('z', d)))
        return copies, mine

    def z_wait(self, rnd, way):
        if self.links.depth > 1:
            whole = self.z_recv.at[rnd]
            all_of = remote(whole, whole, self.z_sems.at[0, rnd, way], self.z_sems.at[1, rnd, way], self.links.step('z', 1))
            all_of.wait_recv()
            all_of.wait_send()

    def swap(self, rnd):
        part = self.out.at[pl.ds(rnd * ROUND_ROWS, ROUND_ROWS)]
        return remote(part, part, self.swap_sems.at[0, rnd], self.swap_sems.at[1, rnd], self.links.peer)

    def store(self, rnd):
        begin = rnd * ROUND_ROWS
        half = self.both.shape[1] // 4
        for first, rows, result, place in self.pieces:
            low, high = max(first, begin), min(first + rows, begin + ROUND_ROWS)
            for core in range(2):
                if low < high:
                    target = result.at[pl.ds(core * half + place + low - first, high - low)]
                    pltpu.make_async_copy(self.both.at[core, pl.ds(low, high - low)], target, self.store_sems.at[rnd]).start()

    def stored(self, rnd):
        wait_for(self.both.at[:, pl.ds(rnd * ROUND_ROWS, ROUND_ROWS)], self.store_sems.at[rnd])

    def stage(self, rnd, k):
        units = (0, 1)
        if k == 0:
            for u in units:
                self.scatter_start(rnd, u, 0)
        elif k == 1:
            for u in units:
                self.mid[rnd, u] = self.scatter_end(rnd, u, 0)
                self.scatter_start(rnd, u, 1)
        elif k == 2:
            for u in units:
                total = self.scatter_end(rnd, u, 1)
                for j in range(5):
                    self.z_src[rnd, u * 5 + j] = total[:, j * 128:(j + 1) * 128]
            self.z_src[rnd, pl.ds(10, 6)] = jnp.zeros((6, 8, 128), F32)
            for copy in self.z_copies(rnd, 0)[0]:
                copy.start()
        elif k == 3:
            self.z_wait(rnd, 0)
            copies, mine = self.z_copies(rnd, 1)
            total = self.z_src[rnd, mine]
            for d in range(self.links.depth - 1):
                total = total + self.z_recv[rnd, d]
            self.z_out[rnd, mine] = total
            for copy in copies:
                copy.start()
        elif k == 4:
            self.z_wait(rnd, 1)
            for u in units:
                first = self.block(rnd, u, 1)[0] + self.links.pos[self.axes(rnd, u)[1]] * 8
                for j in range(5):
                    self.out[pl.ds(pl.multiple_of(first, 8), 8), pl.ds(j * 128, 128)] = self.z_out[rnd, u * 5 + j]
                self.gather_start(rnd, u, 1)
        elif k == 5:
            for u in units:
                self.wait_all(rnd, u, 1, self.ag_sems)
                self.gather_start(rnd, u, 0)
        elif k == 6:
            for u in units:
                self.wait_all(rnd, u, 0, self.ag_sems)
            self.swap(rnd).start()
        else:
            self.swap(rnd).wait()
            self.store(rnd)


def layer_norm(x_ref, rows):
    x_f = x_ref[rows].astype(F32)
    centered = x_f - jnp.mean(x_f, axis=-1, keepdims=True)
    inv_std = lax.rsqrt(jnp.mean(centered * centered, axis=-1, keepdims=True) + LN_EPS)
    return centered * inv_std, inv_std


def padded(parts, rows):
    filled = [part.astype(F32) for part in parts]
    used = sum(part.shape[0] for part in filled)
    return jnp.concatenate(filled + [jnp.zeros((rows - used, filled[0].shape[1]), F32)], axis=0).astype(BF)


def block_body(dim, depth, x_hbm, dy_hbm, wq_hbm, wk_hbm, wv_hbm, wo_hbm, gamma_ref, beta_ref, bo_ref,
               y_ref, gx_ref, dq_ref, dk_ref, dv_ref, dwo_ref, small_ref,
               x_s, normed_s, dy_s, wt_s, wo_s, q_s, k_s, v_s, do_s, o_s, of_s, o_peer, lse_s, kf_s, vf_s, buf_a, buf_b, buf_c,
               kb_s, vb_s, dk_acc, dv_acc, grads, grads_peer, d_w, d_w_all, dx_s, y_s,
               recv1, recv2, mid, z_src, z_recv, z_out, small_s, small_recv,
               load_sems, in_send, in_recv, pass_send, pass_recv, o_sems, grad_sems, out_send, out_recv, small_sems,
               rs_sems, ag_sems, z_sems, swap_sems, store_sems):
    links = Links(depth)
    width, tokens = q_s.shape
    heads, tiles = width // dim, tokens // KEY_TILE
    own, band = tokens // 2, tokens // 4
    scale = dim ** -0.5
    log2_scale = scale * math.log2(math.e)
    fwd_group, bwd_group = 4, 4
    fwd_steps, bwd_steps = tiles // fwd_group, tiles // bwd_group
    zero = jnp.minimum(links.x, 0)
    gamma, beta, bias = (ref[...].reshape(1, ref.shape[0]) for ref in (gamma_ref, beta_ref, bo_ref))
    odd = lax.rem(links.x, 2)
    reduce = GradReduce(links, dim, d_w, d_w_all, (dwo_ref, dq_ref, dk_ref, dv_ref), (recv1, recv2, mid, z_src, z_recv, z_out),
                        (rs_sems, ag_sems, z_sems, swap_sems, store_sems))
    end = heads * bwd_steps + 1
    plan = {}
    for rnd in range(ROUNDS):
        at = rnd * bwd_steps + 1 if rnd else 0
        for k in range(STAGES):
            at += min(k, 1) + ((rnd, k) in SPARE)
            plan.setdefault(at, []).append((rnd, k))
    for at in plan:
        plan[at].sort(key=lambda item: (item[1] in (0, 5) and item[0] < ROUNDS - 1, -item[0]))
    slots = max(plan) + 1 - end

    def tile_rows(tile, base=None):
        return pl.ds(tile * KEY_TILE if base is None else pl.multiple_of(base + tile * KEY_TILE, KEY_TILE), KEY_TILE)

    def head_rows(head, rows=dim):
        return pl.ds(pl.multiple_of(head * rows, 16), rows)

    def q_cols(index):
        return pl.ds(pl.multiple_of(index * Q_BLOCK, Q_BLOCK), Q_BLOCK)

    def my_half(side):
        return pl.ds(pl.multiple_of((links.core if side == 0 else 1 - links.core) * width, 16), width)

    loads = [pltpu.make_async_copy(w_hbm.at[my_half(side)], wt_s.at[side, pl.ds(k * width, width)], load_sems.at[side, k])
             for side in range(2) for k, w_hbm in enumerate((wq_hbm, wk_hbm, wv_hbm))]
    loads += [pltpu.make_async_copy(wo_hbm.at[my_half(side)], wo_s.at[side], load_sems.at[side, 3]) for side in range(2)]

    def maybe_far(place, source, target, send, recv):
        core, x = place
        here = links.is_self(place)
        far = remote(source, target, send, recv, links.at(core=core, x=x))
        near = pltpu.make_async_copy(source, target, recv)

        @pl.when(jnp.logical_not(here))
        def _():
            far.start()

        @pl.when(here)
        def _():
            near.start()

    def all_left(ref, sem):
        rows = ref.shape[0]
        halved = links.x // 2 == links.core

        @pl.when(jnp.logical_not(halved))
        def _():
            wait_for(ref, sem)

        @pl.when(halved)
        def _():
            wait_for(ref.at[pl.ds(0, rows // 2)], sem)

    piece = band // PIECES

    def deliver(which, m, c):
        slot = lax.rem(links.x + m, 2)
        source = (dy_hbm if which else x_hbm).at[m, pl.ds(c * piece, piece)]
        target = (dy_s if which else x_s).at[pl.ds(pl.multiple_of(slot * band + c * piece, 16), piece)]
        maybe_far(links.workers[m], source, target, in_send.at[which], in_recv.at[which, slot, c])

    def hand_over(which, slot, c):
        rows = dy_s if which else x_s
        first = slot * band + c * piece
        return remote(rows.at[pl.ds(first, piece)], rows.at[pl.ds(own + first, piece)],
                      pass_send.at[which], pass_recv.at[which, slot, c], links.peer)

    def arrive(which, slot, c):
        with jax.named_scope(f'arrive{which}{slot}{c}'):
            wait_for((dy_s if which else x_s).at[pl.ds(slot * band + c * piece, piece)], in_recv.at[which, slot, c])
        hand_over(which, slot, c).start()

    def swap_out(head):
        rows = head_rows(head)
        return remote(o_s.at[rows, pl.ds(own, own)], o_peer.at[rows], o_sems.at[0, head], o_sems.at[1, head], links.peer)

    def swap_grads(head):
        rows = head_rows(head)
        return remote(grads.at[:, rows, pl.ds(own, own)], grads_peer.at[:, rows], grad_sems.at[0, head], grad_sems.at[1, head],
                      links.peer)

    part = band // 2
    portion = own // SENDS

    def send_home(which, i):
        cut = SENDS // 2
        second, inner = i // cut, lax.rem(i, cut)
        source = (dx_s if which else y_s).at[pl.ds(pl.multiple_of(i * portion, 16), portion)]
        target = (gx_ref if which else y_ref).at[odd, pl.ds(pl.multiple_of(inner * portion, 16), portion)]
        (core, x0), (_, x1) = links.owners
        maybe_far((core, jnp.where(second == 0, x0, x1)), source, target, out_send.at[which], out_recv.at[which])

    barrier = pltpu.get_barrier_semaphore()
    fixed = [links.peer]
    fixed += [links.step(axis, d) for axis in ('x', 'y') for d in range(1, RING)]
    fixed += [links.step('z', d) for d in range(1, depth)]
    for device in fixed:
        pl.semaphore_signal(barrier, inc=1, device_id=device, device_id_type=MESH)
    count = len(fixed)
    for place in links.owners + links.workers:
        other = jnp.logical_not(links.is_self(place))
        count = count + other.astype(jnp.int32)

        @pl.when(other)
        def _():
            pl.semaphore_signal(barrier, inc=1, device_id=links.at(core=place[0], x=place[1]), device_id_type=MESH)
    for load in loads:
        load.start()
    with jax.named_scope('barrier'):
        pl.semaphore_wait(barrier, count)
    for c in range(PIECES):
        for m in range(2):
            deliver(0, m, c)
    for load in loads:
        load.wait()

    def normalize(first):
        rows = pl.ds(first, piece)
        normed_s[rows] = (layer_norm(x_s, rows)[0] * gamma + beta).astype(BF)

    for c in range(PIECES + 1):
        if c < PIECES:
            for slot in range(2):
                arrive(0, slot, c)
            if c == PIECES - 1:
                for i in range(PIECES):
                    for m in range(2):
                        deliver(1, m, i)
            for slot in range(2):
                normalize(slot * band + c * piece)
        if c:
            for slot in range(2):
                with jax.named_scope(f'handed{slot}{c}'):
                    hand_over(0, slot, c - 1).wait_recv()
                normalize(own + slot * band + (c - 1) * piece)
            if c % 2 == 0:
                for b in range(4):
                    cols = pl.ds(b * band + (c - 2) * piece, 2 * piece)
                    normed = normed_s[cols]
                    for k, out in enumerate((q_s, k_s, v_s)):
                        out[:, cols] = dot_nt(wt_s[0, pl.ds(k * width, width)], normed).astype(BF)

    def forward_step(now, carry):
        head, step = now // fwd_steps, lax.rem(now, fwd_steps)
        rows = head_rows(head)
        for c in range(PIECES):
            @pl.when(now == (c + 1) * heads * fwd_steps // (PIECES + 1))
            def _():
                for slot in range(2):
                    arrive(1, slot, c)

        @pl.when(step == 0)
        def _():
            k_t = k_s[rows]
            kf_s[...] = jnp.concatenate([k_t, k_t, k_t], axis=0).T
            vf_s[0:dim] = v_s[rows]
            vf_s[dim:] = padded([jnp.ones((1, tokens), F32)], AUG - dim)

        bufs = (buf_a, buf_b, buf_c)
        total, lag = tiles * fwd_group, tiles + 1
        query, high, top, probs, out = {}, {}, {}, {}, {}
        for g in range(total + lag + 2):
            if g < total:
                i, t = divmod(g, tiles)
                if t == 0:
                    query[i] = jnp.concatenate(split_parts(q_s[rows, q_cols(step * fwd_group + i)].astype(F32) * log2_scale), axis=0)
                scores = dot_nn(kf_s[tile_rows(t)], query[i])
                bufs[i % 3][tile_rows(t)] = scores
                folded = fold_rows(scores, jnp.maximum)
                high[i] = folded if t == 0 else jnp.maximum(high[i], folded)
                if t == tiles - 1:
                    top[i] = jnp.max(high[i], axis=0, keepdims=True)
            if lag <= g < total + lag:
                i, t = divmod(g - lag, tiles)
                probs[g - lag] = jnp.exp2(bufs[i % 3][tile_rows(t, zero)] - top[i]).astype(BF)
            if g >= lag + 2:
                i, t = divmod(g - lag - 2, tiles)
                product = dot_nn(vf_s[:, tile_rows(t)], probs[g - lag - 2])
                out[i] = product if t == 0 else out[i] + product
                if t == tiles - 1:
                    cols = q_cols(step * fwd_group + i)
                    denom = out[i][dim:dim + 1]
                    value = out[i][:dim] * (1.0 / denom)
                    o_s[rows, cols] = value.astype(BF)
                    of_s[rows, cols] = value
                    lse = (top[i] + jnp.log2(denom)) * (1.0 / log2_scale)
                    lse_s[head_rows(head, 16), cols] = padded(split_parts(lse), 16)

        @pl.when(step == fwd_steps - 1)
        def _():
            swap_out(head).start()

        return carry

    lax.fori_loop(0, heads * fwd_steps, forward_step, 0)
    with jax.named_scope('dyhanded'):
        for c in range(PIECES):
            for slot in range(2):
                hand_over(1, slot, c).wait_recv()
    d_w[pl.ds(0, width)] = dot_nn(o_s[...], dy_s[...])
    for rnd, k in plan[0]:
        reduce.stage(rnd, k)
    with jax.named_scope('oswap'):
        for head in range(heads):
            swap_out(head).wait()
    for i in range(4):
        toks = pl.ds(i * part, part)
        product = dot_tn(o_s[:, toks], wo_s[0]) + dot_tn(o_peer[:, toks], wo_s[1])
        y_s[toks] = (x_s[toks].astype(F32) + product + bias).astype(BF)
    for i in range(tiles):
        cols = pl.ds(i * KEY_TILE, KEY_TILE)
        do_s[:, cols] = dot_nt(wo_s[0], dy_s[cols]).astype(BF)
    for which in range(2):
        rows = (dy_s if which else x_s).at[pl.ds(0, own)]
        all_left(rows, in_send.at[which])
        wait_for(rows, pass_send.at[which])

    def backward_step(now, carry):
        head, step = now // bwd_steps, lax.rem(now, bwd_steps)
        rows = head_rows(head)
        for at in range(end - 1):
            todo = plan.get(at + 1)
            if todo:
                @pl.when(now == at)
                def _():
                    with jax.named_scope(f'step{at}'):
                        for rnd, k in todo:
                            reduce.stage(rnd, k)
        share = SENDS // (heads * bwd_steps)
        for i in range(share):
            send_home(0, now * share + i)

        @pl.when(step == 0)
        def _():
            minus = padded([jnp.full((3, tokens), -1.0, F32)], AUG - dim)
            kb_s[...] = jnp.concatenate([k_s[rows], minus], axis=0).T
            vb_s[...] = jnp.concatenate([v_s[rows], minus], axis=0).T
            dk_acc[...] = jnp.zeros_like(dk_acc)
            dv_acc[...] = jnp.zeros_like(dv_acc)

        total = tiles * bwd_group
        ops, probs, d_scores, dq = {}, {}, {}, {}
        for g in range(total + 2):
            if g < total:
                i, t = divmod(g, tiles)
                if t == 0:
                    cols = q_cols(step * bwd_group + i)
                    q_t, do_t = q_s[rows, cols], do_s[rows, cols]
                    delta = jnp.sum(of_s[rows, cols] * do_t.astype(F32), axis=0, keepdims=True)
                    ops[i] = (cols, q_t, do_t, jnp.concatenate([q_t, lse_s[head_rows(head, 16), cols]], axis=0),
                              jnp.concatenate([do_t, padded(split_parts(delta), 16)], axis=0))
                scores = dot_nn(kb_s[tile_rows(t)], ops[i][3])
                d_probs = dot_nn(vb_s[tile_rows(t)], ops[i][4])
                prob = jnp.exp2(scores * log2_scale)
                probs[g] = prob.astype(BF)
                d_scores[g] = (prob * d_probs).astype(BF)
            if g >= 2:
                i, t = divmod(g - 2, tiles)
                cols, q_t, do_t = ops[i][:3]
                dv_acc[:, tile_rows(t)] += dot_nt(do_t, probs[g - 2])
                product = dot_nn(k_s[rows, tile_rows(t)], d_scores[g - 2])
                dq[i] = product if t == 0 else dq[i] + product
                if t == tiles - 1:
                    grads[0, rows, cols] = (dq[i] * scale).astype(BF)
                dk_acc[:, tile_rows(t)] += dot_nt(q_t, d_scores[g - 2])

        @pl.when(step == bwd_steps - 1)
        def _():
            grads[1, rows] = (dk_acc[...] * scale).astype(BF)
            grads[2, rows] = dv_acc[...].astype(BF)
            swap_grads(head).start()
            stacked = jnp.concatenate([grads[0, rows], grads[1, rows], grads[2, rows]], axis=0)
            d_w[pl.ds(pl.multiple_of(width + head * (3 * dim), 8), 3 * dim)] = dot_nn(stacked, normed_s[...])

        return carry

    lax.fori_loop(0, heads * bwd_steps, backward_step, 0)

    def tail(slot):
        for rnd, k in plan.get(end + slot, ()):
            with jax.named_scope(f'tail{slot}r{rnd}k{k}'):
                reduce.stage(rnd, k)

    tail(0)
    with jax.named_scope('gradswap'):
        for head in range(heads):
            swap_grads(head).wait()
    sums = [jnp.zeros((1, 640), F32)] * 3
    for i in range(4):
        toks = pl.ds(i * part, part)
        mine = jnp.concatenate([grads[k, :, toks] for k in range(3)], axis=0)
        theirs = jnp.concatenate([grads_peer[k, :, toks] for k in range(3)], axis=0)
        d_normed = (dot_tn(mine, wt_s[0]) + dot_tn(theirs, wt_s[1])).astype(BF).astype(F32)
        x_hat, inv_std = layer_norm(x_s, toks)
        d_hat = d_normed * gamma
        mean_one = jnp.mean(d_hat, axis=-1, keepdims=True)
        mean_two = jnp.mean(d_hat * x_hat, axis=-1, keepdims=True)
        dy_f = dy_s[toks].astype(F32)
        dx_s[toks] = (dy_f + inv_std * (d_hat - mean_one - x_hat * mean_two)).astype(BF)
        for k, term in enumerate((d_normed * x_hat, d_normed, dy_f)):
            sums[k] = sums[k] + jnp.sum(term, axis=0, keepdims=True)
        if i == 0:
            for j in range(SENDS // 4):
                send_home(1, j)

    for k in range(3):
        for j in range(5):
            small_s[0, pl.ds(k * 5 + j, 1)] = sums[k][:, j * 128:(j + 1) * 128]
    small_s[0, pl.ds(15, 1)] = jnp.zeros((1, 128), F32)
    small_copy = pltpu.make_async_copy(small_s.at[0], small_ref, load_sems.at[0, 0])
    first, waiting = 0, None
    for hop, axis in enumerate(('z', 'y', 'core', 'x', '')):
        if waiting:
            acc = small_s[hop - 1]
            with jax.named_scope(f'small{hop}'):
                for copy in waiting:
                    copy.wait_recv()
            for d in range(len(waiting)):
                acc = acc + small_recv[first + d]
            for copy in waiting:
                copy.wait_send()
            if axis:
                small_s[hop] = acc
            else:
                small_s[0] = acc
                small_copy.start()
            first += len(waiting)
        elif hop:
            small_s[hop] = small_s[hop - 1]
        if axis:
            far = [links.peer] if axis == 'core' else [links.step(axis, d) for d in range(1, links.size[axis])]
            waiting = [remote(small_s.at[hop], small_recv.at[first + d], small_sems.at[0, first + d], small_sems.at[1, first + d],
                              device) for d, device in enumerate(far)]
            for copy in waiting:
                copy.start()
            tail(1 + hop)
            if hop == 0:
                for i in range(SENDS // 4, SENDS):
                    send_home(1, i)
    for slot in range(5, slots):
        tail(slot)
    with jax.named_scope('home'):
        for which in range(2):
            all_left(dx_s if which else y_s, out_send.at[which])
            wait_for(gx_ref if which else y_ref, out_recv.at[which])
    with jax.named_scope('stored'):
        for rnd in range(ROUNDS):
            reduce.stored(rnd)
    small_copy.wait()


def attention_block(x_in, grad_y, weights, vectors, dim, depth):
    rows, channels = x_in.shape[1:]
    tokens, own = 4 * rows, 2 * rows
    width = weights[0].shape[0] // 2
    heads = width // dim
    total = 4 * width
    half = lambda *shape: pltpu.VMEM(shape, BF)
    full = lambda *shape: pltpu.VMEM(shape, F32)
    dma = lambda *shape: pltpu.SemaphoreType.DMA(shape)
    anywhere = pl.BlockSpec(memory_space=pl.ANY)
    in_vmem = pl.BlockSpec(memory_space=pltpu.VMEM)
    far = max(depth - 1, 1)
    return pl.pallas_call(
        functools.partial(block_body, dim, depth),
        in_specs=[anywhere] * 6 + [in_vmem] * 3,
        out_specs=[anywhere] * 7,
        out_shape=[jax.ShapeDtypeStruct(x_in.shape, BF)] * 2
        + [jax.ShapeDtypeStruct(weights[0].shape, F32)] * 4 + [jax.ShapeDtypeStruct((16, 128), F32)],
        scratch_shapes=[half(tokens, channels)] * 3 + [half(2, 3 * width, channels), half(2, width, channels)]
        + [half(width, tokens)] * 5 + [full(width, tokens), half(width, own), half(16 * heads, tokens),
                                       half(tokens, 3 * dim), half(AUG, tokens)]
        + [full(tokens, Q_BLOCK)] * 3 + [half(tokens, AUG)] * 2 + [full(dim, tokens)] * 2
        + [half(3, width, tokens), half(3, width, own), full(total, channels), full(2, total, channels)]
        + [half(own, channels)] * 2
        + [full(ROUNDS, 2, 3, 32, channels), full(ROUNDS, 2, 3, 8, channels), full(ROUNDS, 2, 32, channels), full(ROUNDS, 16, 8, 128),
           full(ROUNDS, far, 16 // depth, 8, 128), full(ROUNDS, 16, 8, 128), full(4, 16, 128), full(7 + far, 16, 128),
           dma(2, 4)] + [dma(2), dma(2, 2, PIECES)] * 2 + [dma(2, heads)] * 2
        + [dma(2), dma(2), dma(2, 7 + far)] + [dma(2, ROUNDS, 2, 2)] * 2 + [dma(2, ROUNDS, 2), dma(2, ROUNDS), dma(ROUNDS)],
        compiler_params=pltpu.CompilerParams(collective_id=0, has_side_effects=True, vmem_limit_bytes=VMEM_BYTES),
        name='attention_block',
    )(x_in, grad_y, *weights, *vectors)


def settle_body(count, small, *refs):
    sources, targets, refs = refs[:count], refs[count:2 * count], refs[2 * count:]
    vectors, bufs, sems = refs[:3], refs[3:3 + count], refs[3 + count]
    cuts = []
    for i, (source, target, buf) in enumerate(zip(sources, targets, bufs)):
        rows = source.shape[0] // CUTS
        for c in range(CUTS):
            part = pl.ds(c * rows, rows)
            cuts.append((pltpu.make_async_copy(source.at[part], buf.at[part], sems.at[0, i, c]),
                         pltpu.make_async_copy(buf.at[part], target.at[part], sems.at[1, i, c])))
    for read, _ in cuts:
        read.start()
    for read, write in cuts:
        read.wait()
        write.start()
    for k, vector in enumerate(vectors):
        vector[...] = jnp.concatenate([small[k * 5 + j:k * 5 + j + 1] for j in range(5)], axis=1).reshape(vector.shape)
    for _, write in cuts:
        write.wait()


def settle(small, arrays):
    anywhere, in_vmem = pl.BlockSpec(memory_space=pl.ANY), pl.BlockSpec(memory_space=pltpu.VMEM)
    count = len(arrays)
    return pl.pallas_call(
        functools.partial(settle_body, count),
        in_specs=[in_vmem] + [anywhere] * count, out_specs=[anywhere] * count + [in_vmem] * 3,
        out_shape=[jax.ShapeDtypeStruct(a.shape, a.dtype) for a in arrays] + [jax.ShapeDtypeStruct((arrays[0].shape[1],), F32)] * 3,
        scratch_shapes=[pltpu.VMEM(a.shape, a.dtype) for a in arrays] + [pltpu.SemaphoreType.DMA((2, count, CUTS))],
        compiler_params=pltpu.CompilerParams(vmem_limit_bytes=VMEM_BYTES),
        name='settle',
    )(small, *arrays)


def solution(mesh):
    depth = mesh.shape['dp'] // (2 * RING)
    act_spec, rep_spec = P('dp', 'cp', None), P()

    def device_step(x_in, grad_y, ln_gamma, ln_beta, w_q, w_k, w_v, w_o, b_o):
        channels, num_heads, head_dim = w_q.shape
        flat = (num_heads * head_dim, channels)
        weights = [jnp.transpose(w, (1, 2, 0)).reshape(flat) for w in (w_q, w_k, w_v)] + [w_o.reshape(flat)]
        y_out, grad_x, *grads, grad_wo, small = attention_block(x_in, grad_y, weights, (ln_gamma, ln_beta, b_o), head_dim, depth)
        rows = (2 * y_out.shape[1], channels)
        moved = settle(small, [y_out.reshape(rows), grad_x.reshape(rows), *grads, grad_wo])
        y_out, grad_x = (a.reshape(x_in.shape) for a in moved[:2])
        grads, grad_wo = moved[2:5], moved[5]
        grads = [jnp.transpose(grad.reshape(num_heads, head_dim, channels), (2, 0, 1)) for grad in grads]
        return (y_out, grad_x, moved[6], moved[7], *grads, grad_wo.reshape(num_heads, head_dim, channels), moved[8])

    specs = (act_spec, act_spec) + (rep_spec,) * 7
    return jax.shard_map(device_step, mesh=mesh, in_specs=specs, out_specs=specs, check_vma=False)
```

```python
import functools
import math
import jax
import jax.numpy as jnp
from jax import lax
from jax.experimental import pallas as pl
from jax.experimental.pallas import tpu as pltpu
from jax.sharding import PartitionSpec as P

LN_EPS = 1e-5
KEY_TILE = 256
Q_BLOCK = 256
FOLD = 16
AUG = 96
VMEM_BYTES = 67043328
BF = jnp.bfloat16
F32 = jnp.float32


def dot_nn(lhs, rhs):
    return lax.dot_general(lhs, rhs, (((1,), (0,)), ((), ())), preferred_element_type=F32)


def dot_nt(lhs, rhs):
    return lax.dot_general(lhs, rhs, (((1,), (1,)), ((), ())), preferred_element_type=F32)


def dot_tn(lhs, rhs):
    return lax.dot_general(lhs, rhs, (((0,), (0,)), ((), ())), preferred_element_type=F32)


def split_parts(value):
    high = value.astype(BF)
    rest = value - high.astype(F32)
    mid = rest.astype(BF)
    return high, mid, (rest - mid.astype(F32)).astype(BF)


def fold_rows(value, op):
    groups = value.reshape(value.shape[0] // FOLD, FOLD, value.shape[1])
    out = groups[0]
    for i in range(1, groups.shape[0]):
        out = op(out, groups[i])
    return out


MESH = pl.DeviceIdType.MESH
RING = 4
ROUNDS = 5
ROUND_ROWS = 256
STAGES = 8
SPARE = ((0, 1), (1, 1), (2, 1), (3, 1), (0, 6), (1, 5), (2, 6), (3, 5))
PIECES = 4
SENDS = 16
CUTS = 4
ORDER = ('yx', 'yx', 'yy', 'yx', 'yx')


class Links:
    def __init__(self, depth):
        dp, self.x = lax.axis_index('dp'), lax.axis_index('cp')
        self.core = lax.rem(dp, 2)
        self.y = lax.rem(dp // 2, RING)
        self.z = dp // (2 * RING)
        self.depth = depth
        self.pos = {'x': self.x, 'y': self.y, 'z': self.z}
        self.size = {'x': RING, 'y': RING, 'z': depth}
        self.peer = self.at(core=1 - self.core)
        pair, odd = self.x // 2, lax.rem(self.x, 2)
        self.owners = [(pair, 2 * self.core + odd), (pair, 2 * self.core + 1 - odd)]
        self.workers = [(pair, 2 * self.core), (pair, 2 * self.core + 1)]

    def at(self, x=None, y=None, z=None, core=None):
        pick = lambda value, own: own if value is None else value
        return ((pick(z, self.z) * RING + pick(y, self.y)) * 2 + pick(core, self.core), pick(x, self.x))

    def step(self, axis, d):
        return self.at(**{axis: lax.rem(self.pos[axis] + d, self.size[axis])})

    def is_self(self, place):
        return jnp.logical_and(place[0] == self.core, place[1] == self.x)


def remote(source, target, send, recv, device):
    return pltpu.make_async_remote_copy(src_ref=source, dst_ref=target, send_sem=send, recv_sem=recv,
                                        device_id=device, device_id_type=MESH)


def wait_for(ref, sem):
    pltpu.make_async_copy(ref, ref, sem).wait()


class GradReduce:
    def __init__(self, links, dim, grad, out, results, bufs, sems):
        self.links, self.grad, self.both, self.out = links, grad, out, out.at[links.core]
        width = grad.shape[0] // 4
        self.pieces = [(0, width, results[0], 0)]
        self.pieces += [(width + (3 * head + k) * dim, dim, results[1 + k], head * dim) for head in range(width // dim) for k in range(3)]
        self.recv1, self.recv2, self.mid, self.z_src, self.z_recv, self.z_out = bufs
        self.rs_sems, self.ag_sems, self.z_sems, self.swap_sems, self.store_sems = sems

    def axes(self, rnd, unit):
        first = ORDER[rnd][unit]
        return first, ('x' if first == 'y' else 'y')

    def block(self, rnd, unit, phase):
        first = rnd * ROUND_ROWS + unit * 128
        if phase == 0:
            return first, 32
        return first + self.links.pos[self.axes(rnd, unit)[0]] * 32, 8

    def landing(self, rnd, unit, phase):
        return (self.recv1 if phase == 0 else self.recv2).at[rnd, unit]

    def wait_all(self, rnd, unit, phase, sems):
        whole = self.landing(rnd, unit, phase)
        every = remote(whole, whole, sems.at[0, rnd, unit, phase], sems.at[1, rnd, unit, phase], self.links.peer)
        every.wait_recv()
        every.wait_send()

    def source(self, rnd, unit, phase, owner):
        if phase == 0:
            first, rows = self.block(rnd, unit, 0)
            return self.grad.at[pl.ds(pl.multiple_of(first + owner * rows, 8), rows)]
        return self.mid.at[rnd, unit, pl.ds(pl.multiple_of(owner * 8, 8), 8)]

    def scatter_start(self, rnd, unit, phase):
        axis = self.axes(rnd, unit)[phase]
        for d in (2, 1, 3):
            owner = lax.rem(self.links.pos[axis] + d, RING)
            remote(self.source(rnd, unit, phase, owner), self.landing(rnd, unit, phase).at[d - 1],
                   self.rs_sems.at[0, rnd, unit, phase], self.rs_sems.at[1, rnd, unit, phase], self.links.step(axis, d)).start()

    def scatter_end(self, rnd, unit, phase):
        self.wait_all(rnd, unit, phase, self.rs_sems)
        landing = self.landing(rnd, unit, phase)
        mine = self.source(rnd, unit, phase, self.links.pos[self.axes(rnd, unit)[phase]])
        return (mine[...] + landing[0]) + (landing[1] + landing[2])

    def gather_start(self, rnd, unit, phase):
        axis = self.axes(rnd, unit)[phase]
        first, rows = self.block(rnd, unit, phase)
        part = self.out.at[pl.ds(pl.multiple_of(first + self.links.pos[axis] * rows, 8), rows)]
        for d in (2, 1, 3):
            remote(part, part, self.ag_sems.at[0, rnd, unit, phase], self.ag_sems.at[1, rnd, unit, phase],
                   self.links.step(axis, d)).start()

    def z_copies(self, rnd, way):
        links = self.links
        each = 16 // links.depth
        send, recv = self.z_sems.at[0, rnd, way], self.z_sems.at[1, rnd, way]
        mine = pl.ds(links.z * each, each)
        copies = []
        for d in range(1, links.depth):
            far = lax.rem(links.z + d, links.depth)
            if way == 0:
                source, target = self.z_src.at[rnd, pl.ds(far * each, each)], self.z_recv.at[rnd, d - 1]
            else:
                source = target = self.z_out.at[rnd, mine]
            copies.append(remote(source, target, send, recv, links.step('z', d)))
        return copies, mine

    def z_wait(self, rnd, way):
        if self.links.depth > 1:
            whole = self.z_recv.at[rnd]
            all_of = remote(whole, whole, self.z_sems.at[0, rnd, way], self.z_sems.at[1, rnd, way], self.links.step('z', 1))
            all_of.wait_recv()
            all_of.wait_send()

    def swap(self, rnd):
        part = self.out.at[pl.ds(rnd * ROUND_ROWS, ROUND_ROWS)]
        return remote(part, part, self.swap_sems.at[0, rnd], self.swap_sems.at[1, rnd], self.links.peer)

    def store(self, rnd):
        begin = rnd * ROUND_ROWS
        half = self.both.shape[1] // 4
        for first, rows, result, place in self.pieces:
            low, high = max(first, begin), min(first + rows, begin + ROUND_ROWS)
            for core in range(2):
                if low < high:
                    target = result.at[pl.ds(core * half + place + low - first, high - low)]
                    pltpu.make_async_copy(self.both.at[core, pl.ds(low, high - low)], target, self.store_sems.at[rnd]).start()

    def stored(self, rnd):
        wait_for(self.both.at[:, pl.ds(rnd * ROUND_ROWS, ROUND_ROWS)], self.store_sems.at[rnd])

    def stage(self, rnd, k):
        units = (0, 1)
        if k == 0:
            for u in units:
                self.scatter_start(rnd, u, 0)
        elif k == 1:
            for u in units:
                self.mid[rnd, u] = self.scatter_end(rnd, u, 0)
                self.scatter_start(rnd, u, 1)
        elif k == 2:
            for u in units:
                total = self.scatter_end(rnd, u, 1)
                for j in range(5):
                    self.z_src[rnd, u * 5 + j] = total[:, j * 128:(j + 1) * 128]
            self.z_src[rnd, pl.ds(10, 6)] = jnp.zeros((6, 8, 128), F32)
            for copy in self.z_copies(rnd, 0)[0]:
                copy.start()
        elif k == 3:
            self.z_wait(rnd, 0)
            copies, mine = self.z_copies(rnd, 1)
            total = self.z_src[rnd, mine]
            for d in range(self.links.depth - 1):
                total = total + self.z_recv[rnd, d]
            self.z_out[rnd, mine] = total
            for copy in copies:
                copy.start()
        elif k == 4:
            self.z_wait(rnd, 1)
            for u in units:
                first = self.block(rnd, u, 1)[0] + self.links.pos[self.axes(rnd, u)[1]] * 8
                for j in range(5):
                    self.out[pl.ds(pl.multiple_of(first, 8), 8), pl.ds(j * 128, 128)] = self.z_out[rnd, u * 5 + j]
                self.gather_start(rnd, u, 1)
        elif k == 5:
            for u in units:
                self.wait_all(rnd, u, 1, self.ag_sems)
                self.gather_start(rnd, u, 0)
        elif k == 6:
            for u in units:
                self.wait_all(rnd, u, 0, self.ag_sems)
            self.swap(rnd).start()
        else:
            self.swap(rnd).wait()
            self.store(rnd)


def layer_norm(x_ref, rows):
    x_f = x_ref[rows].astype(F32)
    centered = x_f - jnp.mean(x_f, axis=-1, keepdims=True)
    inv_std = lax.rsqrt(jnp.mean(centered * centered, axis=-1, keepdims=True) + LN_EPS)
    return centered * inv_std, inv_std


def padded(parts, rows):
    filled = [part.astype(F32) for part in parts]
    used = sum(part.shape[0] for part in filled)
    return jnp.concatenate(filled + [jnp.zeros((rows - used, filled[0].shape[1]), F32)], axis=0).astype(BF)


def block_body(dim, depth, x_hbm, dy_hbm, wq_hbm, wk_hbm, wv_hbm, wo_hbm, gamma_ref, beta_ref, bo_ref,
               y_ref, gx_ref, dq_ref, dk_ref, dv_ref, dwo_ref, small_ref,
               x_s, normed_s, dy_s, wt_s, wo_s, q_s, k_s, v_s, do_s, o_s, of_s, o_peer, lse_s, kf_s, vf_s, buf_a, buf_b, buf_c,
               kb_s, vb_s, dk_acc, dv_acc, grads, grads_peer, d_w, d_w_all, dx_s, y_s,
               recv1, recv2, mid, z_src, z_recv, z_out, small_s, small_recv,
               load_sems, in_send, in_recv, pass_send, pass_recv, o_sems, grad_sems, out_send, out_recv, small_sems,
               rs_sems, ag_sems, z_sems, swap_sems, store_sems):
    links = Links(depth)
    width, tokens = q_s.shape
    heads, tiles = width // dim, tokens // KEY_TILE
    own, band = tokens // 2, tokens // 4
    scale = dim ** -0.5
    log2_scale = scale * math.log2(math.e)
    fwd_group, bwd_group = 4, 4
    fwd_steps, bwd_steps = tiles // fwd_group, tiles // bwd_group
    zero = jnp.minimum(links.x, 0)
    gamma, beta, bias = (ref[...].reshape(1, ref.shape[0]) for ref in (gamma_ref, beta_ref, bo_ref))
    odd = lax.rem(links.x, 2)
    reduce = GradReduce(links, dim, d_w, d_w_all, (dwo_ref, dq_ref, dk_ref, dv_ref), (recv1, recv2, mid, z_src, z_recv, z_out),
                        (rs_sems, ag_sems, z_sems, swap_sems, store_sems))
    end = heads * bwd_steps + 1
    plan = {}
    for rnd in range(ROUNDS):
        at = rnd * bwd_steps + 1 if rnd else 0
        for k in range(STAGES):
            at += min(k, 1) + ((rnd, k) in SPARE)
            plan.setdefault(at, []).append((rnd, k))
    for at in plan:
        plan[at].sort(key=lambda item: (item[1] in (0, 5) and item[0] < ROUNDS - 1, -item[0]))
    slots = max(plan) + 1 - end

    def tile_rows(tile, base=None):
        return pl.ds(tile * KEY_TILE if base is None else pl.multiple_of(base + tile * KEY_TILE, KEY_TILE), KEY_TILE)

    def head_rows(head, rows=dim):
        return pl.ds(pl.multiple_of(head * rows, 16), rows)

    def q_cols(index):
        return pl.ds(pl.multiple_of(index * Q_BLOCK, Q_BLOCK), Q_BLOCK)

    def my_half(side):
        return pl.ds(pl.multiple_of((links.core if side == 0 else 1 - links.core) * width, 16), width)

    loads = [pltpu.make_async_copy(w_hbm.at[my_half(side)], wt_s.at[side, pl.ds(k * width, width)], load_sems.at[side, k])
             for side in range(2) for k, w_hbm in enumerate((wq_hbm, wk_hbm, wv_hbm))]
    loads += [pltpu.make_async_copy(wo_hbm.at[my_half(side)], wo_s.at[side], load_sems.at[side, 3]) for side in range(2)]

    def maybe_far(place, source, target, send, recv):
        core, x = place
        here = links.is_self(place)
        far = remote(source, target, send, recv, links.at(core=core, x=x))
        near = pltpu.make_async_copy(source, target, recv)

        @pl.when(jnp.logical_not(here))
        def _():
            far.start()

        @pl.when(here)
        def _():
            near.start()

    def all_left(ref, sem):
        rows = ref.shape[0]
        halved = links.x // 2 == links.core

        @pl.when(jnp.logical_not(halved))
        def _():
            wait_for(ref, sem)

        @pl.when(halved)
        def _():
            wait_for(ref.at[pl.ds(0, rows // 2)], sem)

    piece = band // PIECES

    def deliver(which, m, c):
        slot = lax.rem(links.x + m, 2)
        source = (dy_hbm if which else x_hbm).at[m, pl.ds(c * piece, piece)]
        target = (dy_s if which else x_s).at[pl.ds(pl.multiple_of(slot * band + c * piece, 16), piece)]
        maybe_far(links.workers[m], source, target, in_send.at[which], in_recv.at[which, slot, c])

    def hand_over(which, slot, c):
        rows = dy_s if which else x_s
        first = slot * band + c * piece
        return remote(rows.at[pl.ds(first, piece)], rows.at[pl.ds(own + first, piece)],
                      pass_send.at[which], pass_recv.at[which, slot, c], links.peer)

    def arrive(which, slot, c):
        with jax.named_scope(f'arrive{which}{slot}{c}'):
            wait_for((dy_s if which else x_s).at[pl.ds(slot * band + c * piece, piece)], in_recv.at[which, slot, c])
        hand_over(which, slot, c).start()

    def swap_out(head):
        rows = head_rows(head)
        return remote(o_s.at[rows, pl.ds(own, own)], o_peer.at[rows], o_sems.at[0, head], o_sems.at[1, head], links.peer)

    def swap_grads(head):
        rows = head_rows(head)
        return remote(grads.at[:, rows, pl.ds(own, own)], grads_peer.at[:, rows], grad_sems.at[0, head], grad_sems.at[1, head],
                      links.peer)

    part = band // 2
    portion = own // SENDS

    def send_home(which, i):
        cut = SENDS // 2
        second, inner = i // cut, lax.rem(i, cut)
        source = (dx_s if which else y_s).at[pl.ds(pl.multiple_of(i * portion, 16), portion)]
        target = (gx_ref if which else y_ref).at[odd, pl.ds(pl.multiple_of(inner * portion, 16), portion)]
        (core, x0), (_, x1) = links.owners
        maybe_far((core, jnp.where(second == 0, x0, x1)), source, target, out_send.at[which], out_recv.at[which])

    barrier = pltpu.get_barrier_semaphore()
    fixed = [links.peer]
    fixed += [links.step(axis, d) for axis in ('x', 'y') for d in range(1, RING)]
    fixed += [links.step('z', d) for d in range(1, depth)]
    for device in fixed:
        pl.semaphore_signal(barrier, inc=1, device_id=device, device_id_type=MESH)
    count = len(fixed)
    for place in links.owners + links.workers:
        other = jnp.logical_not(links.is_self(place))
        count = count + other.astype(jnp.int32)

        @pl.when(other)
        def _():
            pl.semaphore_signal(barrier, inc=1, device_id=links.at(core=place[0], x=place[1]), device_id_type=MESH)
    for load in loads:
        load.start()
    with jax.named_scope('barrier'):
        pl.semaphore_wait(barrier, count)
    for c in range(PIECES):
        for m in range(2):
            deliver(0, m, c)
    for load in loads:
        load.wait()

    def normalize(first):
        rows = pl.ds(first, piece)
        normed_s[rows] = (layer_norm(x_s, rows)[0] * gamma + beta).astype(BF)

    for c in range(PIECES + 1):
        if c < PIECES:
            for slot in range(2):
                arrive(0, slot, c)
            if c == PIECES - 1:
                for i in range(PIECES):
                    for m in range(2):
                        deliver(1, m, i)
            for slot in range(2):
                normalize(slot * band + c * piece)
        if c:
            for slot in range(2):
                with jax.named_scope(f'handed{slot}{c}'):
                    hand_over(0, slot, c - 1).wait_recv()
                normalize(own + slot * band + (c - 1) * piece)
            if c % 2 == 0:
                for b in range(4):
                    cols = pl.ds(b * band + (c - 2) * piece, 2 * piece)
                    normed = normed_s[cols]
                    for k, out in enumerate((q_s, k_s, v_s)):
                        out[:, cols] = dot_nt(wt_s[0, pl.ds(k * width, width)], normed).astype(BF)

    def forward_step(now, carry):
        head, step = now // fwd_steps, lax.rem(now, fwd_steps)
        rows = head_rows(head)
        for c in range(PIECES):
            @pl.when(now == (c + 1) * heads * fwd_steps // (PIECES + 1))
            def _():
                for slot in range(2):
                    arrive(1, slot, c)

        @pl.when(step == 0)
        def _():
            k_t = k_s[rows]
            kf_s[...] = jnp.concatenate([k_t, k_t, k_t], axis=0).T
            vf_s[0:dim] = v_s[rows]
            vf_s[dim:] = padded([jnp.ones((1, tokens), F32)], AUG - dim)

        bufs = (buf_a, buf_b, buf_c)
        total, lag = tiles * fwd_group, tiles + 2
        query, high, top, probs, out = {}, {}, {}, {}, {}
        for g in range(total + lag + 2):
            if g < total:
                i, t = divmod(g, tiles)
                if t == 0:
                    query[i] = jnp.concatenate(split_parts(q_s[rows, q_cols(step * fwd_group + i)].astype(F32) * log2_scale), axis=0)
                scores = dot_nn(kf_s[tile_rows(t)], query[i])
                bufs[i % 3][tile_rows(t)] = scores
                folded = fold_rows(scores, jnp.maximum)
                high[i] = folded if t == 0 else jnp.maximum(high[i], folded)
                if t == tiles - 1:
                    top[i] = jnp.max(high[i], axis=0, keepdims=True)
            if lag <= g < total + lag:
                i, t = divmod(g - lag, tiles)
                probs[g - lag] = jnp.exp2(bufs[i % 3][tile_rows(t, zero)] - top[i]).astype(BF)
            if g >= lag + 2:
                i, t = divmod(g - lag - 2, tiles)
                product = dot_nn(vf_s[:, tile_rows(t)], probs[g - lag - 2])
                out[i] = product if t == 0 else out[i] + product
                if t == tiles - 1:
                    cols = q_cols(step * fwd_group + i)
                    denom = out[i][dim:dim + 1]
                    value = out[i][:dim] * (1.0 / denom)
                    o_s[rows, cols] = value.astype(BF)
                    of_s[rows, cols] = value
                    lse = (top[i] + jnp.log2(denom)) * (1.0 / log2_scale)
                    lse_s[head_rows(head, 16), cols] = padded(split_parts(lse), 16)

        @pl.when(step == fwd_steps - 1)
        def _():
            swap_out(head).start()

        return carry

    lax.fori_loop(0, heads * fwd_steps, forward_step, 0)
    with jax.named_scope('dyhanded'):
        for c in range(PIECES):
            for slot in range(2):
                hand_over(1, slot, c).wait_recv()
    d_w[pl.ds(0, width)] = dot_nn(o_s[...], dy_s[...])
    for rnd, k in plan[0]:
        reduce.stage(rnd, k)
    with jax.named_scope('oswap'):
        for head in range(heads):
            swap_out(head).wait()
    for i in range(4):
        toks = pl.ds(i * part, part)
        product = dot_tn(o_s[:, toks], wo_s[0]) + dot_tn(o_peer[:, toks], wo_s[1])
        y_s[toks] = (x_s[toks].astype(F32) + product + bias).astype(BF)
    for i in range(tiles):
        cols = pl.ds(i * KEY_TILE, KEY_TILE)
        do_s[:, cols] = dot_nt(wo_s[0], dy_s[cols]).astype(BF)
    for which in range(2):
        rows = (dy_s if which else x_s).at[pl.ds(0, own)]
        all_left(rows, in_send.at[which])
        wait_for(rows, pass_send.at[which])

    def backward_step(now, carry):
        head, step = now // bwd_steps, lax.rem(now, bwd_steps)
        rows = head_rows(head)
        for at in range(end - 1):
            todo = plan.get(at + 1)
            if todo:
                @pl.when(now == at)
                def _():
                    with jax.named_scope(f'step{at}'):
                        for rnd, k in todo:
                            reduce.stage(rnd, k)
        share = SENDS // (heads * bwd_steps)
        for i in range(share):
            send_home(0, now * share + i)

        @pl.when(step == 0)
        def _():
            minus = padded([jnp.full((3, tokens), -1.0, F32)], AUG - dim)
            kb_s[...] = jnp.concatenate([k_s[rows], minus], axis=0).T
            vb_s[...] = jnp.concatenate([v_s[rows], minus], axis=0).T
            dk_acc[...] = jnp.zeros_like(dk_acc)
            dv_acc[...] = jnp.zeros_like(dv_acc)

        total = tiles * bwd_group
        ops, probs, d_scores, dq = {}, {}, {}, {}
        for g in range(total + 2):
            if g < total:
                i, t = divmod(g, tiles)
                if t == 0:
                    cols = q_cols(step * bwd_group + i)
                    q_t, do_t = q_s[rows, cols], do_s[rows, cols]
                    delta = jnp.sum(of_s[rows, cols] * do_t.astype(F32), axis=0, keepdims=True)
                    ops[i] = (cols, q_t, do_t, jnp.concatenate([q_t, lse_s[head_rows(head, 16), cols]], axis=0),
                              jnp.concatenate([do_t, padded(split_parts(delta), 16)], axis=0))
                scores = dot_nn(kb_s[tile_rows(t)], ops[i][3])
                d_probs = dot_nn(vb_s[tile_rows(t)], ops[i][4])
                prob = jnp.exp2(scores * log2_scale)
                probs[g] = prob.astype(BF)
                d_scores[g] = (prob * d_probs).astype(BF)
            if g >= 2:
                i, t = divmod(g - 2, tiles)
                cols, q_t, do_t = ops[i][:3]
                dv_acc[:, tile_rows(t)] += dot_nt(do_t, probs[g - 2])
                product = dot_nn(k_s[rows, tile_rows(t)], d_scores[g - 2])
                dq[i] = product if t == 0 else dq[i] + product
                if t == tiles - 1:
                    grads[0, rows, cols] = (dq[i] * scale).astype(BF)
                dk_acc[:, tile_rows(t)] += dot_nt(q_t, d_scores[g - 2])

        @pl.when(step == bwd_steps - 1)
        def _():
            grads[1, rows] = (dk_acc[...] * scale).astype(BF)
            grads[2, rows] = dv_acc[...].astype(BF)
            swap_grads(head).start()
            stacked = jnp.concatenate([grads[0, rows], grads[1, rows], grads[2, rows]], axis=0)
            d_w[pl.ds(pl.multiple_of(width + head * (3 * dim), 8), 3 * dim)] = dot_nn(stacked, normed_s[...])

        return carry

    lax.fori_loop(0, heads * bwd_steps, backward_step, 0)

    def tail(slot):
        for rnd, k in plan.get(end + slot, ()):
            with jax.named_scope(f'tail{slot}r{rnd}k{k}'):
                reduce.stage(rnd, k)

    tail(0)
    with jax.named_scope('gradswap'):
        for head in range(heads):
            swap_grads(head).wait()
    sums = [jnp.zeros((1, 640), F32)] * 3
    for i in range(4):
        toks = pl.ds(i * part, part)
        mine = jnp.concatenate([grads[k, :, toks] for k in range(3)], axis=0)
        theirs = jnp.concatenate([grads_peer[k, :, toks] for k in range(3)], axis=0)
        d_normed = (dot_tn(mine, wt_s[0]) + dot_tn(theirs, wt_s[1])).astype(BF).astype(F32)
        x_hat, inv_std = layer_norm(x_s, toks)
        d_hat = d_normed * gamma
        mean_one = jnp.mean(d_hat, axis=-1, keepdims=True)
        mean_two = jnp.mean(d_hat * x_hat, axis=-1, keepdims=True)
        dy_f = dy_s[toks].astype(F32)
        dx_s[toks] = (dy_f + inv_std * (d_hat - mean_one - x_hat * mean_two)).astype(BF)
        for k, term in enumerate((d_normed * x_hat, d_normed, dy_f)):
            sums[k] = sums[k] + jnp.sum(term, axis=0, keepdims=True)

    for k in range(3):
        for j in range(5):
            small_s[0, pl.ds(k * 5 + j, 1)] = sums[k][:, j * 128:(j + 1) * 128]
    small_s[0, pl.ds(15, 1)] = jnp.zeros((1, 128), F32)
    small_copy = pltpu.make_async_copy(small_s.at[0], small_ref, load_sems.at[0, 0])
    first, waiting = 0, None
    for hop, axis in enumerate(('z', 'y', 'core', 'x', '')):
        if waiting:
            acc = small_s[hop - 1]
            with jax.named_scope(f'small{hop}'):
                for copy in waiting:
                    copy.wait_recv()
            for d in range(len(waiting)):
                acc = acc + small_recv[first + d]
            for copy in waiting:
                copy.wait_send()
            if axis:
                small_s[hop] = acc
            else:
                small_s[0] = acc
                small_copy.start()
            first += len(waiting)
        elif hop:
            small_s[hop] = small_s[hop - 1]
        if axis:
            far = [links.peer] if axis == 'core' else [links.step(axis, d) for d in range(1, links.size[axis])]
            waiting = [remote(small_s.at[hop], small_recv.at[first + d], small_sems.at[0, first + d], small_sems.at[1, first + d],
                              device) for d, device in enumerate(far)]
            for copy in waiting:
                copy.start()
            tail(1 + hop)
            if hop == 0:
                for i in range(SENDS):
                    send_home(1, i)
    for slot in range(5, slots):
        tail(slot)
    with jax.named_scope('home'):
        for which in range(2):
            all_left(dx_s if which else y_s, out_send.at[which])
            wait_for(gx_ref if which else y_ref, out_recv.at[which])
    with jax.named_scope('stored'):
        for rnd in range(ROUNDS):
            reduce.stored(rnd)
    small_copy.wait()


def attention_block(x_in, grad_y, weights, vectors, dim, depth):
    rows, channels = x_in.shape[1:]
    tokens, own = 4 * rows, 2 * rows
    width = weights[0].shape[0] // 2
    heads = width // dim
    total = 4 * width
    half = lambda *shape: pltpu.VMEM(shape, BF)
    full = lambda *shape: pltpu.VMEM(shape, F32)
    dma = lambda *shape: pltpu.SemaphoreType.DMA(shape)
    anywhere = pl.BlockSpec(memory_space=pl.ANY)
    in_vmem = pl.BlockSpec(memory_space=pltpu.VMEM)
    far = max(depth - 1, 1)
    return pl.pallas_call(
        functools.partial(block_body, dim, depth),
        in_specs=[anywhere] * 6 + [in_vmem] * 3,
        out_specs=[anywhere] * 7,
        out_shape=[jax.ShapeDtypeStruct(x_in.shape, BF)] * 2
        + [jax.ShapeDtypeStruct(weights[0].shape, F32)] * 4 + [jax.ShapeDtypeStruct((16, 128), F32)],
        scratch_shapes=[half(tokens, channels)] * 3 + [half(2, 3 * width, channels), half(2, width, channels)]
        + [half(width, tokens)] * 5 + [full(width, tokens), half(width, own), half(16 * heads, tokens),
                                       half(tokens, 3 * dim), half(AUG, tokens)]
        + [full(tokens, Q_BLOCK)] * 3 + [half(tokens, AUG)] * 2 + [full(dim, tokens)] * 2
        + [half(3, width, tokens), half(3, width, own), full(total, channels), full(2, total, channels)]
        + [half(own, channels)] * 2
        + [full(ROUNDS, 2, 3, 32, channels), full(ROUNDS, 2, 3, 8, channels), full(ROUNDS, 2, 32, channels), full(ROUNDS, 16, 8, 128),
           full(ROUNDS, far, 16 // depth, 8, 128), full(ROUNDS, 16, 8, 128), full(4, 16, 128), full(7 + far, 16, 128),
           dma(2, 4)] + [dma(2), dma(2, 2, PIECES)] * 2 + [dma(2, heads)] * 2
        + [dma(2), dma(2), dma(2, 7 + far)] + [dma(2, ROUNDS, 2, 2)] * 2 + [dma(2, ROUNDS, 2), dma(2, ROUNDS), dma(ROUNDS)],
        compiler_params=pltpu.CompilerParams(collective_id=0, has_side_effects=True, vmem_limit_bytes=VMEM_BYTES),
        name='attention_block',
    )(x_in, grad_y, *weights, *vectors)


def settle_body(count, small_hbm, *refs):
    sources, targets, refs = refs[:count], refs[count:2 * count], refs[2 * count:]
    vectors, bufs, (small, vector_s, sems, vector_sems) = refs[:3], refs[3:3 + count], refs[3 + count:]
    load = pltpu.make_async_copy(small_hbm, small, vector_sems.at[3])
    load.start()
    cuts = []
    for i, (source, target, buf) in enumerate(zip(sources, targets, bufs)):
        rows = source.shape[0] // CUTS
        for c in range(CUTS):
            part = pl.ds(c * rows, rows)
            cuts.append((pltpu.make_async_copy(source.at[part], buf.at[part], sems.at[0, i, c]),
                         pltpu.make_async_copy(buf.at[part], target.at[part], sems.at[1, i, c])))
    for read, _ in cuts:
        read.start()
    load.wait()
    stores = []
    for k, vector in enumerate(vectors):
        vector_s[k][...] = jnp.concatenate([small[k * 5 + j:k * 5 + j + 1] for j in range(5)], axis=1).reshape(vector.shape)
        stores.append(pltpu.make_async_copy(vector_s[k], vector, vector_sems.at[k]))
        stores[k].start()
    for read, write in cuts:
        read.wait()
        write.start()
    for _, write in cuts:
        write.wait()
    for store in stores:
        store.wait()


def settle(small, arrays):
    anywhere = pl.BlockSpec(memory_space=pl.ANY)
    count = len(arrays)
    dma = pltpu.SemaphoreType.DMA
    vector = (arrays[0].shape[1],)
    return pl.pallas_call(
        functools.partial(settle_body, count),
        in_specs=[anywhere] * (count + 1), out_specs=[anywhere] * (count + 3),
        out_shape=[jax.ShapeDtypeStruct(a.shape, a.dtype) for a in arrays] + [jax.ShapeDtypeStruct(vector, F32)] * 3,
        scratch_shapes=[pltpu.VMEM(a.shape, a.dtype) for a in arrays]
        + [pltpu.VMEM(small.shape, F32), [pltpu.VMEM(vector, F32)] * 3, dma((2, count, CUTS)), dma((4,))],
        compiler_params=pltpu.CompilerParams(vmem_limit_bytes=VMEM_BYTES),
        name='settle',
    )(small, *arrays)


def solution(mesh):
    depth = mesh.shape['dp'] // (2 * RING)
    act_spec, rep_spec = P('dp', 'cp', None), P()

    def device_step(x_in, grad_y, ln_gamma, ln_beta, w_q, w_k, w_v, w_o, b_o):
        channels, num_heads, head_dim = w_q.shape
        flat = (num_heads * head_dim, channels)
        weights = [jnp.transpose(w, (1, 2, 0)).reshape(flat) for w in (w_q, w_k, w_v)] + [w_o.reshape(flat)]
        y_out, grad_x, *grads, grad_wo, small = attention_block(x_in, grad_y, weights, (ln_gamma, ln_beta, b_o), head_dim, depth)
        rows = (2 * y_out.shape[1], channels)
        moved = settle(small, [y_out.reshape(rows), grad_x.reshape(rows), *grads, grad_wo])
        y_out, grad_x = (a.reshape(x_in.shape) for a in moved[:2])
        grads, grad_wo = moved[2:5], moved[5]
        grads = [jnp.transpose(grad.reshape(num_heads, head_dim, channels), (2, 0, 1)) for grad in grads]
        return (y_out, grad_x, moved[6], moved[7], *grads, grad_wo.reshape(num_heads, head_dim, channels), moved[8])

    specs = (act_spec, act_spec) + (rep_spec,) * 7
    return jax.shard_map(device_step, mesh=mesh, in_specs=specs, out_specs=specs, check_vma=False)
```

```python
import functools
import math
import jax
import jax.numpy as jnp
from jax import lax
from jax.experimental import pallas as pl
from jax.experimental.pallas import tpu as pltpu
from jax.sharding import PartitionSpec as P

LN_EPS = 1e-5
KEY_TILE = 256
Q_BLOCK = 256
FOLD = 16
AUG = 96
VMEM_BYTES = 67043328
BF = jnp.bfloat16
F32 = jnp.float32


def dot_nn(lhs, rhs):
    return lax.dot_general(lhs, rhs, (((1,), (0,)), ((), ())), preferred_element_type=F32)


def dot_nt(lhs, rhs):
    return lax.dot_general(lhs, rhs, (((1,), (1,)), ((), ())), preferred_element_type=F32)


def dot_tn(lhs, rhs):
    return lax.dot_general(lhs, rhs, (((0,), (0,)), ((), ())), preferred_element_type=F32)


def split_parts(value):
    high = value.astype(BF)
    rest = value - high.astype(F32)
    mid = rest.astype(BF)
    return high, mid, (rest - mid.astype(F32)).astype(BF)


def fold_rows(value, op):
    groups = value.reshape(value.shape[0] // FOLD, FOLD, value.shape[1])
    out = groups[0]
    for i in range(1, groups.shape[0]):
        out = op(out, groups[i])
    return out


MESH = pl.DeviceIdType.MESH
RING = 4
ROUNDS = 5
ROUND_ROWS = 256
STAGES = 8
SPARE = ((0, 1), (1, 1), (2, 1), (3, 1), (0, 6), (1, 5), (2, 6), (3, 5))
PIECES = 4
SENDS = 16
CUTS = 4
ORDER = ('yx', 'yy', 'yy', 'yx', 'yx')


class Links:
    def __init__(self, depth):
        dp, self.x = lax.axis_index('dp'), lax.axis_index('cp')
        self.core = lax.rem(dp, 2)
        self.y = lax.rem(dp // 2, RING)
        self.z = dp // (2 * RING)
        self.depth = depth
        self.pos = {'x': self.x, 'y': self.y, 'z': self.z}
        self.size = {'x': RING, 'y': RING, 'z': depth}
        self.peer = self.at(core=1 - self.core)
        pair, odd = self.x // 2, lax.rem(self.x, 2)
        self.owners = [(pair, 2 * self.core + odd), (pair, 2 * self.core + 1 - odd)]
        self.workers = [(pair, 2 * self.core), (pair, 2 * self.core + 1)]

    def at(self, x=None, y=None, z=None, core=None):
        pick = lambda value, own: own if value is None else value
        return ((pick(z, self.z) * RING + pick(y, self.y)) * 2 + pick(core, self.core), pick(x, self.x))

    def step(self, axis, d):
        return self.at(**{axis: lax.rem(self.pos[axis] + d, self.size[axis])})

    def is_self(self, place):
        return jnp.logical_and(place[0] == self.core, place[1] == self.x)


def remote(source, target, send, recv, device):
    return pltpu.make_async_remote_copy(src_ref=source, dst_ref=target, send_sem=send, recv_sem=recv,
                                        device_id=device, device_id_type=MESH)


def wait_for(ref, sem):
    pltpu.make_async_copy(ref, ref, sem).wait()


class GradReduce:
    def __init__(self, links, dim, grad, out, results, bufs, sems):
        self.links, self.grad, self.both, self.out = links, grad, out, out.at[links.core]
        width = grad.shape[0] // 4
        self.pieces = [(0, width, results[0], 0)]
        self.pieces += [(width + (3 * head + k) * dim, dim, results[1 + k], head * dim) for head in range(width // dim) for k in range(3)]
        self.recv1, self.recv2, self.mid, self.z_src, self.z_recv, self.z_out = bufs
        self.rs_sems, self.ag_sems, self.z_sems, self.swap_sems, self.store_sems = sems

    def axes(self, rnd, unit):
        first = ORDER[rnd][unit]
        return first, ('x' if first == 'y' else 'y')

    def block(self, rnd, unit, phase):
        first = rnd * ROUND_ROWS + unit * 128
        if phase == 0:
            return first, 32
        return first + self.links.pos[self.axes(rnd, unit)[0]] * 32, 8

    def landing(self, rnd, unit, phase):
        return (self.recv1 if phase == 0 else self.recv2).at[rnd, unit]

    def wait_all(self, rnd, unit, phase, sems):
        whole = self.landing(rnd, unit, phase)
        every = remote(whole, whole, sems.at[0, rnd, unit, phase], sems.at[1, rnd, unit, phase], self.links.peer)
        every.wait_recv()
        every.wait_send()

    def source(self, rnd, unit, phase, owner):
        if phase == 0:
            first, rows = self.block(rnd, unit, 0)
            return self.grad.at[pl.ds(pl.multiple_of(first + owner * rows, 8), rows)]
        return self.mid.at[rnd, unit, pl.ds(pl.multiple_of(owner * 8, 8), 8)]

    def scatter_start(self, rnd, unit, phase):
        axis = self.axes(rnd, unit)[phase]
        for d in (2, 1, 3):
            owner = lax.rem(self.links.pos[axis] + d, RING)
            remote(self.source(rnd, unit, phase, owner), self.landing(rnd, unit, phase).at[d - 1],
                   self.rs_sems.at[0, rnd, unit, phase], self.rs_sems.at[1, rnd, unit, phase], self.links.step(axis, d)).start()

    def scatter_end(self, rnd, unit, phase):
        self.wait_all(rnd, unit, phase, self.rs_sems)
        landing = self.landing(rnd, unit, phase)
        mine = self.source(rnd, unit, phase, self.links.pos[self.axes(rnd, unit)[phase]])
        return (mine[...] + landing[0]) + (landing[1] + landing[2])

    def gather_start(self, rnd, unit, phase):
        axis = self.axes(rnd, unit)[phase]
        first, rows = self.block(rnd, unit, phase)
        part = self.out.at[pl.ds(pl.multiple_of(first + self.links.pos[axis] * rows, 8), rows)]
        for d in (2, 1, 3):
            remote(part, part, self.ag_sems.at[0, rnd, unit, phase], self.ag_sems.at[1, rnd, unit, phase],
                   self.links.step(axis, d)).start()

    def z_copies(self, rnd, way):
        links = self.links
        each = 16 // links.depth
        send, recv = self.z_sems.at[0, rnd, way], self.z_sems.at[1, rnd, way]
        mine = pl.ds(links.z * each, each)
        copies = []
        for d in range(1, links.depth):
            far = lax.rem(links.z + d, links.depth)
            if way == 0:
                source, target = self.z_src.at[rnd, pl.ds(far * each, each)], self.z_recv.at[rnd, d - 1]
            else:
                source = target = self.z_out.at[rnd, mine]
            copies.append(remote(source, target, send, recv, links.step('z', d)))
        return copies, mine

    def z_wait(self, rnd, way):
        if self.links.depth > 1:
            whole = self.z_recv.at[rnd]
            all_of = remote(whole, whole, self.z_sems.at[0, rnd, way], self.z_sems.at[1, rnd, way], self.links.step('z', 1))
            all_of.wait_recv()
            all_of.wait_send()

    def swap(self, rnd):
        part = self.out.at[pl.ds(rnd * ROUND_ROWS, ROUND_ROWS)]
        return remote(part, part, self.swap_sems.at[0, rnd], self.swap_sems.at[1, rnd], self.links.peer)

    def store(self, rnd):
        begin = rnd * ROUND_ROWS
        half = self.both.shape[1] // 4
        for first, rows, result, place in self.pieces:
            low, high = max(first, begin), min(first + rows, begin + ROUND_ROWS)
            for core in range(2):
                if low < high:
                    target = result.at[pl.ds(core * half + place + low - first, high - low)]
                    pltpu.make_async_copy(self.both.at[core, pl.ds(low, high - low)], target, self.store_sems.at[rnd]).start()

    def stored(self, rnd):
        wait_for(self.both.at[:, pl.ds(rnd * ROUND_ROWS, ROUND_ROWS)], self.store_sems.at[rnd])

    def stage(self, rnd, k):
        units = (0, 1)
        if k == 0:
            for u in units:
                self.scatter_start(rnd, u, 0)
        elif k == 1:
            for u in units:
                self.mid[rnd, u] = self.scatter_end(rnd, u, 0)
                self.scatter_start(rnd, u, 1)
        elif k == 2:
            for u in units:
                total = self.scatter_end(rnd, u, 1)
                for j in range(5):
                    self.z_src[rnd, u * 5 + j] = total[:, j * 128:(j + 1) * 128]
            self.z_src[rnd, pl.ds(10, 6)] = jnp.zeros((6, 8, 128), F32)
            for copy in self.z_copies(rnd, 0)[0]:
                copy.start()
        elif k == 3:
            self.z_wait(rnd, 0)
            copies, mine = self.z_copies(rnd, 1)
            total = self.z_src[rnd, mine]
            for d in range(self.links.depth - 1):
                total = total + self.z_recv[rnd, d]
            self.z_out[rnd, mine] = total
            for copy in copies:
                copy.start()
        elif k == 4:
            self.z_wait(rnd, 1)
            for u in units:
                first = self.block(rnd, u, 1)[0] + self.links.pos[self.axes(rnd, u)[1]] * 8
                for j in range(5):
                    self.out[pl.ds(pl.multiple_of(first, 8), 8), pl.ds(j * 128, 128)] = self.z_out[rnd, u * 5 + j]
                self.gather_start(rnd, u, 1)
        elif k == 5:
            for u in units:
                self.wait_all(rnd, u, 1, self.ag_sems)
                self.gather_start(rnd, u, 0)
        elif k == 6:
            for u in units:
                self.wait_all(rnd, u, 0, self.ag_sems)
            self.swap(rnd).start()
        else:
            self.swap(rnd).wait()
            self.store(rnd)


def layer_norm(x_ref, rows):
    x_f = x_ref[rows].astype(F32)
    centered = x_f - jnp.mean(x_f, axis=-1, keepdims=True)
    inv_std = lax.rsqrt(jnp.mean(centered * centered, axis=-1, keepdims=True) + LN_EPS)
    return centered * inv_std, inv_std


def padded(parts, rows):
    filled = [part.astype(F32) for part in parts]
    used = sum(part.shape[0] for part in filled)
    return jnp.concatenate(filled + [jnp.zeros((rows - used, filled[0].shape[1]), F32)], axis=0).astype(BF)


def block_body(dim, depth, x_hbm, dy_hbm, wq_hbm, wk_hbm, wv_hbm, wo_hbm, gamma_ref, beta_ref, bo_ref,
               y_ref, gx_ref, dq_ref, dk_ref, dv_ref, dwo_ref, small_ref,
               x_s, normed_s, dy_s, wt_s, wo_s, q_s, k_s, v_s, do_s, o_s, of_s, o_peer, lse_s, kf_s, vf_s, buf_a, buf_b, buf_c,
               kb_s, vb_s, dk_acc, dv_acc, grads, grads_peer, d_w, d_w_all, dx_s, y_s,
               recv1, recv2, mid, z_src, z_recv, z_out, small_s, small_recv,
               load_sems, in_send, in_recv, pass_send, pass_recv, o_sems, grad_sems, out_send, out_recv, small_sems,
               rs_sems, ag_sems, z_sems, swap_sems, store_sems):
    links = Links(depth)
    width, tokens = q_s.shape
    heads, tiles = width // dim, tokens // KEY_TILE
    own, band = tokens // 2, tokens // 4
    scale = dim ** -0.5
    log2_scale = scale * math.log2(math.e)
    fwd_group, bwd_group = tiles, 4
    fwd_steps, bwd_steps = tiles // fwd_group, tiles // bwd_group
    zero = jnp.minimum(links.x, 0)
    gamma, beta, bias = (ref[...].reshape(1, ref.shape[0]) for ref in (gamma_ref, beta_ref, bo_ref))
    odd = lax.rem(links.x, 2)
    reduce = GradReduce(links, dim, d_w, d_w_all, (dwo_ref, dq_ref, dk_ref, dv_ref), (recv1, recv2, mid, z_src, z_recv, z_out),
                        (rs_sems, ag_sems, z_sems, swap_sems, store_sems))
    end = heads * bwd_steps + 1
    plan = {}
    for rnd in range(ROUNDS):
        at = rnd * bwd_steps + 1 if rnd else 0
        for k in range(STAGES):
            at += min(k, 1) + ((rnd, k) in SPARE)
            plan.setdefault(at, []).append((rnd, k))
    for at in plan:
        plan[at].sort(key=lambda item: (item[1] in (0, 5) and item[0] < ROUNDS - 1, -item[0]))
    slots = max(plan) + 1 - end

    def tile_rows(tile, base=None):
        return pl.ds(tile * KEY_TILE if base is None else pl.multiple_of(base + tile * KEY_TILE, KEY_TILE), KEY_TILE)

    def head_rows(head, rows=dim):
        return pl.ds(pl.multiple_of(head * rows, 16), rows)

    def q_cols(index):
        return pl.ds(pl.multiple_of(index * Q_BLOCK, Q_BLOCK), Q_BLOCK)

    def my_half(side):
        return pl.ds(pl.multiple_of((links.core if side == 0 else 1 - links.core) * width, 16), width)

    loads = [pltpu.make_async_copy(w_hbm.at[my_half(side)], wt_s.at[side, pl.ds(k * width, width)], load_sems.at[side, k])
             for side in range(2) for k, w_hbm in enumerate((wq_hbm, wk_hbm, wv_hbm))]
    loads += [pltpu.make_async_copy(wo_hbm.at[my_half(side)], wo_s.at[side], load_sems.at[side, 3]) for side in range(2)]

    def maybe_far(place, source, target, send, recv):
        core, x = place
        here = links.is_self(place)
        far = remote(source, target, send, recv, links.at(core=core, x=x))
        near = pltpu.make_async_copy(source, target, recv)

        @pl.when(jnp.logical_not(here))
        def _():
            far.start()

        @pl.when(here)
        def _():
            near.start()

    def all_left(ref, sem):
        rows = ref.shape[0]
        halved = links.x // 2 == links.core

        @pl.when(jnp.logical_not(halved))
        def _():
            wait_for(ref, sem)

        @pl.when(halved)
        def _():
            wait_for(ref.at[pl.ds(0, rows // 2)], sem)

    piece = band // PIECES

    def deliver(which, m, c):
        slot = lax.rem(links.x + m, 2)
        source = (dy_hbm if which else x_hbm).at[m, pl.ds(c * piece, piece)]
        target = (dy_s if which else x_s).at[pl.ds(pl.multiple_of(slot * band + c * piece, 16), piece)]
        maybe_far(links.workers[m], source, target, in_send.at[which], in_recv.at[which, slot, c])

    def hand_over(which, slot, c):
        rows = dy_s if which else x_s
        first = slot * band + c * piece
        return remote(rows.at[pl.ds(first, piece)], rows.at[pl.ds(own + first, piece)],
                      pass_send.at[which], pass_recv.at[which, slot, c], links.peer)

    def arrive(which, slot, c):
        with jax.named_scope(f'arrive{which}{slot}{c}'):
            wait_for((dy_s if which else x_s).at[pl.ds(slot * band + c * piece, piece)], in_recv.at[which, slot, c])
        hand_over(which, slot, c).start()

    def swap_out(head):
        rows = head_rows(head)
        return remote(o_s.at[rows, pl.ds(own, own)], o_peer.at[rows], o_sems.at[0, head], o_sems.at[1, head], links.peer)

    def swap_grads(head):
        rows = head_rows(head)
        return remote(grads.at[:, rows, pl.ds(own, own)], grads_peer.at[:, rows], grad_sems.at[0, head], grad_sems.at[1, head],
                      links.peer)

    part = band // 2
    portion = own // SENDS

    def send_home(which, i):
        cut = SENDS // 2
        second, inner = i // cut, lax.rem(i, cut)
        source = (dx_s if which else y_s).at[pl.ds(pl.multiple_of(i * portion, 16), portion)]
        target = (gx_ref if which else y_ref).at[odd, pl.ds(pl.multiple_of(inner * portion, 16), portion)]
        (core, x0), (_, x1) = links.owners
        maybe_far((core, jnp.where(second == 0, x0, x1)), source, target, out_send.at[which], out_recv.at[which])

    barrier = pltpu.get_barrier_semaphore()
    fixed = [links.peer]
    fixed += [links.step(axis, d) for axis in ('x', 'y') for d in range(1, RING)]
    fixed += [links.step('z', d) for d in range(1, depth)]
    for device in fixed:
        pl.semaphore_signal(barrier, inc=1, device_id=device, device_id_type=MESH)
    count = len(fixed)
    for place in links.owners + links.workers:
        other = jnp.logical_not(links.is_self(place))
        count = count + other.astype(jnp.int32)

        @pl.when(other)
        def _():
            pl.semaphore_signal(barrier, inc=1, device_id=links.at(core=place[0], x=place[1]), device_id_type=MESH)
    for load in loads:
        load.start()
    with jax.named_scope('barrier'):
        pl.semaphore_wait(barrier, count)
    for c in range(PIECES):
        for m in range(2):
            deliver(0, m, c)
    for load in loads:
        load.wait()

    def normalize(first):
        rows = pl.ds(first, piece)
        normed_s[rows] = (layer_norm(x_s, rows)[0] * gamma + beta).astype(BF)

    def project(b, c):
        cols = pl.ds(b * band + (c - 2) * piece, 2 * piece)
        normed = normed_s[cols]
        for k, out in enumerate((q_s, k_s, v_s)):
            out[:, cols] = dot_nt(wt_s[0, pl.ds(k * width, width)], normed).astype(BF)

    for c in range(PIECES + 1):
        if c < PIECES:
            for slot in range(2):
                arrive(0, slot, c)
            if c == PIECES - 1:
                for i in range(PIECES):
                    for m in range(2):
                        deliver(1, m, i)
            for slot in range(2):
                normalize(slot * band + c * piece)
        if c:
            if c % 2 == 0:
                project(0, c)
                project(1, c)
            for slot in range(2):
                with jax.named_scope(f'handed{slot}{c}'):
                    hand_over(0, slot, c - 1).wait_recv()
                normalize(own + slot * band + (c - 1) * piece)
                if c % 2 == 0:
                    project(2 + slot, c)

    def forward_step(now, carry):
        head, step = now // fwd_steps, lax.rem(now, fwd_steps)
        rows = head_rows(head)
        for c in range(PIECES):
            @pl.when(now == max(c, 1))
            def _():
                for slot in range(2):
                    arrive(1, slot, c)

        @pl.when(step == 0)
        def _():
            k_t = k_s[rows]
            kf_s[...] = jnp.concatenate([k_t, k_t, k_t], axis=0).T
            vf_s[0:dim] = v_s[rows]
            vf_s[dim:] = padded([jnp.ones((1, tokens), F32)], AUG - dim)

        bufs = (buf_a, buf_b, buf_c)
        total, lag = tiles * fwd_group, tiles + 2
        query, high, top, probs, out = {}, {}, {}, {}, {}
        for g in range(total + lag + 2):
            if g < total:
                i, t = divmod(g, tiles)
                if t == 0:
                    query[i] = jnp.concatenate(split_parts(q_s[rows, q_cols(step * fwd_group + i)].astype(F32) * log2_scale), axis=0)
                scores = dot_nn(kf_s[tile_rows(t)], query[i])
                bufs[i % 3][tile_rows(t)] = scores
                folded = fold_rows(scores, jnp.maximum)
                high[i] = folded if t == 0 else jnp.maximum(high[i], folded)
                if t == tiles - 1:
                    top[i] = jnp.max(high[i], axis=0, keepdims=True)
            if lag <= g < total + lag:
                i, t = divmod(g - lag, tiles)
                probs[g - lag] = jnp.exp2(bufs[i % 3][tile_rows(t, zero)] - top[i]).astype(BF)
            if g >= lag + 2:
                i, t = divmod(g - lag - 2, tiles)
                product = dot_nn(vf_s[:, tile_rows(t)], probs[g - lag - 2])
                out[i] = product if t == 0 else out[i] + product
                if t == tiles - 1:
                    cols = q_cols(step * fwd_group + i)
                    denom = out[i][dim:dim + 1]
                    value = out[i][:dim] * (1.0 / denom)
                    o_s[rows, cols] = value.astype(BF)
                    of_s[rows, cols] = value
                    lse = (top[i] + jnp.log2(denom)) * (1.0 / log2_scale)
                    lse_s[head_rows(head, 16), cols] = padded(split_parts(lse), 16)

        @pl.when(step == fwd_steps - 1)
        def _():
            swap_out(head).start()

        return carry

    lax.fori_loop(0, heads * fwd_steps, forward_step, 0)
    with jax.named_scope('dyhanded'):
        for c in range(PIECES):
            for slot in range(2):
                hand_over(1, slot, c).wait_recv()
    d_w[pl.ds(0, width)] = dot_nn(o_s[...], dy_s[...])
    for rnd, k in plan[0]:
        reduce.stage(rnd, k)
    with jax.named_scope('oswap'):
        for head in range(heads):
            swap_out(head).wait()
    for i in range(4):
        toks = pl.ds(i * part, part)
        product = dot_tn(o_s[:, toks], wo_s[0]) + dot_tn(o_peer[:, toks], wo_s[1])
        y_s[toks] = (x_s[toks].astype(F32) + product + bias).astype(BF)
    for i in range(tiles):
        cols = pl.ds(i * KEY_TILE, KEY_TILE)
        do_s[:, cols] = dot_nt(wo_s[0], dy_s[cols]).astype(BF)
    for which in range(2):
        rows = (dy_s if which else x_s).at[pl.ds(0, own)]
        all_left(rows, in_send.at[which])
        wait_for(rows, pass_send.at[which])

    def backward_step(now, carry):
        head, step = now // bwd_steps, lax.rem(now, bwd_steps)
        rows = head_rows(head)
        for at in range(end - 1):
            todo = plan.get(at + 1)
            if todo:
                @pl.when(now == at)
                def _():
                    with jax.named_scope(f'step{at}'):
                        for rnd, k in todo:
                            reduce.stage(rnd, k)
        share = SENDS // (heads * bwd_steps)
        for i in range(share):
            send_home(0, now * share + i)

        @pl.when(step == 0)
        def _():
            minus = padded([jnp.full((3, tokens), -1.0, F32)], AUG - dim)
            kb_s[...] = jnp.concatenate([k_s[rows], minus], axis=0).T
            vb_s[...] = jnp.concatenate([v_s[rows], minus], axis=0).T
            dk_acc[...] = jnp.zeros_like(dk_acc)
            dv_acc[...] = jnp.zeros_like(dv_acc)

        total = tiles * bwd_group
        ops, probs, d_scores, dq = {}, {}, {}, {}
        for g in range(total + 2):
            if g < total:
                i, t = divmod(g, tiles)
                if t == 0:
                    cols = q_cols(step * bwd_group + i)
                    q_t, do_t = q_s[rows, cols], do_s[rows, cols]
                    delta = jnp.sum(of_s[rows, cols] * do_t.astype(F32), axis=0, keepdims=True)
                    ops[i] = (cols, q_t, do_t, jnp.concatenate([q_t, lse_s[head_rows(head, 16), cols]], axis=0),
                              jnp.concatenate([do_t, padded(split_parts(delta), 16)], axis=0))
                scores = dot_nn(kb_s[tile_rows(t)], ops[i][3])
                d_probs = dot_nn(vb_s[tile_rows(t)], ops[i][4])
                prob = jnp.exp2(scores * log2_scale)
                probs[g] = prob.astype(BF)
                d_scores[g] = (prob * d_probs).astype(BF)
            if g >= 2:
                i, t = divmod(g - 2, tiles)
                cols, q_t, do_t = ops[i][:3]
                dv_acc[:, tile_rows(t)] += dot_nt(do_t, probs[g - 2])
                product = dot_nn(k_s[rows, tile_rows(t)], d_scores[g - 2])
                dq[i] = product if t == 0 else dq[i] + product
                if t == tiles - 1:
                    grads[0, rows, cols] = (dq[i] * scale).astype(BF)
                dk_acc[:, tile_rows(t)] += dot_nt(q_t, d_scores[g - 2])

        @pl.when(step == bwd_steps - 1)
        def _():
            grads[1, rows] = (dk_acc[...] * scale).astype(BF)
            grads[2, rows] = dv_acc[...].astype(BF)
            swap_grads(head).start()
            stacked = jnp.concatenate([grads[0, rows], grads[1, rows], grads[2, rows]], axis=0)
            d_w[pl.ds(pl.multiple_of(width + head * (3 * dim), 8), 3 * dim)] = dot_nn(stacked, normed_s[...])

        return carry

    lax.fori_loop(0, heads * bwd_steps, backward_step, 0)

    def tail(slot):
        for rnd, k in plan.get(end + slot, ()):
            with jax.named_scope(f'tail{slot}r{rnd}k{k}'):
                reduce.stage(rnd, k)

    tail(0)
    with jax.named_scope('gradswap'):
        for head in range(heads):
            swap_grads(head).wait()
    sums = [jnp.zeros((1, 640), F32)] * 3
    for i in range(4):
        toks = pl.ds(i * part, part)
        mine = jnp.concatenate([grads[k, :, toks] for k in range(3)], axis=0)
        theirs = jnp.concatenate([grads_peer[k, :, toks] for k in range(3)], axis=0)
        d_normed = (dot_tn(mine, wt_s[0]) + dot_tn(theirs, wt_s[1])).astype(BF).astype(F32)
        x_hat, inv_std = layer_norm(x_s, toks)
        d_hat = d_normed * gamma
        mean_one = jnp.mean(d_hat, axis=-1, keepdims=True)
        mean_two = jnp.mean(d_hat * x_hat, axis=-1, keepdims=True)
        dy_f = dy_s[toks].astype(F32)
        dx_s[toks] = (dy_f + inv_std * (d_hat - mean_one - x_hat * mean_two)).astype(BF)
        for k, term in enumerate((d_normed * x_hat, d_normed, dy_f)):
            sums[k] = sums[k] + jnp.sum(term, axis=0, keepdims=True)

    for k in range(3):
        for j in range(5):
            small_s[0, pl.ds(k * 5 + j, 1)] = sums[k][:, j * 128:(j + 1) * 128]
    small_s[0, pl.ds(15, 1)] = jnp.zeros((1, 128), F32)
    small_copy = pltpu.make_async_copy(small_s.at[0], small_ref, load_sems.at[0, 0])
    first, waiting = 0, None
    for hop, axis in enumerate(('z', 'y', 'core', 'x', '')):
        if not axis:
            for slot in range(5, slots):
                tail(slot)
        if waiting:
            acc = small_s[hop - 1]
            with jax.named_scope(f'small{hop}'):
                for copy in waiting:
                    copy.wait_recv()
            for d in range(len(waiting)):
                acc = acc + small_recv[first + d]
            for copy in waiting:
                copy.wait_send()
            if axis:
                small_s[hop] = acc
            else:
                small_s[0] = acc
                small_copy.start()
            first += len(waiting)
        elif hop:
            small_s[hop] = small_s[hop - 1]
        if axis:
            far = [links.peer] if axis == 'core' else [links.step(axis, d) for d in range(1, links.size[axis])]
            waiting = [remote(small_s.at[hop], small_recv.at[first + d], small_sems.at[0, first + d], small_sems.at[1, first + d],
                              device) for d, device in enumerate(far)]
            for copy in waiting:
                copy.start()
            tail(1 + hop)
            if hop == 0:
                for i in range(SENDS):
                    send_home(1, i)
    with jax.named_scope('home'):
        for which in range(2):
            all_left(dx_s if which else y_s, out_send.at[which])
            wait_for(gx_ref if which else y_ref, out_recv.at[which])
    with jax.named_scope('stored'):
        for rnd in range(ROUNDS):
            reduce.stored(rnd)
    small_copy.wait()


def attention_block(x_in, grad_y, weights, vectors, dim, depth):
    rows, channels = x_in.shape[1:]
    tokens, own = 4 * rows, 2 * rows
    width = weights[0].shape[0] // 2
    heads = width // dim
    total = 4 * width
    half = lambda *shape: pltpu.VMEM(shape, BF)
    full = lambda *shape: pltpu.VMEM(shape, F32)
    dma = lambda *shape: pltpu.SemaphoreType.DMA(shape)
    anywhere = pl.BlockSpec(memory_space=pl.ANY)
    in_vmem = pl.BlockSpec(memory_space=pltpu.VMEM)
    far = max(depth - 1, 1)
    return pl.pallas_call(
        functools.partial(block_body, dim, depth),
        in_specs=[anywhere] * 6 + [in_vmem] * 3,
        out_specs=[anywhere] * 7,
        out_shape=[jax.ShapeDtypeStruct(x_in.shape, BF)] * 2
        + [jax.ShapeDtypeStruct(weights[0].shape, F32)] * 4 + [jax.ShapeDtypeStruct((16, 128), F32)],
        scratch_shapes=[half(tokens, channels)] * 3 + [half(2, 3 * width, channels), half(2, width, channels)]
        + [half(width, tokens)] * 5 + [full(width, tokens), half(width, own), half(16 * heads, tokens),
                                       half(tokens, 3 * dim), half(AUG, tokens)]
        + [full(tokens, Q_BLOCK)] * 3 + [half(tokens, AUG)] * 2 + [full(dim, tokens)] * 2
        + [half(3, width, tokens), half(3, width, own), full(total, channels), full(2, total, channels)]
        + [half(own, channels)] * 2
        + [full(ROUNDS, 2, 3, 32, channels), full(ROUNDS, 2, 3, 8, channels), full(ROUNDS, 2, 32, channels), full(ROUNDS, 16, 8, 128),
           full(ROUNDS, far, 16 // depth, 8, 128), full(ROUNDS, 16, 8, 128), full(4, 16, 128), full(7 + far, 16, 128),
           dma(2, 4)] + [dma(2), dma(2, 2, PIECES)] * 2 + [dma(2, heads)] * 2
        + [dma(2), dma(2), dma(2, 7 + far)] + [dma(2, ROUNDS, 2, 2)] * 2 + [dma(2, ROUNDS, 2), dma(2, ROUNDS), dma(ROUNDS)],
        compiler_params=pltpu.CompilerParams(collective_id=0, has_side_effects=True, vmem_limit_bytes=VMEM_BYTES),
        name='attention_block',
    )(x_in, grad_y, *weights, *vectors)


def settle_body(count, small_hbm, *refs):
    sources, targets, refs = refs[:count], refs[count:2 * count], refs[2 * count:]
    vectors, bufs, (small, vector_s, sems, vector_sems) = refs[:3], refs[3:3 + count], refs[3 + count:]
    load = pltpu.make_async_copy(small_hbm, small, vector_sems.at[3])
    load.start()
    cuts = []
    for i, (source, target, buf) in enumerate(zip(sources, targets, bufs)):
        rows = source.shape[0] // CUTS
        for c in range(CUTS):
            part = pl.ds(c * rows, rows)
            cuts.append((pltpu.make_async_copy(source.at[part], buf.at[part], sems.at[0, i, c]),
                         pltpu.make_async_copy(buf.at[part], target.at[part], sems.at[1, i, c])))
    for read, _ in cuts:
        read.start()
    load.wait()
    stores = []
    for k, vector in enumerate(vectors):
        vector_s[k][...] = jnp.concatenate([small[k * 5 + j:k * 5 + j + 1] for j in range(5)], axis=1).reshape(vector.shape)
        stores.append(pltpu.make_async_copy(vector_s[k], vector, vector_sems.at[k]))
        stores[k].start()
    for read, write in cuts:
        read.wait()
        write.start()
    for _, write in cuts:
        write.wait()
    for store in stores:
        store.wait()


def settle(small, arrays):
    anywhere = pl.BlockSpec(memory_space=pl.ANY)
    count = len(arrays)
    dma = pltpu.SemaphoreType.DMA
    vector = (arrays[0].shape[1],)
    return pl.pallas_call(
        functools.partial(settle_body, count),
        in_specs=[anywhere] * (count + 1), out_specs=[anywhere] * (count + 3),
        out_shape=[jax.ShapeDtypeStruct(a.shape, a.dtype) for a in arrays] + [jax.ShapeDtypeStruct(vector, F32)] * 3,
        scratch_shapes=[pltpu.VMEM(a.shape, a.dtype) for a in arrays]
        + [pltpu.VMEM(small.shape, F32), [pltpu.VMEM(vector, F32)] * 3, dma((2, count, CUTS)), dma((4,))],
        compiler_params=pltpu.CompilerParams(vmem_limit_bytes=VMEM_BYTES),
        name='settle',
    )(small, *arrays)


def solution(mesh):
    depth = mesh.shape['dp'] // (2 * RING)
    act_spec, rep_spec = P('dp', 'cp', None), P()

    def device_step(x_in, grad_y, ln_gamma, ln_beta, w_q, w_k, w_v, w_o, b_o):
        channels, num_heads, head_dim = w_q.shape
        flat = (num_heads * head_dim, channels)
        weights = [jnp.transpose(w, (1, 2, 0)).reshape(flat) for w in (w_q, w_k, w_v)] + [w_o.reshape(flat)]
        y_out, grad_x, *grads, grad_wo, small = attention_block(x_in, grad_y, weights, (ln_gamma, ln_beta, b_o), head_dim, depth)
        rows = (2 * y_out.shape[1], channels)
        moved = settle(small, [y_out.reshape(rows), grad_x.reshape(rows), *grads, grad_wo])
        y_out, grad_x = (a.reshape(x_in.shape) for a in moved[:2])
        grads, grad_wo = moved[2:5], moved[5]
        grads = [jnp.transpose(grad.reshape(num_heads, head_dim, channels), (2, 0, 1)) for grad in grads]
        return (y_out, grad_x, moved[6], moved[7], *grads, grad_wo.reshape(num_heads, head_dim, channels), moved[8])

    specs = (act_spec, act_spec) + (rep_spec,) * 7
    return jax.shard_map(device_step, mesh=mesh, in_specs=specs, out_specs=specs, check_vma=False)
```

```python
import functools
import math
import jax
import jax.numpy as jnp
from jax import lax
from jax.experimental import pallas as pl
from jax.experimental.pallas import tpu as pltpu
from jax.sharding import PartitionSpec as P

LN_EPS = 1e-5
KEY_TILE = 256
Q_BLOCK = 256
FOLD = 16
AUG = 96
VMEM_BYTES = 67043328
BF = jnp.bfloat16
F32 = jnp.float32


def dot_nn(lhs, rhs):
    return lax.dot_general(lhs, rhs, (((1,), (0,)), ((), ())), preferred_element_type=F32)


def dot_nt(lhs, rhs):
    return lax.dot_general(lhs, rhs, (((1,), (1,)), ((), ())), preferred_element_type=F32)


def dot_tn(lhs, rhs):
    return lax.dot_general(lhs, rhs, (((0,), (0,)), ((), ())), preferred_element_type=F32)


def split_parts(value):
    high = value.astype(BF)
    rest = value - high.astype(F32)
    mid = rest.astype(BF)
    return high, mid, (rest - mid.astype(F32)).astype(BF)


def fold_rows(value, op):
    groups = value.reshape(value.shape[0] // FOLD, FOLD, value.shape[1])
    out = groups[0]
    for i in range(1, groups.shape[0]):
        out = op(out, groups[i])
    return out


MESH = pl.DeviceIdType.MESH
RING = 4
ROUNDS = 5
ROUND_ROWS = 256
STAGES = 8
SPARE = ((0, 1), (1, 1), (2, 1), (3, 1), (0, 6), (1, 5), (1, 6), (2, 6), (2, 6), (3, 5))
PIECES = 4
SENDS = 16
CUTS = 4
ORDER = ('yx', 'yy', 'yy', 'yx', 'yx')


class Links:
    def __init__(self, depth):
        dp, self.x = lax.axis_index('dp'), lax.axis_index('cp')
        self.core = lax.rem(dp, 2)
        self.y = lax.rem(dp // 2, RING)
        self.z = dp // (2 * RING)
        self.depth = depth
        self.pos = {'x': self.x, 'y': self.y, 'z': self.z}
        self.size = {'x': RING, 'y': RING, 'z': depth}
        self.peer = self.at(core=1 - self.core)
        pair, odd = self.x // 2, lax.rem(self.x, 2)
        self.owners = [(pair, 2 * self.core + odd), (pair, 2 * self.core + 1 - odd)]
        self.workers = [(pair, 2 * self.core), (pair, 2 * self.core + 1)]

    def at(self, x=None, y=None, z=None, core=None):
        pick = lambda value, own: own if value is None else value
        return ((pick(z, self.z) * RING + pick(y, self.y)) * 2 + pick(core, self.core), pick(x, self.x))

    def step(self, axis, d):
        return self.at(**{axis: lax.rem(self.pos[axis] + d, self.size[axis])})

    def is_self(self, place):
        return jnp.logical_and(place[0] == self.core, place[1] == self.x)


def remote(source, target, send, recv, device):
    return pltpu.make_async_remote_copy(src_ref=source, dst_ref=target, send_sem=send, recv_sem=recv,
                                        device_id=device, device_id_type=MESH)


def wait_for(ref, sem):
    pltpu.make_async_copy(ref, ref, sem).wait()


class GradReduce:
    def __init__(self, links, dim, grad, out, results, bufs, sems):
        self.links, self.grad, self.both, self.out = links, grad, out, out.at[links.core]
        width = grad.shape[0] // 4
        self.pieces = [(0, width, results[0], 0)]
        self.pieces += [(width + (3 * head + k) * dim, dim, results[1 + k], head * dim) for head in range(width // dim) for k in range(3)]
        self.recv1, self.recv2, self.mid, self.z_src, self.z_recv, self.z_out = bufs
        self.rs_sems, self.ag_sems, self.z_sems, self.swap_sems, self.store_sems = sems

    def axes(self, rnd, unit):
        first = ORDER[rnd][unit]
        return first, ('x' if first == 'y' else 'y')

    def block(self, rnd, unit, phase):
        first = rnd * ROUND_ROWS + unit * 128
        if phase == 0:
            return first, 32
        return first + self.links.pos[self.axes(rnd, unit)[0]] * 32, 8

    def landing(self, rnd, unit, phase):
        return (self.recv1 if phase == 0 else self.recv2).at[rnd, unit]

    def wait_all(self, rnd, unit, phase, sems):
        whole = self.landing(rnd, unit, phase)
        every = remote(whole, whole, sems.at[0, rnd, unit, phase], sems.at[1, rnd, unit, phase], self.links.peer)
        every.wait_recv()
        every.wait_send()

    def source(self, rnd, unit, phase, owner):
        if phase == 0:
            first, rows = self.block(rnd, unit, 0)
            return self.grad.at[pl.ds(pl.multiple_of(first + owner * rows, 8), rows)]
        return self.mid.at[rnd, unit, pl.ds(pl.multiple_of(owner * 8, 8), 8)]

    def scatter_start(self, rnd, unit, phase):
        axis = self.axes(rnd, unit)[phase]
        for d in (2, 1, 3):
            owner = lax.rem(self.links.pos[axis] + d, RING)
            remote(self.source(rnd, unit, phase, owner), self.landing(rnd, unit, phase).at[d - 1],
                   self.rs_sems.at[0, rnd, unit, phase], self.rs_sems.at[1, rnd, unit, phase], self.links.step(axis, d)).start()

    def scatter_end(self, rnd, unit, phase):
        self.wait_all(rnd, unit, phase, self.rs_sems)
        landing = self.landing(rnd, unit, phase)
        mine = self.source(rnd, unit, phase, self.links.pos[self.axes(rnd, unit)[phase]])
        return (mine[...] + landing[0]) + (landing[1] + landing[2])

    def gather_start(self, rnd, unit, phase):
        axis = self.axes(rnd, unit)[phase]
        first, rows = self.block(rnd, unit, phase)
        part = self.out.at[pl.ds(pl.multiple_of(first + self.links.pos[axis] * rows, 8), rows)]
        for d in (2, 1, 3):
            remote(part, part, self.ag_sems.at[0, rnd, unit, phase], self.ag_sems.at[1, rnd, unit, phase],
                   self.links.step(axis, d)).start()

    def z_copies(self, rnd, way):
        links = self.links
        each = 16 // links.depth
        send, recv = self.z_sems.at[0, rnd, way], self.z_sems.at[1, rnd, way]
        mine = pl.ds(links.z * each, each)
        copies = []
        for d in range(1, links.depth):
            far = lax.rem(links.z + d, links.depth)
            if way == 0:
                source, target = self.z_src.at[rnd, pl.ds(far * each, each)], self.z_recv.at[rnd, d - 1]
            else:
                source = target = self.z_out.at[rnd, mine]
            copies.append(remote(source, target, send, recv, links.step('z', d)))
        return copies, mine

    def z_wait(self, rnd, way):
        if self.links.depth > 1:
            whole = self.z_recv.at[rnd]
            all_of = remote(whole, whole, self.z_sems.at[0, rnd, way], self.z_sems.at[1, rnd, way], self.links.step('z', 1))
            all_of.wait_recv()
            all_of.wait_send()

    def swap(self, rnd):
        part = self.out.at[pl.ds(rnd * ROUND_ROWS, ROUND_ROWS)]
        return remote(part, part, self.swap_sems.at[0, rnd], self.swap_sems.at[1, rnd], self.links.peer)

    def store(self, rnd):
        begin = rnd * ROUND_ROWS
        half = self.both.shape[1] // 4
        for first, rows, result, place in self.pieces:
            low, high = max(first, begin), min(first + rows, begin + ROUND_ROWS)
            for core in range(2):
                if low < high:
                    target = result.at[pl.ds(core * half + place + low - first, high - low)]
                    pltpu.make_async_copy(self.both.at[core, pl.ds(low, high - low)], target, self.store_sems.at[rnd]).start()

    def stored(self, rnd):
        wait_for(self.both.at[:, pl.ds(rnd * ROUND_ROWS, ROUND_ROWS)], self.store_sems.at[rnd])

    def stage(self, rnd, k):
        units = (0, 1)
        if k == 0:
            for u in units:
                self.scatter_start(rnd, u, 0)
        elif k == 1:
            for u in units:
                self.mid[rnd, u] = self.scatter_end(rnd, u, 0)
                self.scatter_start(rnd, u, 1)
        elif k == 2:
            for u in units:
                total = self.scatter_end(rnd, u, 1)
                for j in range(5):
                    self.z_src[rnd, u * 5 + j] = total[:, j * 128:(j + 1) * 128]
            self.z_src[rnd, pl.ds(10, 6)] = jnp.zeros((6, 8, 128), F32)
            for copy in self.z_copies(rnd, 0)[0]:
                copy.start()
        elif k == 3:
            self.z_wait(rnd, 0)
            copies, mine = self.z_copies(rnd, 1)
            total = self.z_src[rnd, mine]
            for d in range(self.links.depth - 1):
                total = total + self.z_recv[rnd, d]
            self.z_out[rnd, mine] = total
            for copy in copies:
                copy.start()
        elif k == 4:
            self.z_wait(rnd, 1)
            for u in units:
                first = self.block(rnd, u, 1)[0] + self.links.pos[self.axes(rnd, u)[1]] * 8
                for j in range(5):
                    self.out[pl.ds(pl.multiple_of(first, 8), 8), pl.ds(j * 128, 128)] = self.z_out[rnd, u * 5 + j]
                self.gather_start(rnd, u, 1)
        elif k == 5:
            for u in units:
                self.wait_all(rnd, u, 1, self.ag_sems)
                self.gather_start(rnd, u, 0)
        elif k == 6:
            for u in units:
                self.wait_all(rnd, u, 0, self.ag_sems)
            self.swap(rnd).start()
        else:
            self.swap(rnd).wait()
            self.store(rnd)


def layer_norm(x_ref, rows):
    x_f = x_ref[rows].astype(F32)
    centered = x_f - jnp.mean(x_f, axis=-1, keepdims=True)
    inv_std = lax.rsqrt(jnp.mean(centered * centered, axis=-1, keepdims=True) + LN_EPS)
    return centered * inv_std, inv_std


def padded(parts, rows):
    filled = [part.astype(F32) for part in parts]
    used = sum(part.shape[0] for part in filled)
    return jnp.concatenate(filled + [jnp.zeros((rows - used, filled[0].shape[1]), F32)], axis=0).astype(BF)


def block_body(dim, depth, x_hbm, dy_hbm, wq_hbm, wk_hbm, wv_hbm, wo_hbm, gamma_ref, beta_ref, bo_ref,
               y_ref, gx_ref, dq_ref, dk_ref, dv_ref, dwo_ref, small_ref,
               x_s, normed_s, dy_s, wt_s, wo_s, q_s, k_s, v_s, do_s, o_s, of_s, o_peer, lse_s, kf_s, vf_s, buf_a, buf_b, buf_c,
               kb_s, vb_s, dk_acc, dv_acc, grads, grads_peer, d_w, d_w_all, dx_s, y_s,
               recv1, recv2, mid, z_src, z_recv, z_out, small_s, small_recv,
               load_sems, in_send, in_recv, pass_send, pass_recv, o_sems, grad_sems, out_send, out_recv, small_sems,
               rs_sems, ag_sems, z_sems, swap_sems, store_sems):
    links = Links(depth)
    width, tokens = q_s.shape
    heads, tiles = width // dim, tokens // KEY_TILE
    own, band = tokens // 2, tokens // 4
    scale = dim ** -0.5
    log2_scale = scale * math.log2(math.e)
    fwd_group, bwd_group = tiles, 4
    fwd_steps, bwd_steps = tiles // fwd_group, tiles // bwd_group
    zero = jnp.minimum(links.x, 0)
    gamma, beta, bias = (ref[...].reshape(1, ref.shape[0]) for ref in (gamma_ref, beta_ref, bo_ref))
    odd = lax.rem(links.x, 2)
    reduce = GradReduce(links, dim, d_w, d_w_all, (dwo_ref, dq_ref, dk_ref, dv_ref), (recv1, recv2, mid, z_src, z_recv, z_out),
                        (rs_sems, ag_sems, z_sems, swap_sems, store_sems))
    end = heads * bwd_steps + 1
    plan = {}
    for rnd in range(ROUNDS):
        at = rnd * bwd_steps + 1 if rnd else 0
        for k in range(STAGES):
            at += min(k, 1) + SPARE.count((rnd, k))
            plan.setdefault(at, []).append((rnd, k))
    for at in plan:
        plan[at].sort(key=lambda item: (item[1] in (0, 5) and item[0] < ROUNDS - 1, -item[0]))
    slots = max(plan) + 1 - end

    def tile_rows(tile, base=None):
        return pl.ds(tile * KEY_TILE if base is None else pl.multiple_of(base + tile * KEY_TILE, KEY_TILE), KEY_TILE)

    def head_rows(head, rows=dim):
        return pl.ds(pl.multiple_of(head * rows, 16), rows)

    def q_cols(index):
        return pl.ds(pl.multiple_of(index * Q_BLOCK, Q_BLOCK), Q_BLOCK)

    def my_half(side):
        return pl.ds(pl.multiple_of((links.core if side == 0 else 1 - links.core) * width, 16), width)

    loads = [pltpu.make_async_copy(w_hbm.at[my_half(side)], wt_s.at[side, pl.ds(k * width, width)], load_sems.at[side, k])
             for side in range(2) for k, w_hbm in enumerate((wq_hbm, wk_hbm, wv_hbm))]
    loads += [pltpu.make_async_copy(wo_hbm.at[my_half(side)], wo_s.at[side], load_sems.at[side, 3]) for side in range(2)]

    def maybe_far(place, source, target, send, recv):
        core, x = place
        here = links.is_self(place)
        far = remote(source, target, send, recv, links.at(core=core, x=x))
        near = pltpu.make_async_copy(source, target, recv)

        @pl.when(jnp.logical_not(here))
        def _():
            far.start()

        @pl.when(here)
        def _():
            near.start()

    def all_left(ref, sem):
        rows = ref.shape[0]
        halved = links.x // 2 == links.core

        @pl.when(jnp.logical_not(halved))
        def _():
            wait_for(ref, sem)

        @pl.when(halved)
        def _():
            wait_for(ref.at[pl.ds(0, rows // 2)], sem)

    piece = band // PIECES

    def deliver(which, m, c):
        slot = lax.rem(links.x + m, 2)
        source = (dy_hbm if which else x_hbm).at[m, pl.ds(c * piece, piece)]
        target = (dy_s if which else x_s).at[pl.ds(pl.multiple_of(slot * band + c * piece, 16), piece)]
        maybe_far(links.workers[m], source, target, in_send.at[which], in_recv.at[which, slot, c])

    def hand_over(which, slot, c):
        rows = dy_s if which else x_s
        first = slot * band + c * piece
        return remote(rows.at[pl.ds(first, piece)], rows.at[pl.ds(own + first, piece)],
                      pass_send.at[which], pass_recv.at[which, slot, c], links.peer)

    def arrive(which, slot, c):
        with jax.named_scope(f'arrive{which}{slot}{c}'):
            wait_for((dy_s if which else x_s).at[pl.ds(slot * band + c * piece, piece)], in_recv.at[which, slot, c])
        hand_over(which, slot, c).start()

    def swap_out(head):
        rows = head_rows(head)
        return remote(o_s.at[rows, pl.ds(own, own)], o_peer.at[rows], o_sems.at[0, head], o_sems.at[1, head], links.peer)

    def swap_grads(head):
        rows = head_rows(head)
        return remote(grads.at[:, rows, pl.ds(own, own)], grads_peer.at[:, rows], grad_sems.at[0, head], grad_sems.at[1, head],
                      links.peer)

    part = band // 2
    portion = own // SENDS

    def send_home(which, i):
        cut = SENDS // 2
        second, inner = i // cut, lax.rem(i, cut)
        source = (dx_s if which else y_s).at[pl.ds(pl.multiple_of(i * portion, 16), portion)]
        target = (gx_ref if which else y_ref).at[odd, pl.ds(pl.multiple_of(inner * portion, 16), portion)]
        (core, x0), (_, x1) = links.owners
        maybe_far((core, jnp.where(second == 0, x0, x1)), source, target, out_send.at[which], out_recv.at[which])

    barrier = pltpu.get_barrier_semaphore()
    fixed = [links.peer]
    fixed += [links.step(axis, d) for axis in ('x', 'y') for d in range(1, RING)]
    fixed += [links.step('z', d) for d in range(1, depth)]
    for device in fixed:
        pl.semaphore_signal(barrier, inc=1, device_id=device, device_id_type=MESH)
    count = len(fixed)
    for place in links.owners + links.workers:
        other = jnp.logical_not(links.is_self(place))
        count = count + other.astype(jnp.int32)

        @pl.when(other)
        def _():
            pl.semaphore_signal(barrier, inc=1, device_id=links.at(core=place[0], x=place[1]), device_id_type=MESH)
    for load in loads:
        load.start()
    with jax.named_scope('barrier'):
        pl.semaphore_wait(barrier, count)
    for c in range(PIECES):
        for m in range(2):
            deliver(0, m, c)
    for load in loads:
        load.wait()

    def normalize(first):
        rows = pl.ds(first, piece)
        normed_s[rows] = (layer_norm(x_s, rows)[0] * gamma + beta).astype(BF)

    def project(b, c):
        cols = pl.ds(b * band + (c - 2) * piece, 2 * piece)
        normed = normed_s[cols]
        for k, out in enumerate((q_s, k_s, v_s)):
            out[:, cols] = dot_nt(wt_s[0, pl.ds(k * width, width)], normed).astype(BF)

    for c in range(PIECES + 1):
        if c < PIECES:
            for slot in range(2):
                arrive(0, slot, c)
            if c == PIECES - 1:
                for i in range(PIECES):
                    for m in range(2):
                        deliver(1, m, i)
            for slot in range(2):
                normalize(slot * band + c * piece)
        if c:
            if c % 2 == 0:
                project(0, c)
                project(1, c)
            for slot in range(2):
                with jax.named_scope(f'handed{slot}{c}'):
                    hand_over(0, slot, c - 1).wait_recv()
                normalize(own + slot * band + (c - 1) * piece)
                if c % 2 == 0:
                    project(2 + slot, c)

    def forward_step(now, carry):
        head, step = now // fwd_steps, lax.rem(now, fwd_steps)
        rows = head_rows(head)
        for c in range(PIECES):
            @pl.when(now == max(c, 1))
            def _():
                for slot in range(2):
                    arrive(1, slot, c)

        @pl.when(step == 0)
        def _():
            k_t = k_s[rows]
            kf_s[...] = jnp.concatenate([k_t, k_t, k_t], axis=0).T
            vf_s[0:dim] = v_s[rows]
            vf_s[dim:] = padded([jnp.ones((1, tokens), F32)], AUG - dim)

        bufs = (buf_a, buf_b, buf_c)
        total, lag = tiles * fwd_group, tiles + 2
        query, high, top, probs, out = {}, {}, {}, {}, {}
        for g in range(total + lag + 2):
            if g < total:
                i, t = divmod(g, tiles)
                if t == 0:
                    query[i] = jnp.concatenate(split_parts(q_s[rows, q_cols(step * fwd_group + i)].astype(F32) * log2_scale), axis=0)
                scores = dot_nn(kf_s[tile_rows(t)], query[i])
                bufs[i % 3][tile_rows(t)] = scores
                folded = fold_rows(scores, jnp.maximum)
                high[i] = folded if t == 0 else jnp.maximum(high[i], folded)
                if t == tiles - 1:
                    top[i] = jnp.max(high[i], axis=0, keepdims=True)
            if lag <= g < total + lag:
                i, t = divmod(g - lag, tiles)
                probs[g - lag] = jnp.exp2(bufs[i % 3][tile_rows(t, zero)] - top[i]).astype(BF)
            if g >= lag + 2:
                i, t = divmod(g - lag - 2, tiles)
                product = dot_nn(vf_s[:, tile_rows(t)], probs[g - lag - 2])
                out[i] = product if t == 0 else out[i] + product
                if t == tiles - 1:
                    cols = q_cols(step * fwd_group + i)
                    denom = out[i][dim:dim + 1]
                    value = out[i][:dim] * (1.0 / denom)
                    o_s[rows, cols] = value.astype(BF)
                    of_s[rows, cols] = value
                    lse = (top[i] + jnp.log2(denom)) * (1.0 / log2_scale)
                    lse_s[head_rows(head, 16), cols] = padded(split_parts(lse), 16)

        @pl.when(step == fwd_steps - 1)
        def _():
            swap_out(head).start()

        return carry

    lax.fori_loop(0, heads * fwd_steps, forward_step, 0)
    with jax.named_scope('dyhanded'):
        for c in range(PIECES):
            for slot in range(2):
                hand_over(1, slot, c).wait_recv()
    d_w[pl.ds(0, width)] = dot_nn(o_s[...], dy_s[...])
    for rnd, k in plan[0]:
        reduce.stage(rnd, k)
    for i in range(tiles):
        cols = pl.ds(i * KEY_TILE, KEY_TILE)
        do_s[:, cols] = dot_nt(wo_s[0], dy_s[cols]).astype(BF)
    with jax.named_scope('oswap'):
        for head in range(heads):
            swap_out(head).wait()
    for i in range(4):
        toks = pl.ds(i * part, part)
        product = dot_tn(o_s[:, toks], wo_s[0]) + dot_tn(o_peer[:, toks], wo_s[1])
        y_s[toks] = (x_s[toks].astype(F32) + product + bias).astype(BF)
    for which in range(2):
        rows = (dy_s if which else x_s).at[pl.ds(0, own)]
        all_left(rows, in_send.at[which])
        wait_for(rows, pass_send.at[which])

    def backward_step(now, carry):
        head, step = now // bwd_steps, lax.rem(now, bwd_steps)
        rows = head_rows(head)
        for at in range(end - 1):
            todo = plan.get(at + 1)
            if todo:
                @pl.when(now == at)
                def _():
                    with jax.named_scope(f'step{at}'):
                        for rnd, k in todo:
                            reduce.stage(rnd, k)
        share = SENDS // (heads * bwd_steps)
        for i in range(share):
            send_home(0, now * share + i)

        @pl.when(step == 0)
        def _():
            minus = padded([jnp.full((3, tokens), -1.0, F32)], AUG - dim)
            kb_s[...] = jnp.concatenate([k_s[rows], minus], axis=0).T
            vb_s[...] = jnp.concatenate([v_s[rows], minus], axis=0).T
            dk_acc[...] = jnp.zeros_like(dk_acc)
            dv_acc[...] = jnp.zeros_like(dv_acc)

        total = tiles * bwd_group
        ops, probs, d_scores, dq = {}, {}, {}, {}
        for g in range(total + 2):
            if g < total:
                i, t = divmod(g, tiles)
                if t == 0:
                    cols = q_cols(step * bwd_group + i)
                    q_t, do_t = q_s[rows, cols], do_s[rows, cols]
                    delta = jnp.sum(of_s[rows, cols] * do_t.astype(F32), axis=0, keepdims=True)
                    ops[i] = (cols, q_t, do_t, jnp.concatenate([q_t, lse_s[head_rows(head, 16), cols]], axis=0),
                              jnp.concatenate([do_t, padded(split_parts(delta), 16)], axis=0))
                scores = dot_nn(kb_s[tile_rows(t)], ops[i][3])
                d_probs = dot_nn(vb_s[tile_rows(t)], ops[i][4])
                prob = jnp.exp2(scores * log2_scale)
                probs[g] = prob.astype(BF)
                d_scores[g] = (prob * d_probs).astype(BF)
            if g >= 2:
                i, t = divmod(g - 2, tiles)
                cols, q_t, do_t = ops[i][:3]
                dv_acc[:, tile_rows(t)] += dot_nt(do_t, probs[g - 2])
                product = dot_nn(k_s[rows, tile_rows(t)], d_scores[g - 2])
                dq[i] = product if t == 0 else dq[i] + product
                if t == tiles - 1:
                    grads[0, rows, cols] = (dq[i] * scale).astype(BF)
                dk_acc[:, tile_rows(t)] += dot_nt(q_t, d_scores[g - 2])

        @pl.when(step == bwd_steps - 1)
        def _():
            grads[1, rows] = (dk_acc[...] * scale).astype(BF)
            grads[2, rows] = dv_acc[...].astype(BF)
            swap_grads(head).start()
            stacked = jnp.concatenate([grads[0, rows], grads[1, rows], grads[2, rows]], axis=0)
            d_w[pl.ds(pl.multiple_of(width + head * (3 * dim), 8), 3 * dim)] = dot_nn(stacked, normed_s[...])

        return carry

    lax.fori_loop(0, heads * bwd_steps, backward_step, 0)

    def tail(slot):
        for rnd, k in plan.get(end + slot, ()):
            with jax.named_scope(f'tail{slot}r{rnd}k{k}'):
                reduce.stage(rnd, k)

    tail(0)
    with jax.named_scope('gradswap'):
        for head in range(heads):
            swap_grads(head).wait()
    sums = [jnp.zeros((1, 640), F32)] * 3
    for i in range(4):
        toks = pl.ds(i * part, part)
        mine = jnp.concatenate([grads[k, :, toks] for k in range(3)], axis=0)
        theirs = jnp.concatenate([grads_peer[k, :, toks] for k in range(3)], axis=0)
        d_normed = (dot_tn(mine, wt_s[0]) + dot_tn(theirs, wt_s[1])).astype(BF).astype(F32)
        x_hat, inv_std = layer_norm(x_s, toks)
        d_hat = d_normed * gamma
        mean_one = jnp.mean(d_hat, axis=-1, keepdims=True)
        mean_two = jnp.mean(d_hat * x_hat, axis=-1, keepdims=True)
        dy_f = dy_s[toks].astype(F32)
        dx_s[toks] = (dy_f + inv_std * (d_hat - mean_one - x_hat * mean_two)).astype(BF)
        for k, term in enumerate((d_normed * x_hat, d_normed, dy_f)):
            sums[k] = sums[k] + jnp.sum(term, axis=0, keepdims=True)

    for k in range(3):
        for j in range(5):
            small_s[0, pl.ds(k * 5 + j, 1)] = sums[k][:, j * 128:(j + 1) * 128]
    small_s[0, pl.ds(15, 1)] = jnp.zeros((1, 128), F32)
    small_copy = pltpu.make_async_copy(small_s.at[4], small_ref, load_sems.at[0, 0])
    first, waiting = 0, ()
    for hop, axis in enumerate(('z', 'y', 'core', 'x', '')):
        if hop:
            for slot in range(hop, hop + 1 if axis else slots):
                tail(slot)
            if hop == 1:
                for i in range(SENDS):
                    send_home(1, i)
            acc = small_s[hop - 1]
            with jax.named_scope(f'small{hop}'):
                for copy in waiting:
                    copy.wait_recv()
            for d in range(len(waiting)):
                acc = acc + small_recv[first + d]
            for copy in waiting:
                copy.wait_send()
            first += len(waiting)
            small_s[hop] = acc
        if axis:
            far = [links.peer] if axis == 'core' else [links.step(axis, d) for d in range(1, links.size[axis])]
            waiting = [remote(small_s.at[hop], small_recv.at[first + d], small_sems.at[0, first + d], small_sems.at[1, first + d],
                              device) for d, device in enumerate(far)]
            for copy in waiting:
                copy.start()
    small_copy.start()
    with jax.named_scope('home'):
        for which in range(2):
            all_left(dx_s if which else y_s, out_send.at[which])
            wait_for(gx_ref if which else y_ref, out_recv.at[which])
    with jax.named_scope('stored'):
        for rnd in range(ROUNDS):
            reduce.stored(rnd)
    small_copy.wait()


def attention_block(x_in, grad_y, weights, vectors, dim, depth):
    rows, channels = x_in.shape[1:]
    tokens, own = 4 * rows, 2 * rows
    width = weights[0].shape[0] // 2
    heads = width // dim
    total = 4 * width
    half = lambda *shape: pltpu.VMEM(shape, BF)
    full = lambda *shape: pltpu.VMEM(shape, F32)
    dma = lambda *shape: pltpu.SemaphoreType.DMA(shape)
    anywhere = pl.BlockSpec(memory_space=pl.ANY)
    in_vmem = pl.BlockSpec(memory_space=pltpu.VMEM)
    far = max(depth - 1, 1)
    return pl.pallas_call(
        functools.partial(block_body, dim, depth),
        in_specs=[anywhere] * 6 + [in_vmem] * 3,
        out_specs=[anywhere] * 7,
        out_shape=[jax.ShapeDtypeStruct(x_in.shape, BF)] * 2
        + [jax.ShapeDtypeStruct(weights[0].shape, F32)] * 4 + [jax.ShapeDtypeStruct((16, 128), F32)],
        scratch_shapes=[half(tokens, channels)] * 3 + [half(2, 3 * width, channels), half(2, width, channels)]
        + [half(width, tokens)] * 5 + [full(width, tokens), half(width, own), half(16 * heads, tokens),
                                       half(tokens, 3 * dim), half(AUG, tokens)]
        + [full(tokens, Q_BLOCK)] * 3 + [half(tokens, AUG)] * 2 + [full(dim, tokens)] * 2
        + [half(3, width, tokens), half(3, width, own), full(total, channels), full(2, total, channels)]
        + [half(own, channels)] * 2
        + [full(ROUNDS, 2, 3, 32, channels), full(ROUNDS, 2, 3, 8, channels), full(ROUNDS, 2, 32, channels), full(ROUNDS, 16, 8, 128),
           full(ROUNDS, far, 16 // depth, 8, 128), full(ROUNDS, 16, 8, 128), full(5, 16, 128), full(7 + far, 16, 128),
           dma(2, 4)] + [dma(2), dma(2, 2, PIECES)] * 2 + [dma(2, heads)] * 2
        + [dma(2), dma(2), dma(2, 7 + far)] + [dma(2, ROUNDS, 2, 2)] * 2 + [dma(2, ROUNDS, 2), dma(2, ROUNDS), dma(ROUNDS)],
        compiler_params=pltpu.CompilerParams(collective_id=0, has_side_effects=True, vmem_limit_bytes=VMEM_BYTES),
        name='attention_block',
    )(x_in, grad_y, *weights, *vectors)


def settle_body(count, small_hbm, *refs):
    sources, targets, refs = refs[:count], refs[count:2 * count], refs[2 * count:]
    vectors, bufs, (small, vector_s, sems, vector_sems) = refs[:3], refs[3:3 + count], refs[3 + count:]
    load = pltpu.make_async_copy(small_hbm, small, vector_sems.at[3])
    load.start()
    cuts = []
    for i, (source, target, buf) in enumerate(zip(sources, targets, bufs)):
        rows = source.shape[0] // CUTS
        for c in range(CUTS):
            part = pl.ds(c * rows, rows)
            cuts.append((pltpu.make_async_copy(source.at[part], buf.at[part], sems.at[0, i, c]),
                         pltpu.make_async_copy(buf.at[part], target.at[part], sems.at[1, i, c])))
    for read, _ in cuts:
        read.start()
    load.wait()
    stores = []
    for k, vector in enumerate(vectors):
        vector_s[k][...] = jnp.concatenate([small[k * 5 + j:k * 5 + j + 1] for j in range(5)], axis=1).reshape(vector.shape)
        stores.append(pltpu.make_async_copy(vector_s[k], vector, vector_sems.at[k]))
        stores[k].start()
    for read, write in cuts:
        read.wait()
        write.start()
    for _, write in cuts:
        write.wait()
    for store in stores:
        store.wait()


def settle(small, arrays):
    anywhere = pl.BlockSpec(memory_space=pl.ANY)
    count = len(arrays)
    dma = pltpu.SemaphoreType.DMA
    vector = (arrays[0].shape[1],)
    return pl.pallas_call(
        functools.partial(settle_body, count),
        in_specs=[anywhere] * (count + 1), out_specs=[anywhere] * (count + 3),
        out_shape=[jax.ShapeDtypeStruct(a.shape, a.dtype) for a in arrays] + [jax.ShapeDtypeStruct(vector, F32)] * 3,
        scratch_shapes=[pltpu.VMEM(a.shape, a.dtype) for a in arrays]
        + [pltpu.VMEM(small.shape, F32), [pltpu.VMEM(vector, F32)] * 3, dma((2, count, CUTS)), dma((4,))],
        compiler_params=pltpu.CompilerParams(vmem_limit_bytes=VMEM_BYTES),
        name='settle',
    )(small, *arrays)


def solution(mesh):
    depth = mesh.shape['dp'] // (2 * RING)
    act_spec, rep_spec = P('dp', 'cp', None), P()

    def device_step(x_in, grad_y, ln_gamma, ln_beta, w_q, w_k, w_v, w_o, b_o):
        channels, num_heads, head_dim = w_q.shape
        flat = (num_heads * head_dim, channels)
        weights = [jnp.transpose(w, (1, 2, 0)).reshape(flat) for w in (w_q, w_k, w_v)] + [w_o.reshape(flat)]
        y_out, grad_x, *grads, grad_wo, small = attention_block(x_in, grad_y, weights, (ln_gamma, ln_beta, b_o), head_dim, depth)
        rows = (2 * y_out.shape[1], channels)
        moved = settle(small, [y_out.reshape(rows), grad_x.reshape(rows), *grads, grad_wo])
        y_out, grad_x = (a.reshape(x_in.shape) for a in moved[:2])
        grads, grad_wo = moved[2:5], moved[5]
        grads = [jnp.transpose(grad.reshape(num_heads, head_dim, channels), (2, 0, 1)) for grad in grads]
        return (y_out, grad_x, moved[6], moved[7], *grads, grad_wo.reshape(num_heads, head_dim, channels), moved[8])

    specs = (act_spec, act_spec) + (rep_spec,) * 7
    return jax.shard_map(device_step, mesh=mesh, in_specs=specs, out_specs=specs, check_vma=False)
```

```python
import functools
import math
import jax
import jax.numpy as jnp
from jax import lax
from jax.experimental import pallas as pl
from jax.experimental.pallas import tpu as pltpu
from jax.sharding import PartitionSpec as P

LN_EPS = 1e-5
KEY_TILE = 256
Q_BLOCK = 256
FOLD = 16
AUG = 96
VMEM_BYTES = 67043328
BF = jnp.bfloat16
F32 = jnp.float32


def dot_nn(lhs, rhs):
    return lax.dot_general(lhs, rhs, (((1,), (0,)), ((), ())), preferred_element_type=F32)


def dot_nt(lhs, rhs):
    return lax.dot_general(lhs, rhs, (((1,), (1,)), ((), ())), preferred_element_type=F32)


def dot_tn(lhs, rhs):
    return lax.dot_general(lhs, rhs, (((0,), (0,)), ((), ())), preferred_element_type=F32)


def split_parts(value):
    high = value.astype(BF)
    rest = value - high.astype(F32)
    mid = rest.astype(BF)
    return high, mid, (rest - mid.astype(F32)).astype(BF)


def fold_rows(value, op):
    groups = value.reshape(value.shape[0] // FOLD, FOLD, value.shape[1])
    out = groups[0]
    for i in range(1, groups.shape[0]):
        out = op(out, groups[i])
    return out


MESH = pl.DeviceIdType.MESH
RING = 4
ROUNDS = 5
ROUND_ROWS = 256
STAGES = 8
SPARE = ((0, 1), (1, 1), (2, 1), (3, 1), (0, 6), (1, 5), (1, 6), (2, 6), (2, 6))
PIECES = 4
SENDS = 16
CUTS = 4
ORDER = ('yx', 'yy', 'yy', 'yx', 'yx')


class Links:
    def __init__(self, depth):
        dp, self.x = lax.axis_index('dp'), lax.axis_index('cp')
        self.core = lax.rem(dp, 2)
        self.y = lax.rem(dp // 2, RING)
        self.z = dp // (2 * RING)
        self.depth = depth
        self.pos = {'x': self.x, 'y': self.y, 'z': self.z}
        self.size = {'x': RING, 'y': RING, 'z': depth}
        self.peer = self.at(core=1 - self.core)
        pair, odd = self.x // 2, lax.rem(self.x, 2)
        self.owners = [(pair, 2 * self.core + odd), (pair, 2 * self.core + 1 - odd)]
        self.workers = [(pair, 2 * self.core), (pair, 2 * self.core + 1)]

    def at(self, x=None, y=None, z=None, core=None):
        pick = lambda value, own: own if value is None else value
        return ((pick(z, self.z) * RING + pick(y, self.y)) * 2 + pick(core, self.core), pick(x, self.x))

    def step(self, axis, d):
        return self.at(**{axis: lax.rem(self.pos[axis] + d, self.size[axis])})

    def is_self(self, place):
        return jnp.logical_and(place[0] == self.core, place[1] == self.x)


def remote(source, target, send, recv, device):
    return pltpu.make_async_remote_copy(src_ref=source, dst_ref=target, send_sem=send, recv_sem=recv,
                                        device_id=device, device_id_type=MESH)


def wait_for(ref, sem):
    pltpu.make_async_copy(ref, ref, sem).wait()


class GradReduce:
    def __init__(self, links, dim, grad, out, results, bufs, sems):
        self.links, self.grad, self.both, self.out = links, grad, out, out.at[links.core]
        width = grad.shape[0] // 4
        self.pieces = [(0, width, results[0], 0)]
        self.pieces += [(width + (3 * head + k) * dim, dim, results[1 + k], head * dim) for head in range(width // dim) for k in range(3)]
        self.recv1, self.recv2, self.mid, self.z_src, self.z_recv, self.z_out = bufs
        self.rs_sems, self.ag_sems, self.z_sems, self.swap_sems, self.store_sems = sems

    def axes(self, rnd, unit):
        first = ORDER[rnd][unit]
        return first, ('x' if first == 'y' else 'y')

    def block(self, rnd, unit, phase):
        first = rnd * ROUND_ROWS + unit * 128
        if phase == 0:
            return first, 32
        return first + self.links.pos[self.axes(rnd, unit)[0]] * 32, 8

    def landing(self, rnd, unit, phase):
        return (self.recv1 if phase == 0 else self.recv2).at[rnd, unit]

    def wait_all(self, rnd, unit, phase, sems):
        whole = self.landing(rnd, unit, phase)
        every = remote(whole, whole, sems.at[0, rnd, unit, phase], sems.at[1, rnd, unit, phase], self.links.peer)
        every.wait_recv()
        every.wait_send()

    def source(self, rnd, unit, phase, owner):
        if phase == 0:
            first, rows = self.block(rnd, unit, 0)
            return self.grad.at[pl.ds(pl.multiple_of(first + owner * rows, 8), rows)]
        return self.mid.at[rnd, unit, pl.ds(pl.multiple_of(owner * 8, 8), 8)]

    def scatter_start(self, rnd, unit, phase):
        axis = self.axes(rnd, unit)[phase]
        for d in (2, 1, 3):
            owner = lax.rem(self.links.pos[axis] + d, RING)
            remote(self.source(rnd, unit, phase, owner), self.landing(rnd, unit, phase).at[d - 1],
                   self.rs_sems.at[0, rnd, unit, phase], self.rs_sems.at[1, rnd, unit, phase], self.links.step(axis, d)).start()

    def scatter_end(self, rnd, unit, phase):
        self.wait_all(rnd, unit, phase, self.rs_sems)
        landing = self.landing(rnd, unit, phase)
        mine = self.source(rnd, unit, phase, self.links.pos[self.axes(rnd, unit)[phase]])
        return (mine[...] + landing[0]) + (landing[1] + landing[2])

    def gather_start(self, rnd, unit, phase):
        axis = self.axes(rnd, unit)[phase]
        first, rows = self.block(rnd, unit, phase)
        part = self.out.at[pl.ds(pl.multiple_of(first + self.links.pos[axis] * rows, 8), rows)]
        for d in (2, 1, 3):
            remote(part, part, self.ag_sems.at[0, rnd, unit, phase], self.ag_sems.at[1, rnd, unit, phase],
                   self.links.step(axis, d)).start()

    def z_copies(self, rnd, way):
        links = self.links
        each = 16 // links.depth
        send, recv = self.z_sems.at[0, rnd, way], self.z_sems.at[1, rnd, way]
        mine = pl.ds(links.z * each, each)
        copies = []
        for d in range(1, links.depth):
            far = lax.rem(links.z + d, links.depth)
            if way == 0:
                source, target = self.z_src.at[rnd, pl.ds(far * each, each)], self.z_recv.at[rnd, d - 1]
            else:
                source = target = self.z_out.at[rnd, mine]
            copies.append(remote(source, target, send, recv, links.step('z', d)))
        return copies, mine

    def z_wait(self, rnd, way):
        if self.links.depth > 1:
            whole = self.z_recv.at[rnd]
            all_of = remote(whole, whole, self.z_sems.at[0, rnd, way], self.z_sems.at[1, rnd, way], self.links.step('z', 1))
            all_of.wait_recv()
            all_of.wait_send()

    def swap(self, rnd):
        part = self.out.at[pl.ds(rnd * ROUND_ROWS, ROUND_ROWS)]
        return remote(part, part, self.swap_sems.at[0, rnd], self.swap_sems.at[1, rnd], self.links.peer)

    def store(self, rnd):
        begin = rnd * ROUND_ROWS
        half = self.both.shape[1] // 4
        for first, rows, result, place in self.pieces:
            low, high = max(first, begin), min(first + rows, begin + ROUND_ROWS)
            for core in range(2):
                if low < high:
                    target = result.at[pl.ds(core * half + place + low - first, high - low)]
                    pltpu.make_async_copy(self.both.at[core, pl.ds(low, high - low)], target, self.store_sems.at[rnd]).start()

    def stored(self, rnd):
        wait_for(self.both.at[:, pl.ds(rnd * ROUND_ROWS, ROUND_ROWS)], self.store_sems.at[rnd])

    def stage(self, rnd, k):
        units = (0, 1)
        if k == 0:
            for u in units:
                self.scatter_start(rnd, u, 0)
        elif k == 1:
            for u in units:
                self.mid[rnd, u] = self.scatter_end(rnd, u, 0)
                self.scatter_start(rnd, u, 1)
        elif k == 2:
            for u in units:
                total = self.scatter_end(rnd, u, 1)
                for j in range(5):
                    self.z_src[rnd, u * 5 + j] = total[:, j * 128:(j + 1) * 128]
            self.z_src[rnd, pl.ds(10, 6)] = jnp.zeros((6, 8, 128), F32)
            for copy in self.z_copies(rnd, 0)[0]:
                copy.start()
        elif k == 3:
            self.z_wait(rnd, 0)
            copies, mine = self.z_copies(rnd, 1)
            total = self.z_src[rnd, mine]
            for d in range(self.links.depth - 1):
                total = total + self.z_recv[rnd, d]
            self.z_out[rnd, mine] = total
            for copy in copies:
                copy.start()
        elif k == 4:
            self.z_wait(rnd, 1)
            for u in units:
                first = self.block(rnd, u, 1)[0] + self.links.pos[self.axes(rnd, u)[1]] * 8
                for j in range(5):
                    self.out[pl.ds(pl.multiple_of(first, 8), 8), pl.ds(j * 128, 128)] = self.z_out[rnd, u * 5 + j]
                self.gather_start(rnd, u, 1)
        elif k == 5:
            for u in units:
                self.wait_all(rnd, u, 1, self.ag_sems)
                self.gather_start(rnd, u, 0)
        elif k == 6:
            for u in units:
                self.wait_all(rnd, u, 0, self.ag_sems)
            self.swap(rnd).start()
        else:
            self.swap(rnd).wait()
            self.store(rnd)


def layer_norm(x_ref, rows):
    x_f = x_ref[rows].astype(F32)
    centered = x_f - jnp.mean(x_f, axis=-1, keepdims=True)
    inv_std = lax.rsqrt(jnp.mean(centered * centered, axis=-1, keepdims=True) + LN_EPS)
    return centered * inv_std, inv_std


def padded(parts, rows):
    filled = [part.astype(F32) for part in parts]
    used = sum(part.shape[0] for part in filled)
    return jnp.concatenate(filled + [jnp.zeros((rows - used, filled[0].shape[1]), F32)], axis=0).astype(BF)


def block_body(dim, depth, x_hbm, dy_hbm, wq_hbm, wk_hbm, wv_hbm, wo_hbm, gamma_ref, beta_ref, bo_ref,
               y_ref, gx_ref, dq_ref, dk_ref, dv_ref, dwo_ref, small_ref,
               x_s, normed_s, dy_s, wt_s, wo_s, q_s, k_s, v_s, do_s, o_s, of_s, o_peer, lse_s, kf_s, vf_s, buf_a, buf_b, buf_c,
               kb_s, vb_s, dk_acc, dv_acc, grads, grads_peer, d_w, d_w_all, dx_s, y_s,
               recv1, recv2, mid, z_src, z_recv, z_out, small_s, small_recv,
               load_sems, in_send, in_recv, pass_send, pass_recv, o_sems, grad_sems, out_send, out_recv, small_sems,
               rs_sems, ag_sems, z_sems, swap_sems, store_sems):
    links = Links(depth)
    width, tokens = q_s.shape
    heads, tiles = width // dim, tokens // KEY_TILE
    own, band = tokens // 2, tokens // 4
    scale = dim ** -0.5
    log2_scale = scale * math.log2(math.e)
    fwd_group, bwd_group = tiles, 4
    fwd_steps, bwd_steps = tiles // fwd_group, tiles // bwd_group
    zero = jnp.minimum(links.x, 0)
    gamma, beta, bias = (ref[...].reshape(1, ref.shape[0]) for ref in (gamma_ref, beta_ref, bo_ref))
    odd = lax.rem(links.x, 2)
    reduce = GradReduce(links, dim, d_w, d_w_all, (dwo_ref, dq_ref, dk_ref, dv_ref), (recv1, recv2, mid, z_src, z_recv, z_out),
                        (rs_sems, ag_sems, z_sems, swap_sems, store_sems))
    end = heads * bwd_steps + 1
    plan = {}
    for rnd in range(ROUNDS):
        at = rnd * bwd_steps + 1 if rnd else 0
        for k in range(STAGES):
            at += min(k, 1) + SPARE.count((rnd, k))
            plan.setdefault(at, []).append((rnd, k))
    for at in plan:
        plan[at].sort(key=lambda item: (item[1] in (0, 5) and item[0] < ROUNDS - 1, -item[0]))
    slots = max(plan) + 1 - end

    def tile_rows(tile, base=None):
        return pl.ds(tile * KEY_TILE if base is None else pl.multiple_of(base + tile * KEY_TILE, KEY_TILE), KEY_TILE)

    def head_rows(head, rows=dim):
        return pl.ds(pl.multiple_of(head * rows, 16), rows)

    def q_cols(index):
        return pl.ds(pl.multiple_of(index * Q_BLOCK, Q_BLOCK), Q_BLOCK)

    def my_half(side):
        return pl.ds(pl.multiple_of((links.core if side == 0 else 1 - links.core) * width, 16), width)

    loads = [pltpu.make_async_copy(w_hbm.at[my_half(side)], wt_s.at[side, pl.ds(k * width, width)], load_sems.at[side, k])
             for side in range(2) for k, w_hbm in enumerate((wq_hbm, wk_hbm, wv_hbm))]
    loads += [pltpu.make_async_copy(wo_hbm.at[my_half(side)], wo_s.at[side], load_sems.at[side, 3]) for side in range(2)]

    def maybe_far(place, source, target, send, recv):
        core, x = place
        here = links.is_self(place)
        far = remote(source, target, send, recv, links.at(core=core, x=x))
        near = pltpu.make_async_copy(source, target, recv)

        @pl.when(jnp.logical_not(here))
        def _():
            far.start()

        @pl.when(here)
        def _():
            near.start()

    def all_left(ref, sem):
        rows = ref.shape[0]
        halved = links.x // 2 == links.core

        @pl.when(jnp.logical_not(halved))
        def _():
            wait_for(ref, sem)

        @pl.when(halved)
        def _():
            wait_for(ref.at[pl.ds(0, rows // 2)], sem)

    piece = band // PIECES

    def deliver(which, m, c):
        slot = lax.rem(links.x + m, 2)
        source = (dy_hbm if which else x_hbm).at[m, pl.ds(c * piece, piece)]
        target = (dy_s if which else x_s).at[pl.ds(pl.multiple_of(slot * band + c * piece, 16), piece)]
        maybe_far(links.workers[m], source, target, in_send.at[which], in_recv.at[which, slot, c])

    def hand_over(which, slot, c):
        rows = dy_s if which else x_s
        first = slot * band + c * piece
        return remote(rows.at[pl.ds(first, piece)], rows.at[pl.ds(own + first, piece)],
                      pass_send.at[which], pass_recv.at[which, slot, c], links.peer)

    def arrive(which, slot, c):
        wait_for((dy_s if which else x_s).at[pl.ds(slot * band + c * piece, piece)], in_recv.at[which, slot, c])
        hand_over(which, slot, c).start()

    def swap_out(head):
        rows = head_rows(head)
        return remote(o_s.at[rows, pl.ds(own, own)], o_peer.at[rows], o_sems.at[0, head], o_sems.at[1, head], links.peer)

    def swap_grads(head):
        rows = head_rows(head)
        return remote(grads.at[:, rows, pl.ds(own, own)], grads_peer.at[:, rows], grad_sems.at[0, head], grad_sems.at[1, head],
                      links.peer)

    part = band // 2
    portion = own // SENDS

    def send_home(which, i):
        cut = SENDS // 2
        second, inner = i // cut, lax.rem(i, cut)
        source = (dx_s if which else y_s).at[pl.ds(pl.multiple_of(i * portion, 16), portion)]
        target = (gx_ref if which else y_ref).at[odd, pl.ds(pl.multiple_of(inner * portion, 16), portion)]
        (core, x0), (_, x1) = links.owners
        maybe_far((core, jnp.where(second == 0, x0, x1)), source, target, out_send.at[which], out_recv.at[which])

    barrier = pltpu.get_barrier_semaphore()
    fixed = [links.peer]
    fixed += [links.step(axis, d) for axis in ('x', 'y') for d in range(1, RING)]
    fixed += [links.step('z', d) for d in range(1, depth)]
    for device in fixed:
        pl.semaphore_signal(barrier, inc=1, device_id=device, device_id_type=MESH)
    count = len(fixed)
    for place in links.owners + links.workers:
        other = jnp.logical_not(links.is_self(place))
        count = count + other.astype(jnp.int32)

        @pl.when(other)
        def _():
            pl.semaphore_signal(barrier, inc=1, device_id=links.at(core=place[0], x=place[1]), device_id_type=MESH)
    for load in loads:
        load.start()
    pl.semaphore_wait(barrier, count)
    for c in range(PIECES):
        for m in range(2):
            deliver(0, m, c)
    for load in loads:
        load.wait()

    def normalize(first):
        rows = pl.ds(first, piece)
        normed_s[rows] = (layer_norm(x_s, rows)[0] * gamma + beta).astype(BF)

    def project(b, c):
        cols = pl.ds(b * band + (c - 2) * piece, 2 * piece)
        normed = normed_s[cols]
        for k, out in enumerate((q_s, k_s, v_s)):
            out[:, cols] = dot_nt(wt_s[0, pl.ds(k * width, width)], normed).astype(BF)

    for c in range(PIECES + 1):
        if c < PIECES:
            for slot in range(2):
                arrive(0, slot, c)
            if c == PIECES - 1:
                for i in range(PIECES):
                    for m in range(2):
                        deliver(1, m, i)
            for slot in range(2):
                normalize(slot * band + c * piece)
        if c:
            if c % 2 == 0:
                project(0, c)
                project(1, c)
            for slot in range(2):
                hand_over(0, slot, c - 1).wait_recv()
                normalize(own + slot * band + (c - 1) * piece)
                if c % 2 == 0:
                    project(2 + slot, c)

    def forward_step(now, carry):
        head, step = now // fwd_steps, lax.rem(now, fwd_steps)
        rows = head_rows(head)
        for c in range(PIECES):
            @pl.when(now == max(c, 1))
            def _():
                for slot in range(2):
                    arrive(1, slot, c)

        @pl.when(step == 0)
        def _():
            k_t = k_s[rows]
            kf_s[...] = jnp.concatenate([k_t, k_t, k_t], axis=0).T
            vf_s[0:dim] = v_s[rows]
            vf_s[dim:] = padded([jnp.ones((1, tokens), F32)], AUG - dim)

        bufs = (buf_a, buf_b, buf_c)
        total, lag = tiles * fwd_group, tiles + 2
        query, high, top, probs, out = {}, {}, {}, {}, {}
        for g in range(total + lag + 2):
            if g < total:
                i, t = divmod(g, tiles)
                if t == 0:
                    query[i] = jnp.concatenate(split_parts(q_s[rows, q_cols(step * fwd_group + i)].astype(F32) * log2_scale), axis=0)
                scores = dot_nn(kf_s[tile_rows(t)], query[i])
                bufs[i % 3][tile_rows(t)] = scores
                folded = fold_rows(scores, jnp.maximum)
                high[i] = folded if t == 0 else jnp.maximum(high[i], folded)
                if t == tiles - 1:
                    top[i] = jnp.max(high[i], axis=0, keepdims=True)
            if lag <= g < total + lag:
                i, t = divmod(g - lag, tiles)
                probs[g - lag] = jnp.exp2(bufs[i % 3][tile_rows(t, zero)] - top[i]).astype(BF)
            if g >= lag + 2:
                i, t = divmod(g - lag - 2, tiles)
                product = dot_nn(vf_s[:, tile_rows(t)], probs[g - lag - 2])
                out[i] = product if t == 0 else out[i] + product
                if t == tiles - 1:
                    cols = q_cols(step * fwd_group + i)
                    denom = out[i][dim:dim + 1]
                    value = out[i][:dim] * (1.0 / denom)
                    o_s[rows, cols] = value.astype(BF)
                    of_s[rows, cols] = value
                    lse = (top[i] + jnp.log2(denom)) * (1.0 / log2_scale)
                    lse_s[head_rows(head, 16), cols] = padded(split_parts(lse), 16)

        @pl.when(step == fwd_steps - 1)
        def _():
            swap_out(head).start()

        return carry

    lax.fori_loop(0, heads * fwd_steps, forward_step, 0)
    for c in range(PIECES):
        for slot in range(2):
            hand_over(1, slot, c).wait_recv()
    d_w[pl.ds(0, width)] = dot_nn(o_s[...], dy_s[...])
    for rnd, k in plan[0]:
        reduce.stage(rnd, k)
    for i in range(tiles):
        cols = pl.ds(i * KEY_TILE, KEY_TILE)
        do_s[:, cols] = dot_nt(wo_s[0], dy_s[cols]).astype(BF)
    for head in range(heads):
        swap_out(head).wait()
    for i in range(4):
        toks = pl.ds(i * part, part)
        product = dot_tn(o_s[:, toks], wo_s[0]) + dot_tn(o_peer[:, toks], wo_s[1])
        y_s[toks] = (x_s[toks].astype(F32) + product + bias).astype(BF)
    for which in range(2):
        rows = (dy_s if which else x_s).at[pl.ds(0, own)]
        all_left(rows, in_send.at[which])
        wait_for(rows, pass_send.at[which])

    def backward_step(now, carry):
        head, step = now // bwd_steps, lax.rem(now, bwd_steps)
        rows = head_rows(head)
        for at in range(end - 1):
            todo = plan.get(at + 1)
            if todo:
                @pl.when(now == at)
                def _():
                    for rnd, k in todo:
                        reduce.stage(rnd, k)
        share = SENDS // (heads * bwd_steps)
        for i in range(share):
            send_home(0, now * share + i)

        @pl.when(step == 0)
        def _():
            minus = padded([jnp.full((3, tokens), -1.0, F32)], AUG - dim)
            kb_s[...] = jnp.concatenate([k_s[rows], minus], axis=0).T
            vb_s[...] = jnp.concatenate([v_s[rows], minus], axis=0).T
            dk_acc[...] = jnp.zeros_like(dk_acc)
            dv_acc[...] = jnp.zeros_like(dv_acc)

        total = tiles * bwd_group
        ops, probs, d_scores, dq = {}, {}, {}, {}
        for g in range(total + 2):
            if g < total:
                i, t = divmod(g, tiles)
                if t == 0:
                    cols = q_cols(step * bwd_group + i)
                    q_t, do_t = q_s[rows, cols], do_s[rows, cols]
                    delta = jnp.sum(of_s[rows, cols] * do_t.astype(F32), axis=0, keepdims=True)
                    ops[i] = (cols, q_t, do_t, jnp.concatenate([q_t, lse_s[head_rows(head, 16), cols]], axis=0),
                              jnp.concatenate([do_t, padded(split_parts(delta), 16)], axis=0))
                scores = dot_nn(kb_s[tile_rows(t)], ops[i][3])
                d_probs = dot_nn(vb_s[tile_rows(t)], ops[i][4])
                prob = jnp.exp2(scores * log2_scale)
                probs[g] = prob.astype(BF)
                d_scores[g] = (prob * d_probs).astype(BF)
            if g >= 2:
                i, t = divmod(g - 2, tiles)
                cols, q_t, do_t = ops[i][:3]
                dv_acc[:, tile_rows(t)] += dot_nt(do_t, probs[g - 2])
                product = dot_nn(k_s[rows, tile_rows(t)], d_scores[g - 2])
                dq[i] = product if t == 0 else dq[i] + product
                if t == tiles - 1:
                    grads[0, rows, cols] = (dq[i] * scale).astype(BF)
                dk_acc[:, tile_rows(t)] += dot_nt(q_t, d_scores[g - 2])

        @pl.when(step == bwd_steps - 1)
        def _():
            grads[1, rows] = (dk_acc[...] * scale).astype(BF)
            grads[2, rows] = dv_acc[...].astype(BF)
            swap_grads(head).start()
            stacked = jnp.concatenate([grads[0, rows], grads[1, rows], grads[2, rows]], axis=0)
            d_w[pl.ds(pl.multiple_of(width + head * (3 * dim), 8), 3 * dim)] = dot_nn(stacked, normed_s[...])

        return carry

    lax.fori_loop(0, heads * bwd_steps, backward_step, 0)

    def tail(slot):
        for rnd, k in plan.get(end + slot, ()):
            reduce.stage(rnd, k)

    tail(0)
    for head in range(heads):
        swap_grads(head).wait()
    sums = [jnp.zeros((1, 640), F32)] * 3
    for i in range(4):
        toks = pl.ds(i * part, part)
        mine = jnp.concatenate([grads[k, :, toks] for k in range(3)], axis=0)
        theirs = jnp.concatenate([grads_peer[k, :, toks] for k in range(3)], axis=0)
        d_normed = (dot_tn(mine, wt_s[0]) + dot_tn(theirs, wt_s[1])).astype(BF).astype(F32)
        x_hat, inv_std = layer_norm(x_s, toks)
        d_hat = d_normed * gamma
        mean_one = jnp.mean(d_hat, axis=-1, keepdims=True)
        mean_two = jnp.mean(d_hat * x_hat, axis=-1, keepdims=True)
        dy_f = dy_s[toks].astype(F32)
        dx_s[toks] = (dy_f + inv_std * (d_hat - mean_one - x_hat * mean_two)).astype(BF)
        for k, term in enumerate((d_normed * x_hat, d_normed, dy_f)):
            sums[k] = sums[k] + jnp.sum(term, axis=0, keepdims=True)

    for k in range(3):
        for j in range(5):
            small_s[0, pl.ds(k * 5 + j, 1)] = sums[k][:, j * 128:(j + 1) * 128]
    small_s[0, pl.ds(15, 1)] = jnp.zeros((1, 128), F32)
    small_copy = pltpu.make_async_copy(small_s.at[4], small_ref, load_sems.at[0, 0])
    first, waiting = 0, ()
    for hop, axis in enumerate(('z', 'core', 'y', 'x', '')):
        if hop:
            for slot in range(hop, hop + 1 if axis else slots):
                tail(slot)
            if hop == 1:
                for i in range(SENDS):
                    send_home(1, i)
            acc = small_s[hop - 1]
            for d, copy in enumerate(waiting):
                copy.wait_recv()
                acc = acc + small_recv[first + d]
            for copy in waiting:
                copy.wait_send()
            first += len(waiting)
            small_s[hop] = acc
        if axis:
            far = [links.peer] if axis == 'core' else [links.step(axis, d) for d in range(1, links.size[axis])]
            waiting = [remote(small_s.at[hop], small_recv.at[first + d], small_sems.at[0, first + d], small_sems.at[1, first + d],
                              device) for d, device in enumerate(far)]
            for copy in waiting:
                copy.start()
    small_copy.start()
    for which in range(2):
        all_left(dx_s if which else y_s, out_send.at[which])
        wait_for(gx_ref if which else y_ref, out_recv.at[which])
    for rnd in range(ROUNDS):
        reduce.stored(rnd)
    small_copy.wait()


def attention_block(x_in, grad_y, weights, vectors, dim, depth):
    rows, channels = x_in.shape[1:]
    tokens, own = 4 * rows, 2 * rows
    width = weights[0].shape[0] // 2
    heads = width // dim
    total = 4 * width
    half = lambda *shape: pltpu.VMEM(shape, BF)
    full = lambda *shape: pltpu.VMEM(shape, F32)
    dma = lambda *shape: pltpu.SemaphoreType.DMA(shape)
    anywhere = pl.BlockSpec(memory_space=pl.ANY)
    in_vmem = pl.BlockSpec(memory_space=pltpu.VMEM)
    far = max(depth - 1, 1)
    return pl.pallas_call(
        functools.partial(block_body, dim, depth),
        in_specs=[anywhere] * 6 + [in_vmem] * 3,
        out_specs=[anywhere] * 7,
        out_shape=[jax.ShapeDtypeStruct(x_in.shape, BF)] * 2
        + [jax.ShapeDtypeStruct(weights[0].shape, F32)] * 4 + [jax.ShapeDtypeStruct((16, 128), F32)],
        scratch_shapes=[half(tokens, channels)] * 3 + [half(2, 3 * width, channels), half(2, width, channels)]
        + [half(width, tokens)] * 5 + [full(width, tokens), half(width, own), half(16 * heads, tokens),
                                       half(tokens, 3 * dim), half(AUG, tokens)]
        + [full(tokens, Q_BLOCK)] * 3 + [half(tokens, AUG)] * 2 + [full(dim, tokens)] * 2
        + [half(3, width, tokens), half(3, width, own), full(total, channels), full(2, total, channels)]
        + [half(own, channels)] * 2
        + [full(ROUNDS, 2, 3, 32, channels), full(ROUNDS, 2, 3, 8, channels), full(ROUNDS, 2, 32, channels), full(ROUNDS, 16, 8, 128),
           full(ROUNDS, far, 16 // depth, 8, 128), full(ROUNDS, 16, 8, 128), full(5, 16, 128), full(7 + far, 16, 128),
           dma(2, 4)] + [dma(2), dma(2, 2, PIECES)] * 2 + [dma(2, heads)] * 2
        + [dma(2), dma(2), dma(2, 7 + far)] + [dma(2, ROUNDS, 2, 2)] * 2 + [dma(2, ROUNDS, 2), dma(2, ROUNDS), dma(ROUNDS)],
        compiler_params=pltpu.CompilerParams(collective_id=0, has_side_effects=True, vmem_limit_bytes=VMEM_BYTES),
        name='attention_block',
    )(x_in, grad_y, *weights, *vectors)


def settle_body(count, small_hbm, *refs):
    sources, targets, refs = refs[:count], refs[count:2 * count], refs[2 * count:]
    vectors, bufs, (small, vector_s, sems, vector_sems) = refs[:3], refs[3:3 + count], refs[3 + count:]
    load = pltpu.make_async_copy(small_hbm, small, vector_sems.at[3])
    load.start()
    cuts = []
    for i, (source, target, buf) in enumerate(zip(sources, targets, bufs)):
        rows = source.shape[0] // CUTS
        for c in range(CUTS):
            part = pl.ds(c * rows, rows)
            cuts.append((pltpu.make_async_copy(source.at[part], buf.at[part], sems.at[0, i, c]),
                         pltpu.make_async_copy(buf.at[part], target.at[part], sems.at[1, i, c])))
    for read, _ in cuts:
        read.start()
    load.wait()
    stores = []
    for k, vector in enumerate(vectors):
        vector_s[k][...] = jnp.concatenate([small[k * 5 + j:k * 5 + j + 1] for j in range(5)], axis=1).reshape(vector.shape)
        stores.append(pltpu.make_async_copy(vector_s[k], vector, vector_sems.at[k]))
        stores[k].start()
    for read, write in cuts:
        read.wait()
        write.start()
    for _, write in cuts:
        write.wait()
    for store in stores:
        store.wait()


def settle(small, arrays):
    anywhere = pl.BlockSpec(memory_space=pl.ANY)
    count = len(arrays)
    dma = pltpu.SemaphoreType.DMA
    vector = (arrays[0].shape[1],)
    return pl.pallas_call(
        functools.partial(settle_body, count),
        in_specs=[anywhere] * (count + 1), out_specs=[anywhere] * (count + 3),
        out_shape=[jax.ShapeDtypeStruct(a.shape, a.dtype) for a in arrays] + [jax.ShapeDtypeStruct(vector, F32)] * 3,
        scratch_shapes=[pltpu.VMEM(a.shape, a.dtype) for a in arrays]
        + [pltpu.VMEM(small.shape, F32), [pltpu.VMEM(vector, F32)] * 3, dma((2, count, CUTS)), dma((4,))],
        compiler_params=pltpu.CompilerParams(vmem_limit_bytes=VMEM_BYTES),
        name='settle',
    )(small, *arrays)


def solution(mesh):
    depth = mesh.shape['dp'] // (2 * RING)
    act_spec, rep_spec = P('dp', 'cp', None), P()

    def device_step(x_in, grad_y, ln_gamma, ln_beta, w_q, w_k, w_v, w_o, b_o):
        channels, num_heads, head_dim = w_q.shape
        flat = (num_heads * head_dim, channels)
        weights = [jnp.transpose(w, (1, 2, 0)).reshape(flat) for w in (w_q, w_k, w_v)] + [w_o.reshape(flat)]
        y_out, grad_x, *grads, grad_wo, small = attention_block(x_in, grad_y, weights, (ln_gamma, ln_beta, b_o), head_dim, depth)
        rows = (2 * y_out.shape[1], channels)
        moved = settle(small, [y_out.reshape(rows), grad_x.reshape(rows), *grads, grad_wo])
        y_out, grad_x = (a.reshape(x_in.shape) for a in moved[:2])
        grads, grad_wo = moved[2:5], moved[5]
        grads = [jnp.transpose(grad.reshape(num_heads, head_dim, channels), (2, 0, 1)) for grad in grads]
        return (y_out, grad_x, moved[6], moved[7], *grads, grad_wo.reshape(num_heads, head_dim, channels), moved[8])

    specs = (act_spec, act_spec) + (rep_spec,) * 7
    return jax.shard_map(device_step, mesh=mesh, in_specs=specs, out_specs=specs, check_vma=False)
```

```python
import functools
import math
import jax
import jax.numpy as jnp
from jax import lax
from jax.experimental import pallas as pl
from jax.experimental.pallas import tpu as pltpu
from jax.sharding import PartitionSpec as P

LN_EPS = 1e-5
KEY_TILE = 256
Q_BLOCK = 256
FOLD = 16
AUG = 96
VMEM_BYTES = 67043328
BF = jnp.bfloat16
F32 = jnp.float32


def dot_nn(lhs, rhs):
    return lax.dot_general(lhs, rhs, (((1,), (0,)), ((), ())), preferred_element_type=F32)


def dot_nt(lhs, rhs):
    return lax.dot_general(lhs, rhs, (((1,), (1,)), ((), ())), preferred_element_type=F32)


def dot_tn(lhs, rhs):
    return lax.dot_general(lhs, rhs, (((0,), (0,)), ((), ())), preferred_element_type=F32)


def split_parts(value):
    high = value.astype(BF)
    rest = value - high.astype(F32)
    mid = rest.astype(BF)
    return high, mid, (rest - mid.astype(F32)).astype(BF)


def fold_rows(value, op):
    groups = value.reshape(value.shape[0] // FOLD, FOLD, value.shape[1])
    out = groups[0]
    for i in range(1, groups.shape[0]):
        out = op(out, groups[i])
    return out


MESH = pl.DeviceIdType.MESH
RING = 4
ROUNDS = 5
ROUND_ROWS = 256
STAGES = 8
SPARE = ((0, 1), (0, 2), (1, 1), (2, 1), (3, 1), (0, 6), (1, 5), (1, 6), (2, 6), (2, 6))
PIECES = 4
SENDS = 16
CUTS = 8
ORDER = ('yx', 'yy', 'yy', 'yx', 'yx')


class Links:
    def __init__(self, depth):
        dp, self.x = lax.axis_index('dp'), lax.axis_index('cp')
        self.core = lax.rem(dp, 2)
        self.y = lax.rem(dp // 2, RING)
        self.z = dp // (2 * RING)
        self.depth = depth
        self.pos = {'x': self.x, 'y': self.y, 'z': self.z}
        self.size = {'x': RING, 'y': RING, 'z': depth}
        self.peer = self.at(core=1 - self.core)
        pair, odd = self.x // 2, lax.rem(self.x, 2)
        self.owners = [(pair, 2 * self.core + odd), (pair, 2 * self.core + 1 - odd)]
        self.workers = [(pair, 2 * self.core), (pair, 2 * self.core + 1)]

    def at(self, x=None, y=None, z=None, core=None):
        pick = lambda value, own: own if value is None else value
        return ((pick(z, self.z) * RING + pick(y, self.y)) * 2 + pick(core, self.core), pick(x, self.x))

    def step(self, axis, d):
        return self.at(**{axis: lax.rem(self.pos[axis] + d, self.size[axis])})

    def is_self(self, place):
        return jnp.logical_and(place[0] == self.core, place[1] == self.x)


def remote(source, target, send, recv, device):
    return pltpu.make_async_remote_copy(src_ref=source, dst_ref=target, send_sem=send, recv_sem=recv,
                                        device_id=device, device_id_type=MESH)


def wait_for(ref, sem):
    pltpu.make_async_copy(ref, ref, sem).wait()


class GradReduce:
    def __init__(self, links, dim, grad, out, results, bufs, sems):
        self.links, self.grad, self.both, self.out = links, grad, out, out.at[links.core]
        width = grad.shape[0] // 4
        self.pieces = [(0, width, results[0], 0)]
        self.pieces += [(width + (3 * head + k) * dim, dim, results[1 + k], head * dim) for head in range(width // dim) for k in range(3)]
        self.recv1, self.recv2, self.mid, self.z_src, self.z_recv, self.z_out = bufs
        self.rs_sems, self.ag_sems, self.z_sems, self.swap_sems, self.store_sems = sems

    def axes(self, rnd, unit):
        first = ORDER[rnd][unit]
        return first, ('x' if first == 'y' else 'y')

    def block(self, rnd, unit, phase):
        first = rnd * ROUND_ROWS + unit * 128
        if phase == 0:
            return first, 32
        return first + self.links.pos[self.axes(rnd, unit)[0]] * 32, 8

    def landing(self, rnd, unit, phase):
        return (self.recv1 if phase == 0 else self.recv2).at[rnd, unit]

    def wait_all(self, rnd, unit, phase, sems):
        whole = self.landing(rnd, unit, phase)
        every = remote(whole, whole, sems.at[0, rnd, unit, phase], sems.at[1, rnd, unit, phase], self.links.peer)
        every.wait_recv()
        every.wait_send()

    def source(self, rnd, unit, phase, owner):
        if phase == 0:
            first, rows = self.block(rnd, unit, 0)
            return self.grad.at[pl.ds(pl.multiple_of(first + owner * rows, 8), rows)]
        return self.mid.at[rnd, unit, pl.ds(pl.multiple_of(owner * 8, 8), 8)]

    def scatter_start(self, rnd, unit, phase):
        axis = self.axes(rnd, unit)[phase]
        for d in (2, 1, 3):
            owner = lax.rem(self.links.pos[axis] + d, RING)
            remote(self.source(rnd, unit, phase, owner), self.landing(rnd, unit, phase).at[d - 1],
                   self.rs_sems.at[0, rnd, unit, phase], self.rs_sems.at[1, rnd, unit, phase], self.links.step(axis, d)).start()

    def scatter_end(self, rnd, unit, phase):
        self.wait_all(rnd, unit, phase, self.rs_sems)
        landing = self.landing(rnd, unit, phase)
        mine = self.source(rnd, unit, phase, self.links.pos[self.axes(rnd, unit)[phase]])
        return (mine[...] + landing[0]) + (landing[1] + landing[2])

    def gather_start(self, rnd, unit, phase):
        axis = self.axes(rnd, unit)[phase]
        first, rows = self.block(rnd, unit, phase)
        part = self.out.at[pl.ds(pl.multiple_of(first + self.links.pos[axis] * rows, 8), rows)]
        for d in (2, 1, 3):
            remote(part, part, self.ag_sems.at[0, rnd, unit, phase], self.ag_sems.at[1, rnd, unit, phase],
                   self.links.step(axis, d)).start()

    def z_copies(self, rnd, way):
        links = self.links
        each = 16 // links.depth
        send, recv = self.z_sems.at[0, rnd, way], self.z_sems.at[1, rnd, way]
        mine = pl.ds(links.z * each, each)
        copies = []
        for d in range(1, links.depth):
            far = lax.rem(links.z + d, links.depth)
            if way == 0:
                source, target = self.z_src.at[rnd, pl.ds(far * each, each)], self.z_recv.at[rnd, d - 1]
            else:
                source = target = self.z_out.at[rnd, mine]
            copies.append(remote(source, target, send, recv, links.step('z', d)))
        return copies, mine

    def z_wait(self, rnd, way):
        if self.links.depth > 1:
            whole = self.z_recv.at[rnd]
            all_of = remote(whole, whole, self.z_sems.at[0, rnd, way], self.z_sems.at[1, rnd, way], self.links.step('z', 1))
            all_of.wait_recv()
            all_of.wait_send()

    def swap(self, rnd):
        part = self.out.at[pl.ds(rnd * ROUND_ROWS, ROUND_ROWS)]
        return remote(part, part, self.swap_sems.at[0, rnd], self.swap_sems.at[1, rnd], self.links.peer)

    def store(self, rnd):
        begin = rnd * ROUND_ROWS
        half = self.both.shape[1] // 4
        for first, rows, result, place in self.pieces:
            low, high = max(first, begin), min(first + rows, begin + ROUND_ROWS)
            for core in range(2):
                if low < high:
                    target = result.at[pl.ds(core * half + place + low - first, high - low)]
                    pltpu.make_async_copy(self.both.at[core, pl.ds(low, high - low)], target, self.store_sems.at[rnd]).start()

    def stored(self, rnd):
        wait_for(self.both.at[:, pl.ds(rnd * ROUND_ROWS, ROUND_ROWS)], self.store_sems.at[rnd])

    def stage(self, rnd, k):
        units = (0, 1)
        if k == 0:
            for u in units:
                self.scatter_start(rnd, u, 0)
        elif k == 1:
            for u in units:
                self.mid[rnd, u] = self.scatter_end(rnd, u, 0)
                self.scatter_start(rnd, u, 1)
        elif k == 2:
            for u in units:
                total = self.scatter_end(rnd, u, 1)
                for j in range(5):
                    self.z_src[rnd, u * 5 + j] = total[:, j * 128:(j + 1) * 128]
            self.z_src[rnd, pl.ds(10, 6)] = jnp.zeros((6, 8, 128), F32)
            for copy in self.z_copies(rnd, 0)[0]:
                copy.start()
        elif k == 3:
            self.z_wait(rnd, 0)
            copies, mine = self.z_copies(rnd, 1)
            total = self.z_src[rnd, mine]
            for d in range(self.links.depth - 1):
                total = total + self.z_recv[rnd, d]
            self.z_out[rnd, mine] = total
            for copy in copies:
                copy.start()
        elif k == 4:
            self.z_wait(rnd, 1)
            for u in units:
                first = self.block(rnd, u, 1)[0] + self.links.pos[self.axes(rnd, u)[1]] * 8
                for j in range(5):
                    self.out[pl.ds(pl.multiple_of(first, 8), 8), pl.ds(j * 128, 128)] = self.z_out[rnd, u * 5 + j]
                self.gather_start(rnd, u, 1)
        elif k == 5:
            for u in units:
                self.wait_all(rnd, u, 1, self.ag_sems)
                self.gather_start(rnd, u, 0)
        elif k == 6:
            for u in units:
                self.wait_all(rnd, u, 0, self.ag_sems)
            self.swap(rnd).start()
        else:
            self.swap(rnd).wait()
            self.store(rnd)


def layer_norm(x_ref, rows):
    x_f = x_ref[rows].astype(F32)
    centered = x_f - jnp.mean(x_f, axis=-1, keepdims=True)
    inv_std = lax.rsqrt(jnp.mean(centered * centered, axis=-1, keepdims=True) + LN_EPS)
    return centered * inv_std, inv_std


def padded(parts, rows):
    filled = [part.astype(F32) for part in parts]
    used = sum(part.shape[0] for part in filled)
    return jnp.concatenate(filled + [jnp.zeros((rows - used, filled[0].shape[1]), F32)], axis=0).astype(BF)


def block_body(dim, depth, x_hbm, dy_hbm, wq_hbm, wk_hbm, wv_hbm, wo_hbm, gamma_ref, beta_ref, bo_ref,
               y_ref, gx_ref, dq_ref, dk_ref, dv_ref, dwo_ref, small_ref,
               x_s, normed_s, dy_s, wt_s, wo_s, q_s, k_s, v_s, do_s, o_s, of_s, o_peer, lse_s, kf_s, vf_s, buf_a, buf_b, buf_c,
               kb_s, vb_s, dk_acc, dv_acc, grads, grads_peer, d_w, d_w_all, dx_s, y_s,
               recv1, recv2, mid, z_src, z_recv, z_out, small_s, small_recv,
               load_sems, in_send, in_recv, pass_send, pass_recv, o_sems, grad_sems, out_send, out_recv, small_sems,
               rs_sems, ag_sems, z_sems, swap_sems, store_sems):
    links = Links(depth)
    width, tokens = q_s.shape
    heads, tiles = width // dim, tokens // KEY_TILE
    own, band = tokens // 2, tokens // 4
    scale = dim ** -0.5
    log2_scale = scale * math.log2(math.e)
    fwd_group, bwd_group = tiles, 4
    fwd_steps, bwd_steps = tiles // fwd_group, tiles // bwd_group
    zero = jnp.minimum(links.x, 0)
    gamma, beta, bias = (ref[...].reshape(1, ref.shape[0]) for ref in (gamma_ref, beta_ref, bo_ref))
    odd = lax.rem(links.x, 2)
    reduce = GradReduce(links, dim, d_w, d_w_all, (dwo_ref, dq_ref, dk_ref, dv_ref), (recv1, recv2, mid, z_src, z_recv, z_out),
                        (rs_sems, ag_sems, z_sems, swap_sems, store_sems))
    end = heads * bwd_steps + 1
    plan = {}
    for rnd in range(ROUNDS):
        at = rnd * bwd_steps + 1 if rnd else 0
        for k in range(STAGES):
            at += min(k, 1) + SPARE.count((rnd, k))
            plan.setdefault(at, []).append((rnd, k))
    for at in plan:
        plan[at].sort(key=lambda item: (item[1] in (0, 5) and item[0] < ROUNDS - 1, -item[0]))
    slots = max(plan) + 1 - end

    def tile_rows(tile, base=None):
        return pl.ds(tile * KEY_TILE if base is None else pl.multiple_of(base + tile * KEY_TILE, KEY_TILE), KEY_TILE)

    def head_rows(head, rows=dim):
        return pl.ds(pl.multiple_of(head * rows, 16), rows)

    def q_cols(index):
        return pl.ds(pl.multiple_of(index * Q_BLOCK, Q_BLOCK), Q_BLOCK)

    def my_half(side):
        return pl.ds(pl.multiple_of((links.core if side == 0 else 1 - links.core) * width, 16), width)

    loads = [pltpu.make_async_copy(w_hbm.at[my_half(side)], wt_s.at[side, pl.ds(k * width, width)], load_sems.at[side, k])
             for side in range(2) for k, w_hbm in enumerate((wq_hbm, wk_hbm, wv_hbm))]
    loads += [pltpu.make_async_copy(wo_hbm.at[my_half(side)], wo_s.at[side], load_sems.at[side, 3]) for side in range(2)]

    def maybe_far(place, source, target, send, recv):
        core, x = place
        here = links.is_self(place)
        far = remote(source, target, send, recv, links.at(core=core, x=x))
        near = pltpu.make_async_copy(source, target, recv)

        @pl.when(jnp.logical_not(here))
        def _():
            far.start()

        @pl.when(here)
        def _():
            near.start()

    def all_left(ref, sem):
        rows = ref.shape[0]
        halved = links.x // 2 == links.core

        @pl.when(jnp.logical_not(halved))
        def _():
            wait_for(ref, sem)

        @pl.when(halved)
        def _():
            wait_for(ref.at[pl.ds(0, rows // 2)], sem)

    piece = band // PIECES

    def deliver(which, m, c):
        slot = lax.rem(links.x + m, 2)
        source = (dy_hbm if which else x_hbm).at[m, pl.ds(c * piece, piece)]
        target = (dy_s if which else x_s).at[pl.ds(pl.multiple_of(slot * band + c * piece, 16), piece)]
        maybe_far(links.workers[m], source, target, in_send.at[which], in_recv.at[which, slot, c])

    def hand_over(which, slot, c):
        rows = dy_s if which else x_s
        first = slot * band + c * piece
        return remote(rows.at[pl.ds(first, piece)], rows.at[pl.ds(own + first, piece)],
                      pass_send.at[which], pass_recv.at[which, slot, c], links.peer)

    def arrive(which, slot, c):
        wait_for((dy_s if which else x_s).at[pl.ds(slot * band + c * piece, piece)], in_recv.at[which, slot, c])
        hand_over(which, slot, c).start()

    def swap_out(head):
        rows = head_rows(head)
        return remote(o_s.at[rows, pl.ds(own, own)], o_peer.at[rows], o_sems.at[0, head], o_sems.at[1, head], links.peer)

    def swap_grads(head):
        rows = head_rows(head)
        return remote(grads.at[:, rows, pl.ds(own, own)], grads_peer.at[:, rows], grad_sems.at[0, head], grad_sems.at[1, head],
                      links.peer)

    part = band // 2
    portion = own // SENDS

    def send_home(which, i):
        cut = SENDS // 2
        second, inner = i // cut, lax.rem(i, cut)
        source = (dx_s if which else y_s).at[pl.ds(pl.multiple_of(i * portion, 16), portion)]
        target = (gx_ref if which else y_ref).at[odd, pl.ds(pl.multiple_of(inner * portion, 16), portion)]
        (core, x0), (_, x1) = links.owners
        maybe_far((core, jnp.where(second == 0, x0, x1)), source, target, out_send.at[which], out_recv.at[which])

    barrier = pltpu.get_barrier_semaphore()
    fixed = [links.peer]
    fixed += [links.step(axis, d) for axis in ('x', 'y') for d in range(1, RING)]
    fixed += [links.step('z', d) for d in range(1, depth)]
    for device in fixed:
        pl.semaphore_signal(barrier, inc=1, device_id=device, device_id_type=MESH)
    count = len(fixed)
    for place in links.owners + links.workers:
        other = jnp.logical_not(links.is_self(place))
        count = count + other.astype(jnp.int32)

        @pl.when(other)
        def _():
            pl.semaphore_signal(barrier, inc=1, device_id=links.at(core=place[0], x=place[1]), device_id_type=MESH)
    for load in loads:
        load.start()
    pl.semaphore_wait(barrier, count)
    for c in range(PIECES):
        for m in range(2):
            deliver(0, m, c)
    for load in loads:
        load.wait()

    def normalize(first):
        rows = pl.ds(first, piece)
        normed_s[rows] = (layer_norm(x_s, rows)[0] * gamma + beta).astype(BF)

    def project(b, c):
        cols = pl.ds(b * band + (c - 2) * piece, 2 * piece)
        normed = normed_s[cols]
        for k, out in enumerate((q_s, k_s, v_s)):
            out[:, cols] = dot_nt(wt_s[0, pl.ds(k * width, width)], normed).astype(BF)

    for c in range(PIECES + 1):
        if c < PIECES:
            for slot in range(2):
                arrive(0, slot, c)
            if c == PIECES - 1:
                for i in range(PIECES):
                    for m in range(2):
                        deliver(1, m, i)
            for slot in range(2):
                normalize(slot * band + c * piece)
        if c:
            if c % 2 == 0:
                project(0, c)
                project(1, c)
            for slot in range(2):
                hand_over(0, slot, c - 1).wait_recv()
                normalize(own + slot * band + (c - 1) * piece)
                if c % 2 == 0:
                    project(2 + slot, c)

    def forward_step(now, carry):
        head, step = now // fwd_steps, lax.rem(now, fwd_steps)
        rows = head_rows(head)
        for c in range(PIECES):
            @pl.when(now == max(c, 1))
            def _():
                for slot in range(2):
                    arrive(1, slot, c)

        @pl.when(step == 0)
        def _():
            k_t = k_s[rows]
            kf_s[...] = jnp.concatenate([k_t, k_t, k_t], axis=0).T
            vf_s[0:dim] = v_s[rows]
            vf_s[dim:] = padded([jnp.ones((1, tokens), F32)], AUG - dim)

        bufs = (buf_a, buf_b, buf_c)
        total, lag = tiles * fwd_group, tiles + 2
        query, high, top, probs, out = {}, {}, {}, {}, {}
        for g in range(total + lag + 2):
            if g < total:
                i, t = divmod(g, tiles)
                if t == 0:
                    query[i] = jnp.concatenate(split_parts(q_s[rows, q_cols(step * fwd_group + i)].astype(F32) * log2_scale), axis=0)
                scores = dot_nn(kf_s[tile_rows(t)], query[i])
                bufs[i % 3][tile_rows(t)] = scores
                folded = fold_rows(scores, jnp.maximum)
                high[i] = folded if t == 0 else jnp.maximum(high[i], folded)
                if t == tiles - 1:
                    top[i] = jnp.max(high[i], axis=0, keepdims=True)
            if lag <= g < total + lag:
                i, t = divmod(g - lag, tiles)
                probs[g - lag] = jnp.exp2(bufs[i % 3][tile_rows(t, zero)] - top[i]).astype(BF)
            if g >= lag + 2:
                i, t = divmod(g - lag - 2, tiles)
                product = dot_nn(vf_s[:, tile_rows(t)], probs[g - lag - 2])
                out[i] = product if t == 0 else out[i] + product
                if t == tiles - 1:
                    cols = q_cols(step * fwd_group + i)
                    denom = out[i][dim:dim + 1]
                    value = out[i][:dim] * (1.0 / denom)
                    o_s[rows, cols] = value.astype(BF)
                    of_s[rows, cols] = value
                    lse = (top[i] + jnp.log2(denom)) * (1.0 / log2_scale)
                    lse_s[head_rows(head, 16), cols] = padded(split_parts(lse), 16)

        @pl.when(step == fwd_steps - 1)
        def _():
            swap_out(head).start()

        return carry

    lax.fori_loop(0, heads * fwd_steps, forward_step, 0)
    for c in range(PIECES):
        for slot in range(2):
            hand_over(1, slot, c).wait_recv()
    d_w[pl.ds(0, width)] = dot_nn(o_s[...], dy_s[...])
    for rnd, k in plan[0]:
        reduce.stage(rnd, k)
    for i in range(tiles):
        cols = pl.ds(i * KEY_TILE, KEY_TILE)
        do_s[:, cols] = dot_nt(wo_s[0], dy_s[cols]).astype(BF)
    for head in range(heads):
        swap_out(head).wait()
    for i in range(4):
        toks = pl.ds(i * part, part)
        product = dot_tn(o_s[:, toks], wo_s[0]) + dot_tn(o_peer[:, toks], wo_s[1])
        y_s[toks] = (x_s[toks].astype(F32) + product + bias).astype(BF)
    for which in range(2):
        rows = (dy_s if which else x_s).at[pl.ds(0, own)]
        all_left(rows, in_send.at[which])
        wait_for(rows, pass_send.at[which])

    def backward_step(now, carry):
        head, step = now // bwd_steps, lax.rem(now, bwd_steps)
        rows = head_rows(head)
        for at in range(end - 1):
            todo = plan.get(at + 1)
            if todo:
                @pl.when(now == at)
                def _():
                    for rnd, k in todo:
                        reduce.stage(rnd, k)
        share = SENDS // (heads * bwd_steps)
        for i in range(share):
            send_home(0, now * share + i)

        @pl.when(step == 0)
        def _():
            minus = padded([jnp.full((3, tokens), -1.0, F32)], AUG - dim)
            kb_s[...] = jnp.concatenate([k_s[rows], minus], axis=0).T
            vb_s[...] = jnp.concatenate([v_s[rows], minus], axis=0).T
            dk_acc[...] = jnp.zeros_like(dk_acc)
            dv_acc[...] = jnp.zeros_like(dv_acc)

        total = tiles * bwd_group
        ops, probs, d_scores, dq = {}, {}, {}, {}
        for g in range(total + 2):
            if g < total:
                i, t = divmod(g, tiles)
                if t == 0:
                    cols = q_cols(step * bwd_group + i)
                    q_t, do_t = q_s[rows, cols], do_s[rows, cols]
                    delta = jnp.sum(of_s[rows, cols] * do_t.astype(F32), axis=0, keepdims=True)
                    ops[i] = (cols, q_t, do_t, jnp.concatenate([q_t, lse_s[head_rows(head, 16), cols]], axis=0),
                              jnp.concatenate([do_t, padded(split_parts(delta), 16)], axis=0))
                scores = dot_nn(kb_s[tile_rows(t)], ops[i][3])
                d_probs = dot_nn(vb_s[tile_rows(t)], ops[i][4])
                prob = jnp.exp2(scores * log2_scale)
                probs[g] = prob.astype(BF)
                d_scores[g] = (prob * d_probs).astype(BF)
            if g >= 2:
                i, t = divmod(g - 2, tiles)
                cols, q_t, do_t = ops[i][:3]
                dv_acc[:, tile_rows(t)] += dot_nt(do_t, probs[g - 2])
                product = dot_nn(k_s[rows, tile_rows(t)], d_scores[g - 2])
                dq[i] = product if t == 0 else dq[i] + product
                if t == tiles - 1:
                    grads[0, rows, cols] = (dq[i] * scale).astype(BF)
                dk_acc[:, tile_rows(t)] += dot_nt(q_t, d_scores[g - 2])

        @pl.when(step == bwd_steps - 1)
        def _():
            grads[1, rows] = (dk_acc[...] * scale).astype(BF)
            grads[2, rows] = dv_acc[...].astype(BF)
            swap_grads(head).start()
            stacked = jnp.concatenate([grads[0, rows], grads[1, rows], grads[2, rows]], axis=0)
            d_w[pl.ds(pl.multiple_of(width + head * (3 * dim), 8), 3 * dim)] = dot_nn(stacked, normed_s[...])

        return carry

    lax.fori_loop(0, heads * bwd_steps, backward_step, 0)

    def tail(slot):
        for rnd, k in plan.get(end + slot, ()):
            reduce.stage(rnd, k)

    tail(0)
    for head in range(heads):
        swap_grads(head).wait()
    sums = [jnp.zeros((1, 640), F32)] * 3
    for i in range(4):
        toks = pl.ds(i * part, part)
        mine = jnp.concatenate([grads[k, :, toks] for k in range(3)], axis=0)
        theirs = jnp.concatenate([grads_peer[k, :, toks] for k in range(3)], axis=0)
        d_normed = (dot_tn(mine, wt_s[0]) + dot_tn(theirs, wt_s[1])).astype(BF).astype(F32)
        x_hat, inv_std = layer_norm(x_s, toks)
        d_hat = d_normed * gamma
        mean_one = jnp.mean(d_hat, axis=-1, keepdims=True)
        mean_two = jnp.mean(d_hat * x_hat, axis=-1, keepdims=True)
        dy_f = dy_s[toks].astype(F32)
        dx_s[toks] = (dy_f + inv_std * (d_hat - mean_one - x_hat * mean_two)).astype(BF)
        for k, term in enumerate((d_normed * x_hat, d_normed, dy_f)):
            sums[k] = sums[k] + jnp.sum(term, axis=0, keepdims=True)

    for k in range(3):
        for j in range(5):
            small_s[0, pl.ds(k * 5 + j, 1)] = sums[k][:, j * 128:(j + 1) * 128]
    small_s[0, pl.ds(15, 1)] = jnp.zeros((1, 128), F32)
    small_copy = pltpu.make_async_copy(small_s.at[4], small_ref, load_sems.at[0, 0])
    first, waiting = 0, ()
    for hop, axis in enumerate(('z', 'core', 'y', 'x', '')):
        if hop:
            for slot in range(hop, hop + 1 if axis else slots):
                tail(slot)
            if hop == 1:
                for i in range(SENDS):
                    send_home(1, i)
            acc = small_s[hop - 1]
            for d, copy in enumerate(waiting):
                copy.wait_recv()
                acc = acc + small_recv[first + d]
            for copy in waiting:
                copy.wait_send()
            first += len(waiting)
            small_s[hop] = acc
        if axis:
            far = [links.peer] if axis == 'core' else [links.step(axis, d) for d in range(1, links.size[axis])]
            waiting = [remote(small_s.at[hop], small_recv.at[first + d], small_sems.at[0, first + d], small_sems.at[1, first + d],
                              device) for d, device in enumerate(far)]
            for copy in waiting:
                copy.start()
    small_copy.start()
    for which in range(2):
        all_left(dx_s if which else y_s, out_send.at[which])
        wait_for(gx_ref if which else y_ref, out_recv.at[which])
    for rnd in range(ROUNDS):
        reduce.stored(rnd)
    small_copy.wait()


def attention_block(x_in, grad_y, weights, vectors, dim, depth):
    rows, channels = x_in.shape[1:]
    tokens, own = 4 * rows, 2 * rows
    width = weights[0].shape[0] // 2
    heads = width // dim
    total = 4 * width
    half = lambda *shape: pltpu.VMEM(shape, BF)
    full = lambda *shape: pltpu.VMEM(shape, F32)
    dma = lambda *shape: pltpu.SemaphoreType.DMA(shape)
    anywhere = pl.BlockSpec(memory_space=pl.ANY)
    in_vmem = pl.BlockSpec(memory_space=pltpu.VMEM)
    far = max(depth - 1, 1)
    return pl.pallas_call(
        functools.partial(block_body, dim, depth),
        in_specs=[anywhere] * 6 + [in_vmem] * 3,
        out_specs=[anywhere] * 7,
        out_shape=[jax.ShapeDtypeStruct(x_in.shape, BF)] * 2
        + [jax.ShapeDtypeStruct(weights[0].shape, F32)] * 4 + [jax.ShapeDtypeStruct((16, 128), F32)],
        scratch_shapes=[half(tokens, channels)] * 3 + [half(2, 3 * width, channels), half(2, width, channels)]
        + [half(width, tokens)] * 5 + [full(width, tokens), half(width, own), half(16 * heads, tokens),
                                       half(tokens, 3 * dim), half(AUG, tokens)]
        + [full(tokens, Q_BLOCK)] * 3 + [half(tokens, AUG)] * 2 + [full(dim, tokens)] * 2
        + [half(3, width, tokens), half(3, width, own), full(total, channels), full(2, total, channels)]
        + [half(own, channels)] * 2
        + [full(ROUNDS, 2, 3, 32, channels), full(ROUNDS, 2, 3, 8, channels), full(ROUNDS, 2, 32, channels), full(ROUNDS, 16, 8, 128),
           full(ROUNDS, far, 16 // depth, 8, 128), full(ROUNDS, 16, 8, 128), full(5, 16, 128), full(7 + far, 16, 128),
           dma(2, 4)] + [dma(2), dma(2, 2, PIECES)] * 2 + [dma(2, heads)] * 2
        + [dma(2), dma(2), dma(2, 7 + far)] + [dma(2, ROUNDS, 2, 2)] * 2 + [dma(2, ROUNDS, 2), dma(2, ROUNDS), dma(ROUNDS)],
        compiler_params=pltpu.CompilerParams(collective_id=0, has_side_effects=True, vmem_limit_bytes=VMEM_BYTES),
        name='attention_block',
    )(x_in, grad_y, *weights, *vectors)


def settle_body(count, small_hbm, *refs):
    sources, targets, refs = refs[:count], refs[count:2 * count], refs[2 * count:]
    vectors, bufs, (small, vector_s, sems, vector_sems) = refs[:3], refs[3:3 + count], refs[3 + count:]
    load = pltpu.make_async_copy(small_hbm, small, vector_sems.at[3])
    load.start()
    cuts = []
    for i, (source, target, buf) in enumerate(zip(sources, targets, bufs)):
        rows = source.shape[0] // CUTS
        for c in range(CUTS):
            part = pl.ds(c * rows, rows)
            cuts.append((pltpu.make_async_copy(source.at[part], buf.at[part], sems.at[0, i, c]),
                         pltpu.make_async_copy(buf.at[part], target.at[part], sems.at[1, i, c])))
    for read, _ in cuts:
        read.start()
    load.wait()
    stores = []
    for k, vector in enumerate(vectors):
        vector_s[k][...] = jnp.concatenate([small[k * 5 + j:k * 5 + j + 1] for j in range(5)], axis=1).reshape(vector.shape)
        stores.append(pltpu.make_async_copy(vector_s[k], vector, vector_sems.at[k]))
        stores[k].start()
    for read, write in cuts:
        read.wait()
        write.start()
    for _, write in cuts:
        write.wait()
    for store in stores:
        store.wait()


def settle(small, arrays):
    anywhere = pl.BlockSpec(memory_space=pl.ANY)
    count = len(arrays)
    dma = pltpu.SemaphoreType.DMA
    vector = (arrays[0].shape[1],)
    return pl.pallas_call(
        functools.partial(settle_body, count),
        in_specs=[anywhere] * (count + 1), out_specs=[anywhere] * (count + 3),
        out_shape=[jax.ShapeDtypeStruct(a.shape, a.dtype) for a in arrays] + [jax.ShapeDtypeStruct(vector, F32)] * 3,
        scratch_shapes=[pltpu.VMEM(a.shape, a.dtype) for a in arrays]
        + [pltpu.VMEM(small.shape, F32), [pltpu.VMEM(vector, F32)] * 3, dma((2, count, CUTS)), dma((4,))],
        compiler_params=pltpu.CompilerParams(vmem_limit_bytes=VMEM_BYTES),
        name='settle',
    )(small, *arrays)


def solution(mesh):
    depth = mesh.shape['dp'] // (2 * RING)
    act_spec, rep_spec = P('dp', 'cp', None), P()

    def device_step(x_in, grad_y, ln_gamma, ln_beta, w_q, w_k, w_v, w_o, b_o):
        channels, num_heads, head_dim = w_q.shape
        flat = (num_heads * head_dim, channels)
        weights = [jnp.transpose(w, (1, 2, 0)).reshape(flat) for w in (w_q, w_k, w_v)] + [w_o.reshape(flat)]
        y_out, grad_x, *grads, grad_wo, small = attention_block(x_in, grad_y, weights, (ln_gamma, ln_beta, b_o), head_dim, depth)
        rows = (2 * y_out.shape[1], channels)
        moved = settle(small, [y_out.reshape(rows), grad_x.reshape(rows), *grads, grad_wo])
        y_out, grad_x = (a.reshape(x_in.shape) for a in moved[:2])
        grads, grad_wo = moved[2:5], moved[5]
        grads = [jnp.transpose(grad.reshape(num_heads, head_dim, channels), (2, 0, 1)) for grad in grads]
        return (y_out, grad_x, moved[6], moved[7], *grads, grad_wo.reshape(num_heads, head_dim, channels), moved[8])

    specs = (act_spec, act_spec) + (rep_spec,) * 7
    return jax.shard_map(device_step, mesh=mesh, in_specs=specs, out_specs=specs, check_vma=False)
```
